32 devices in a mesh: section: 2 (over core), gx: 4 (over z), gy: 4 (over y, x).
Axes of the slice: x: 2, y: 2, z: 4, core: 2. Of those that a mesh axis runs over, the one named last changes fastest.
Arguments:
- inputs: bfloat16 [4, 4, 128, 2048], P(None, 'gy', 'gx'), may hold values from -6 to 6
- out_grad: bfloat16 [4, 4, 128, 2048], P(None, 'gy', 'gx'), may hold values from -6 to 6
- segments: int32 [4, 4, 128], P(None, 'gy'), may hold values from 0 to 3, never falling along the last dimension, each value on 1 to 64 neighbouring positions
- routes: int32 [2, 4, 4, 128, 8], P('section', None, 'gy', 'gx'), may hold values from 0 to 15, all different within a row; in each aligned block of 32 rows (0 to 31, 32 to 63, ..., all dimensions but the last counted through in order) at most 32 rows name the same one
- gates: float32 [2, 4, 4, 128, 8], P('section', None, 'gy', 'gx'), may hold values from 0.05 to 0.3
- gain_attn: float32 [2, 2048], P('section'), may hold values from 0.5 to 1.5
- gain_ffn: float32 [2, 2048], P('section'), may hold values from 0.5 to 1.5
- gain_query: float32 [2, 128], P('section'), may hold values from 0.5 to 1.5
- gain_key: float32 [2, 128], P('section'), may hold values from 0.5 to 1.5
- w_query: bfloat16 [2, 2048, 4096], P('section', 'gy', 'gx'), may hold values from -0.125 to 0.125
- w_key: bfloat16 [2, 2048, 512], P('section', 'gy'), may hold values from -0.125 to 0.125
- w_value: bfloat16 [2, 2048, 512], P('section', 'gy'), may hold values from -0.125 to 0.125
- w_out: bfloat16 [2, 2048, 4096], P('section', 'gy', 'gx'), may hold values from -0.5 to 0.5
- w_gate: bfloat16 [2, 16, 2048, 768], P('section', ('gx', 'gy')), may hold values from -0.125 to 0.125
- w_up: bfloat16 [2, 16, 2048, 768], P('section', ('gx', 'gy')), may hold values from -0.125 to 0.125
- w_down: bfloat16 [2, 16, 768, 2048], P('section', ('gx', 'gy')), may hold values from -0.625 to 0.625
Outputs:
- layer_out: bfloat16 [2, 4, 4, 128, 2048], P('section', None, 'gy', 'gx')
- input_grad: bfloat16 [2, 4, 4, 128, 2048], P('section', None, 'gy', 'gx')
- grad_gain_attn: float32 [2, 2048], P('section')
- grad_gain_ffn: float32 [2, 2048], P('section')
- grad_gain_query: float32 [2, 128], P('section')
- grad_gain_key: float32 [2, 128], P('section')
- grad_w_query: float32 [2, 2048, 4096], P('section', 'gy', 'gx')
- grad_w_key: float32 [2, 2048, 512], P('section', 'gy')
- grad_w_value: float32 [2, 2048, 512], P('section', 'gy')
- grad_w_out: float32 [2, 2048, 4096], P('section', 'gy', 'gx')
- grad_w_gate: float32 [2, 16, 2048, 768], P('section', ('gx', 'gy'))
- grad_w_up: float32 [2, 16, 2048, 768], P('section', ('gx', 'gy'))
- grad_w_down: float32 [2, 16, 768, 2048], P('section', ('gx', 'gy'))
The draws below stay inside these ranges and needn't reach their ends.
Inputs may be any that keep to these rules, and one draw needn't show every extreme that they name: `routes`: each row names 8 different experts. Within each aligned block of 32 rows (the tokens of one device for one layer and micro-batch) no expert is named by more than 32 rows, a bound that some block reaches. `segments`: along a group's 128 tokens the sequence numbers never fall; each sequence has 1 to 64 tokens and one has exactly 64.
All inputs are finite; a program needn't handle non-finite values.
Results may differ from the reference program's by a relative error of at most 0.028.
Values may be sent and summed in bfloat16 or wider, within the bound.
A program may use at most 448 MiB of HBM per device.

```python
import math
import jax
import jax.numpy as jnp
import numpy as np
from jax import lax

D = 2048
HQ = 32
KVH = 4
HD = 128
FF = 768
TOPK = 8
MICRO = 4
SEQS = 4
TOK_DEV = 32
LAYERS = 2
GROUPS = 4
TOK_G = 128
MAXLEN = 64
EXPERTS = 16
CAP = 32
N_GX = 4
N_GY = 4


def levels(key, shape, shards, low, top_value):
    loudness, own = 1.0, jax.random.fold_in(key, 6)
    for position, blocks in shards:
        steps = jnp.exp(jax.random.uniform(jax.random.fold_in(own, position), (blocks,), jnp.float32, low / len(shards), top_value / len(shards)))
        loudness = loudness * jnp.repeat(steps, shape[position] // blocks).reshape([-1 if axis == position else 1 for axis in range(len(shape))])
    return loudness


def split_up(count, total, reach, skew):
    loads = [(1 << 20) // math.isqrt(rank ** skew) + 1 for rank in range(2, count + 1)]
    spare, given = total - reach - (count - 1), [1] * (count - 1)
    while spare > 0:
        free = [i for i in range(count - 1) if given[i] < reach]
        whole, budget = sum([loads[i] for i in free]), spare
        for i in free:
            addition = min(reach - given[i], max(1, budget * loads[i] // whole), spare)
            given[i] = given[i] + addition
            spare = spare - addition
    return np.array([reach] + given)


def uneven_parts(key, count, total, reach, skew):
    if count == 2:
        one = jax.random.randint(key, (), max(1, total - reach), min(reach, total - 1) + 1)
        return jnp.stack([one, total - one])
    sizes = jnp.asarray(split_up(count, total, reach, skew), jnp.int32)
    twos = (count - 1) // 2
    donor, taker = sizes[1:1 + 2 * twos:2], sizes[2:2 + 2 * twos:2]
    slack = jnp.minimum(donor - 1, reach - taker)
    shifted = jax.random.randint(jax.random.fold_in(key, 1), (twos,), 0, 1 << 20) % (slack + 1)
    sizes = sizes.at[1:1 + 2 * twos:2].set(donor - shifted).at[2:2 + 2 * twos:2].set(taker + shifted)
    return sizes[jax.random.permutation(jax.random.fold_in(key, 2), count)]


def shared_out(own_key, own, number, rows, amount, top, bound, slope):
    order = jax.random.permutation(own_key, amount)
    crowded, usual = load_shares(amount, rows * top, bound, slope, True), load_shares(amount, rows * top, bound, slope, False)
    places = jnp.arange(amount)

    def named(lengths, offset_by):
        used = int((lengths > 0).sum())
        fixed = max(1, used // 4)
        passed = fixed + (places - fixed + offset_by * (used - fixed)) % max(1, amount - fixed)
        return jnp.zeros((amount,), jnp.int32).at[order[jnp.where(places < fixed, places, passed)]].set(jnp.asarray(lengths, jnp.int32))

    lengths = jnp.where(number % 4 == 0, named(crowded, number // 4), named(usual, number - number // 4 - 1))
    mixed = jax.random.permutation(jax.random.fold_in(own, 3), amount)
    source_of, taker = mixed[0:amount // 2 * 2:2], mixed[1:amount // 2 * 2:2]
    margin = jnp.minimum(lengths[source_of] - 1, bound - lengths[taker]) // 2
    margin = jnp.where((source_of == order[0]) | (taker == order[0]) | (lengths[taker] == 0), 0, jnp.maximum(margin, 0))
    passed = jax.random.randint(jax.random.fold_in(own, 4), (amount // 2,), 0, 1 << 20) % (margin + 1)
    lengths = lengths.at[source_of].add(-passed).at[taker].add(passed)
    members = jnp.searchsorted(jnp.cumsum(lengths), jnp.arange(rows * top), side="right").astype(jnp.int32)
    listing = members.reshape(top, rows).T
    listing = listing[jax.random.permutation(jax.random.fold_in(own, 1), rows)]
    offset_by = jax.random.randint(jax.random.fold_in(own, 2), (rows, 1), 0, top)
    return jnp.take_along_axis(listing, (jnp.arange(top)[None, :] + offset_by) % top, axis=1)


def load_shares(number_of, total, reach, lean, full):
    loads = [(1 << 20) // math.isqrt(rank ** lean) + 1 for rank in range(1, number_of + 1)]
    largest = reach if full else min(reach, max(-(-total // number_of), total * loads[0] // sum(loads)))
    least = 1 if total - largest >= number_of - 1 else 0
    given, spare = [largest] + [least] * (number_of - 1), total - largest - least * (number_of - 1)
    while spare > 0:
        movable = [i for i in range(1, number_of) if given[i] < largest] or [i for i in range(1, number_of) if given[i] < reach]
        pool, budget = sum([loads[i] for i in movable]), spare
        for i in movable:
            addition = min(reach - given[i], max(1, budget * loads[i] // pool), spare)
            given[i] = given[i] + addition
            spare = spare - addition
    return np.array(given)


def gaussian(own_key, extent, deviation, most, shards=(), kind=jnp.bfloat16):
    gain = levels(own_key, extent, shards, -0.22, 0.18) if shards else 1.0
    values = jax.random.normal(own_key, extent, jnp.float32) * deviation * gain
    return jnp.minimum(jnp.maximum(values, -most), most).astype(kind)


def setup_inputs(seed: int = 0) -> dict:
    arg_keys = jax.random.split(jax.random.key(seed), 17)
    inputs = gaussian(arg_keys[0], (MICRO, GROUPS, TOK_G, D), 1.0, 6.0, ((1, 4), (2, 4)))
    out_grad = gaussian(arg_keys[1], (MICRO, GROUPS, TOK_G, D), 1.0, 6.0, ((1, 4), (2, 4)))
    segments = jax.vmap(lambda own: jnp.searchsorted(jnp.cumsum(uneven_parts(own, SEQS, TOK_G, MAXLEN, 2)), jnp.arange(TOK_G), side="right"))(jax.random.split(arg_keys[2], MICRO * GROUPS)).reshape((MICRO, GROUPS, TOK_G)).astype(jnp.int32)
    routes_keys = jax.random.split(jax.random.fold_in(arg_keys[3], 1), LAYERS * MICRO * GROUPS * TOK_G // TOK_DEV)
    routes_turns = jax.random.permutation(jax.random.fold_in(arg_keys[3], 3), LAYERS * MICRO * GROUPS * TOK_G // TOK_DEV)
    routes = jax.vmap(lambda own, number: shared_out(jax.random.fold_in(arg_keys[3], 2), own, number, TOK_DEV, EXPERTS, TOPK, CAP, 2))(routes_keys, routes_turns).reshape((LAYERS, MICRO, GROUPS, TOK_G, TOPK))
    gates = jnp.clip(0.05 + 0.25 * jax.random.uniform(arg_keys[4], (LAYERS, MICRO, GROUPS, TOK_G, TOPK), jnp.float32) ** levels(arg_keys[4], (LAYERS, MICRO, GROUPS, TOK_G, TOPK), ((0, 2), (2, 4), (3, 4)), -0.2, 0.2), 0.05, 0.3)
    gain_attn = jnp.clip(1.0 + 0.1 * jax.random.normal(arg_keys[5], (LAYERS, D), jnp.float32), 0.5, 1.5)
    gain_ffn = jnp.clip(1.0 + 0.1 * jax.random.normal(arg_keys[6], (LAYERS, D), jnp.float32), 0.5, 1.5)
    gain_query = jnp.clip(1.0 + 0.1 * jax.random.normal(arg_keys[7], (LAYERS, HD), jnp.float32), 0.5, 1.5)
    gain_key = jnp.clip(1.0 + 0.1 * jax.random.normal(arg_keys[8], (LAYERS, HD), jnp.float32), 0.5, 1.5)
    w_query = gaussian(arg_keys[9], (LAYERS, D, HQ * HD), D ** -0.5, 0.125, ((0, 2), (1, 4), (2, 4)))
    w_key = gaussian(arg_keys[10], (LAYERS, D, KVH * HD), D ** -0.5, 0.125, ((0, 2), (1, 4)))
    w_value = gaussian(arg_keys[11], (LAYERS, D, KVH * HD), D ** -0.5, 0.125, ((0, 2), (1, 4)))
    w_out = gaussian(arg_keys[12], (LAYERS, D, HQ * HD), (HQ * HD // 32) ** -0.5, 0.5, ((0, 2), (1, 4), (2, 4)))
    w_gate = gaussian(arg_keys[13], (LAYERS, EXPERTS, D, FF), D ** -0.5, 0.125, ((0, 2), (1, 16)))
    w_up = gaussian(arg_keys[14], (LAYERS, EXPERTS, D, FF), D ** -0.5, 0.125, ((0, 2), (1, 16)))
    w_down = gaussian(arg_keys[15], (LAYERS, EXPERTS, FF, D), (FF // 8) ** -0.5, 0.625, ((0, 2), (1, 16)))
    return dict(inputs=inputs, out_grad=out_grad, segments=segments, routes=routes, gates=gates, gain_attn=gain_attn, gain_ffn=gain_ffn, gain_query=gain_query, gain_key=gain_key, w_query=w_query, w_key=w_key, w_value=w_value, w_out=w_out, w_gate=w_gate, w_up=w_up, w_down=w_down)


EPSILON = 1e-06
ROPE_BASE = 1000000.0

def normalize(tensor):
    scaling = lax.rsqrt(lax.optimization_barrier(jnp.mean(tensor * tensor, axis=-1, keepdims=True)) + EPSILON)
    return (tensor * scaling, scaling)

def norm_back(gradient, unit_vec, scaling):
    return scaling * (gradient - unit_vec * lax.optimization_barrier(jnp.mean(gradient * unit_vec, axis=-1, keepdims=True)))

def rotate(tensor, cosine, sine_part):
    halfway = tensor.shape[-1] // 2
    leading = tensor[..., :halfway]
    trailing = tensor[..., halfway:]
    return jnp.concatenate([leading * cosine - trailing * sine_part, trailing * cosine + leading * sine_part], axis=-1)

def rotate_back(gradient, cosine, sine_part):
    halfway = gradient.shape[-1] // 2
    leading = gradient[..., :halfway]
    trailing = gradient[..., halfway:]
    return jnp.concatenate([leading * cosine + trailing * sine_part, trailing * cosine - leading * sine_part], axis=-1)

def seq_tables(segment_ids):
    length_all = segment_ids.shape[0]
    position_ids = jnp.arange(length_all, dtype=jnp.int32)
    allowed = (segment_ids[:, None] == segment_ids[None, :]) & (position_ids[:, None] >= position_ids[None, :])
    positions = lax.optimization_barrier(jnp.sum(allowed.astype(jnp.int32), axis=1)) - 1
    halfway = HD // 2
    inverse = ROPE_BASE ** (-2.0 * jnp.arange(halfway, dtype=jnp.float32) / HD)
    angles = positions.astype(jnp.float32)[:, None] * inverse[None, :]
    return (allowed, jnp.cos(angles), jnp.sin(angles))

def settle(tensor):
    return lax.optimization_barrier(tensor.astype(jnp.bfloat16)).astype(jnp.float32)

def attend(packed):
    query_rope, key_rope, value_low, segment_ids = packed
    allowed = seq_tables(segment_ids)[0]
    repeat_count = HQ // KVH
    key_all = jnp.repeat(key_rope.astype(jnp.float32), repeat_count, axis=1)
    value_all = jnp.repeat(value_low.astype(jnp.float32), repeat_count, axis=1)
    scores = jnp.einsum('thd,shd->hts', query_rope.astype(jnp.float32), key_all) * (1.0 / math.sqrt(HD))
    exponent = jnp.where(allowed[None], jnp.exp(scores), 0.0)
    log_total = jnp.log(lax.optimization_barrier(jnp.sum(exponent, axis=-1)))
    probability = jnp.where(allowed[None], jnp.exp(scores - log_total[..., None]), 0.0)
    mixed_heads = jnp.einsum('hts,shd->thd', settle(probability), value_all).astype(jnp.bfloat16)
    return (mixed_heads, log_total)

def attend_back(packed):
    query_rope, key_rope, value_low, mixed_heads, grad_heads, log_total, segment_ids = packed
    allowed = seq_tables(segment_ids)[0]
    repeat_count = HQ // KVH
    key_all = jnp.repeat(key_rope.astype(jnp.float32), repeat_count, axis=1)
    value_all = jnp.repeat(value_low.astype(jnp.float32), repeat_count, axis=1)
    scores = jnp.einsum('thd,shd->hts', query_rope.astype(jnp.float32), key_all) * (1.0 / math.sqrt(HD))
    probability = jnp.where(allowed[None], jnp.exp(scores - log_total[..., None]), 0.0)
    grad_float = grad_heads.astype(jnp.float32)
    grad_value = jnp.einsum('hts,thd->shd', settle(probability), grad_float)
    grad_prob = jnp.einsum('thd,shd->hts', grad_float, value_all)
    delta_rows = lax.optimization_barrier(jnp.sum(grad_float * mixed_heads.astype(jnp.float32), axis=-1)).T
    grad_scores = settle(probability * (grad_prob - delta_rows[..., None]))
    grad_query = jnp.einsum('hts,shd->thd', grad_scores, key_all) * (1.0 / math.sqrt(HD))
    grad_key = jnp.einsum('hts,thd->shd', grad_scores, query_rope.astype(jnp.float32)) * (1.0 / math.sqrt(HD))
    return (grad_query, grad_key, grad_value)

def expert_rows(route_ids, gate_vals, expert):
    is_hit = route_ids == expert
    member = jnp.any(is_hit, axis=1)
    weight = lax.optimization_barrier(jnp.sum(jnp.where(is_hit, gate_vals, 0.0), axis=1))
    slot_total = N_GX * N_GY * CAP
    row_index = jnp.nonzero(member, size=slot_total, fill_value=0)[0]
    is_valid = jnp.arange(slot_total) < jnp.sum(member.astype(jnp.int32))
    return (row_index, jnp.where(is_valid, weight[row_index], 0.0))

def moe_forward(expert_in, route_ids, gate_vals, w_gate, w_up, w_down):

    def step_fn(running, expert_item):
        expert, gate_mat, up_mat, down_mat = expert_item
        row_index, weight = expert_rows(route_ids, gate_vals, expert)
        picked = expert_in[row_index]
        gate_pre = jnp.dot(picked, gate_mat, preferred_element_type=jnp.float32)
        up_proj = jnp.dot(picked, up_mat, preferred_element_type=jnp.float32)
        inner_act = (jax.nn.silu(gate_pre) * up_proj).astype(jnp.bfloat16)
        result = jnp.dot(inner_act, down_mat, preferred_element_type=jnp.float32).astype(jnp.bfloat16)
        return (running.at[row_index].add(result.astype(jnp.float32) * weight[:, None]), None)
    start_sum = jnp.zeros((expert_in.shape[0], D), jnp.float32)
    running, _ = lax.scan(step_fn, start_sum, (jnp.arange(EXPERTS, dtype=jnp.int32), w_gate, w_up, w_down))
    return running

def moe_backward(expert_in, route_ids, gate_vals, w_gate, w_up, w_down, gradient):

    def step_fn(running, expert_item):
        expert, gate_mat, up_mat, down_mat = expert_item
        row_index, weight = expert_rows(route_ids, gate_vals, expert)
        picked = expert_in[row_index]
        gate_pre = jnp.dot(picked, gate_mat, preferred_element_type=jnp.float32)
        up_proj = jnp.dot(picked, up_mat, preferred_element_type=jnp.float32)
        sigmoid_gate = jax.nn.sigmoid(gate_pre)
        silu_gate = gate_pre * sigmoid_gate
        inner_act = (jax.nn.silu(gate_pre) * up_proj).astype(jnp.bfloat16)
        grad_result = (gradient[row_index] * weight[:, None]).astype(jnp.bfloat16)
        grad_inner = jnp.dot(grad_result, down_mat.T, preferred_element_type=jnp.float32)
        grad_down = jnp.dot(inner_act.T, grad_result, preferred_element_type=jnp.float32)
        grad_gate_pre = (grad_inner * up_proj * sigmoid_gate * (1.0 + gate_pre * (1.0 - sigmoid_gate))).astype(jnp.bfloat16)
        grad_up_proj = (grad_inner * silu_gate).astype(jnp.bfloat16)
        grad_gate = jnp.dot(picked.T, grad_gate_pre, preferred_element_type=jnp.float32)
        grad_up = jnp.dot(picked.T, grad_up_proj, preferred_element_type=jnp.float32)
        grad_picked = (jnp.dot(grad_gate_pre, gate_mat.T, preferred_element_type=jnp.float32) + jnp.dot(grad_up_proj, up_mat.T, preferred_element_type=jnp.float32)).astype(jnp.bfloat16)
        return (running.at[row_index].add(grad_picked.astype(jnp.float32)), (grad_gate, grad_up, grad_down))
    start_sum = jnp.zeros((expert_in.shape[0], D), jnp.float32)
    running, grads = lax.scan(step_fn, start_sum, (jnp.arange(EXPERTS, dtype=jnp.int32), w_gate, w_up, w_down))
    return (running, grads)

def layer_forward(layer_in, segment_ids, route_ids, gate_vals, weights):
    w_query, w_key, w_value, w_out, gain_attn, gain_ffn, gain_query, gain_key, w_gate, w_up, w_down = weights
    group_count, group_len, _ = layer_in.shape
    hidden = layer_in.astype(jnp.float32).reshape(group_count * group_len, D)
    attn_unit, attn_scale = normalize(hidden)
    normed = (attn_unit * gain_attn).astype(jnp.bfloat16)
    queries = jnp.dot(normed, w_query, preferred_element_type=jnp.float32).reshape(group_count, group_len, HQ, HD)
    key_proj = jnp.dot(normed, w_key, preferred_element_type=jnp.float32).reshape(group_count, group_len, KVH, HD)
    value_low = jnp.dot(normed, w_value, preferred_element_type=jnp.float32).astype(jnp.bfloat16).reshape(group_count, group_len, KVH, HD)
    tables = jax.vmap(seq_tables)(segment_ids)
    cosine = tables[1][:, :, None, :]
    sine_part = tables[2][:, :, None, :]
    query_unit, query_scale = normalize(queries)
    key_unit, key_scale = normalize(key_proj)
    query_rope = rotate(query_unit * gain_query, cosine, sine_part).astype(jnp.bfloat16)
    key_rope = rotate(key_unit * gain_key, cosine, sine_part).astype(jnp.bfloat16)
    mixed_heads, log_total = lax.map(attend, (query_rope, key_rope, value_low, segment_ids))
    attn_out = jnp.dot(mixed_heads.reshape(group_count * group_len, HQ * HD), w_out.T, preferred_element_type=jnp.float32)
    middle = hidden + attn_out
    ffn_unit, ffn_scale = normalize(middle)
    expert_in = (ffn_unit * gain_ffn).astype(jnp.bfloat16)
    expert_sum = moe_forward(expert_in, route_ids.reshape(-1, TOPK), gate_vals.reshape(-1, TOPK), w_gate, w_up, w_down)
    result_low = (middle + expert_sum).astype(jnp.bfloat16).reshape(group_count, group_len, D)
    saved = (attn_unit, attn_scale, normed, query_unit, query_scale, key_unit, key_scale, cosine, sine_part, query_rope, key_rope, value_low, mixed_heads, log_total, ffn_unit, ffn_scale, expert_in)
    return (result_low, saved)

def layer_backward(grad_out, saved, segment_ids, route_ids, gate_vals, weights):
    w_query, w_key, w_value, w_out, gain_attn, gain_ffn, gain_query, gain_key, w_gate, w_up, w_down = weights
    attn_unit, attn_scale, normed, query_unit, query_scale, key_unit, key_scale, cosine, sine_part, query_rope, key_rope, value_low, mixed_heads, log_total, ffn_unit, ffn_scale, expert_in = saved
    group_count, group_len = segment_ids.shape
    row_total = group_count * group_len
    gradient = grad_out.reshape(row_total, D)
    grad_expert_in, moe_grads = moe_backward(expert_in, route_ids.reshape(-1, TOPK), gate_vals.reshape(-1, TOPK), w_gate, w_up, w_down, gradient)
    grad_ffn = lax.optimization_barrier(jnp.sum(grad_expert_in * ffn_unit, axis=0))
    grad_middle = gradient + norm_back(grad_expert_in * gain_ffn, ffn_unit, ffn_scale)
    middle_low = grad_middle.astype(jnp.bfloat16)
    mixed_flat = mixed_heads.reshape(row_total, HQ * HD)
    grad_out_w = jnp.dot(middle_low.T, mixed_flat, preferred_element_type=jnp.float32)
    grad_heads = jnp.dot(middle_low, w_out, preferred_element_type=jnp.float32).astype(jnp.bfloat16).reshape(group_count, group_len, HQ, HD)
    grad_query, grad_key, grad_value = lax.map(attend_back, (query_rope, key_rope, value_low, mixed_heads, grad_heads, log_total, segment_ids))
    repeat_count = HQ // KVH
    key_unit_all = jnp.repeat(key_unit, repeat_count, axis=2)
    key_scale_all = jnp.repeat(key_scale, repeat_count, axis=2)
    query_turn = rotate_back(grad_query, cosine, sine_part)
    grad_query_gain = lax.optimization_barrier(jnp.sum(query_turn * query_unit, axis=(0, 1, 2)))
    grad_query_pre = norm_back(query_turn * gain_query, query_unit, query_scale)
    key_turn = rotate_back(grad_key, cosine, sine_part)
    grad_key_gain = lax.optimization_barrier(jnp.sum(key_turn * key_unit_all, axis=(0, 1, 2)))
    grad_key_pre = norm_back(key_turn * gain_key, key_unit_all, key_scale_all)
    query_low = grad_query_pre.reshape(row_total, HQ * HD).astype(jnp.bfloat16)
    key_low = grad_key_pre.reshape(row_total, HQ * HD).astype(jnp.bfloat16)
    value_grad_low = grad_value.reshape(row_total, HQ * HD).astype(jnp.bfloat16)
    grad_q = jnp.dot(normed.T, query_low, preferred_element_type=jnp.float32)
    grad_k = jnp.dot(normed.T, key_low, preferred_element_type=jnp.float32).reshape(D, KVH, repeat_count, HD).sum(axis=2).reshape(D, KVH * HD)
    grad_v = jnp.dot(normed.T, value_grad_low, preferred_element_type=jnp.float32).reshape(D, KVH, repeat_count, HD).sum(axis=2).reshape(D, KVH * HD)
    key_wide = jnp.repeat(w_key.reshape(D, KVH, HD), repeat_count, axis=1).reshape(D, HQ * HD)
    value_wide = jnp.repeat(w_value.reshape(D, KVH, HD), repeat_count, axis=1).reshape(D, HQ * HD)
    grad_normed = jnp.dot(query_low, w_query.T, preferred_element_type=jnp.float32) + jnp.dot(key_low, key_wide.T, preferred_element_type=jnp.float32) + jnp.dot(value_grad_low, value_wide.T, preferred_element_type=jnp.float32)
    grad_attn = lax.optimization_barrier(jnp.sum(grad_normed * attn_unit, axis=0))
    grad_input = (grad_middle + norm_back(grad_normed * gain_attn, attn_unit, attn_scale)).astype(jnp.bfloat16)
    grads = (grad_attn, grad_ffn, grad_query_gain, grad_key_gain, grad_q, grad_k, grad_v, grad_out_w) + tuple(moe_grads)
    return (grad_input.reshape(group_count, group_len, D), grads)

def reference(inputs, out_grad, segments, routes, gates, gain_attn, gain_ffn, gain_query, gain_key, w_query, w_key, w_value, w_out, w_gate, w_up, w_down):
    stacked = (w_query, w_key, w_value, w_out, gain_attn, gain_ffn, gain_query, gain_key, w_gate, w_up, w_down)
    layer_params = [tuple((array[layer_index] for array in stacked)) for layer_index in range(LAYERS)]
    out_lists = [[] for _ in range(LAYERS)]
    grad_lists = [[] for _ in range(LAYERS)]
    totals = [None for _ in range(LAYERS)]
    for batch_index in range(MICRO):
        current = inputs[batch_index]
        saved_list = []
        for layer_index in range(LAYERS):
            current, saved = layer_forward(current, segments[batch_index], routes[layer_index, batch_index], gates[layer_index, batch_index], layer_params[layer_index])
            saved_list.append(saved)
            out_lists[layer_index].append(current)
        cotangent = out_grad[batch_index].astype(jnp.float32)
        for layer_index in reversed(range(LAYERS)):
            grad_low, grads = layer_backward(cotangent, saved_list[layer_index], segments[batch_index], routes[layer_index, batch_index], gates[layer_index, batch_index], layer_params[layer_index])
            grad_lists[layer_index].append(grad_low)
            cotangent = grad_low.astype(jnp.float32)
            if totals[layer_index] is None:
                totals[layer_index] = grads
            else:
                totals[layer_index] = jax.tree.map(lambda left, right: left + right, totals[layer_index], grads)
    layer_out = jnp.stack([jnp.stack(out_lists[layer_index]) for layer_index in range(LAYERS)])
    input_grad = jnp.stack([jnp.stack(grad_lists[layer_index]) for layer_index in range(LAYERS)])
    merged = [jnp.stack([totals[layer_index][slot] for layer_index in range(LAYERS)]) for slot in range(11)]
    return (layer_out, input_grad, merged[0], merged[1], merged[2], merged[3], merged[4], merged[5], merged[6], merged[7], merged[8], merged[9], merged[10])
```

```python
import functools
import math

import jax
import jax.numpy as jnp
from jax import lax
from jax.experimental import pallas as pl
from jax.experimental.pallas import tpu as pltpu
from jax.sharding import PartitionSpec as P

HQ = 32
KVH = 4
HD = 128
TOPK = 8

EPSILON = 1e-06
ROPE_BASE = 1000000.0
ROW_PAIR = (((0,), (0,)), ((), ()))
COL_PAIR = (((1,), (1,)), ((), ()))
F32 = jnp.float32
BF16 = jnp.bfloat16
MOST_ROWS = 1024


def normalize(tensor):
    scaling = lax.rsqrt(jnp.mean(tensor * tensor, axis=-1, keepdims=True) + EPSILON)
    return (tensor * scaling, scaling)


def norm_back(gradient, unit_vec, scaling):
    return scaling * (gradient - unit_vec * jnp.mean(gradient * unit_vec, axis=-1, keepdims=True))


def rotate(tensor, cosine, sine_part):
    halfway = tensor.shape[-1] // 2
    leading = tensor[..., :halfway]
    trailing = tensor[..., halfway:]
    return jnp.concatenate(
        [leading * cosine - trailing * sine_part, trailing * cosine + leading * sine_part], axis=-1
    )


def rotate_back(gradient, cosine, sine_part):
    return rotate(gradient, cosine, -sine_part)


def seq_tables(segment_ids, head_dim):
    length_all = segment_ids.shape[-1]
    position_ids = jnp.arange(length_all, dtype=jnp.int32)
    allowed = (segment_ids[:, :, None] == segment_ids[:, None, :]) & (
        position_ids[:, None] >= position_ids[None, :]
    )
    positions = jnp.sum(allowed.astype(jnp.int32), axis=-1) - 1
    halfway = head_dim // 2
    inverse = ROPE_BASE ** (-2.0 * jnp.arange(halfway, dtype=jnp.float32) / head_dim)
    angles = positions.astype(jnp.float32)[..., None] * inverse
    return (allowed, jnp.cos(angles), jnp.sin(angles))


def dot32(left, right, dims=None):
    if dims is None:
        return jnp.dot(left, right, preferred_element_type=F32)
    return lax.dot_general(left, right, dims, preferred_element_type=F32)


def gather_z(rows):
    return lax.all_gather(rows, "gx", axis=1, tiled=True)


def scatter_z(rows):
    return lax.psum_scatter(rows, "gx", scatter_dimension=1, tiled=True)


def gather_all(rows):
    return lax.all_gather(rows, ("gx", "gy"), axis=0, tiled=True)


def scatter_all(rows):
    return lax.psum_scatter(rows, ("gx", "gy"), scatter_dimension=0, tiled=True)


def both_layers(tensor):
    return lax.all_gather(tensor, "section", axis=0, tiled=False)


def dense_gates(route_ids, gate_vals, experts):
    onehot = route_ids[..., None] == jnp.arange(experts, dtype=jnp.int32)
    return jnp.sum(jnp.where(onehot, gate_vals[..., None], 0.0), axis=-2)


def swap_sections(tensor):
    return lax.ppermute(tensor, "section", [(0, 1), (1, 0)])


def remote(src, dst, send_sem, recv_sem, **where):
    return pltpu.make_async_remote_copy(
        src_ref=src,
        dst_ref=dst,
        send_sem=send_sem,
        recv_sem=recv_sem,
        device_id=where,
        device_id_type=pl.DeviceIdType.MESH,
    )


def hello(n, me, gy, with_plane):
    barrier = pltpu.get_barrier_semaphore()
    mesh_ids = pl.DeviceIdType.MESH

    @pl.when(me + 1 < n)
    def _():
        pl.semaphore_signal(barrier, 1, device_id={"gx": me + 1}, device_id_type=mesh_ids)

    @pl.when(me > 0)
    def _():
        pl.semaphore_signal(barrier, 1, device_id={"gx": me - 1}, device_id_type=mesh_ids)

    if with_plane:
        for bit in (1, 2):
            pl.semaphore_signal(
                barrier, 1, device_id={"gy": gy_flip(gy, bit)}, device_id_type=mesh_ids
            )
    peers = 2 if with_plane else 0
    at_end = (me == 0) | (me == n - 1)

    @pl.when(at_end)
    def _():
        pl.semaphore_wait(barrier, peers + 1)

    @pl.when(jnp.logical_not(at_end))
    def _():
        pl.semaphore_wait(barrier, peers + 2)


def gy_flip(gy, bits):
    low = lax.rem(gy, 2)
    high = gy // 2
    if bits & 1:
        low = 1 - low
    if bits & 2:
        high = 1 - high
    return high * 2 + low


def z_gather_steps(n, me, slot, sems, after):
    send_up, recv_up, send_down, recv_down = sems
    sends = []

    def up(k):
        return remote(slot(me - k), slot(me - k), send_up.at[k], recv_up.at[k], gx=me + 1)

    def down(k):
        return remote(slot(me + k), slot(me + k), send_down.at[k], recv_down.at[k], gx=me - 1)

    for k in range(n):
        @pl.when(me - k >= 0)
        def _():
            if k:
                remote(
                    slot(me - k), slot(me - k), send_up.at[k - 1], recv_up.at[k - 1], gx=me
                ).wait_recv()
            if k < n - 1:

                @pl.when(me + 1 < n)
                def _():
                    up(k).start()

            if k == 0:

                @pl.when(me > 0)
                def _():
                    down(0).start()

            after(me - k, k)

        if k:

            @pl.when(me + k < n)
            def _():
                remote(
                    slot(me + k), slot(me + k), send_down.at[k - 1], recv_down.at[k - 1], gx=me
                ).wait_recv()
                if k < n - 1:

                    @pl.when(me > 0)
                    def _():
                        down(k).start()

                after(me + k, k)


def z_gather_drain(n, me, slot, sems):
    send_up, recv_up, send_down, recv_down = sems
    for k in range(n - 1):

        @pl.when((me - k >= 0) & (me + 1 < n))
        def _():
            remote(slot(me - k), slot(me - k), send_up.at[k], recv_up.at[k], gx=me + 1).wait_send()

        @pl.when((me + k < n) & (me > 0))
        def _():
            remote(
                slot(me + k), slot(me + k), send_down.at[k], recv_down.at[k], gx=me - 1
            ).wait_send()


def flip_by(gy, step):
    low = lax.rem(lax.rem(gy, 2) + lax.rem(step, 2), 2)
    high = lax.rem(gy // 2 + step // 2, 2)
    return high * 2 + low


class Plane:
    def __init__(self, n, sems):
        self.n = n
        self.me = lax.axis_index("gx")
        self.gy = lax.axis_index("gy")
        self.cx, self.cy, self.cd = (gy_flip(self.gy, bits) for bits in (1, 2, 3))
        self.gather_sems = sems[:10]
        self.scatter_sems = sems[10:20]
        self.z_list = []
        for k in range((n + 1) // 2):
            self.z_list += [n - 1 - k] + ([k] if k != n - 1 - k else [])


    def gather_own_column(self, slot):
        su, ru, sd, rd, sx, rx, sy, ry, sf, rf = self.gather_sems
        c = self.gy

        def after(z, k):
            remote(slot(z, c), slot(z, c), sx.at[z], rx.at[z], gy=self.cx).start()
            remote(slot(z, c), slot(z, c), sy.at[z], ry.at[z], gy=self.cy).start()

        z_gather_steps(self.n, self.me, lambda z: slot(z, c), (su, ru, sd, rd), after)

    def gather_pass_on(self, slot):
        su, ru, sd, rd, sx, rx, sy, ry, sf, rf = self.gather_sems

        def forward(z):
            remote(slot(z, self.cx), slot(z, self.cx), sx.at[z], rx.at[z], gy=self.cx).wait_recv()
            remote(slot(z, self.cy), slot(z, self.cy), sy.at[z], ry.at[z], gy=self.cy).wait_recv()

            @pl.when(lax.rem(z, 2) == 0)
            def _():
                remote(
                    slot(z, self.cy), slot(z, self.cy), sf.at[z], rf.at[z], gy=self.cx
                ).start()

            @pl.when(lax.rem(z, 2) == 1)
            def _():
                remote(
                    slot(z, self.cx), slot(z, self.cx), sf.at[z], rf.at[z], gy=self.cy
                ).start()

        for k in range(self.n):

            @pl.when(self.me - k >= 0)
            def _():
                forward(self.me - k)

            if k:

                @pl.when(self.me + k < self.n)
                def _():
                    forward(self.me + k)

    def gather_far_column(self, slot):
        sf, rf = self.gather_sems[8:]
        for z in range(self.n):
            remote(slot(z, self.cd), slot(z, self.cd), sf.at[z], rf.at[z], gy=self.cx).wait_recv()

    def gather_drain(self, slot):
        su, ru, sd, rd, sx, rx, sy, ry, sf, rf = self.gather_sems
        z_gather_drain(self.n, self.me, lambda z: slot(z, self.gy), (su, ru, sd, rd))
        for z in range(self.n):
            one = slot(z, self.gy)
            remote(one, one, sx.at[z], rx.at[z], gy=self.cx).wait_send()
            remote(one, one, sy.at[z], ry.at[z], gy=self.cy).wait_send()
            remote(one, one, sf.at[z], rf.at[z], gy=self.cx).wait_send()


    def to_x(self, z):
        sx, rx = self.scatter_sems[4:6]
        return remote(self.part(z, self.cx), self.xin.at[z], sx.at[z], rx.at[z], gy=self.cx)

    def to_y(self, z):
        sy, ry = self.scatter_sems[6:8]
        return remote(self.part(z, self.cy), self.yin.at[z], sy.at[z], ry.at[z], gy=self.cy)

    def far(self, z):
        sf, rf = self.scatter_sems[8:]
        return remote(
            self.part(z, self.cd),
            self.din.at[z],
            sf.at[z],
            rf.at[z],
            gy=self.cx if z % 2 == 0 else self.cy,
        )

    def scatter_setup(self, part, xin, yin, din, zup, zdn, stage, acc):
        self.part, self.xin, self.yin, self.din = part, xin, yin, din
        self.zup, self.zdn, self.stage, self.acc = zup, zdn, stage, acc

    def scatter_x(self):
        for z in self.z_list:
            if z % 2 == 0:
                self.to_x(z).start()

    def scatter_y(self):
        for z in self.z_list:
            if z % 2 == 1:
                self.to_y(z).start()

    def scatter_far(self):
        for z in self.z_list:
            self.far(z).start()

    def scatter_pass_on(self, z):
        self.far(z).wait_recv()
        mine = self.part(z, self.cy if z % 2 == 0 else self.cx)
        add_rows(mine, mine, self.din.at[z])
        (self.to_y if z % 2 == 0 else self.to_x)(z).start()

    def scatter_line(self, z, total):
        n, me, acc = self.n, self.me, self.acc
        su, ru, sd, rd = self.scatter_sems[:4]
        self.to_x(z).wait_recv()
        self.to_y(z).wait_recv()
        add_rows(acc, self.part(z, self.gy), self.xin.at[z], self.yin.at[z])
        up = remote(self.stage.at[z], self.zup.at[z], su.at[z], ru.at[z], gx=me + 1)
        down = remote(self.stage.at[z], self.zdn.at[z], sd.at[z], rd.at[z], gx=me - 1)

        @pl.when((me < z) & (me > 0))
        def _():
            up.wait_recv()
            add_rows(acc, acc, self.zup.at[z])

        @pl.when((me > z) & (me < n - 1))
        def _():
            down.wait_recv()
            add_rows(acc, acc, self.zdn.at[z])

        @pl.when(me != z)
        def _():
            add_rows(self.stage.at[z], acc)

        @pl.when(me < z)
        def _():
            up.start()

        @pl.when(me > z)
        def _():
            down.start()

        @pl.when(me == z)
        def _():
            add_rows(total, acc)

    def scatter_finish(self, total):
        n, me = self.n, self.me
        su, ru, sd, rd = self.scatter_sems[:4]

        @pl.when(me > 0)
        def _():
            remote(self.stage.at[me], self.zup.at[me], su.at[me], ru.at[me], gx=me - 1).wait_recv()
            add_rows(total, total, self.zup.at[me])

        @pl.when(me < n - 1)
        def _():
            remote(self.stage.at[me], self.zdn.at[me], sd.at[me], rd.at[me], gx=me + 1).wait_recv()
            add_rows(total, total, self.zdn.at[me])

        for z in self.z_list:
            self.to_x(z).wait_send()
            self.to_y(z).wait_send()
            self.far(z).wait_send()

            @pl.when(me < z)
            def _():
                remote(self.stage.at[z], self.zup.at[z], su.at[z], ru.at[z], gx=me + 1).wait_send()

            @pl.when(me > z)
            def _():
                remote(self.stage.at[z], self.zdn.at[z], sd.at[z], rd.at[z], gx=me - 1).wait_send()


def add_rows(out, *terms):
    rows = out.shape[0]
    step = 16

    def body(i, carry):
        at = pl.ds(pl.multiple_of(i * step, step), step)
        value = terms[0][at].astype(F32)
        for term in terms[1:]:
            value = value + term[at].astype(F32)
        out[at] = value.astype(out.dtype)
        return carry

    lax.fori_loop(0, rows // step, body, 0)


def fetch_layer(layer, own, other, held, sems):
    section = lax.axis_index("section")

    @pl.when(section == layer)
    def _():
        for k, ref in enumerate(own):
            pltpu.make_async_copy(ref, held[k], sems.at[k]).start()

    @pl.when(section != layer)
    def _():
        for k, ref in enumerate(other):
            pltpu.make_async_copy(ref, held[k], sems.at[k]).start()


def fetch_wait(own, held, sems, which):
    for k in which:
        pltpu.make_async_copy(own[k], held[k], sems.at[k]).wait()


def moe_forward_kernel(
    n,
    layer,
    mid_ref,
    pay_ref,
    wg_own,
    wu_own,
    wd_own,
    wg_other,
    wu_other,
    wd_other,
    out_ref,
    arrived_ref,
    weight_ref,
    gp_ref,
    up_ref,
    inner_ref,
    pay,
    wg,
    wu,
    wd,
    part,
    xin,
    yin,
    din,
    zup,
    zdn,
    stage,
    acc,
    total,
    gp,
    up,
    inner,
    wsem,
    osem,
    *sems,
):
    r, d = mid_ref.shape
    ff = wg.shape[1]
    rows = n * r
    experts = 4 * n
    own, other, held = (
        (wg_own, wu_own, wd_own),
        (wg_other, wu_other, wd_other),
        (wg, wu, wd),
    )
    fetch_layer(layer, own, other, held, wsem)
    plane = Plane(n, sems)
    me, gy = plane.me, plane.gy
    hello(n, me, gy, True)
    pay[pl.ds(pl.multiple_of((gy * n + me) * r, r), r)] = pay_ref[...]

    def slot(z, c):
        return pay.at[pl.ds((c * n + z) * r, r)]

    plane.scatter_setup(lambda z, c: part.at[c * n + z], xin, yin, din, zup, zdn, stage, acc)
    plane.gather_own_column(slot)
    fetch_wait(own, held, wsem, range(3))
    expert = me * 4 + gy

    def column(s, carry):
        c = flip_by(gy, s)

        @pl.when(s == 1)
        def _():
            plane.gather_pass_on(slot)

        @pl.when(s == 3)
        def _():
            plane.gather_far_column(slot)

        at = pl.ds(pl.multiple_of(c * rows, rows), rows)
        gate_cols = pay[at, d : d + 128].astype(F32)
        lane = lax.broadcasted_iota(jnp.int32, (rows, 128), 1)
        hit = ((lane == expert) | (lane == expert + experts)) & (lane < 2 * experts)
        weight = jnp.sum(jnp.where(hit, gate_cols, 0.0), axis=1, keepdims=True)
        weight_ref[at] = weight
        block = pay[at, :d]
        for j in range(ff // 256):
            cols = slice(j * 256, (j + 1) * 256)
            g = jnp.dot(block, wg[:, cols], preferred_element_type=F32)
            u = jnp.dot(block, wu[:, cols], preferred_element_type=F32)
            gp[at, cols] = g.astype(BF16)
            up[at, cols] = u.astype(BF16)
            inner[at, cols] = (g / (1.0 + jnp.exp(-g)) * u).astype(BF16)
        act = inner[at]
        for j in range(d // 256):
            cols = slice(j * 256, (j + 1) * 256)
            res = jnp.dot(act, wd[:, cols], preferred_element_type=F32) * weight
            part[pl.ds(pl.multiple_of(c * n, n), n), :, cols] = (
                res.astype(BF16).reshape(n, r, 256)
            )

        @pl.when(s == 1)
        def _():
            plane.scatter_x()

        @pl.when(s == 2)
        def _():
            plane.scatter_y()

        return carry

    lax.fori_loop(0, 4, column, 0)
    plane.scatter_far()
    saves = [
        pltpu.make_async_copy(pay.at[:, pl.ds(0, d)], arrived_ref, osem.at[0]),
        pltpu.make_async_copy(gp, gp_ref, osem.at[1]),
        pltpu.make_async_copy(up, up_ref, osem.at[2]),
        pltpu.make_async_copy(inner, inner_ref, osem.at[3]),
    ]
    for save in saves:
        save.start()
    for z in plane.z_list:
        plane.scatter_pass_on(z)
    for z in plane.z_list:
        plane.scatter_line(z, total)
    plane.scatter_finish(total)
    add_rows(out_ref, mid_ref, total)
    plane.gather_drain(slot)
    for save in saves:
        save.wait()


def scatter_buffers(n, r, d):
    return [pltpu.VMEM((4 * n, r, d), BF16)] + [pltpu.VMEM((n, r, d), BF16)] * 6 + [
        pltpu.VMEM((r, d), F32)
    ] * 2


def in_vmem(count):
    return [pl.BlockSpec(memory_space=pltpu.VMEM)] * count


def in_place(count):
    return [pl.BlockSpec(memory_space=pl.ANY)] * count


def moe_forward(layer, n, mid, payload, own, other, cid):
    r, d = mid.shape
    ff = own[0].shape[1]
    total_rows = 4 * n * r
    width = payload.shape[1]
    return pl.pallas_call(
        functools.partial(moe_forward_kernel, n, layer),
        out_shape=(
            jax.ShapeDtypeStruct((r, d), BF16),
            jax.ShapeDtypeStruct((total_rows, d), BF16),
            jax.ShapeDtypeStruct((total_rows, 1), F32),
            jax.ShapeDtypeStruct((total_rows, ff), BF16),
            jax.ShapeDtypeStruct((total_rows, ff), BF16),
            jax.ShapeDtypeStruct((total_rows, ff), BF16),
        ),
        in_specs=in_vmem(2) + in_place(6),
        out_specs=tuple(in_vmem(1) + in_place(1) + in_vmem(1) + in_place(3)),
        scratch_shapes=[
            pltpu.VMEM((total_rows, width), BF16),
            pltpu.VMEM((d, ff), BF16),
            pltpu.VMEM((d, ff), BF16),
            pltpu.VMEM((ff, d), BF16),
        ]
        + scatter_buffers(n, r, d)
        + [pltpu.VMEM((total_rows, ff), BF16)] * 3
        + [pltpu.SemaphoreType.DMA((3,)), pltpu.SemaphoreType.DMA((4,))]
        + [pltpu.SemaphoreType.DMA((n,))] * 20,
        compiler_params=pltpu.CompilerParams(
            collective_id=cid, has_side_effects=True, vmem_limit_bytes=63 << 20
        ),
        name="moe_forward",
    )(mid, payload, *own, *other)


def moe_backward_kernel(
    n,
    layer,
    cot_ref,
    mid_ref,
    gain_ref,
    weight_ref,
    arrived_hbm,
    gp_hbm,
    up_hbm,
    inner_hbm,
    wg_own,
    wu_own,
    wd_own,
    wg_other,
    wu_other,
    wd_other,
    dmid_ref,
    dgain_ref,
    grad_gate_ref,
    grad_up_ref,
    grad_down_ref,
    cots,
    wg,
    wu,
    wd,
    part,
    xin,
    yin,
    din,
    zup,
    zdn,
    stage,
    acc,
    total,
    arrived,
    gp,
    up,
    inner,
    de,
    out_gate,
    out_up,
    out_down,
    wsem,
    isem,
    osem,
    *sems,
):
    r, d = mid_ref.shape
    ff = wg.shape[1]
    rows = n * r
    own, other, held = (
        (wg_own, wu_own, wd_own),
        (wg_other, wu_other, wd_other),
        (wg, wu, wd),
    )
    loads = [
        pltpu.make_async_copy(gp_hbm, gp, isem.at[0]),
        pltpu.make_async_copy(up_hbm, up, isem.at[1]),
        pltpu.make_async_copy(arrived_hbm, arrived, isem.at[2]),
        pltpu.make_async_copy(inner_hbm, inner, isem.at[3]),
    ]
    fetch_layer(layer, own, other, held, wsem)
    for load in loads:
        load.start()
    plane = Plane(n, sems)
    me, gy = plane.me, plane.gy
    hello(n, me, gy, True)
    cots[pl.ds(pl.multiple_of((gy * n + me) * r, r), r)] = cot_ref[...]

    def slot(z, c):
        return cots.at[pl.ds((c * n + z) * r, r)]

    plane.scatter_setup(lambda z, c: part.at[c * n + z], xin, yin, din, zup, zdn, stage, acc)
    plane.gather_own_column(slot)
    fetch_wait(own, held, wsem, range(3))
    for load in loads:
        load.wait()

    def column(s, carry):
        c = flip_by(gy, s)

        @pl.when(s == 1)
        def _():
            plane.gather_pass_on(slot)

        @pl.when(s == 3)
        def _():
            plane.gather_far_column(slot)

        at = pl.ds(pl.multiple_of(c * rows, rows), rows)
        de[at] = (cots[at].astype(F32) * weight_ref[at]).astype(BF16)
        block = de[at]
        for j in range(ff // 256):
            cols = slice(j * 256, (j + 1) * 256)
            dz = dot32(block, wd[cols], COL_PAIR)
            g = gp[at, cols].astype(F32)
            u = up[at, cols].astype(F32)
            sg = 1.0 / (1.0 + jnp.exp(-g))
            gp[at, cols] = (dz * u * sg * (1.0 + g * (1.0 - sg))).astype(BF16)
            up[at, cols] = (dz * g * sg).astype(BF16)
        dgp = gp[at]
        dup = up[at]
        for j in range(d // 256):
            cols = slice(j * 256, (j + 1) * 256)
            res = dot32(dgp, wg[cols], COL_PAIR) + dot32(dup, wu[cols], COL_PAIR)
            part[pl.ds(pl.multiple_of(c * n, n), n), :, cols] = (
                res.astype(BF16).reshape(n, r, 256)
            )

        @pl.when(s == 1)
        def _():
            plane.scatter_x()

        @pl.when(s == 2)
        def _():
            plane.scatter_y()

        return carry

    lax.fori_loop(0, 4, column, 0)
    plane.scatter_far()

    def chunk_saves(i):
        at = pl.ds(pl.multiple_of(i * 256, 256), 256)
        return (
            pltpu.make_async_copy(out_gate.at[at], grad_gate_ref.at[at], osem.at[0, i]),
            pltpu.make_async_copy(out_up.at[at], grad_up_ref.at[at], osem.at[1, i]),
            pltpu.make_async_copy(out_down.at[:, at], grad_down_ref.at[:, at], osem.at[2, i]),
        )

    def weight_grads(first, last):
        def chunk(i, carry):
            at = pl.ds(pl.multiple_of(i * 256, 256), 256)
            left = arrived[:, at]
            out_gate[at] = dot32(left, gp[...], ROW_PAIR).astype(BF16)
            out_up[at] = dot32(left, up[...], ROW_PAIR).astype(BF16)
            out_down[:, at] = dot32(inner[...], de[:, at], ROW_PAIR).astype(BF16)
            for save in chunk_saves(i):
                save.start()
            return carry

        lax.fori_loop(first, last, chunk, 0)

    chunks = d // 256
    cut = [0, chunks * 2 // 8, chunks * 4 // 8, chunks * 6 // 8, chunks]
    weight_grads(cut[0], cut[1])
    for z in plane.z_list:
        plane.scatter_pass_on(z)
    weight_grads(cut[1], cut[2])
    for k, z in enumerate(plane.z_list):
        plane.scatter_line(z, total)
        if k == 0:
            weight_grads(cut[2], cut[3])
    weight_grads(cut[3], cut[4])
    plane.scatter_finish(total)

    mid = mid_ref[...]
    scale = lax.rsqrt(jnp.mean(mid * mid, axis=-1, keepdims=True) + EPSILON)
    unit = mid * scale
    db = total[...]
    dgain_ref[...] = jnp.sum(db * unit, axis=0, keepdims=True)
    dmid_ref[...] = cot_ref[...].astype(F32) + norm_back(db * gain_ref[...], unit, scale)
    plane.gather_drain(slot)
    for i in range(chunks):
        for save in chunk_saves(i):
            save.wait()


def moe_backward(layer, n, cot, mid, gain, weight, arrived, gp, up, inner, own, other, cid):
    r, d = mid.shape
    ff = own[0].shape[1]
    total_rows = 4 * n * r
    return pl.pallas_call(
        functools.partial(moe_backward_kernel, n, layer),
        out_shape=(
            jax.ShapeDtypeStruct((r, d), F32),
            jax.ShapeDtypeStruct((1, d), F32),
            jax.ShapeDtypeStruct((d, ff), BF16),
            jax.ShapeDtypeStruct((d, ff), BF16),
            jax.ShapeDtypeStruct((ff, d), BF16),
        ),
        in_specs=in_vmem(4) + in_place(10),
        out_specs=tuple(in_vmem(2) + in_place(3)),
        scratch_shapes=[
            pltpu.VMEM((total_rows, d), BF16),
            pltpu.VMEM((d, ff), BF16),
            pltpu.VMEM((d, ff), BF16),
            pltpu.VMEM((ff, d), BF16),
        ]
        + scatter_buffers(n, r, d)
        + [pltpu.VMEM((total_rows, d), BF16)]
        + [pltpu.VMEM((total_rows, ff), BF16)] * 3
        + [pltpu.VMEM((total_rows, d), BF16)]
        + [pltpu.VMEM((d, ff), BF16)] * 2
        + [pltpu.VMEM((ff, d), BF16)]
        + [
            pltpu.SemaphoreType.DMA((3,)),
            pltpu.SemaphoreType.DMA((4,)),
            pltpu.SemaphoreType.DMA((3, d // 256)),
        ]
        + [pltpu.SemaphoreType.DMA((n,))] * 20,
        compiler_params=pltpu.CompilerParams(
            collective_id=cid, has_side_effects=True, vmem_limit_bytes=63 << 20
        ),
        name="moe_backward",
    )(cot, mid, gain, weight, arrived, gp, up, inner, *own, *other)


class Line:
    def __init__(self, n, sems, zup, zdn, stage, acc):
        self.n = n
        self.me = lax.axis_index("gx")
        self.sems = sems
        self.zup, self.zdn, self.stage, self.acc = zup, zdn, stage, acc
        self.z_list = []
        for k in range((n + 1) // 2):
            self.z_list += [n - 1 - k] + ([k] if k != n - 1 - k else [])

    def up(self, z):
        su, ru = self.sems[:2]
        return remote(self.stage.at[z], self.zup.at[z], su.at[z], ru.at[z], gx=self.me + 1)

    def down(self, z):
        sd, rd = self.sems[2:]
        return remote(self.stage.at[z], self.zdn.at[z], sd.at[z], rd.at[z], gx=self.me - 1)

    def move(self, z, total):
        n, me, acc = self.n, self.me, self.acc

        @pl.when((me < z) & (me > 0))
        def _():
            self.up(z).wait_recv()
            add_rows(acc, acc, self.zup.at[z])

        @pl.when((me > z) & (me < n - 1))
        def _():
            self.down(z).wait_recv()
            add_rows(acc, acc, self.zdn.at[z])

        @pl.when(me != z)
        def _():
            add_rows(self.stage.at[z], acc)

        @pl.when(me < z)
        def _():
            self.up(z).start()

        @pl.when(me > z)
        def _():
            self.down(z).start()

        @pl.when(me == z)
        def _():
            add_rows(total, acc)

    def finish(self, total):
        n, me = self.n, self.me

        @pl.when(me > 0)
        def _():
            self.up(me).wait_recv()
            add_rows(total, total, self.zup.at[me])

        @pl.when(me < n - 1)
        def _():
            self.down(me).wait_recv()
            add_rows(total, total, self.zdn.at[me])

        for z in self.z_list:

            @pl.when(me < z)
            def _():
                self.up(z).wait_send()

            @pl.when(me > z)
            def _():
                self.down(z).wait_send()


def unit_of(value):
    scale = lax.rsqrt(jnp.mean(value * value, axis=-1, keepdims=True) + EPSILON)
    return value * scale, scale


def half_turn(value):
    return pltpu.roll(value, value.shape[-1] // 2, axis=value.ndim - 1)


def attn_forward_kernel(
    n,
    layer,
    heads,
    x_ref,
    gain_attn,
    gain_ffn,
    gain_query,
    gain_key,
    cos_ref,
    sin_ref,
    mask_ref,
    gates_ref,
    win_own,
    wout_own,
    win_other,
    wout_other,
    mid_ref,
    pay_ref,
    normed_hbm,
    proj_hbm,
    qr_hbm,
    kr_ref,
    v_ref,
    prob_hbm,
    mixed_hbm,
    win,
    wout,
    normed,
    proj,
    qr,
    prob,
    mixed,
    col,
    zup,
    zdn,
    stage,
    acc,
    total,
    wsem,
    osem,
    *sems,
):
    mb, length, d = normed.shape
    t = length // n
    r = mb * t
    span = heads * HD
    me = lax.axis_index("gx")
    own, other, held = (win_own, wout_own), (win_other, wout_other), (win, wout)
    fetch_layer(layer, own, other, held, wsem)
    hello(n, me, None, False)
    hidden = x_ref[...].astype(F32)
    unit, _ = unit_of(hidden)
    low = (unit * gain_attn[...]).astype(BF16)
    normed[:, pl.ds(pl.multiple_of(me * t, t), t)] = low.reshape(mb, t, d)

    def slot(z):
        return normed.at[:, pl.ds(z * t, t)]

    z_gather_steps(n, me, slot, sems[:4], lambda z, k: None)
    saves = [
        pltpu.make_async_copy(normed, normed_hbm, osem.at[0]),
        pltpu.make_async_copy(proj, proj_hbm, osem.at[1]),
        pltpu.make_async_copy(qr, qr_hbm, osem.at[2]),
        pltpu.make_async_copy(prob, prob_hbm, osem.at[3]),
        pltpu.make_async_copy(mixed, mixed_hbm, osem.at[4]),
    ]
    saves[0].start()
    fetch_wait(own, held, wsem, (0,))
    every = normed[...].reshape(mb * length, d)
    for j in range((span + 2 * HD) // 256):
        cols = slice(j * 256, (j + 1) * 256)
        proj[:, cols] = jnp.dot(every, win[:, cols], preferred_element_type=F32)
    saves[1].start()
    cosine, sine = cos_ref[...], sin_ref[...]
    key_unit, _ = unit_of(proj[:, span : span + HD])
    key = key_unit * gain_key[...]
    kr_ref[...] = (key * cosine + half_turn(key) * sine).astype(BF16)
    v_ref[...] = proj[:, span + HD :].astype(BF16)

    def head(h, carry):
        at = pl.ds(pl.multiple_of(h * HD, HD), HD)
        query_unit, _ = unit_of(proj[:, at])
        query = query_unit * gain_query[...]
        turned = (query * cosine + half_turn(query) * sine).astype(BF16)
        qr[:, at] = turned
        for m in range(mb):
            rows = slice(m * length, (m + 1) * length)
            scores = dot32(turned[rows], kr_ref[rows], COL_PAIR) * (1.0 / math.sqrt(HD))
            exponent = jnp.where(mask_ref[m] > 0.5, jnp.exp(scores), 0.0)
            p = (exponent / jnp.sum(exponent, axis=-1, keepdims=True)).astype(BF16)
            prob[m * heads + h] = p
            mixed[rows, at] = jnp.dot(p, v_ref[rows], preferred_element_type=F32).astype(BF16)
        return carry

    lax.fori_loop(0, heads, head, 0)
    saves[2].start()
    saves[3].start()
    saves[4].start()
    fetch_wait(own, held, wsem, (1,))
    both = mixed[...]

    def out_cols(j, carry):
        at = pl.ds(pl.multiple_of(j * 256, 256), 256)
        res = dot32(both, wout[at], COL_PAIR).astype(BF16)
        for m in range(mb):
            for z in range(n):
                col[z, m * t : (m + 1) * t, at] = res[m * length + z * t : m * length + (z + 1) * t]
        return carry

    lax.fori_loop(0, d // 256, out_cols, 0)
    line = Line(n, sems[4:], zup, zdn, stage, acc)
    for z in line.z_list:
        add_rows(acc, col.at[z])
        line.move(z, total)
    line.finish(total)
    mid = x_ref[...].astype(F32) + total[...]
    mid_ref[...] = mid
    unit, _ = unit_of(mid)
    pay_ref[:, :d] = (unit * gain_ffn[...]).astype(BF16)
    pay_ref[:, d:] = gates_ref[...]
    z_gather_drain(n, me, slot, sems[:4])
    for save in saves:
        save.wait()


def line_buffers(n, r, d):
    return [pltpu.VMEM((n, r, d), BF16)] * 4 + [pltpu.VMEM((r, d), F32)] * 2


def attn_forward(layer, n, x, gains, tables, gate_cols, own, other, cid, mb):
    r, d = x.shape
    cosine, sine, mask = tables
    total_rows = cosine.shape[0]
    length = total_rows // mb
    width = own[0].shape[1]
    heads = own[1].shape[1] // HD
    span = heads * HD
    shape = jax.ShapeDtypeStruct
    return pl.pallas_call(
        functools.partial(attn_forward_kernel, n, layer, heads),
        out_shape=(
            shape((r, d), F32),
            shape((r, d + 128), BF16),
            shape((mb, length, d), BF16),
            shape((total_rows, width), F32),
            shape((total_rows, span), BF16),
            shape((total_rows, HD), BF16),
            shape((total_rows, HD), BF16),
            shape((mb * heads, length, length), BF16),
            shape((total_rows, span), BF16),
        ),
        in_specs=in_vmem(9) + in_place(4),
        out_specs=tuple(in_vmem(2) + in_place(3) + in_vmem(2) + in_place(2)),
        scratch_shapes=[
            pltpu.VMEM((d, width), BF16),
            pltpu.VMEM((d, span), BF16),
            pltpu.VMEM((mb, length, d), BF16),
            pltpu.VMEM((total_rows, width), F32),
            pltpu.VMEM((total_rows, span), BF16),
            pltpu.VMEM((mb * heads, length, length), BF16),
            pltpu.VMEM((total_rows, span), BF16),
        ]
        + line_buffers(n, r, d)
        + [pltpu.SemaphoreType.DMA((2,)), pltpu.SemaphoreType.DMA((5,))]
        + [pltpu.SemaphoreType.DMA((n,))] * 8,
        compiler_params=pltpu.CompilerParams(
            collective_id=cid, has_side_effects=True, vmem_limit_bytes=60 << 20
        ),
        name="attn_forward",
    )(x, *gains, cosine, sine, mask, gate_cols, *own, *other)


def attn_backward_kernel(
    n,
    layer,
    heads,
    dmid_ref,
    x_ref,
    gain_attn,
    gain_query,
    gain_key,
    cos_ref,
    sin_ref,
    kr_ref,
    v_ref,
    normed_hbm,
    proj_hbm,
    qr_hbm,
    prob_hbm,
    mixed_hbm,
    win_own,
    wout_own,
    win_other,
    wout_other,
    cot_ref,
    dgain_attn,
    dgain_query,
    dgain_key,
    grad_in_hbm,
    grad_out_hbm,
    win,
    wout,
    normed,
    proj,
    qr,
    prob,
    mixed,
    dmids,
    dheads,
    dproj,
    dkey,
    dvalue,
    grad_in,
    grad_out,
    col,
    zup,
    zdn,
    stage,
    acc,
    total,
    wsem,
    isem,
    osem,
    *sems,
):
    mb, length, d = normed.shape
    t = length // n
    span = heads * HD
    me = lax.axis_index("gx")
    inv_root = 1.0 / math.sqrt(HD)
    own, other, held = (wout_own, win_own), (wout_other, win_other), (wout, win)
    fetch_layer(layer, own, other, held, wsem)
    loads = [
        pltpu.make_async_copy(prob_hbm, prob, isem.at[0]),
        pltpu.make_async_copy(mixed_hbm, mixed, isem.at[1]),
        pltpu.make_async_copy(qr_hbm, qr, isem.at[2]),
        pltpu.make_async_copy(proj_hbm, proj, isem.at[3]),
        pltpu.make_async_copy(normed_hbm, normed, isem.at[4]),
    ]
    for load in loads:
        load.start()
    hello(n, me, None, False)
    dmids[:, pl.ds(pl.multiple_of(me * t, t), t)] = dmid_ref[...].astype(BF16).reshape(mb, t, d)

    def slot(z):
        return dmids.at[:, pl.ds(z * t, t)]

    z_gather_steps(n, me, slot, sems[:4], lambda z, k: None)
    fetch_wait(own, held, wsem, (0,))
    every = dmids[...].reshape(mb * length, d)
    for j in range(span // 256):
        cols = slice(j * 256, (j + 1) * 256)
        dheads[:, cols] = jnp.dot(every, wout[:, cols], preferred_element_type=F32).astype(BF16)
    for load in loads:
        load.wait()
    cosine, sine = cos_ref[...], sin_ref[...]
    dkey[...] = jnp.zeros_like(dkey)
    dvalue[...] = jnp.zeros_like(dvalue)
    dgain_query[...] = jnp.zeros_like(dgain_query)

    def head(h, carry):
        at = pl.ds(pl.multiple_of(h * HD, HD), HD)
        for m in range(mb):
            rows = slice(m * length, (m + 1) * length)
            p = prob[m * heads + h]
            dh = dheads[rows, at]
            dvalue[rows] += dot32(p, dh, ROW_PAIR)
            dp = dot32(dh, v_ref[rows], COL_PAIR)
            delta = jnp.sum(
                dh.astype(F32) * mixed[rows, at].astype(F32), axis=-1, keepdims=True
            )
            ds = (p.astype(F32) * (dp - delta)).astype(BF16)
            dkey[rows] += dot32(ds, qr[rows, at], ROW_PAIR) * inv_root
            dq = jnp.dot(ds, kr_ref[rows], preferred_element_type=F32) * inv_root
            turned = dq * cosine[rows] - half_turn(dq) * sine[rows]
            unit, scale = unit_of(proj[rows, at])
            dgain_query[...] += jnp.sum(turned * unit, axis=0, keepdims=True)
            dproj[rows, at] = norm_back(turned * gain_query[...], unit, scale).astype(BF16)
        return carry

    lax.fori_loop(0, heads, head, 0)
    dk = dkey[...]
    turned = dk * cosine - half_turn(dk) * sine
    unit, scale = unit_of(proj[:, span : span + HD])
    dgain_key[...] = jnp.sum(turned * unit, axis=0, keepdims=True)
    dproj[:, span : span + HD] = norm_back(turned * gain_key[...], unit, scale).astype(BF16)
    dproj[:, span + HD :] = dvalue[...].astype(BF16)
    fetch_wait(own, held, wsem, (1,))
    both = dproj[...]

    def in_cols(j, carry):
        at = pl.ds(pl.multiple_of(j * 256, 256), 256)
        res = dot32(both, win[at], COL_PAIR).astype(BF16)
        for m in range(mb):
            for z in range(n):
                col[z, m * t : (m + 1) * t, at] = res[m * length + z * t : m * length + (z + 1) * t]
        return carry

    lax.fori_loop(0, d // 256, in_cols, 0)
    line = Line(n, sems[4:], zup, zdn, stage, acc)

    def chunk_saves(i):
        at = pl.ds(pl.multiple_of(i * 256, 256), 256)
        return (
            pltpu.make_async_copy(grad_in.at[at], grad_in_hbm.at[at], osem.at[0, i]),
            pltpu.make_async_copy(grad_out.at[at], grad_out_hbm.at[at], osem.at[1, i]),
        )

    def weight_grads(first, last):
        def chunk(i, carry):
            at = pl.ds(pl.multiple_of(i * 256, 256), 256)
            left = normed[:, :, at].reshape(mb * length, 256)
            grad_in[at] = dot32(left, dproj[...], ROW_PAIR).astype(BF16)
            left = dmids[:, :, at].reshape(mb * length, 256)
            grad_out[at] = dot32(left, mixed[...], ROW_PAIR).astype(BF16)
            for save in chunk_saves(i):
                save.start()
            return carry

        lax.fori_loop(first, last, chunk, 0)

    chunks = d // 256
    for k, z in enumerate(line.z_list):
        add_rows(acc, col.at[z])
        line.move(z, total)
        weight_grads(chunks * k // len(line.z_list), chunks * (k + 1) // len(line.z_list))
    line.finish(total)
    hidden = x_ref[...].astype(F32)
    unit, scale = unit_of(hidden)
    da = total[...]
    dgain_attn[...] = jnp.sum(da * unit, axis=0, keepdims=True)
    cot_ref[...] = (dmid_ref[...] + norm_back(da * gain_attn[...], unit, scale)).astype(BF16)
    z_gather_drain(n, me, slot, sems[:4])
    for i in range(chunks):
        for save in chunk_saves(i):
            save.wait()


def attn_backward(layer, n, dmid, x, gains, tables, kept, own, other, cid, mb):
    r, d = x.shape
    cosine, sine, _ = tables
    normed, proj, qr, kr, v, prob, mixed = kept
    total_rows = cosine.shape[0]
    length = total_rows // mb
    width = own[0].shape[1]
    heads = own[1].shape[1] // HD
    span = heads * HD
    shape = jax.ShapeDtypeStruct
    return pl.pallas_call(
        functools.partial(attn_backward_kernel, n, layer, heads),
        out_shape=(
            shape((r, d), BF16),
            shape((1, d), F32),
            shape((1, HD), F32),
            shape((1, HD), F32),
            shape((d, width), BF16),
            shape((d, span), BF16),
        ),
        in_specs=in_vmem(9) + in_place(9),
        out_specs=tuple(in_vmem(4) + in_place(2)),
        scratch_shapes=[
            pltpu.VMEM((d, width), BF16),
            pltpu.VMEM((d, span), BF16),
            pltpu.VMEM((mb, length, d), BF16),
            pltpu.VMEM((total_rows, width), F32),
            pltpu.VMEM((total_rows, span), BF16),
            pltpu.VMEM((mb * heads, length, length), BF16),
            pltpu.VMEM((total_rows, span), BF16),
            pltpu.VMEM((mb, length, d), BF16),
            pltpu.VMEM((total_rows, span), BF16),
            pltpu.VMEM((total_rows, width), BF16),
            pltpu.VMEM((total_rows, HD), F32),
            pltpu.VMEM((total_rows, HD), F32),
            pltpu.VMEM((d, width), BF16),
            pltpu.VMEM((d, span), BF16),
        ]
        + line_buffers(n, r, d)
        + [
            pltpu.SemaphoreType.DMA((2,)),
            pltpu.SemaphoreType.DMA((5,)),
            pltpu.SemaphoreType.DMA((2, d // 256)),
        ]
        + [pltpu.SemaphoreType.DMA((n,))] * 8,
        compiler_params=pltpu.CompilerParams(
            collective_id=cid, has_side_effects=True, vmem_limit_bytes=60 << 20
        ),
        name="attn_backward",
    )(
        dmid,
        x,
        *gains,
        cosine,
        sine,
        kr,
        v,
        normed,
        proj,
        qr,
        prob,
        mixed,
        *own,
        *other,
    )


def local_wide(
    inputs,
    out_grad,
    segments,
    routes,
    gates,
    gain_attn,
    gain_ffn,
    gain_query,
    gain_key,
    w_query,
    w_key,
    w_value,
    w_out,
    w_gate,
    w_up,
    w_down,
):
    micro_count, _, local_rows, width = inputs.shape
    n_sec = lax.axis_size("section")
    n_gx = lax.axis_size("gx")
    n_gy = lax.axis_size("gy")
    heads = w_query.shape[2] // HD
    span = heads * HD
    experts = n_gx * n_gy
    group_len = segments.shape[2]
    mb = micro_count // n_sec
    rows_own = mb * local_rows
    rows_attn = mb * group_len
    section = lax.axis_index("section")
    gx = lax.axis_index("gx")
    gy = lax.axis_index("gy")
    expert_own = gx * n_gy + gy
    inv_root = 1.0 / math.sqrt(HD)
    first = section * mb

    kv_head = gx * heads // (HQ // KVH)
    key_own = lax.dynamic_slice_in_dim(w_key[0], kv_head * HD, HD, 1)
    value_own = lax.dynamic_slice_in_dim(w_value[0], kv_head * HD, HD, 1)
    w_in_shard = jnp.concatenate([w_query[0], key_own, value_own], axis=1)
    w_in_all = both_layers(lax.all_gather(w_in_shard, "gy", axis=0, tiled=True))
    w_out_all = both_layers(lax.all_gather(w_out[0], "gy", axis=0, tiled=True))
    w_gate_all = both_layers(w_gate[0, 0])
    w_up_all = both_layers(w_up[0, 0])
    w_down_all = both_layers(w_down[0, 0])
    table = dense_gates(routes[0, :, 0], gates[0, :, 0], experts)
    small = jnp.concatenate(
        [
            table.reshape(-1),
            gain_attn[0],
            gain_ffn[0],
            gain_query[0],
            gain_key[0],
        ]
    )
    small_all = both_layers(small)
    table_size = micro_count * local_rows * experts
    table_all = small_all[:, :table_size].reshape(n_sec, micro_count, local_rows, experts)
    gains_all = small_all[:, table_size:]

    table_mine = lax.dynamic_slice_in_dim(table_all, first, mb, 1).reshape(
        n_sec, rows_own, experts
    )
    x_mine = lax.dynamic_slice_in_dim(inputs[:, 0], first, mb, 0).reshape(rows_own, width)
    cot_mine = lax.dynamic_slice_in_dim(out_grad[:, 0], first, mb, 0).reshape(rows_own, width)
    segs = lax.dynamic_slice_in_dim(segments[:, 0], first, mb, 0)
    allowed, cosine, sine = seq_tables(segs, HD)
    cos_q = cosine.reshape(rows_attn, 1, HD // 2)
    sin_q = sine.reshape(rows_attn, 1, HD // 2)
    cos_k = cosine.reshape(rows_attn, HD // 2)
    sin_k = sine.reshape(rows_attn, HD // 2)

    def split_gains(layer):
        g = gains_all[layer]
        return (
            g[:width],
            g[width : 2 * width],
            g[2 * width : 2 * width + HD],
            g[2 * width + HD :],
        )

    saved_all = []
    outs = []
    layer_in = x_mine
    for layer in range(n_sec):
        g_attn, g_ffn, g_query, g_key = split_gains(layer)
        hidden = layer_in.astype(F32)
        attn_unit, attn_scale = normalize(hidden)
        normed = (attn_unit * g_attn).astype(BF16)
        normed_all = gather_z(normed.reshape(mb, local_rows, width)).reshape(rows_attn, width)
        projected = dot32(normed_all, w_in_all[layer])
        query = projected[:, :span].reshape(rows_attn, heads, HD)
        key = projected[:, span : span + HD]
        value_low = projected[:, span + HD :].astype(BF16).reshape(mb, group_len, HD)
        query_unit, query_scale = normalize(query)
        key_unit, key_scale = normalize(key)
        query_rope = (
            rotate(query_unit * g_query, cos_q, sin_q)
            .astype(BF16)
            .reshape(mb, group_len, heads, HD)
        )
        key_rope = rotate(key_unit * g_key, cos_k, sin_k).astype(BF16).reshape(mb, group_len, HD)
        scores = (
            jnp.einsum("mthd,msd->mhts", query_rope, key_rope, preferred_element_type=F32)
            * inv_root
        )
        exponent = jnp.where(allowed[:, None], jnp.exp(scores), 0.0)
        log_total = jnp.log(jnp.sum(exponent, axis=-1, keepdims=True))
        prob = jnp.where(allowed[:, None], jnp.exp(scores - log_total), 0.0)
        mixed = (
            jnp.einsum("mhts,msd->mthd", prob.astype(BF16), value_low, preferred_element_type=F32)
            .astype(BF16)
            .reshape(rows_attn, span)
        )
        attn_part = dot32(mixed, w_out_all[layer], COL_PAIR).astype(BF16)
        attn_out = scatter_z(attn_part.reshape(mb, group_len, width)).reshape(rows_own, width)
        middle = hidden + attn_out.astype(F32)
        ffn_unit, ffn_scale = normalize(middle)
        expert_in = (ffn_unit * g_ffn).astype(BF16)
        tab = table_mine[layer]
        tab_hi = tab.astype(BF16)
        tab_lo = (tab - tab_hi.astype(F32)).astype(BF16)
        payload = jnp.concatenate([expert_in, tab_hi, tab_lo], axis=1)
        arrived_all = gather_all(payload)
        arrived = arrived_all[:, :width]
        gate_cols = arrived_all[:, width:].astype(F32)
        is_mine = jnp.arange(2 * experts) % experts == expert_own
        weight = jnp.sum(jnp.where(is_mine[None], gate_cols, 0.0), axis=1, keepdims=True)
        gate_pre = dot32(arrived, w_gate_all[layer])
        up_proj = dot32(arrived, w_up_all[layer])
        inner = (jax.nn.silu(gate_pre) * up_proj).astype(BF16)
        result = dot32(inner, w_down_all[layer])
        weighted = (result * weight).astype(BF16)
        expert_sum = scatter_all(weighted)
        layer_out = (middle + expert_sum.astype(F32)).astype(BF16)
        outs.append(layer_out)
        layer_in = layer_out
        saved_all.append(
            (
                attn_unit,
                attn_scale,
                normed_all,
                query_unit,
                query_scale,
                key_unit,
                key_scale,
                query_rope,
                key_rope,
                value_low,
                prob,
                mixed,
                ffn_unit,
                ffn_scale,
                arrived,
                weight,
                gate_pre,
                up_proj,
                inner,
            )
        )

    cot = cot_mine
    in_grads = [None] * n_sec
    expert_grads = [None] * n_sec
    attn_grads = [None] * n_sec
    gain_grads = [None] * n_sec
    for layer in reversed(range(n_sec)):
        g_attn, g_ffn, g_query, g_key = split_gains(layer)
        (
            attn_unit,
            attn_scale,
            normed_all,
            query_unit,
            query_scale,
            key_unit,
            key_scale,
            query_rope,
            key_rope,
            value_low,
            prob,
            mixed,
            ffn_unit,
            ffn_scale,
            arrived,
            weight,
            gate_pre,
            up_proj,
            inner,
        ) = saved_all[layer]
        gradient = cot.astype(F32)
        grad_all = gather_all(cot)
        grad_result = (grad_all.astype(F32) * weight).astype(BF16)
        grad_inner = dot32(grad_result, w_down_all[layer], COL_PAIR)
        grad_down = dot32(inner, grad_result, ROW_PAIR)
        sig = jax.nn.sigmoid(gate_pre)
        grad_gate_pre = (grad_inner * up_proj * sig * (1.0 + gate_pre * (1.0 - sig))).astype(BF16)
        grad_up_proj = (grad_inner * gate_pre * sig).astype(BF16)
        grad_gate = dot32(arrived, grad_gate_pre, ROW_PAIR)
        grad_up = dot32(arrived, grad_up_proj, ROW_PAIR)
        grad_arrived = (
            dot32(grad_gate_pre, w_gate_all[layer], COL_PAIR)
            + dot32(grad_up_proj, w_up_all[layer], COL_PAIR)
        ).astype(BF16)
        expert_grads[layer] = (grad_gate, grad_up, grad_down)
        grad_expert_in = scatter_all(grad_arrived).astype(F32)
        grad_ffn_gain = jnp.sum(grad_expert_in * ffn_unit, axis=0)
        grad_middle = gradient + norm_back(grad_expert_in * g_ffn, ffn_unit, ffn_scale)
        middle_low = grad_middle.astype(BF16)
        middle_all = gather_z(middle_low.reshape(mb, local_rows, width)).reshape(rows_attn, width)
        grad_out_w = dot32(middle_all, mixed, ROW_PAIR)
        grad_heads = (
            dot32(middle_all, w_out_all[layer]).astype(BF16).reshape(mb, group_len, heads, HD)
        )
        grad_value = jnp.einsum(
            "mhts,mthd->mshd", prob.astype(BF16), grad_heads, preferred_element_type=F32
        )
        grad_prob = jnp.einsum(
            "mthd,msd->mhts", grad_heads, value_low, preferred_element_type=F32
        )
        mixed_split = mixed.reshape(mb, group_len, heads, HD)
        delta = jnp.sum(grad_heads.astype(F32) * mixed_split.astype(F32), axis=-1)
        delta = jnp.swapaxes(delta, 1, 2)[..., None]
        grad_scores = (prob * (grad_prob - delta)).astype(BF16)
        grad_query = (
            jnp.einsum("mhts,msd->mthd", grad_scores, key_rope, preferred_element_type=F32)
            * inv_root
        ).reshape(rows_attn, heads, HD)
        grad_key = (
            jnp.einsum("mhts,mthd->mshd", grad_scores, query_rope, preferred_element_type=F32)
            * inv_root
        ).reshape(rows_attn, heads, HD)
        query_turn = rotate_back(grad_query, cos_q, sin_q)
        grad_query_gain = jnp.sum(query_turn * query_unit, axis=(0, 1))
        grad_query_pre = norm_back(query_turn * g_query, query_unit, query_scale)
        key_turn = rotate_back(jnp.sum(grad_key, axis=1), cos_k, sin_k)
        grad_key_gain = jnp.sum(key_turn * key_unit, axis=0)
        grad_key_pre = norm_back(key_turn * g_key, key_unit, key_scale)
        grad_proj = jnp.concatenate(
            [
                grad_query_pre.reshape(rows_attn, span),
                grad_key_pre,
                jnp.sum(grad_value, axis=2).reshape(rows_attn, HD),
            ],
            axis=1,
        ).astype(BF16)
        grad_in_w = dot32(normed_all, grad_proj, ROW_PAIR)
        normed_part = dot32(grad_proj, w_in_all[layer], COL_PAIR).astype(BF16)
        grad_normed = (
            scatter_z(normed_part.reshape(mb, group_len, width))
            .reshape(rows_own, width)
            .astype(F32)
        )
        grad_attn_gain = jnp.sum(grad_normed * attn_unit, axis=0)
        cot = (grad_middle + norm_back(grad_normed * g_attn, attn_unit, attn_scale)).astype(BF16)
        in_grads[layer] = cot
        attn_grads[layer] = jnp.concatenate([grad_in_w, grad_out_w], axis=1).astype(BF16)
        gain_grads[layer] = jnp.concatenate(
            [grad_attn_gain, grad_ffn_gain, grad_query_gain, grad_key_gain]
        )

    def own_layer_sum(pieces):
        return lax.psum_scatter(
            jnp.stack([piece.astype(BF16) for piece in pieces]),
            "section",
            scatter_dimension=0,
            tiled=True,
        ).astype(F32)

    grad_gate, grad_up, grad_down = (
        own_layer_sum([expert_grads[layer][k] for layer in range(n_sec)]) for k in range(3)
    )
    attn_sum = lax.psum_scatter(
        jnp.concatenate(attn_grads, axis=0), ("section", "gy"), scatter_dimension=0, tiled=True
    ).astype(F32)
    query_grad = attn_sum[:, :span]
    out_w_grad = attn_sum[:, span + 2 * HD :]
    kv_all = lax.all_gather(attn_sum[:, span : span + 2 * HD], "gx", axis=0, tiled=False)
    kv_all = jnp.sum(kv_all.reshape(KVH, n_gx // KVH, -1, 2, HD), axis=1)
    key_part = jnp.swapaxes(kv_all[:, :, 0], 0, 1).reshape(-1, KVH * HD)
    value_part = jnp.swapaxes(kv_all[:, :, 1], 0, 1).reshape(-1, KVH * HD)
    gain_sum = lax.psum(jnp.stack(gain_grads), ("section", "gx", "gy"))
    gain_sum = lax.dynamic_index_in_dim(gain_sum, section, 0, keepdims=True)

    def own_layer_rows(pieces):
        stacked = jnp.stack(pieces).reshape(n_sec, mb, local_rows, width)
        return lax.all_to_all(stacked, "section", split_axis=0, concat_axis=0, tiled=True).reshape(
            1, micro_count, 1, local_rows, width
        )

    return (
        own_layer_rows(outs),
        own_layer_rows(in_grads),
        gain_sum[:, :width],
        gain_sum[:, width : 2 * width],
        gain_sum[:, 2 * width : 2 * width + HD],
        gain_sum[:, 2 * width + HD :],
        query_grad[None],
        key_part[None],
        value_part[None],
        out_w_grad[None],
        grad_gate[:, None],
        grad_up[:, None],
        grad_down[:, None],
    )


def local_fused(
    inputs,
    out_grad,
    segments,
    routes,
    gates,
    gain_attn,
    gain_ffn,
    gain_query,
    gain_key,
    w_query,
    w_key,
    w_value,
    w_out,
    w_gate,
    w_up,
    w_down,
):
    micro_count, _, local_rows, width = inputs.shape
    n_sec = lax.axis_size("section")
    n_gx = lax.axis_size("gx")
    n_gy = lax.axis_size("gy")
    heads = w_query.shape[2] // HD
    span = heads * HD
    experts = n_gx * n_gy
    group_len = segments.shape[2]
    mb = micro_count // n_sec
    rows_own = mb * local_rows
    rows_attn = mb * group_len
    section = lax.axis_index("section")
    gx = lax.axis_index("gx")
    first = section * mb

    kv_head = gx * heads // (HQ // KVH)
    key_own = lax.dynamic_slice_in_dim(w_key[0], kv_head * HD, HD, 1)
    value_own = lax.dynamic_slice_in_dim(w_value[0], kv_head * HD, HD, 1)
    w_in_shard = jnp.concatenate([w_query[0], key_own, value_own], axis=1)
    attn_own = (
        lax.all_gather(w_in_shard, "gy", axis=0, tiled=True),
        lax.all_gather(w_out[0], "gy", axis=0, tiled=True),
    )
    moe_own = (w_gate[0, 0], w_up[0, 0], w_down[0, 0])
    attn_other = tuple(swap_sections(w) for w in attn_own)
    moe_other = tuple(swap_sections(w) for w in moe_own)
    table = dense_gates(routes[0, :, 0], gates[0, :, 0], experts)
    small = jnp.concatenate(
        [table.reshape(-1), gain_attn[0], gain_ffn[0], gain_query[0], gain_key[0]]
    )
    small_all = both_layers(small)
    table_size = micro_count * local_rows * experts
    table_all = small_all[:, :table_size].reshape(n_sec, micro_count, local_rows, experts)
    gains_all = small_all[:, table_size:]
    table_mine = lax.dynamic_slice_in_dim(table_all, first, mb, 1).reshape(
        n_sec, rows_own, experts
    )
    x_mine = lax.dynamic_slice_in_dim(inputs[:, 0], first, mb, 0).reshape(rows_own, width)
    cot = lax.dynamic_slice_in_dim(out_grad[:, 0], first, mb, 0).reshape(rows_own, width)
    segs = lax.dynamic_slice_in_dim(segments[:, 0], first, mb, 0)
    allowed, cosine, sine = seq_tables(segs, HD)
    tables = (
        jnp.concatenate([cosine, cosine], axis=-1).reshape(rows_attn, HD),
        jnp.concatenate([-sine, sine], axis=-1).reshape(rows_attn, HD),
        allowed.astype(F32),
    )

    def split_gains(layer):
        g = gains_all[layer : layer + 1]
        return (
            g[:, :width],
            g[:, width : 2 * width],
            g[:, 2 * width : 2 * width + HD],
            g[:, 2 * width + HD :],
        )

    kept = []
    outs = []
    layer_in = x_mine
    for layer in range(n_sec):
        tab = table_mine[layer]
        tab_hi = tab.astype(BF16)
        tab_lo = (tab - tab_hi.astype(F32)).astype(BF16)
        pad = jnp.zeros((rows_own, 128 - 2 * experts), BF16)
        gate_cols = jnp.concatenate([tab_hi, tab_lo, pad], axis=1)
        mid, payload, normed, proj, qr, kr, v, prob, mixed = attn_forward(
            layer,
            n_gx,
            layer_in,
            split_gains(layer),
            tables,
            gate_cols,
            attn_own,
            attn_other,
            1 + layer,
            mb,
        )
        layer_out, *moe_kept = moe_forward(
            layer, n_gx, mid, payload, moe_own, moe_other, 3 + layer
        )
        kept.append((layer_in, mid, (normed, proj, qr, kr, v, prob, mixed), moe_kept))
        outs.append(layer_out)
        layer_in = layer_out

    in_grads = [None] * n_sec
    moe_grads = [None] * n_sec
    attn_grads = [None] * n_sec
    gain_grads = [None] * n_sec
    for layer in reversed(range(n_sec)):
        g_attn, g_ffn, g_query, g_key = split_gains(layer)
        layer_in, mid, attn_kept, (arrived, weight, gp, up, inner) = kept[layer]
        dmid, d_ffn, *moe_grads[layer] = moe_backward(
            layer,
            n_gx,
            cot,
            mid,
            g_ffn,
            weight,
            arrived,
            gp,
            up,
            inner,
            moe_own,
            moe_other,
            5 + layer,
        )
        cot, d_attn, d_query, d_key, *attn_grads[layer] = attn_backward(
            layer,
            n_gx,
            dmid,
            layer_in,
            (g_attn, g_query, g_key),
            tables,
            attn_kept,
            attn_own,
            attn_other,
            7 + layer,
            mb,
        )
        in_grads[layer] = cot
        gain_grads[layer] = jnp.concatenate([d_attn, d_ffn, d_query, d_key], axis=1)

    def own_layer_sum(pieces):
        from_other = [
            lax.ppermute(piece, "section", [(1 - layer, layer)])
            for layer, piece in enumerate(pieces)
        ]
        sums = [a.astype(F32) + b.astype(F32) for a, b in zip(pieces, from_other)]
        return jnp.where(section == 0, sums[0], sums[1])

    grad_gate, grad_up, grad_down = (
        own_layer_sum([moe_grads[layer][k] for layer in range(n_sec)])[None] for k in range(3)
    )
    grad_in, grad_out = (
        lax.psum_scatter(
            own_layer_sum([attn_grads[layer][k] for layer in range(n_sec)]).astype(BF16),
            "gy",
            scatter_dimension=0,
            tiled=True,
        ).astype(F32)
        for k in range(2)
    )
    query_grad = grad_in[:, :span]
    kv_all = lax.all_gather(grad_in[:, span:], "gx", axis=0, tiled=False)
    kv_all = jnp.sum(kv_all.reshape(KVH, n_gx // KVH, -1, 2, HD), axis=1)
    key_part = jnp.swapaxes(kv_all[:, :, 0], 0, 1).reshape(-1, KVH * HD)
    value_part = jnp.swapaxes(kv_all[:, :, 1], 0, 1).reshape(-1, KVH * HD)
    gain_sum = lax.psum(jnp.concatenate(gain_grads, axis=0), ("section", "gx", "gy"))
    gain_sum = lax.dynamic_index_in_dim(gain_sum, section, 0, keepdims=True)

    def own_layer_rows(pieces):
        stacked = jnp.stack(pieces).reshape(n_sec, mb, local_rows, width)
        return lax.all_to_all(stacked, "section", split_axis=0, concat_axis=0, tiled=True).reshape(
            1, micro_count, 1, local_rows, width
        )

    return (
        own_layer_rows(outs),
        own_layer_rows(in_grads),
        gain_sum[:, :width],
        gain_sum[:, width : 2 * width],
        gain_sum[:, 2 * width : 2 * width + HD],
        gain_sum[:, 2 * width + HD :],
        query_grad[None],
        key_part[None],
        value_part[None],
        grad_out[None],
        grad_gate[:, None],
        grad_up[:, None],
        grad_down[:, None],
    )


def local(*args):
    inputs = args[0]
    n = lax.axis_size("gx")
    rows_own = inputs.shape[0] // lax.axis_size("section") * inputs.shape[2]
    if 4 * n * rows_own > MOST_ROWS:
        return local_wide(*args)
    return local_fused(*args)


def solution(mesh):
    return jax.shard_map(
        local,
        mesh=mesh,
        in_specs=(
            P(None, "gy", "gx", None),
            P(None, "gy", "gx", None),
            P(None, "gy", None),
            P("section", None, "gy", "gx", None),
            P("section", None, "gy", "gx", None),
            P("section", None),
            P("section", None),
            P("section", None),
            P("section", None),
            P("section", "gy", "gx"),
            P("section", "gy", None),
            P("section", "gy", None),
            P("section", "gy", "gx"),
            P("section", ("gx", "gy"), None, None),
            P("section", ("gx", "gy"), None, None),
            P("section", ("gx", "gy"), None, None),
        ),
        out_specs=(
            P("section", None, "gy", "gx", None),
            P("section", None, "gy", "gx", None),
            P("section", None),
            P("section", None),
            P("section", None),
            P("section", None),
            P("section", "gy", "gx"),
            P("section", "gy", None),
            P("section", "gy", None),
            P("section", "gy", "gx"),
            P("section", ("gx", "gy"), None, None),
            P("section", ("gx", "gy"), None, None),
            P("section", ("gx", "gy"), None, None),
        ),
        check_vma=False,
    )
```

```python
import functools
import math

import jax
import jax.numpy as jnp
from jax import lax
from jax.experimental import pallas as pl
from jax.experimental.pallas import tpu as pltpu
from jax.sharding import PartitionSpec as P

HQ = 32
KVH = 4
HD = 128
TOPK = 8

EPSILON = 1e-06
ROPE_BASE = 1000000.0
ROW_PAIR = (((0,), (0,)), ((), ()))
COL_PAIR = (((1,), (1,)), ((), ()))
F32 = jnp.float32
BF16 = jnp.bfloat16
MOST_ROWS = 1024


def normalize(tensor):
    scaling = lax.rsqrt(jnp.mean(tensor * tensor, axis=-1, keepdims=True) + EPSILON)
    return (tensor * scaling, scaling)


def norm_back(gradient, unit_vec, scaling):
    return scaling * (gradient - unit_vec * jnp.mean(gradient * unit_vec, axis=-1, keepdims=True))


def rotate(tensor, cosine, sine_part):
    halfway = tensor.shape[-1] // 2
    leading = tensor[..., :halfway]
    trailing = tensor[..., halfway:]
    return jnp.concatenate(
        [leading * cosine - trailing * sine_part, trailing * cosine + leading * sine_part], axis=-1
    )


def rotate_back(gradient, cosine, sine_part):
    return rotate(gradient, cosine, -sine_part)


def seq_tables(segment_ids, head_dim):
    length_all = segment_ids.shape[-1]
    position_ids = jnp.arange(length_all, dtype=jnp.int32)
    allowed = (segment_ids[:, :, None] == segment_ids[:, None, :]) & (
        position_ids[:, None] >= position_ids[None, :]
    )
    positions = jnp.sum(allowed.astype(jnp.int32), axis=-1) - 1
    halfway = head_dim // 2
    inverse = ROPE_BASE ** (-2.0 * jnp.arange(halfway, dtype=jnp.float32) / head_dim)
    angles = positions.astype(jnp.float32)[..., None] * inverse
    return (allowed, jnp.cos(angles), jnp.sin(angles))


def dot32(left, right, dims=None):
    if dims is None:
        return jnp.dot(left, right, preferred_element_type=F32)
    return lax.dot_general(left, right, dims, preferred_element_type=F32)


def gather_z(rows):
    return lax.all_gather(rows, "gx", axis=1, tiled=True)


def scatter_z(rows):
    return lax.psum_scatter(rows, "gx", scatter_dimension=1, tiled=True)


def gather_all(rows):
    return lax.all_gather(rows, ("gx", "gy"), axis=0, tiled=True)


def scatter_all(rows):
    return lax.psum_scatter(rows, ("gx", "gy"), scatter_dimension=0, tiled=True)


def both_layers(tensor):
    return lax.all_gather(tensor, "section", axis=0, tiled=False)


def dense_gates(route_ids, gate_vals, experts):
    onehot = route_ids[..., None] == jnp.arange(experts, dtype=jnp.int32)
    return jnp.sum(jnp.where(onehot, gate_vals[..., None], 0.0), axis=-2)


def swap_sections(tensor):
    return lax.ppermute(tensor, "section", [(0, 1), (1, 0)])


def remote(src, dst, send_sem, recv_sem, **where):
    return pltpu.make_async_remote_copy(
        src_ref=src,
        dst_ref=dst,
        send_sem=send_sem,
        recv_sem=recv_sem,
        device_id=where,
        device_id_type=pl.DeviceIdType.MESH,
    )


def hello(n, me, gy, with_plane, with_section=False):
    barrier = pltpu.get_barrier_semaphore()
    mesh_ids = pl.DeviceIdType.MESH

    @pl.when(me + 1 < n)
    def _():
        pl.semaphore_signal(barrier, 1, device_id={"gx": me + 1}, device_id_type=mesh_ids)

    @pl.when(me > 0)
    def _():
        pl.semaphore_signal(barrier, 1, device_id={"gx": me - 1}, device_id_type=mesh_ids)

    peers = 0
    if with_plane:
        for bit in (1, 2):
            pl.semaphore_signal(
                barrier, 1, device_id={"gy": gy_flip(gy, bit)}, device_id_type=mesh_ids
            )
        peers += 2
    if with_section:
        other = 1 - lax.axis_index("section")
        pl.semaphore_signal(barrier, 1, device_id={"section": other}, device_id_type=mesh_ids)
        peers += 1
    at_end = (me == 0) | (me == n - 1)

    @pl.when(at_end)
    def _():
        pl.semaphore_wait(barrier, peers + 1)

    @pl.when(jnp.logical_not(at_end))
    def _():
        pl.semaphore_wait(barrier, peers + 2)


def gy_flip(gy, bits):
    low = lax.rem(gy, 2)
    high = gy // 2
    if bits & 1:
        low = 1 - low
    if bits & 2:
        high = 1 - high
    return high * 2 + low


def z_gather_steps(n, me, slot, sems, after):
    send_up, recv_up, send_down, recv_down = sems
    sends = []

    def up(k):
        return remote(slot(me - k), slot(me - k), send_up.at[k], recv_up.at[k], gx=me + 1)

    def down(k):
        return remote(slot(me + k), slot(me + k), send_down.at[k], recv_down.at[k], gx=me - 1)

    for k in range(n):
        @pl.when(me - k >= 0)
        def _():
            if k:
                remote(
                    slot(me - k), slot(me - k), send_up.at[k - 1], recv_up.at[k - 1], gx=me
                ).wait_recv()
            if k < n - 1:

                @pl.when(me + 1 < n)
                def _():
                    up(k).start()

            if k == 0:

                @pl.when(me > 0)
                def _():
                    down(0).start()

            after(me - k, k)

        if k:

            @pl.when(me + k < n)
            def _():
                remote(
                    slot(me + k), slot(me + k), send_down.at[k - 1], recv_down.at[k - 1], gx=me
                ).wait_recv()
                if k < n - 1:

                    @pl.when(me > 0)
                    def _():
                        down(k).start()

                after(me + k, k)


def z_gather_drain(n, me, slot, sems):
    send_up, recv_up, send_down, recv_down = sems
    for k in range(n - 1):

        @pl.when((me - k >= 0) & (me + 1 < n))
        def _():
            remote(slot(me - k), slot(me - k), send_up.at[k], recv_up.at[k], gx=me + 1).wait_send()

        @pl.when((me + k < n) & (me > 0))
        def _():
            remote(
                slot(me + k), slot(me + k), send_down.at[k], recv_down.at[k], gx=me - 1
            ).wait_send()


def flip_by(gy, step):
    low = lax.rem(lax.rem(gy, 2) + lax.rem(step, 2), 2)
    high = lax.rem(gy // 2 + step // 2, 2)
    return high * 2 + low


class Plane:
    def __init__(self, n, sems):
        self.n = n
        self.me = lax.axis_index("gx")
        self.gy = lax.axis_index("gy")
        self.cx, self.cy, self.cd = (gy_flip(self.gy, bits) for bits in (1, 2, 3))
        self.gather_sems = sems[:10]
        self.scatter_sems = sems[10:20]
        self.z_list = []
        for k in range((n + 1) // 2):
            self.z_list += [n - 1 - k] + ([k] if k != n - 1 - k else [])


    def gather_own_column(self, slot):
        su, ru, sd, rd, sx, rx, sy, ry, sf, rf = self.gather_sems
        c = self.gy

        def after(z, k):
            remote(slot(z, c), slot(z, c), sx.at[z], rx.at[z], gy=self.cx).start()
            remote(slot(z, c), slot(z, c), sy.at[z], ry.at[z], gy=self.cy).start()

        z_gather_steps(self.n, self.me, lambda z: slot(z, c), (su, ru, sd, rd), after)

    def gather_pass_on(self, slot):
        su, ru, sd, rd, sx, rx, sy, ry, sf, rf = self.gather_sems

        def forward(z):
            remote(slot(z, self.cx), slot(z, self.cx), sx.at[z], rx.at[z], gy=self.cx).wait_recv()
            remote(slot(z, self.cy), slot(z, self.cy), sy.at[z], ry.at[z], gy=self.cy).wait_recv()

            @pl.when(lax.rem(z, 2) == 0)
            def _():
                remote(
                    slot(z, self.cy), slot(z, self.cy), sf.at[z], rf.at[z], gy=self.cx
                ).start()

            @pl.when(lax.rem(z, 2) == 1)
            def _():
                remote(
                    slot(z, self.cx), slot(z, self.cx), sf.at[z], rf.at[z], gy=self.cy
                ).start()

        for k in range(self.n):

            @pl.when(self.me - k >= 0)
            def _():
                forward(self.me - k)

            if k:

                @pl.when(self.me + k < self.n)
                def _():
                    forward(self.me + k)

    def gather_far_column(self, slot):
        sf, rf = self.gather_sems[8:]
        for z in range(self.n):
            remote(slot(z, self.cd), slot(z, self.cd), sf.at[z], rf.at[z], gy=self.cx).wait_recv()

    def gather_drain(self, slot):
        su, ru, sd, rd, sx, rx, sy, ry, sf, rf = self.gather_sems
        z_gather_drain(self.n, self.me, lambda z: slot(z, self.gy), (su, ru, sd, rd))
        for z in range(self.n):
            one = slot(z, self.gy)
            remote(one, one, sx.at[z], rx.at[z], gy=self.cx).wait_send()
            remote(one, one, sy.at[z], ry.at[z], gy=self.cy).wait_send()
            remote(one, one, sf.at[z], rf.at[z], gy=self.cx).wait_send()


    def to_x(self, z):
        sx, rx = self.scatter_sems[4:6]
        return remote(self.part(z, self.cx), self.xin.at[z], sx.at[z], rx.at[z], gy=self.cx)

    def to_y(self, z):
        sy, ry = self.scatter_sems[6:8]
        return remote(self.part(z, self.cy), self.yin.at[z], sy.at[z], ry.at[z], gy=self.cy)

    def far(self, z):
        sf, rf = self.scatter_sems[8:]
        return remote(
            self.part(z, self.cd),
            self.din.at[z],
            sf.at[z],
            rf.at[z],
            gy=self.cx if z % 2 == 0 else self.cy,
        )

    def scatter_setup(self, part, xin, yin, din, zup, zdn, stage, acc):
        self.part, self.xin, self.yin, self.din = part, xin, yin, din
        self.zup, self.zdn, self.stage, self.acc = zup, zdn, stage, acc

    def scatter_x(self):
        for z in self.z_list:
            if z % 2 == 0:
                self.to_x(z).start()

    def scatter_y(self):
        for z in self.z_list:
            if z % 2 == 1:
                self.to_y(z).start()

    def scatter_far(self):
        for z in self.z_list:
            self.far(z).start()

    def scatter_pass_on(self, z):
        self.far(z).wait_recv()
        mine = self.part(z, self.cy if z % 2 == 0 else self.cx)
        add_rows(mine, mine, self.din.at[z])
        (self.to_y if z % 2 == 0 else self.to_x)(z).start()

    def scatter_line(self, z, total):
        n, me, acc = self.n, self.me, self.acc
        su, ru, sd, rd = self.scatter_sems[:4]
        self.to_x(z).wait_recv()
        self.to_y(z).wait_recv()
        add_rows(acc, self.part(z, self.gy), self.xin.at[z], self.yin.at[z])
        up = remote(self.stage.at[z], self.zup.at[z], su.at[z], ru.at[z], gx=me + 1)
        down = remote(self.stage.at[z], self.zdn.at[z], sd.at[z], rd.at[z], gx=me - 1)

        @pl.when((me < z) & (me > 0))
        def _():
            up.wait_recv()
            add_rows(acc, acc, self.zup.at[z])

        @pl.when((me > z) & (me < n - 1))
        def _():
            down.wait_recv()
            add_rows(acc, acc, self.zdn.at[z])

        @pl.when(me != z)
        def _():
            add_rows(self.stage.at[z], acc)

        @pl.when(me < z)
        def _():
            up.start()

        @pl.when(me > z)
        def _():
            down.start()

        @pl.when(me == z)
        def _():
            add_rows(total, acc)

    def scatter_finish(self, total):
        n, me = self.n, self.me
        su, ru, sd, rd = self.scatter_sems[:4]

        @pl.when(me > 0)
        def _():
            remote(self.stage.at[me], self.zup.at[me], su.at[me], ru.at[me], gx=me - 1).wait_recv()
            add_rows(total, total, self.zup.at[me])

        @pl.when(me < n - 1)
        def _():
            remote(self.stage.at[me], self.zdn.at[me], sd.at[me], rd.at[me], gx=me + 1).wait_recv()
            add_rows(total, total, self.zdn.at[me])

        for z in self.z_list:
            self.to_x(z).wait_send()
            self.to_y(z).wait_send()
            self.far(z).wait_send()

            @pl.when(me < z)
            def _():
                remote(self.stage.at[z], self.zup.at[z], su.at[z], ru.at[z], gx=me + 1).wait_send()

            @pl.when(me > z)
            def _():
                remote(self.stage.at[z], self.zdn.at[z], sd.at[z], rd.at[z], gx=me - 1).wait_send()


def add_rows(out, *terms):
    rows = out.shape[0]
    step = 16

    def body(i, carry):
        at = pl.ds(pl.multiple_of(i * step, step), step)
        value = terms[0][at].astype(F32)
        for term in terms[1:]:
            value = value + term[at].astype(F32)
        out[at] = value.astype(out.dtype)
        return carry

    lax.fori_loop(0, rows // step, body, 0)


def fetch_layer(layer, own, other, held, sems):
    section = lax.axis_index("section")

    @pl.when(section == layer)
    def _():
        for k, ref in enumerate(own):
            pltpu.make_async_copy(ref, held[k], sems.at[k]).start()

    @pl.when(section != layer)
    def _():
        for k, ref in enumerate(other):
            pltpu.make_async_copy(ref, held[k], sems.at[k]).start()


def fetch_wait(own, held, sems, which):
    for k in which:
        pltpu.make_async_copy(own[k], held[k], sems.at[k]).wait()


def moe_forward_kernel(
    n,
    layer,
    mid_ref,
    pay_ref,
    wg_own,
    wu_own,
    wd_own,
    wg_other,
    wu_other,
    wd_other,
    out_ref,
    arrived_ref,
    weight_ref,
    gp_ref,
    up_ref,
    inner_ref,
    pay,
    wg,
    wu,
    wd,
    part,
    xin,
    yin,
    din,
    zup,
    zdn,
    stage,
    acc,
    total,
    gp,
    up,
    inner,
    wsem,
    osem,
    *sems,
):
    r, d = mid_ref.shape
    ff = wg.shape[1]
    rows = n * r
    experts = 4 * n
    own, other, held = (
        (wg_own, wu_own, wd_own),
        (wg_other, wu_other, wd_other),
        (wg, wu, wd),
    )
    fetch_layer(layer, own, other, held, wsem)
    plane = Plane(n, sems)
    me, gy = plane.me, plane.gy
    hello(n, me, gy, True)
    pay[pl.ds(pl.multiple_of((gy * n + me) * r, r), r)] = pay_ref[...]

    def slot(z, c):
        return pay.at[pl.ds((c * n + z) * r, r)]

    plane.scatter_setup(lambda z, c: part.at[c * n + z], xin, yin, din, zup, zdn, stage, acc)
    plane.gather_own_column(slot)
    fetch_wait(own, held, wsem, range(3))
    expert = me * 4 + gy

    def column(s, carry):
        c = flip_by(gy, s)

        @pl.when(s == 1)
        def _():
            plane.gather_pass_on(slot)

        @pl.when(s == 3)
        def _():
            plane.gather_far_column(slot)

        at = pl.ds(pl.multiple_of(c * rows, rows), rows)
        gate_cols = pay[at, d : d + 128].astype(F32)
        lane = lax.broadcasted_iota(jnp.int32, (rows, 128), 1)
        hit = ((lane == expert) | (lane == expert + experts)) & (lane < 2 * experts)
        weight = jnp.sum(jnp.where(hit, gate_cols, 0.0), axis=1, keepdims=True)
        weight_ref[at] = weight
        block = pay[at, :d]
        for j in range(ff // 256):
            cols = slice(j * 256, (j + 1) * 256)
            g = jnp.dot(block, wg[:, cols], preferred_element_type=F32)
            u = jnp.dot(block, wu[:, cols], preferred_element_type=F32)
            gp[at, cols] = g.astype(BF16)
            up[at, cols] = u.astype(BF16)
            inner[at, cols] = (g / (1.0 + jnp.exp(-g)) * u).astype(BF16)
        act = inner[at]
        for j in range(d // 256):
            cols = slice(j * 256, (j + 1) * 256)
            res = jnp.dot(act, wd[:, cols], preferred_element_type=F32) * weight
            part[pl.ds(pl.multiple_of(c * n, n), n), :, cols] = (
                res.astype(BF16).reshape(n, r, 256)
            )

        @pl.when(s == 1)
        def _():
            plane.scatter_x()

        @pl.when(s == 2)
        def _():
            plane.scatter_y()

        return carry

    lax.fori_loop(0, 4, column, 0)
    plane.scatter_far()
    saves = [
        pltpu.make_async_copy(pay.at[:, pl.ds(0, d)], arrived_ref, osem.at[0]),
        pltpu.make_async_copy(gp, gp_ref, osem.at[1]),
        pltpu.make_async_copy(up, up_ref, osem.at[2]),
        pltpu.make_async_copy(inner, inner_ref, osem.at[3]),
    ]
    for save in saves:
        save.start()
    for z in plane.z_list:
        plane.scatter_pass_on(z)
    for z in plane.z_list:
        plane.scatter_line(z, total)
    plane.scatter_finish(total)
    add_rows(out_ref, mid_ref, total)
    plane.gather_drain(slot)
    for save in saves:
        save.wait()


def scatter_buffers(n, r, d):
    return [pltpu.VMEM((4 * n, r, d), BF16)] + [pltpu.VMEM((n, r, d), BF16)] * 6 + [
        pltpu.VMEM((r, d), F32)
    ] * 2


def in_vmem(count):
    return [pl.BlockSpec(memory_space=pltpu.VMEM)] * count


def in_place(count):
    return [pl.BlockSpec(memory_space=pl.ANY)] * count


def moe_forward(layer, n, mid, payload, own, other, cid):
    r, d = mid.shape
    ff = own[0].shape[1]
    total_rows = 4 * n * r
    width = payload.shape[1]
    return pl.pallas_call(
        functools.partial(moe_forward_kernel, n, layer),
        out_shape=(
            jax.ShapeDtypeStruct((r, d), BF16),
            jax.ShapeDtypeStruct((total_rows, d), BF16),
            jax.ShapeDtypeStruct((total_rows, 1), F32),
            jax.ShapeDtypeStruct((total_rows, ff), BF16),
            jax.ShapeDtypeStruct((total_rows, ff), BF16),
            jax.ShapeDtypeStruct((total_rows, ff), BF16),
        ),
        in_specs=in_vmem(2) + in_place(6),
        out_specs=tuple(in_vmem(1) + in_place(1) + in_vmem(1) + in_place(3)),
        scratch_shapes=[
            pltpu.VMEM((total_rows, width), BF16),
            pltpu.VMEM((d, ff), BF16),
            pltpu.VMEM((d, ff), BF16),
            pltpu.VMEM((ff, d), BF16),
        ]
        + scatter_buffers(n, r, d)
        + [pltpu.VMEM((total_rows, ff), BF16)] * 3
        + [pltpu.SemaphoreType.DMA((3,)), pltpu.SemaphoreType.DMA((4,))]
        + [pltpu.SemaphoreType.DMA((n,))] * 20,
        compiler_params=pltpu.CompilerParams(
            collective_id=cid, has_side_effects=True, vmem_limit_bytes=63 << 20
        ),
        name="moe_forward",
    )(mid, payload, *own, *other)


def moe_backward_kernel(
    n,
    layer,
    cot_ref,
    mid_ref,
    gain_ref,
    weight_ref,
    arrived_hbm,
    gp_hbm,
    up_hbm,
    inner_hbm,
    wg_own,
    wu_own,
    wd_own,
    wg_other,
    wu_other,
    wd_other,
    *rest,
):
    rest = rest[0 if layer else 6 :]
    dmid_ref, dgain_ref = rest[:2]
    keep_refs, give_refs = rest[2:5], rest[5:8]
    (
    cots,
    wg,
    wu,
    wd,
    part,
    xin,
    yin,
    din,
    zup,
    zdn,
    stage,
    acc,
    total,
    arrived,
    gp,
    up,
    inner,
    de,
    out_gate,
    out_up,
    out_down,
    wsem,
    isem,
    osem,
    *sems,
    ) = rest[8:]
    section = lax.axis_index("section")
    r, d = mid_ref.shape
    ff = wg.shape[1]
    rows = n * r
    own, other, held = (
        (wg_own, wu_own, wd_own),
        (wg_other, wu_other, wd_other),
        (wg, wu, wd),
    )
    loads = [
        pltpu.make_async_copy(gp_hbm, gp, isem.at[0]),
        pltpu.make_async_copy(up_hbm, up, isem.at[1]),
        pltpu.make_async_copy(arrived_hbm, arrived, isem.at[2]),
        pltpu.make_async_copy(inner_hbm, inner, isem.at[3]),
    ]
    fetch_layer(layer, own, other, held, wsem)
    for load in loads:
        load.start()
    plane = Plane(n, sems)
    me, gy = plane.me, plane.gy
    hello(n, me, gy, True)
    cots[pl.ds(pl.multiple_of((gy * n + me) * r, r), r)] = cot_ref[...]

    def slot(z, c):
        return cots.at[pl.ds((c * n + z) * r, r)]

    plane.scatter_setup(lambda z, c: part.at[c * n + z], xin, yin, din, zup, zdn, stage, acc)
    plane.gather_own_column(slot)
    fetch_wait(own, held, wsem, range(3))
    for load in loads:
        load.wait()

    def column(s, carry):
        c = flip_by(gy, s)

        @pl.when(s == 1)
        def _():
            plane.gather_pass_on(slot)

        @pl.when(s == 3)
        def _():
            plane.gather_far_column(slot)

        at = pl.ds(pl.multiple_of(c * rows, rows), rows)
        de[at] = (cots[at].astype(F32) * weight_ref[at]).astype(BF16)
        block = de[at]
        for j in range(ff // 256):
            cols = slice(j * 256, (j + 1) * 256)
            dz = dot32(block, wd[cols], COL_PAIR)
            g = gp[at, cols].astype(F32)
            u = up[at, cols].astype(F32)
            sg = 1.0 / (1.0 + jnp.exp(-g))
            gp[at, cols] = (dz * u * sg * (1.0 + g * (1.0 - sg))).astype(BF16)
            up[at, cols] = (dz * g * sg).astype(BF16)
        dgp = gp[at]
        dup = up[at]
        for j in range(d // 256):
            cols = slice(j * 256, (j + 1) * 256)
            res = dot32(dgp, wg[cols], COL_PAIR) + dot32(dup, wu[cols], COL_PAIR)
            part[pl.ds(pl.multiple_of(c * n, n), n), :, cols] = (
                res.astype(BF16).reshape(n, r, 256)
            )

        @pl.when(s == 1)
        def _():
            plane.scatter_x()

        @pl.when(s == 2)
        def _():
            plane.scatter_y()

        return carry

    lax.fori_loop(0, 4, column, 0)
    plane.scatter_far()

    def saving(i, refs):
        at = pl.ds(pl.multiple_of(i * 256, 256), 256)
        for k, (src, ref) in enumerate(zip((out_gate, out_up, out_down), refs)):
            where = (slice(None), at) if k == 2 else (at, slice(None))
            yield pltpu.make_async_copy(src.at[where], ref.at[where], osem.at[k, i])

    def weight_grads(first, last):
        def chunk(i, carry):
            at = pl.ds(pl.multiple_of(i * 256, 256), 256)
            left = arrived[:, at]
            out_gate[at] = dot32(left, gp[...], ROW_PAIR).astype(BF16)
            out_up[at] = dot32(left, up[...], ROW_PAIR).astype(BF16)
            out_down[:, at] = dot32(inner[...], de[:, at], ROW_PAIR).astype(BF16)

            @pl.when(section == layer)
            def _():
                for copy in saving(i, keep_refs):
                    copy.start()

            @pl.when(section != layer)
            def _():
                for copy in saving(i, give_refs):
                    copy.start()

            return carry

        lax.fori_loop(first, last, chunk, 0)

    chunks = d // 256
    cut = [0, chunks * 2 // 8, chunks * 4 // 8, chunks * 6 // 8, chunks]
    weight_grads(cut[0], cut[1])
    for z in plane.z_list:
        plane.scatter_pass_on(z)
    weight_grads(cut[1], cut[2])
    for k, z in enumerate(plane.z_list):
        plane.scatter_line(z, total)
        if k == 0:
            weight_grads(cut[2], cut[3])
    weight_grads(cut[3], cut[4])
    plane.scatter_finish(total)

    mid = mid_ref[...]
    scale = lax.rsqrt(jnp.mean(mid * mid, axis=-1, keepdims=True) + EPSILON)
    unit = mid * scale
    db = total[...]
    dgain_ref[...] = jnp.sum(db * unit, axis=0, keepdims=True)
    dmid_ref[...] = cot_ref[...].astype(F32) + norm_back(db * gain_ref[...], unit, scale)
    plane.gather_drain(slot)

    def settle(i, carry):
        for copy in saving(i, keep_refs):
            copy.wait()
        return carry

    lax.fori_loop(0, chunks, settle, 0)


def moe_backward(layer, n, cot, mid, gain, weight, arrived, gp, up, inner, own, other, so_far, cid):
    r, d = mid.shape
    ff = own[0].shape[1]
    total_rows = 4 * n * r
    sums = [jax.ShapeDtypeStruct(shape, BF16) for shape in ((d, ff), (d, ff), (ff, d))] * 2
    return pl.pallas_call(
        functools.partial(moe_backward_kernel, n, layer),
        out_shape=(
            jax.ShapeDtypeStruct((r, d), F32),
            jax.ShapeDtypeStruct((1, d), F32),
            *sums,
        ),
        in_specs=in_vmem(4) + in_place(10 + len(so_far)),
        out_specs=tuple(in_vmem(2) + in_place(6)),
        input_output_aliases={14 + k: 2 + k for k in range(len(so_far))},
        scratch_shapes=[
            pltpu.VMEM((total_rows, d), BF16),
            pltpu.VMEM((d, ff), BF16),
            pltpu.VMEM((d, ff), BF16),
            pltpu.VMEM((ff, d), BF16),
        ]
        + scatter_buffers(n, r, d)
        + [pltpu.VMEM((total_rows, d), BF16)]
        + [pltpu.VMEM((total_rows, ff), BF16)] * 3
        + [pltpu.VMEM((total_rows, d), BF16)]
        + [pltpu.VMEM((d, ff), BF16)] * 2
        + [pltpu.VMEM((ff, d), BF16)]
        + [
            pltpu.SemaphoreType.DMA((3,)),
            pltpu.SemaphoreType.DMA((4,)),
        ]
        + [pltpu.SemaphoreType.DMA((3, d // 256))]
        + [pltpu.SemaphoreType.DMA((n,))] * 20,
        compiler_params=pltpu.CompilerParams(
            collective_id=cid, has_side_effects=True, vmem_limit_bytes=63 << 20
        ),
        name="moe_backward",
    )(cot, mid, gain, weight, arrived, gp, up, inner, *own, *other, *so_far)


class Share:
    def __init__(self, layer, shard, full, scratch):
        self.shard, self.full = shard, full
        self.held, self.plane_sems, self.to_sems, self.from_sems = scratch
        self.section = lax.axis_index("section")
        self.mine = self.section == layer
        gy = lax.axis_index("gy")
        self.cols = [gy_flip(gy, bits) if bits else gy for bits in range(4)]
        self.rows = shard.shape[0]

    def at(self, column, half=None):
        rows = self.rows
        if half is None:
            return self.full.at[pl.ds(pl.multiple_of(column * rows, rows), rows)]
        few = rows // 2
        return self.full.at[pl.ds(pl.multiple_of(column * rows + half * few, few), few)]

    def own(self, step):
        src, dst = ((self.shard, self.held), (self.held, self.at(self.cols[0])))[step]
        return pltpu.make_async_copy(src, dst, self.plane_sems.at[9 * step])

    def direct(self, bit):
        s = self.plane_sems
        k = 1 if bit == 1 else 3
        return remote(
            self.shard, self.at(self.cols[0]), s.at[k], s.at[k + 1], gy=self.cols[bit]
        )

    def onward(self, bit):
        s = self.plane_sems
        k = 5 if bit == 1 else 7
        half = 1 if bit == 1 else 0
        ref = self.at(self.cols[3 - bit], half)
        return remote(ref, ref, s.at[k], s.at[k + 1], gy=self.cols[bit])

    def hand(self, k):
        if k == 0:
            src, dst = self.shard, self.at(self.cols[0])
        elif k < 3:
            src = dst = self.at(self.cols[k])
        else:
            src = dst = self.at(self.cols[3], k - 3)
        return remote(src, dst, self.to_sems.at[k], self.from_sems.at[k], section=1 - self.section)

    def start(self):
        @pl.when(self.mine)
        def _():
            self.direct(1).start()
            self.direct(2).start()
            self.own(0).start()
            self.hand(0).start()

    def pass_on(self):
        @pl.when(self.mine)
        def _():
            self.own(0).wait()
            self.own(1).start()
            self.direct(1).wait_recv()
            self.onward(2).start()
            self.hand(1).start()
            self.direct(2).wait_recv()
            self.onward(1).start()
            self.hand(2).start()

    def finish(self):
        @pl.when(self.mine)
        def _():
            self.onward(2).wait_recv()
            self.hand(3).start()
            self.onward(1).wait_recv()
            self.hand(4).start()
            self.own(1).wait()

        @pl.when(jnp.logical_not(self.mine))
        def _():
            for k in range(5):
                self.hand(k).wait_recv()

    def drain(self):
        @pl.when(self.mine)
        def _():
            for bit in (1, 2):
                self.direct(bit).wait_send()
                self.onward(bit).wait_send()
            for k in range(5):
                self.hand(k).wait_send()


def share_scratch(shard):
    dma = pltpu.SemaphoreType.DMA
    return [pltpu.VMEM(shard.shape, BF16), dma((10,)), dma((5,)), dma((5,))]


def share_kernel(n, layer, count, *refs):
    shards, fulls, scratch = refs[:count], refs[count : 2 * count], refs[2 * count :]
    shares = [
        Share(layer, shards[k], fulls[k], scratch[4 * k : 4 * k + 4]) for k in range(count)
    ]
    hello(n, lax.axis_index("gx"), lax.axis_index("gy"), True, True)
    for share in shares:
        share.start()
    for share in shares:
        share.pass_on()
    for share in shares:
        share.finish()
    for share in shares:
        share.drain()


def share_weights(layer, n, shards, cid):
    return pl.pallas_call(
        functools.partial(share_kernel, n, layer, len(shards)),
        out_shape=tuple(jax.ShapeDtypeStruct((4 * w.shape[0], w.shape[1]), BF16) for w in shards),
        in_specs=in_place(len(shards)),
        out_specs=tuple(in_place(len(shards))),
        scratch_shapes=[item for shard in shards for item in share_scratch(shard)],
        compiler_params=pltpu.CompilerParams(collective_id=cid, has_side_effects=True),
        name="share_weights",
    )(*shards)


def finish_kernel(
    n,
    gains_ref,
    kv_ref,
    lo_ref,
    ig_ref,
    gain_ref,
    kv_all_ref,
    lo_all_ref,
    ig_all_ref,
    gbuf,
    stage,
    incoming,
    lsem,
    psem,
    qsem,
    rsem,
    *sems,
):
    me = lax.axis_index("gx")
    gy = lax.axis_index("gy")
    section = lax.axis_index("section")
    other = 1 - section
    gbuf[me] = gains_ref[...]
    kv_all_ref[me] = kv_ref[...]
    hello(n, me, gy, True, True)
    z_gather_steps(n, me, lambda z: gbuf.at[z], sems[:4], lambda z, k: None)
    z_gather_steps(n, me, lambda z: kv_all_ref.at[z], sems[4:8], lambda z, k: None)
    keeps = []
    for k, (src, dst) in enumerate(((lo_ref, lo_all_ref), (ig_ref, ig_all_ref))):
        keep = pltpu.make_async_copy(src.at[section], dst.at[section], lsem.at[k])
        give = remote(src.at[other], dst.at[section], psem.at[k], qsem.at[k], section=other)
        keep.start()
        give.start()
        keeps.append((keep, give))
    total = gbuf[0]
    for z in range(1, n):
        total = total + gbuf[z]
    for k, where in enumerate(({"gy": gy_flip(gy, 1)}, {"gy": gy_flip(gy, 2)}, {"section": other})):
        stage[k] = total
        swap = remote(stage.at[k], incoming.at[k], rsem.at[0, k], rsem.at[1, k], **where)
        swap.start()
        swap.wait()
        total = total + incoming[k]

    @pl.when(section == 0)
    def _():
        gain_ref[...] = total[0:1]

    @pl.when(section == 1)
    def _():
        gain_ref[...] = total[1:2]

    for keep, give in keeps:
        keep.wait()
        give.wait()
    z_gather_drain(n, me, lambda z: gbuf.at[z], sems[:4])
    z_gather_drain(n, me, lambda z: kv_all_ref.at[z], sems[4:8])


def finish(n, gains, kv, lo, ig, cid):
    dma = pltpu.SemaphoreType.DMA
    shape = jax.ShapeDtypeStruct
    return pl.pallas_call(
        functools.partial(finish_kernel, n),
        out_shape=(
            shape((1, gains.shape[1]), F32),
            shape((n,) + kv.shape, BF16),
            shape(lo.shape, BF16),
            shape(ig.shape, BF16),
        ),
        in_specs=in_vmem(4),
        out_specs=tuple(in_vmem(4)),
        scratch_shapes=[
            pltpu.VMEM((n,) + gains.shape, F32),
            pltpu.VMEM((3,) + gains.shape, F32),
            pltpu.VMEM((3,) + gains.shape, F32),
            dma((2,)),
            dma((2,)),
            dma((2,)),
            dma((2, 3)),
        ]
        + [dma((n,))] * 8,
        compiler_params=pltpu.CompilerParams(collective_id=cid, has_side_effects=True),
        name="finish",
    )(gains, kv, lo, ig)


class Reduce:
    def __init__(self, layer, part, inbox, xin, yin, din, sems):
        self.part, self.inbox = part, inbox
        self.xin, self.yin, self.din = xin, yin, din
        self.give_sems, self.take_sems, self.send_sems, self.recv_sems = sems
        self.section = lax.axis_index("section")
        self.mine = self.section == layer
        gy = lax.axis_index("gy")
        self.cols = [gy_flip(gy, bits) if bits else gy for bits in range(4)]
        self.few = xin.shape[0] // 2

    def give(self, k, src):
        return remote(
            src,
            self.inbox.at[self.cols[k]],
            self.give_sems.at[k],
            self.take_sems.at[k],
            section=1 - self.section,
        )

    def half(self, ref, h):
        return ref.at[pl.ds(h * self.few, self.few)]

    def far(self, bit):
        k = bit - 1
        src = self.half(self.part(self.cols[3]), k)
        return remote(
            src, self.din.at[k], self.send_sems.at[k], self.recv_sems.at[k], gy=self.cols[bit]
        )

    def near(self, bit, h):
        k = 2 * bit + h
        into = self.xin if bit == 1 else self.yin
        return remote(
            self.half(self.part(self.cols[bit]), h),
            self.half(into, h),
            self.send_sems.at[k],
            self.recv_sems.at[k],
            gy=self.cols[bit],
        )

    def send_terms(self):
        def add(k):
            self.give(k, self.part(self.cols[k])).wait_recv()
            ref = self.part(self.cols[k])
            add_rows(ref, ref, self.inbox.at[self.cols[k]])

        @pl.when(self.mine)
        def _():
            add(3)
            self.far(1).start()
            self.far(2).start()
            add(1)
            self.near(1, 0).start()
            add(2)
            self.near(2, 1).start()
            add(0)

    def pass_on(self):
        @pl.when(self.mine)
        def _():
            self.far(1).wait_recv()
            ref = self.half(self.part(self.cols[2]), 0)
            add_rows(ref, ref, self.din.at[0])
            self.near(2, 0).start()
            self.far(2).wait_recv()
            ref = self.half(self.part(self.cols[1]), 1)
            add_rows(ref, ref, self.din.at[1])
            self.near(1, 1).start()

    def close(self, outs):
        @pl.when(self.mine)
        def _():
            for bit in (1, 2):
                for h in (0, 1):
                    self.near(bit, h).wait_recv()
            for ref, first, last in outs:
                cols = slice(first, last)
                own = self.part(self.cols[0])
                add_rows(ref, own.at[:, cols], self.xin.at[:, cols], self.yin.at[:, cols])
            for bit in (1, 2):
                self.far(bit).wait_send()
                for h in (0, 1):
                    self.near(bit, h).wait_send()


def reduce_sems():
    dma = pltpu.SemaphoreType.DMA
    return [dma((4,)), dma((4,)), dma((6,)), dma((6,))]


class Line:
    def __init__(self, n, sems, zup, zdn, stage, acc):
        self.n = n
        self.me = lax.axis_index("gx")
        self.sems = sems
        self.zup, self.zdn, self.stage, self.acc = zup, zdn, stage, acc
        self.z_list = []
        for k in range((n + 1) // 2):
            self.z_list += [n - 1 - k] + ([k] if k != n - 1 - k else [])

    def up(self, z):
        su, ru = self.sems[:2]
        return remote(self.stage.at[z], self.zup.at[z], su.at[z], ru.at[z], gx=self.me + 1)

    def down(self, z):
        sd, rd = self.sems[2:]
        return remote(self.stage.at[z], self.zdn.at[z], sd.at[z], rd.at[z], gx=self.me - 1)

    def move(self, z, total):
        n, me, acc = self.n, self.me, self.acc

        @pl.when((me < z) & (me > 0))
        def _():
            self.up(z).wait_recv()
            add_rows(acc, acc, self.zup.at[z])

        @pl.when((me > z) & (me < n - 1))
        def _():
            self.down(z).wait_recv()
            add_rows(acc, acc, self.zdn.at[z])

        @pl.when(me != z)
        def _():
            add_rows(self.stage.at[z], acc)

        @pl.when(me < z)
        def _():
            self.up(z).start()

        @pl.when(me > z)
        def _():
            self.down(z).start()

        @pl.when(me == z)
        def _():
            add_rows(total, acc)

    def finish(self, total):
        n, me = self.n, self.me

        @pl.when(me > 0)
        def _():
            self.up(me).wait_recv()
            add_rows(total, total, self.zup.at[me])

        @pl.when(me < n - 1)
        def _():
            self.down(me).wait_recv()
            add_rows(total, total, self.zdn.at[me])

        for z in self.z_list:

            @pl.when(me < z)
            def _():
                self.up(z).wait_send()

            @pl.when(me > z)
            def _():
                self.down(z).wait_send()


def unit_of(value):
    scale = lax.rsqrt(jnp.mean(value * value, axis=-1, keepdims=True) + EPSILON)
    return value * scale, scale


def half_turn(value):
    return pltpu.roll(value, value.shape[-1] // 2, axis=value.ndim - 1)


def attn_forward_kernel(
    n,
    layer,
    heads,
    x_ref,
    gain_attn,
    gain_ffn,
    gain_query,
    gain_key,
    cos_ref,
    sin_ref,
    mask_ref,
    gates_ref,
    win_hbm,
    wout_hbm,
    *rest,
):
    count = 2 if layer == 0 else 0
    shards, rest = rest[:count], rest[count:]
    mid_ref, pay_ref, normed_hbm, proj_hbm, qr_hbm, kr_ref, v_ref, prob_hbm, mixed_hbm = rest[:9]
    fulls, rest = rest[9 : 9 + count], rest[9 + count :]
    (
    win,
    wout,
    normed,
    proj,
    qr,
    prob,
    mixed,
    col,
    zup,
    zdn,
    stage,
    acc,
    total,
    wsem,
    osem,
    *sems,
    ) = rest
    mb, length, d = normed.shape
    t = length // n
    r = mb * t
    span = heads * HD
    me = lax.axis_index("gx")
    shares = [
        Share(1, shards[k], fulls[k], sems[8 + 4 * k : 12 + 4 * k]) for k in range(count)
    ]
    fetch_in = pltpu.make_async_copy(win_hbm, win, wsem.at[0])
    fetch_out = pltpu.make_async_copy(wout_hbm, wout, wsem.at[1])
    fetch_in.start()
    fetch_out.start()
    hello(n, me, lax.axis_index("gy"), count > 0, count > 0)
    for share in shares:
        share.start()
    hidden = x_ref[...].astype(F32)
    unit, _ = unit_of(hidden)
    low = (unit * gain_attn[...]).astype(BF16)
    normed[:, pl.ds(pl.multiple_of(me * t, t), t)] = low.reshape(mb, t, d)

    def slot(z):
        return normed.at[:, pl.ds(z * t, t)]

    z_gather_steps(n, me, slot, sems[:4], lambda z, k: None)
    saves = [
        pltpu.make_async_copy(normed, normed_hbm, osem.at[0]),
        pltpu.make_async_copy(proj, proj_hbm, osem.at[1]),
        pltpu.make_async_copy(qr, qr_hbm, osem.at[2]),
        pltpu.make_async_copy(prob, prob_hbm, osem.at[3]),
        pltpu.make_async_copy(mixed, mixed_hbm, osem.at[4]),
    ]
    saves[0].start()
    fetch_in.wait()
    every = normed[...].reshape(mb * length, d)
    for j in range((span + 2 * HD) // 256):
        cols = slice(j * 256, (j + 1) * 256)
        proj[:, cols] = jnp.dot(every, win[:, cols], preferred_element_type=F32)
    saves[1].start()
    cosine, sine = cos_ref[...], sin_ref[...]
    key_unit, _ = unit_of(proj[:, span : span + HD])
    key = key_unit * gain_key[...]
    kr_ref[...] = (key * cosine + half_turn(key) * sine).astype(BF16)
    v_ref[...] = proj[:, span + HD :].astype(BF16)

    def head(h, carry):
        at = pl.ds(pl.multiple_of(h * HD, HD), HD)
        query_unit, _ = unit_of(proj[:, at])
        query = query_unit * gain_query[...]
        turned = (query * cosine + half_turn(query) * sine).astype(BF16)
        qr[:, at] = turned
        for m in range(mb):
            rows = slice(m * length, (m + 1) * length)
            scores = dot32(turned[rows], kr_ref[rows], COL_PAIR) * (1.0 / math.sqrt(HD))
            exponent = jnp.where(mask_ref[m] > 0.5, jnp.exp(scores), 0.0)
            p = (exponent / jnp.sum(exponent, axis=-1, keepdims=True)).astype(BF16)
            prob[m * heads + h] = p
            mixed[rows, at] = jnp.dot(p, v_ref[rows], preferred_element_type=F32).astype(BF16)
        return carry

    lax.fori_loop(0, heads, head, 0)
    saves[2].start()
    saves[3].start()
    saves[4].start()
    for share in shares:
        share.pass_on()
    fetch_out.wait()
    both = mixed[...]

    def out_cols(j, carry):
        at = pl.ds(pl.multiple_of(j * 256, 256), 256)
        res = dot32(both, wout[at], COL_PAIR).astype(BF16)
        for m in range(mb):
            for z in range(n):
                col[z, m * t : (m + 1) * t, at] = res[m * length + z * t : m * length + (z + 1) * t]
        return carry

    lax.fori_loop(0, d // 256, out_cols, 0)
    line = Line(n, sems[4:8], zup, zdn, stage, acc)
    for z in line.z_list:
        add_rows(acc, col.at[z])
        line.move(z, total)
    line.finish(total)
    mid = x_ref[...].astype(F32) + total[...]
    mid_ref[...] = mid
    unit, _ = unit_of(mid)
    pay_ref[:, :d] = (unit * gain_ffn[...]).astype(BF16)
    pay_ref[:, d:] = gates_ref[...]
    for share in shares:
        share.finish()
    for share in shares:
        share.drain()
    z_gather_drain(n, me, slot, sems[:4])
    for save in saves:
        save.wait()


def line_buffers(n, r, d):
    return [pltpu.VMEM((n, r, d), BF16)] * 4 + [pltpu.VMEM((r, d), F32)] * 2


def attn_forward(layer, n, x, gains, tables, gate_cols, w_in, w_out, shards, cid, mb):
    r, d = x.shape
    cosine, sine, mask = tables
    total_rows = cosine.shape[0]
    length = total_rows // mb
    width = w_in.shape[1]
    heads = w_out.shape[1] // HD
    span = heads * HD
    shape = jax.ShapeDtypeStruct
    return pl.pallas_call(
        functools.partial(attn_forward_kernel, n, layer, heads),
        out_shape=(
            shape((r, d), F32),
            shape((r, d + 128), BF16),
            shape((mb, length, d), BF16),
            shape((total_rows, width), F32),
            shape((total_rows, span), BF16),
            shape((total_rows, HD), BF16),
            shape((total_rows, HD), BF16),
            shape((mb * heads, length, length), BF16),
            shape((total_rows, span), BF16),
            *(shape((4 * w.shape[0], w.shape[1]), BF16) for w in shards),
        ),
        in_specs=in_vmem(9) + in_place(2 + len(shards)),
        out_specs=tuple(in_vmem(2) + in_place(3) + in_vmem(2) + in_place(2 + len(shards))),
        scratch_shapes=[
            pltpu.VMEM((d, width), BF16),
            pltpu.VMEM((d, span), BF16),
            pltpu.VMEM((mb, length, d), BF16),
            pltpu.VMEM((total_rows, width), F32),
            pltpu.VMEM((total_rows, span), BF16),
            pltpu.VMEM((mb * heads, length, length), BF16),
            pltpu.VMEM((total_rows, span), BF16),
        ]
        + line_buffers(n, r, d)
        + [pltpu.SemaphoreType.DMA((2,)), pltpu.SemaphoreType.DMA((5,))]
        + [pltpu.SemaphoreType.DMA((n,))] * 8
        + [item for shard in shards for item in share_scratch(shard)],
        compiler_params=pltpu.CompilerParams(
            collective_id=cid, has_side_effects=True, vmem_limit_bytes=60 << 20
        ),
        name="attn_forward",
    )(x, *gains, cosine, sine, mask, gate_cols, w_in, w_out, *shards)


def attn_backward_kernel(
    n,
    layer,
    heads,
    dmid_ref,
    x_ref,
    gain_attn,
    gain_query,
    gain_key,
    cos_ref,
    sin_ref,
    kr_ref,
    v_ref,
    normed_hbm,
    proj_hbm,
    qr_hbm,
    prob_hbm,
    mixed_hbm,
    win_hbm,
    wout_hbm,
    *rest,
):
    last = layer == 0
    if last:
        later_hbm, gives, rest = rest[0], rest[1:4], rest[4:]
    cot_ref, dgain_attn, dgain_query, dgain_key = rest[:4]
    outs, rest = rest[4 : 10 if last else 5], rest[10 if last else 5 :]
    (
    win,
    wout,
    normed,
    proj,
    qr,
    prob,
    mixed,
    dmids,
    dheads,
    dproj,
    dkey,
    dvalue,
    grads,
    col,
    zup,
    zdn,
    stage,
    acc,
    total,
    wsem,
    isem,
    osem,
    *sems,
    ) = rest
    mb, length, d = normed.shape
    t = length // n
    span = heads * HD
    me = lax.axis_index("gx")
    inv_root = 1.0 / math.sqrt(HD)
    gy = lax.axis_index("gy")
    section = lax.axis_index("section")
    fetch_out = pltpu.make_async_copy(wout_hbm, wout, wsem.at[0])
    fetch_in = pltpu.make_async_copy(win_hbm, win, wsem.at[1])
    fetch_out.start()
    fetch_in.start()
    loads = [
        pltpu.make_async_copy(prob_hbm, prob, isem.at[0]),
        pltpu.make_async_copy(mixed_hbm, mixed, isem.at[1]),
        pltpu.make_async_copy(qr_hbm, qr, isem.at[2]),
        pltpu.make_async_copy(proj_hbm, proj, isem.at[3]),
        pltpu.make_async_copy(normed_hbm, normed, isem.at[4]),
    ]
    for load in loads:
        load.start()
    if last:
        later, inbox, xin, yin, din = sems[8:13]
        block = d // 4
        job_later = Reduce(
            1, lambda c: later.at[pl.ds(c * block, block)], inbox, xin, yin, din, sems[13:17]
        )
        job = Reduce(
            0, lambda c: grads.at[pl.ds(c * block, block)], inbox, xin, yin, din, sems[17:21]
        )
        swaps = [
            remote(gives[k], outs[3 + k], sems[21].at[k], sems[22].at[k], section=1 - section)
            for k in range(3)
        ]
        load_later = pltpu.make_async_copy(later_hbm, later, osem.at[0])

        @pl.when(job_later.mine)
        def _():
            load_later.start()

        hello(n, me, gy, True, True)

        @pl.when(jnp.logical_not(job_later.mine))
        def _():
            for k in (3, 1, 2, 0):
                c = job_later.cols[k]
                job_later.give(k, later_hbm.at[pl.ds(c * block, block)]).start()

        for swap in swaps:
            swap.start()
    else:
        hello(n, me, None, False)
    dmids[:, pl.ds(pl.multiple_of(me * t, t), t)] = dmid_ref[...].astype(BF16).reshape(mb, t, d)

    def slot(z):
        return dmids.at[:, pl.ds(z * t, t)]

    z_gather_steps(n, me, slot, sems[:4], lambda z, k: None)
    if last:

        @pl.when(job_later.mine)
        def _():
            load_later.wait()

        job_later.send_terms()
    fetch_out.wait()
    every = dmids[...].reshape(mb * length, d)
    for j in range(span // 256):
        cols = slice(j * 256, (j + 1) * 256)
        dheads[:, cols] = jnp.dot(every, wout[:, cols], preferred_element_type=F32).astype(BF16)
    for load in loads:
        load.wait()
    cosine, sine = cos_ref[...], sin_ref[...]
    dkey[...] = jnp.zeros_like(dkey)
    dvalue[...] = jnp.zeros_like(dvalue)
    dgain_query[...] = jnp.zeros_like(dgain_query)

    def head(h, carry):
        at = pl.ds(pl.multiple_of(h * HD, HD), HD)
        for m in range(mb):
            rows = slice(m * length, (m + 1) * length)
            p = prob[m * heads + h]
            dh = dheads[rows, at]
            dvalue[rows] += dot32(p, dh, ROW_PAIR)
            dp = dot32(dh, v_ref[rows], COL_PAIR)
            delta = jnp.sum(
                dh.astype(F32) * mixed[rows, at].astype(F32), axis=-1, keepdims=True
            )
            ds = (p.astype(F32) * (dp - delta)).astype(BF16)
            dkey[rows] += dot32(ds, qr[rows, at], ROW_PAIR) * inv_root
            dq = jnp.dot(ds, kr_ref[rows], preferred_element_type=F32) * inv_root
            turned = dq * cosine[rows] - half_turn(dq) * sine[rows]
            unit, scale = unit_of(proj[rows, at])
            dgain_query[...] += jnp.sum(turned * unit, axis=0, keepdims=True)
            dproj[rows, at] = norm_back(turned * gain_query[...], unit, scale).astype(BF16)
        return carry

    lax.fori_loop(0, heads, head, 0)
    if last:
        job_later.pass_on()
    dk = dkey[...]
    turned = dk * cosine - half_turn(dk) * sine
    unit, scale = unit_of(proj[:, span : span + HD])
    dgain_key[...] = jnp.sum(turned * unit, axis=0, keepdims=True)
    dproj[:, span : span + HD] = norm_back(turned * gain_key[...], unit, scale).astype(BF16)
    dproj[:, span + HD :] = dvalue[...].astype(BF16)
    fetch_in.wait()
    both = dproj[...]

    def in_cols(j, carry):
        at = pl.ds(pl.multiple_of(j * 256, 256), 256)
        res = dot32(both, win[at], COL_PAIR).astype(BF16)
        for m in range(mb):
            for z in range(n):
                col[z, m * t : (m + 1) * t, at] = res[m * length + z * t : m * length + (z + 1) * t]
        return carry

    lax.fori_loop(0, d // 256, in_cols, 0)
    line = Line(n, sems[4:8], zup, zdn, stage, acc)

    def weight_grads(begin, end):
        def chunk(i, carry):
            at = pl.ds(pl.multiple_of(i * 256, 256), 256)
            left = normed[:, :, at].reshape(mb * length, 256)
            grads[at, : span + 2 * HD] = dot32(left, dproj[...], ROW_PAIR).astype(BF16)
            left = dmids[:, :, at].reshape(mb * length, 256)
            grads[at, span + 2 * HD :] = dot32(left, mixed[...], ROW_PAIR).astype(BF16)
            return carry

        lax.fori_loop(begin, end, chunk, 0)

    chunks = d // 256
    for k, z in enumerate(line.z_list):
        add_rows(acc, col.at[z])
        line.move(z, total)
        weight_grads(chunks * k // len(line.z_list), chunks * (k + 1) // len(line.z_list))
    if last:

        @pl.when(jnp.logical_not(job.mine))
        def _():
            for k in (3, 1, 2, 0):
                job.give(k, job.part(job.cols[k])).start()

        job.send_terms()
    else:
        save = pltpu.make_async_copy(grads, outs[0], osem.at[0])
        save.start()
    line.finish(total)
    hidden = x_ref[...].astype(F32)
    unit, scale = unit_of(hidden)
    da = total[...]
    dgain_attn[...] = jnp.sum(da * unit, axis=0, keepdims=True)
    cot_ref[...] = (dmid_ref[...] + norm_back(da * gain_attn[...], unit, scale)).astype(BF16)
    z_gather_drain(n, me, slot, sems[:4])
    if not last:
        save.wait()
        return
    job.pass_on()
    closing = [(outs[0], 0, span), (outs[1], span, span + 2 * HD), (outs[2], span + 2 * HD, None)]
    job_later.close(closing)
    job.close(closing)
    for swap in swaps:
        swap.wait()

    @pl.when(jnp.logical_not(job.mine))
    def _():
        for k in range(4):
            job.give(k, job.part(job.cols[k])).wait_send()

    @pl.when(jnp.logical_not(job_later.mine))
    def _():
        for k in range(4):
            c = job_later.cols[k]
            job_later.give(k, later_hbm.at[pl.ds(c * block, block)]).wait_send()


def attn_backward(layer, n, dmid, x, gains, tables, kept, w_in, w_out, later, gives, cid, mb):
    r, d = x.shape
    cosine, sine, _ = tables
    normed, proj, qr, kr, v, prob, mixed = kept
    total_rows = cosine.shape[0]
    length = total_rows // mb
    width = w_in.shape[1]
    heads = w_out.shape[1] // HD
    span = heads * HD
    shape = jax.ShapeDtypeStruct
    both = width + span
    grad_shapes = [shape((d, both), BF16)]
    extra = []
    if later:
        block = d // 4
        grad_shapes = [
            shape((block, span), F32),
            shape((block, 2 * HD), BF16),
            shape((block, span), F32),
            *(shape(piece.shape, BF16) for piece in gives),
        ]
        extra = [
            pltpu.VMEM((d, both), BF16),
            pltpu.VMEM((4, block, both), BF16),
            pltpu.VMEM((block, both), BF16),
            pltpu.VMEM((block, both), BF16),
            pltpu.VMEM((2, block // 2, both), BF16),
        ] + reduce_sems() * 2 + [pltpu.SemaphoreType.DMA((3,))] * 2
    return pl.pallas_call(
        functools.partial(attn_backward_kernel, n, layer, heads),
        out_shape=(
            shape((r, d), BF16),
            shape((1, d), F32),
            shape((1, HD), F32),
            shape((1, HD), F32),
            *grad_shapes,
        ),
        in_specs=in_vmem(9) + in_place(7 + len(later) + len(gives)),
        out_specs=tuple(in_vmem(4) + (in_vmem(3) + in_place(3) if later else in_place(1))),
        scratch_shapes=[
            pltpu.VMEM((d, width), BF16),
            pltpu.VMEM((d, span), BF16),
            pltpu.VMEM((mb, length, d), BF16),
            pltpu.VMEM((total_rows, width), F32),
            pltpu.VMEM((total_rows, span), BF16),
            pltpu.VMEM((mb * heads, length, length), BF16),
            pltpu.VMEM((total_rows, span), BF16),
            pltpu.VMEM((mb, length, d), BF16),
            pltpu.VMEM((total_rows, span), BF16),
            pltpu.VMEM((total_rows, width), BF16),
            pltpu.VMEM((total_rows, HD), F32),
            pltpu.VMEM((total_rows, HD), F32),
            pltpu.VMEM((d, both), BF16),
        ]
        + line_buffers(n, r, d)
        + [
            pltpu.SemaphoreType.DMA((2,)),
            pltpu.SemaphoreType.DMA((5,)),
            pltpu.SemaphoreType.DMA((1,)),
        ]
        + [pltpu.SemaphoreType.DMA((n,))] * 8
        + extra,
        compiler_params=pltpu.CompilerParams(
            collective_id=cid, has_side_effects=True, vmem_limit_bytes=63 << 20
        ),
        name="attn_backward",
    )(
        dmid,
        x,
        *gains,
        cosine,
        sine,
        kr,
        v,
        normed,
        proj,
        qr,
        prob,
        mixed,
        w_in,
        w_out,
        *later,
        *gives,
    )


def local_wide(
    inputs,
    out_grad,
    segments,
    routes,
    gates,
    gain_attn,
    gain_ffn,
    gain_query,
    gain_key,
    w_query,
    w_key,
    w_value,
    w_out,
    w_gate,
    w_up,
    w_down,
):
    micro_count, _, local_rows, width = inputs.shape
    n_sec = lax.axis_size("section")
    n_gx = lax.axis_size("gx")
    n_gy = lax.axis_size("gy")
    heads = w_query.shape[2] // HD
    span = heads * HD
    experts = n_gx * n_gy
    group_len = segments.shape[2]
    mb = micro_count // n_sec
    rows_own = mb * local_rows
    rows_attn = mb * group_len
    section = lax.axis_index("section")
    gx = lax.axis_index("gx")
    gy = lax.axis_index("gy")
    expert_own = gx * n_gy + gy
    inv_root = 1.0 / math.sqrt(HD)
    first = section * mb

    kv_head = gx * heads // (HQ // KVH)
    key_own = lax.dynamic_slice_in_dim(w_key[0], kv_head * HD, HD, 1)
    value_own = lax.dynamic_slice_in_dim(w_value[0], kv_head * HD, HD, 1)
    w_in_shard = jnp.concatenate([w_query[0], key_own, value_own], axis=1)
    w_in_all = both_layers(lax.all_gather(w_in_shard, "gy", axis=0, tiled=True))
    w_out_all = both_layers(lax.all_gather(w_out[0], "gy", axis=0, tiled=True))
    w_gate_all = both_layers(w_gate[0, 0])
    w_up_all = both_layers(w_up[0, 0])
    w_down_all = both_layers(w_down[0, 0])
    table = dense_gates(routes[0, :, 0], gates[0, :, 0], experts)
    small = jnp.concatenate(
        [
            table.reshape(-1),
            gain_attn[0],
            gain_ffn[0],
            gain_query[0],
            gain_key[0],
        ]
    )
    small_all = both_layers(small)
    table_size = micro_count * local_rows * experts
    table_all = small_all[:, :table_size].reshape(n_sec, micro_count, local_rows, experts)
    gains_all = small_all[:, table_size:]

    table_mine = lax.dynamic_slice_in_dim(table_all, first, mb, 1).reshape(
        n_sec, rows_own, experts
    )
    x_mine = lax.dynamic_slice_in_dim(inputs[:, 0], first, mb, 0).reshape(rows_own, width)
    cot_mine = lax.dynamic_slice_in_dim(out_grad[:, 0], first, mb, 0).reshape(rows_own, width)
    segs = lax.dynamic_slice_in_dim(segments[:, 0], first, mb, 0)
    allowed, cosine, sine = seq_tables(segs, HD)
    cos_q = cosine.reshape(rows_attn, 1, HD // 2)
    sin_q = sine.reshape(rows_attn, 1, HD // 2)
    cos_k = cosine.reshape(rows_attn, HD // 2)
    sin_k = sine.reshape(rows_attn, HD // 2)

    def split_gains(layer):
        g = gains_all[layer]
        return (
            g[:width],
            g[width : 2 * width],
            g[2 * width : 2 * width + HD],
            g[2 * width + HD :],
        )

    saved_all = []
    outs = []
    layer_in = x_mine
    for layer in range(n_sec):
        g_attn, g_ffn, g_query, g_key = split_gains(layer)
        hidden = layer_in.astype(F32)
        attn_unit, attn_scale = normalize(hidden)
        normed = (attn_unit * g_attn).astype(BF16)
        normed_all = gather_z(normed.reshape(mb, local_rows, width)).reshape(rows_attn, width)
        projected = dot32(normed_all, w_in_all[layer])
        query = projected[:, :span].reshape(rows_attn, heads, HD)
        key = projected[:, span : span + HD]
        value_low = projected[:, span + HD :].astype(BF16).reshape(mb, group_len, HD)
        query_unit, query_scale = normalize(query)
        key_unit, key_scale = normalize(key)
        query_rope = (
            rotate(query_unit * g_query, cos_q, sin_q)
            .astype(BF16)
            .reshape(mb, group_len, heads, HD)
        )
        key_rope = rotate(key_unit * g_key, cos_k, sin_k).astype(BF16).reshape(mb, group_len, HD)
        scores = (
            jnp.einsum("mthd,msd->mhts", query_rope, key_rope, preferred_element_type=F32)
            * inv_root
        )
        exponent = jnp.where(allowed[:, None], jnp.exp(scores), 0.0)
        log_total = jnp.log(jnp.sum(exponent, axis=-1, keepdims=True))
        prob = jnp.where(allowed[:, None], jnp.exp(scores - log_total), 0.0)
        mixed = (
            jnp.einsum("mhts,msd->mthd", prob.astype(BF16), value_low, preferred_element_type=F32)
            .astype(BF16)
            .reshape(rows_attn, span)
        )
        attn_part = dot32(mixed, w_out_all[layer], COL_PAIR).astype(BF16)
        attn_out = scatter_z(attn_part.reshape(mb, group_len, width)).reshape(rows_own, width)
        middle = hidden + attn_out.astype(F32)
        ffn_unit, ffn_scale = normalize(middle)
        expert_in = (ffn_unit * g_ffn).astype(BF16)
        tab = table_mine[layer]
        tab_hi = tab.astype(BF16)
        tab_lo = (tab - tab_hi.astype(F32)).astype(BF16)
        payload = jnp.concatenate([expert_in, tab_hi, tab_lo], axis=1)
        arrived_all = gather_all(payload)
        arrived = arrived_all[:, :width]
        gate_cols = arrived_all[:, width:].astype(F32)
        is_mine = jnp.arange(2 * experts) % experts == expert_own
        weight = jnp.sum(jnp.where(is_mine[None], gate_cols, 0.0), axis=1, keepdims=True)
        gate_pre = dot32(arrived, w_gate_all[layer])
        up_proj = dot32(arrived, w_up_all[layer])
        inner = (jax.nn.silu(gate_pre) * up_proj).astype(BF16)
        result = dot32(inner, w_down_all[layer])
        weighted = (result * weight).astype(BF16)
        expert_sum = scatter_all(weighted)
        layer_out = (middle + expert_sum.astype(F32)).astype(BF16)
        outs.append(layer_out)
        layer_in = layer_out
        saved_all.append(
            (
                attn_unit,
                attn_scale,
                normed_all,
                query_unit,
                query_scale,
                key_unit,
                key_scale,
                query_rope,
                key_rope,
                value_low,
                prob,
                mixed,
                ffn_unit,
                ffn_scale,
                arrived,
                weight,
                gate_pre,
                up_proj,
                inner,
            )
        )

    cot = cot_mine
    in_grads = [None] * n_sec
    expert_grads = [None] * n_sec
    attn_grads = [None] * n_sec
    gain_grads = [None] * n_sec
    for layer in reversed(range(n_sec)):
        g_attn, g_ffn, g_query, g_key = split_gains(layer)
        (
            attn_unit,
            attn_scale,
            normed_all,
            query_unit,
            query_scale,
            key_unit,
            key_scale,
            query_rope,
            key_rope,
            value_low,
            prob,
            mixed,
            ffn_unit,
            ffn_scale,
            arrived,
            weight,
            gate_pre,
            up_proj,
            inner,
        ) = saved_all[layer]
        gradient = cot.astype(F32)
        grad_all = gather_all(cot)
        grad_result = (grad_all.astype(F32) * weight).astype(BF16)
        grad_inner = dot32(grad_result, w_down_all[layer], COL_PAIR)
        grad_down = dot32(inner, grad_result, ROW_PAIR)
        sig = jax.nn.sigmoid(gate_pre)
        grad_gate_pre = (grad_inner * up_proj * sig * (1.0 + gate_pre * (1.0 - sig))).astype(BF16)
        grad_up_proj = (grad_inner * gate_pre * sig).astype(BF16)
        grad_gate = dot32(arrived, grad_gate_pre, ROW_PAIR)
        grad_up = dot32(arrived, grad_up_proj, ROW_PAIR)
        grad_arrived = (
            dot32(grad_gate_pre, w_gate_all[layer], COL_PAIR)
            + dot32(grad_up_proj, w_up_all[layer], COL_PAIR)
        ).astype(BF16)
        expert_grads[layer] = (grad_gate, grad_up, grad_down)
        grad_expert_in = scatter_all(grad_arrived).astype(F32)
        grad_ffn_gain = jnp.sum(grad_expert_in * ffn_unit, axis=0)
        grad_middle = gradient + norm_back(grad_expert_in * g_ffn, ffn_unit, ffn_scale)
        middle_low = grad_middle.astype(BF16)
        middle_all = gather_z(middle_low.reshape(mb, local_rows, width)).reshape(rows_attn, width)
        grad_out_w = dot32(middle_all, mixed, ROW_PAIR)
        grad_heads = (
            dot32(middle_all, w_out_all[layer]).astype(BF16).reshape(mb, group_len, heads, HD)
        )
        grad_value = jnp.einsum(
            "mhts,mthd->mshd", prob.astype(BF16), grad_heads, preferred_element_type=F32
        )
        grad_prob = jnp.einsum(
            "mthd,msd->mhts", grad_heads, value_low, preferred_element_type=F32
        )
        mixed_split = mixed.reshape(mb, group_len, heads, HD)
        delta = jnp.sum(grad_heads.astype(F32) * mixed_split.astype(F32), axis=-1)
        delta = jnp.swapaxes(delta, 1, 2)[..., None]
        grad_scores = (prob * (grad_prob - delta)).astype(BF16)
        grad_query = (
            jnp.einsum("mhts,msd->mthd", grad_scores, key_rope, preferred_element_type=F32)
            * inv_root
        ).reshape(rows_attn, heads, HD)
        grad_key = (
            jnp.einsum("mhts,mthd->mshd", grad_scores, query_rope, preferred_element_type=F32)
            * inv_root
        ).reshape(rows_attn, heads, HD)
        query_turn = rotate_back(grad_query, cos_q, sin_q)
        grad_query_gain = jnp.sum(query_turn * query_unit, axis=(0, 1))
        grad_query_pre = norm_back(query_turn * g_query, query_unit, query_scale)
        key_turn = rotate_back(jnp.sum(grad_key, axis=1), cos_k, sin_k)
        grad_key_gain = jnp.sum(key_turn * key_unit, axis=0)
        grad_key_pre = norm_back(key_turn * g_key, key_unit, key_scale)
        grad_proj = jnp.concatenate(
            [
                grad_query_pre.reshape(rows_attn, span),
                grad_key_pre,
                jnp.sum(grad_value, axis=2).reshape(rows_attn, HD),
            ],
            axis=1,
        ).astype(BF16)
        grad_in_w = dot32(normed_all, grad_proj, ROW_PAIR)
        normed_part = dot32(grad_proj, w_in_all[layer], COL_PAIR).astype(BF16)
        grad_normed = (
            scatter_z(normed_part.reshape(mb, group_len, width))
            .reshape(rows_own, width)
            .astype(F32)
        )
        grad_attn_gain = jnp.sum(grad_normed * attn_unit, axis=0)
        cot = (grad_middle + norm_back(grad_normed * g_attn, attn_unit, attn_scale)).astype(BF16)
        in_grads[layer] = cot
        attn_grads[layer] = jnp.concatenate([grad_in_w, grad_out_w], axis=1).astype(BF16)
        gain_grads[layer] = jnp.concatenate(
            [grad_attn_gain, grad_ffn_gain, grad_query_gain, grad_key_gain]
        )

    def own_layer_sum(pieces):
        return lax.psum_scatter(
            jnp.stack([piece.astype(BF16) for piece in pieces]),
            "section",
            scatter_dimension=0,
            tiled=True,
        ).astype(F32)

    grad_gate, grad_up, grad_down = (
        own_layer_sum([expert_grads[layer][k] for layer in range(n_sec)]) for k in range(3)
    )
    attn_sum = lax.psum_scatter(
        jnp.concatenate(attn_grads, axis=0), ("section", "gy"), scatter_dimension=0, tiled=True
    ).astype(F32)
    query_grad = attn_sum[:, :span]
    out_w_grad = attn_sum[:, span + 2 * HD :]
    kv_all = lax.all_gather(attn_sum[:, span : span + 2 * HD], "gx", axis=0, tiled=False)
    kv_all = jnp.sum(kv_all.reshape(KVH, n_gx // KVH, -1, 2, HD), axis=1)
    key_part = jnp.swapaxes(kv_all[:, :, 0], 0, 1).reshape(-1, KVH * HD)
    value_part = jnp.swapaxes(kv_all[:, :, 1], 0, 1).reshape(-1, KVH * HD)
    gain_sum = lax.psum(jnp.stack(gain_grads), ("section", "gx", "gy"))
    gain_sum = lax.dynamic_index_in_dim(gain_sum, section, 0, keepdims=True)

    def own_layer_rows(pieces):
        stacked = jnp.stack(pieces).reshape(n_sec, mb, local_rows, width)
        return lax.all_to_all(stacked, "section", split_axis=0, concat_axis=0, tiled=True).reshape(
            1, micro_count, 1, local_rows, width
        )

    return (
        own_layer_rows(outs),
        own_layer_rows(in_grads),
        gain_sum[:, :width],
        gain_sum[:, width : 2 * width],
        gain_sum[:, 2 * width : 2 * width + HD],
        gain_sum[:, 2 * width + HD :],
        query_grad[None],
        key_part[None],
        value_part[None],
        out_w_grad[None],
        grad_gate[:, None],
        grad_up[:, None],
        grad_down[:, None],
    )


def local_fused(
    inputs,
    out_grad,
    segments,
    routes,
    gates,
    gain_attn,
    gain_ffn,
    gain_query,
    gain_key,
    w_query,
    w_key,
    w_value,
    w_out,
    w_gate,
    w_up,
    w_down,
):
    micro_count, _, local_rows, width = inputs.shape
    n_sec = lax.axis_size("section")
    n_gx = lax.axis_size("gx")
    n_gy = lax.axis_size("gy")
    heads = w_query.shape[2] // HD
    span = heads * HD
    experts = n_gx * n_gy
    group_len = segments.shape[2]
    mb = micro_count // n_sec
    rows_own = mb * local_rows
    rows_attn = mb * group_len
    section = lax.axis_index("section")
    gx = lax.axis_index("gx")
    first = section * mb

    kv_head = gx * heads // (HQ // KVH)
    key_own = lax.dynamic_slice_in_dim(w_key[0], kv_head * HD, HD, 1)
    value_own = lax.dynamic_slice_in_dim(w_value[0], kv_head * HD, HD, 1)
    w_in_shard = jnp.concatenate([w_query[0], key_own, value_own], axis=1)
    attn_shards = (w_in_shard, w_out[0])
    attn_all = [share_weights(0, n_gx, attn_shards, 9)]
    moe_own = (w_gate[0, 0], w_up[0, 0], w_down[0, 0])
    moe_other = tuple(swap_sections(w) for w in moe_own)
    table = dense_gates(routes[0, :, 0], gates[0, :, 0], experts)
    small = jnp.concatenate(
        [table.reshape(-1), gain_attn[0], gain_ffn[0], gain_query[0], gain_key[0]]
    )
    small_other = swap_sections(small)
    is_first = section == 0
    small_all = jnp.stack(
        [jnp.where(is_first, small, small_other), jnp.where(is_first, small_other, small)]
    )
    table_size = micro_count * local_rows * experts
    table_all = small_all[:, :table_size].reshape(n_sec, micro_count, local_rows, experts)
    gains_all = small_all[:, table_size:]
    table_mine = lax.dynamic_slice_in_dim(table_all, first, mb, 1).reshape(
        n_sec, rows_own, experts
    )
    x_mine = lax.dynamic_slice_in_dim(inputs[:, 0], first, mb, 0).reshape(rows_own, width)
    cot = lax.dynamic_slice_in_dim(out_grad[:, 0], first, mb, 0).reshape(rows_own, width)
    segs = lax.dynamic_slice_in_dim(segments[:, 0], first, mb, 0)
    allowed, cosine, sine = seq_tables(segs, HD)
    tables = (
        jnp.concatenate([cosine, cosine], axis=-1).reshape(rows_attn, HD),
        jnp.concatenate([-sine, sine], axis=-1).reshape(rows_attn, HD),
        allowed.astype(F32),
    )

    def split_gains(layer):
        g = gains_all[layer : layer + 1]
        return (
            g[:, :width],
            g[:, width : 2 * width],
            g[:, 2 * width : 2 * width + HD],
            g[:, 2 * width + HD :],
        )

    kept = []
    outs = []
    layer_in = x_mine
    for layer in range(n_sec):
        tab = table_mine[layer]
        tab_hi = tab.astype(BF16)
        tab_lo = (tab - tab_hi.astype(F32)).astype(BF16)
        pad = jnp.zeros((rows_own, 128 - 2 * experts), BF16)
        gate_cols = jnp.concatenate([tab_hi, tab_lo, pad], axis=1)
        mid, payload, normed, proj, qr, kr, v, prob, mixed, *next_all = attn_forward(
            layer,
            n_gx,
            layer_in,
            split_gains(layer),
            tables,
            gate_cols,
            *attn_all[layer],
            attn_shards if layer == 0 else (),
            1 + layer,
            mb,
        )
        attn_all.append(next_all)
        layer_out, *moe_kept = moe_forward(
            layer, n_gx, mid, payload, moe_own, moe_other, 3 + layer
        )
        kept.append((layer_in, mid, (normed, proj, qr, kr, v, prob, mixed), moe_kept))
        outs.append(layer_out)
        layer_in = layer_out

    in_grads = [None] * n_sec
    moe_sums = ()
    later = ()
    gain_grads = [None] * n_sec
    for layer in reversed(range(n_sec)):
        g_attn, g_ffn, g_query, g_key = split_gains(layer)
        layer_in, mid, attn_kept, (arrived, weight, gp, up, inner) = kept[layer]
        dmid, d_ffn, *moe_sums = moe_backward(
            layer,
            n_gx,
            cot,
            mid,
            g_ffn,
            weight,
            arrived,
            gp,
            up,
            inner,
            moe_own,
            moe_other,
            moe_sums,
            5 + layer,
        )
        cot, d_attn, d_query, d_key, *later = attn_backward(
            layer,
            n_gx,
            dmid,
            layer_in,
            (g_attn, g_query, g_key),
            tables,
            attn_kept,
            *attn_all[layer],
            later,
            moe_sums[3:] if layer == 0 else (),
            7 + layer,
            mb,
        )
        in_grads[layer] = cot
        gain_grads[layer] = jnp.concatenate([d_attn, d_ffn, d_query, d_key], axis=1)

    query_grad, kv_shard, out_grad_w, *from_other = later
    grad_gate, grad_up, grad_down = (
        (moe_sums[k].astype(F32) + from_other[k].astype(F32))[None] for k in range(3)
    )
    gain_sum, kv_all, out_rows, grad_rows = finish(
        n_gx,
        jnp.concatenate(gain_grads[::1], axis=0),
        kv_shard,
        jnp.stack(outs),
        jnp.stack(in_grads),
        10,
    )
    kv_all = jnp.sum(kv_all.reshape(KVH, n_gx // KVH, -1, 2, HD).astype(F32), axis=1)
    key_part = jnp.swapaxes(kv_all[:, :, 0], 0, 1).reshape(-1, KVH * HD)
    value_part = jnp.swapaxes(kv_all[:, :, 1], 0, 1).reshape(-1, KVH * HD)
    whole_rows = (1, micro_count, 1, local_rows, width)

    return (
        out_rows.reshape(whole_rows),
        grad_rows.reshape(whole_rows),
        gain_sum[:, :width],
        gain_sum[:, width : 2 * width],
        gain_sum[:, 2 * width : 2 * width + HD],
        gain_sum[:, 2 * width + HD :],
        query_grad[None],
        key_part[None],
        value_part[None],
        out_grad_w[None],
        grad_gate[:, None],
        grad_up[:, None],
        grad_down[:, None],
    )


def local(*args):
    inputs = args[0]
    n = lax.axis_size("gx")
    rows_own = inputs.shape[0] // lax.axis_size("section") * inputs.shape[2]
    if 4 * n * rows_own > MOST_ROWS:
        return local_wide(*args)
    return local_fused(*args)


def solution(mesh):
    return jax.shard_map(
        local,
        mesh=mesh,
        in_specs=(
            P(None, "gy", "gx", None),
            P(None, "gy", "gx", None),
            P(None, "gy", None),
            P("section", None, "gy", "gx", None),
            P("section", None, "gy", "gx", None),
            P("section", None),
            P("section", None),
            P("section", None),
            P("section", None),
            P("section", "gy", "gx"),
            P("section", "gy", None),
            P("section", "gy", None),
            P("section", "gy", "gx"),
            P("section", ("gx", "gy"), None, None),
            P("section", ("gx", "gy"), None, None),
            P("section", ("gx", "gy"), None, None),
        ),
        out_specs=(
            P("section", None, "gy", "gx", None),
            P("section", None, "gy", "gx", None),
            P("section", None),
            P("section", None),
            P("section", None),
            P("section", None),
            P("section", "gy", "gx"),
            P("section", "gy", None),
            P("section", "gy", None),
            P("section", "gy", "gx"),
            P("section", ("gx", "gy"), None, None),
            P("section", ("gx", "gy"), None, None),
            P("section", ("gx", "gy"), None, None),
        ),
        check_vma=False,
    )
```

```python
import functools
import math

import jax
import jax.numpy as jnp
from jax import lax
from jax.experimental import pallas as pl
from jax.experimental.pallas import tpu as pltpu
from jax.sharding import PartitionSpec as P

HQ = 32
KVH = 4
HD = 128
TOPK = 8

EPSILON = 1e-06
ROPE_BASE = 1000000.0
ROW_PAIR = (((0,), (0,)), ((), ()))
COL_PAIR = (((1,), (1,)), ((), ()))
F32 = jnp.float32
BF16 = jnp.bfloat16
MOST_ROWS = 1024


def normalize(tensor):
    scaling = lax.rsqrt(jnp.mean(tensor * tensor, axis=-1, keepdims=True) + EPSILON)
    return (tensor * scaling, scaling)


def norm_back(gradient, unit_vec, scaling):
    return scaling * (gradient - unit_vec * jnp.mean(gradient * unit_vec, axis=-1, keepdims=True))


def rotate(tensor, cosine, sine_part):
    halfway = tensor.shape[-1] // 2
    leading = tensor[..., :halfway]
    trailing = tensor[..., halfway:]
    return jnp.concatenate(
        [leading * cosine - trailing * sine_part, trailing * cosine + leading * sine_part], axis=-1
    )


def rotate_back(gradient, cosine, sine_part):
    return rotate(gradient, cosine, -sine_part)


def seq_tables(segment_ids, head_dim):
    length_all = segment_ids.shape[-1]
    position_ids = jnp.arange(length_all, dtype=jnp.int32)
    allowed = (segment_ids[:, :, None] == segment_ids[:, None, :]) & (
        position_ids[:, None] >= position_ids[None, :]
    )
    positions = jnp.sum(allowed.astype(jnp.int32), axis=-1) - 1
    halfway = head_dim // 2
    inverse = ROPE_BASE ** (-2.0 * jnp.arange(halfway, dtype=jnp.float32) / head_dim)
    angles = positions.astype(jnp.float32)[..., None] * inverse
    return (allowed, jnp.cos(angles), jnp.sin(angles))


def dot32(left, right, dims=None):
    if dims is None:
        return jnp.dot(left, right, preferred_element_type=F32)
    return lax.dot_general(left, right, dims, preferred_element_type=F32)


def gather_z(rows):
    return lax.all_gather(rows, "gx", axis=1, tiled=True)


def scatter_z(rows):
    return lax.psum_scatter(rows, "gx", scatter_dimension=1, tiled=True)


def gather_all(rows):
    return lax.all_gather(rows, ("gx", "gy"), axis=0, tiled=True)


def scatter_all(rows):
    return lax.psum_scatter(rows, ("gx", "gy"), scatter_dimension=0, tiled=True)


def both_layers(tensor):
    return lax.all_gather(tensor, "section", axis=0, tiled=False)


def dense_gates(route_ids, gate_vals, experts):
    onehot = route_ids[..., None] == jnp.arange(experts, dtype=jnp.int32)
    return jnp.sum(jnp.where(onehot, gate_vals[..., None], 0.0), axis=-2)


def swap_sections(tensor):
    return lax.ppermute(tensor, "section", [(0, 1), (1, 0)])


def remote(src, dst, send_sem, recv_sem, **where):
    return pltpu.make_async_remote_copy(
        src_ref=src,
        dst_ref=dst,
        send_sem=send_sem,
        recv_sem=recv_sem,
        device_id=where,
        device_id_type=pl.DeviceIdType.MESH,
    )


def hello(n, me, gy, with_plane, with_section=False):
    barrier = pltpu.get_barrier_semaphore()
    mesh_ids = pl.DeviceIdType.MESH

    @pl.when(me + 1 < n)
    def _():
        pl.semaphore_signal(barrier, 1, device_id={"gx": me + 1}, device_id_type=mesh_ids)

    @pl.when(me > 0)
    def _():
        pl.semaphore_signal(barrier, 1, device_id={"gx": me - 1}, device_id_type=mesh_ids)

    peers = 0
    if with_plane:
        for bit in (1, 2):
            pl.semaphore_signal(
                barrier, 1, device_id={"gy": gy_flip(gy, bit)}, device_id_type=mesh_ids
            )
        peers += 2
    if with_section:
        other = 1 - lax.axis_index("section")
        pl.semaphore_signal(barrier, 1, device_id={"section": other}, device_id_type=mesh_ids)
        peers += 1
    at_end = (me == 0) | (me == n - 1)

    @pl.when(at_end)
    def _():
        pl.semaphore_wait(barrier, peers + 1)

    @pl.when(jnp.logical_not(at_end))
    def _():
        pl.semaphore_wait(barrier, peers + 2)


def gy_flip(gy, bits):
    low = lax.rem(gy, 2)
    high = gy // 2
    if bits & 1:
        low = 1 - low
    if bits & 2:
        high = 1 - high
    return high * 2 + low


def z_gather_steps(n, me, slot, sems, after):
    send_up, recv_up, send_down, recv_down = sems
    sends = []

    def up(k):
        return remote(slot(me - k), slot(me - k), send_up.at[k], recv_up.at[k], gx=me + 1)

    def down(k):
        return remote(slot(me + k), slot(me + k), send_down.at[k], recv_down.at[k], gx=me - 1)

    for k in range(n):
        @pl.when(me - k >= 0)
        def _():
            if k:
                remote(
                    slot(me - k), slot(me - k), send_up.at[k - 1], recv_up.at[k - 1], gx=me
                ).wait_recv()
            if k < n - 1:

                @pl.when(me + 1 < n)
                def _():
                    up(k).start()

            if k == 0:

                @pl.when(me > 0)
                def _():
                    down(0).start()

            after(me - k, k)

        if k:

            @pl.when(me + k < n)
            def _():
                remote(
                    slot(me + k), slot(me + k), send_down.at[k - 1], recv_down.at[k - 1], gx=me
                ).wait_recv()
                if k < n - 1:

                    @pl.when(me > 0)
                    def _():
                        down(k).start()

                after(me + k, k)


def z_gather_drain(n, me, slot, sems):
    send_up, recv_up, send_down, recv_down = sems
    for k in range(n - 1):

        @pl.when((me - k >= 0) & (me + 1 < n))
        def _():
            remote(slot(me - k), slot(me - k), send_up.at[k], recv_up.at[k], gx=me + 1).wait_send()

        @pl.when((me + k < n) & (me > 0))
        def _():
            remote(
                slot(me + k), slot(me + k), send_down.at[k], recv_down.at[k], gx=me - 1
            ).wait_send()


def flip_by(gy, step):
    low = lax.rem(lax.rem(gy, 2) + lax.rem(step, 2), 2)
    high = lax.rem(gy // 2 + step // 2, 2)
    return high * 2 + low


class Plane:
    def __init__(self, n, sems):
        self.n = n
        self.me = lax.axis_index("gx")
        self.gy = lax.axis_index("gy")
        self.cx, self.cy, self.cd = (gy_flip(self.gy, bits) for bits in (1, 2, 3))
        self.gather_sems = sems[:10]
        self.scatter_sems = sems[10:]


    def gather_own_column(self, slot):
        su, ru, sd, rd, sx, rx, sy, ry, sf, rf = self.gather_sems
        c = self.gy

        def after(z, k):
            remote(slot(z, c), slot(z, c), sx.at[z], rx.at[z], gy=self.cx).start()
            remote(slot(z, c), slot(z, c), sy.at[z], ry.at[z], gy=self.cy).start()

        z_gather_steps(self.n, self.me, lambda z: slot(z, c), (su, ru, sd, rd), after)

    def gather_pass_on(self, slot):
        su, ru, sd, rd, sx, rx, sy, ry, sf, rf = self.gather_sems

        def forward(z):
            remote(slot(z, self.cx), slot(z, self.cx), sx.at[z], rx.at[z], gy=self.cx).wait_recv()
            remote(slot(z, self.cy), slot(z, self.cy), sy.at[z], ry.at[z], gy=self.cy).wait_recv()

            @pl.when(lax.rem(z, 2) == 0)
            def _():
                remote(
                    slot(z, self.cy), slot(z, self.cy), sf.at[z], rf.at[z], gy=self.cx
                ).start()

            @pl.when(lax.rem(z, 2) == 1)
            def _():
                remote(
                    slot(z, self.cx), slot(z, self.cx), sf.at[z], rf.at[z], gy=self.cy
                ).start()

        for k in range(self.n):

            @pl.when(self.me - k >= 0)
            def _():
                forward(self.me - k)

            if k:

                @pl.when(self.me + k < self.n)
                def _():
                    forward(self.me + k)

    def gather_far_column(self, slot):
        sf, rf = self.gather_sems[8:]
        for z in range(self.n):
            remote(slot(z, self.cd), slot(z, self.cd), sf.at[z], rf.at[z], gy=self.cx).wait_recv()

    def gather_drain(self, slot):
        su, ru, sd, rd, sx, rx, sy, ry, sf, rf = self.gather_sems
        z_gather_drain(self.n, self.me, lambda z: slot(z, self.gy), (su, ru, sd, rd))
        for z in range(self.n):
            one = slot(z, self.gy)
            remote(one, one, sx.at[z], rx.at[z], gy=self.cx).wait_send()
            remote(one, one, sy.at[z], ry.at[z], gy=self.cy).wait_send()
            remote(one, one, sf.at[z], rf.at[z], gy=self.cx).wait_send()


    def scatter_setup(self, part, sides, din, zup, zdn, stage, acc):
        self.part, self.sides, self.din = part, sides, din
        self.zup, self.zdn, self.stage, self.acc = zup, zdn, stage, acc

    def column_of(self, side):
        return self.cx * (1 - side) + self.cy * side

    def near(self, side, z):
        send, recv = self.scatter_sems[4:6]
        column = self.column_of(side)
        return remote(
            self.part(z, column), self.sides.at[side, z], send.at[side, z], recv.at[side, z], gy=column
        )

    def far(self, z):
        send, recv = self.scatter_sems[6:]
        return remote(
            self.part(z, self.cd),
            self.din.at[z],
            send.at[z],
            recv.at[z],
            gy=self.column_of(lax.rem(z, 2)),
        )

    def each(self, call):
        for k in [sign * far for far in reversed(range(1, self.n)) for sign in (-1, 1)] + [0]:

            @pl.when((self.me + k >= 0) & (self.me + k < self.n))
            def _():
                call(self.me + k, k)

    def scatter_near(self, side):
        def send(z, k):
            @pl.when(lax.rem(z, 2) == side)
            def _():
                self.near(side, z).start()

        self.each(send)

    def scatter_far(self):
        self.each(lambda z, k: self.far(z).start())

    def scatter_pass_on(self, z, k):
        self.far(z).wait_recv()
        side = 1 - lax.rem(z, 2)
        mine = self.part(z, self.column_of(side))
        add_rows(mine, mine, self.din.at[z])
        self.near(side, z).start()

    def along(self, z, up):
        send, recv = self.scatter_sems[:2] if up else self.scatter_sems[2:4]
        into = self.zup if up else self.zdn
        return remote(
            self.stage.at[z],
            into.at[z],
            send.at[z],
            recv.at[z],
            gx=self.me + 1 if up else self.me - 1,
        )

    def scatter_line(self, total, z, k):
        n, me, acc = self.n, self.me, self.acc
        self.near(0, z).wait_recv()
        self.near(1, z).wait_recv()
        terms = (self.part(z, self.gy), self.sides.at[0, z], self.sides.at[1, z])
        if k == 0:
            add_rows(total, *terms)
            return
        came = me > 0 if k > 0 else me < n - 1

        @pl.when(came)
        def _():
            self.along(z, k > 0).wait_recv()
            add_rows(self.stage.at[z], *terms, (self.zup if k > 0 else self.zdn).at[z])

        @pl.when(jnp.logical_not(came))
        def _():
            add_rows(self.stage.at[z], *terms)

        self.along(z, k > 0).start()

    def scatter_finish(self, total):
        n, me = self.n, self.me

        @pl.when(me > 0)
        def _():
            self.along(me, True).wait_recv()
            add_rows(total, total, self.zup.at[me])

        @pl.when(me < n - 1)
        def _():
            self.along(me, False).wait_recv()
            add_rows(total, total, self.zdn.at[me])

        for z in range(n):
            self.near(0, z).wait_send()
            self.near(1, z).wait_send()
            self.far(z).wait_send()

            @pl.when(me < z)
            def _():
                self.along(z, True).wait_send()

            @pl.when(me > z)
            def _():
                self.along(z, False).wait_send()


def add_rows(out, *terms):
    rows = out.shape[0]
    step = 16

    def body(i, carry):
        at = pl.ds(pl.multiple_of(i * step, step), step)
        value = terms[0][at].astype(F32)
        for term in terms[1:]:
            value = value + term[at].astype(F32)
        out[at] = value.astype(out.dtype)
        return carry

    lax.fori_loop(0, rows // step, body, 0)


def fetch_layer(layer, own, other, held, sems):
    section = lax.axis_index("section")

    @pl.when(section == layer)
    def _():
        for k, ref in enumerate(own):
            pltpu.make_async_copy(ref, held[k], sems.at[k]).start()

    @pl.when(section != layer)
    def _():
        for k, ref in enumerate(other):
            pltpu.make_async_copy(ref, held[k], sems.at[k]).start()


def fetch_wait(own, held, sems, which):
    for k in which:
        pltpu.make_async_copy(own[k], held[k], sems.at[k]).wait()


def moe_forward_kernel(
    n,
    layer,
    mid_ref,
    pay_ref,
    wg_own,
    wu_own,
    wd_own,
    wg_other,
    wu_other,
    wd_other,
    out_ref,
    arrived_ref,
    weight_ref,
    gp_ref,
    up_ref,
    inner_ref,
    pay,
    wg,
    wu,
    wd,
    part,
    sides,
    din,
    zup,
    zdn,
    stage,
    acc,
    total,
    gp,
    up,
    inner,
    wsem,
    osem,
    *sems,
):
    r, d = mid_ref.shape
    ff = wg.shape[1]
    rows = n * r
    experts = 4 * n
    own, other, held = (
        (wg_own, wu_own, wd_own),
        (wg_other, wu_other, wd_other),
        (wg, wu, wd),
    )
    fetch_layer(layer, own, other, held, wsem)
    plane = Plane(n, sems)
    me, gy = plane.me, plane.gy
    hello(n, me, gy, True)
    pay[pl.ds(pl.multiple_of((gy * n + me) * r, r), r)] = pay_ref[...]

    def slot(z, c):
        return pay.at[pl.ds((c * n + z) * r, r)]

    plane.scatter_setup(lambda z, c: part.at[c * n + z], sides, din, zup, zdn, stage, acc)
    plane.gather_own_column(slot)
    fetch_wait(own, held, wsem, range(3))
    expert = me * 4 + gy

    def column(s, carry):
        c = flip_by(gy, s)

        @pl.when(s == 1)
        def _():
            plane.gather_pass_on(slot)

        @pl.when(s == 3)
        def _():
            plane.gather_far_column(slot)

        at = pl.ds(pl.multiple_of(c * rows, rows), rows)
        gate_cols = pay[at, d : d + 128].astype(F32)
        lane = lax.broadcasted_iota(jnp.int32, (rows, 128), 1)
        hit = ((lane == expert) | (lane == expert + experts)) & (lane < 2 * experts)
        weight = jnp.sum(jnp.where(hit, gate_cols, 0.0), axis=1, keepdims=True)
        weight_ref[at] = weight
        block = pay[at, :d]
        for j in range(ff // 256):
            cols = slice(j * 256, (j + 1) * 256)
            g = jnp.dot(block, wg[:, cols], preferred_element_type=F32)
            u = jnp.dot(block, wu[:, cols], preferred_element_type=F32)
            gp[at, cols] = g.astype(BF16)
            up[at, cols] = u.astype(BF16)
            inner[at, cols] = (g / (1.0 + jnp.exp(-g)) * u).astype(BF16)
        act = inner[at]
        for j in range(d // 256):
            cols = slice(j * 256, (j + 1) * 256)
            res = jnp.dot(act, wd[:, cols], preferred_element_type=F32) * weight
            part[pl.ds(pl.multiple_of(c * n, n), n), :, cols] = (
                res.astype(BF16).reshape(n, r, 256)
            )

        @pl.when(s == 1)
        def _():
            plane.scatter_near(0)

        @pl.when(s == 2)
        def _():
            plane.scatter_near(1)

        return carry

    lax.fori_loop(0, 4, column, 0)
    plane.scatter_far()
    saves = [
        pltpu.make_async_copy(pay.at[:, pl.ds(0, d)], arrived_ref, osem.at[0]),
        pltpu.make_async_copy(gp, gp_ref, osem.at[1]),
        pltpu.make_async_copy(up, up_ref, osem.at[2]),
        pltpu.make_async_copy(inner, inner_ref, osem.at[3]),
    ]
    for save in saves:
        save.start()
    plane.each(plane.scatter_pass_on)
    plane.each(functools.partial(plane.scatter_line, total))
    plane.scatter_finish(total)
    add_rows(out_ref, mid_ref, total)
    plane.gather_drain(slot)
    for save in saves:
        save.wait()


def scatter_buffers(n, r, d):
    block = pltpu.VMEM((n, r, d), BF16)
    return [
        pltpu.VMEM((4 * n, r, d), BF16),
        pltpu.VMEM((2, n, r, d), BF16),
        *[block] * 4,
        *[pltpu.VMEM((r, d), F32)] * 2,
    ]


def in_vmem(count):
    return [pl.BlockSpec(memory_space=pltpu.VMEM)] * count


def in_place(count):
    return [pl.BlockSpec(memory_space=pl.ANY)] * count


def moe_forward(layer, n, mid, payload, own, other, cid):
    r, d = mid.shape
    ff = own[0].shape[1]
    total_rows = 4 * n * r
    width = payload.shape[1]
    return pl.pallas_call(
        functools.partial(moe_forward_kernel, n, layer),
        out_shape=(
            jax.ShapeDtypeStruct((r, d), BF16),
            jax.ShapeDtypeStruct((total_rows, d), BF16),
            jax.ShapeDtypeStruct((total_rows, 1), F32),
            jax.ShapeDtypeStruct((total_rows, ff), BF16),
            jax.ShapeDtypeStruct((total_rows, ff), BF16),
            jax.ShapeDtypeStruct((total_rows, ff), BF16),
        ),
        in_specs=in_vmem(2) + in_place(6),
        out_specs=tuple(in_vmem(1) + in_place(1) + in_vmem(1) + in_place(3)),
        scratch_shapes=[
            pltpu.VMEM((total_rows, width), BF16),
            pltpu.VMEM((d, ff), BF16),
            pltpu.VMEM((d, ff), BF16),
            pltpu.VMEM((ff, d), BF16),
        ]
        + scatter_buffers(n, r, d)
        + [pltpu.VMEM((total_rows, ff), BF16)] * 3
        + [pltpu.SemaphoreType.DMA((3,)), pltpu.SemaphoreType.DMA((4,))]
        + [pltpu.SemaphoreType.DMA((n,))] * 14
        + [pltpu.SemaphoreType.DMA((2, n))] * 2
        + [pltpu.SemaphoreType.DMA((n,))] * 2,
        compiler_params=pltpu.CompilerParams(
            collective_id=cid, has_side_effects=True, vmem_limit_bytes=63 << 20
        ),
        name="moe_forward",
    )(mid, payload, *own, *other)


def moe_backward_kernel(
    n,
    layer,
    cot_ref,
    mid_ref,
    gain_ref,
    weight_ref,
    arrived_hbm,
    gp_hbm,
    up_hbm,
    inner_hbm,
    wg_own,
    wu_own,
    wd_own,
    wg_other,
    wu_other,
    wd_other,
    *rest,
):
    rest = rest[0 if layer else 6 :]
    dmid_ref, dgain_ref = rest[:2]
    keep_refs, give_refs = rest[2:5], rest[5:8]
    (
    cots,
    wg,
    wu,
    wd,
    part,
    sides,
    din,
    zup,
    zdn,
    stage,
    acc,
    total,
    arrived,
    gp,
    up,
    inner,
    de,
    out_gate,
    out_up,
    out_down,
    wsem,
    isem,
    osem,
    *sems,
    ) = rest[8:]
    section = lax.axis_index("section")
    r, d = mid_ref.shape
    ff = wg.shape[1]
    rows = n * r
    own, other, held = (
        (wg_own, wu_own, wd_own),
        (wg_other, wu_other, wd_other),
        (wg, wu, wd),
    )
    loads = [
        pltpu.make_async_copy(gp_hbm, gp, isem.at[0]),
        pltpu.make_async_copy(up_hbm, up, isem.at[1]),
        pltpu.make_async_copy(arrived_hbm, arrived, isem.at[2]),
        pltpu.make_async_copy(inner_hbm, inner, isem.at[3]),
    ]
    fetch_layer(layer, own, other, held, wsem)
    for load in loads:
        load.start()
    plane = Plane(n, sems)
    me, gy = plane.me, plane.gy
    hello(n, me, gy, True)
    cots[pl.ds(pl.multiple_of((gy * n + me) * r, r), r)] = cot_ref[...]

    def slot(z, c):
        return cots.at[pl.ds((c * n + z) * r, r)]

    plane.scatter_setup(lambda z, c: part.at[c * n + z], sides, din, zup, zdn, stage, acc)
    plane.gather_own_column(slot)
    fetch_wait(own, held, wsem, range(3))
    for load in loads:
        load.wait()

    def column(s, carry):
        c = flip_by(gy, s)

        @pl.when(s == 1)
        def _():
            plane.gather_pass_on(slot)

        @pl.when(s == 3)
        def _():
            plane.gather_far_column(slot)

        at = pl.ds(pl.multiple_of(c * rows, rows), rows)
        de[at] = (cots[at].astype(F32) * weight_ref[at]).astype(BF16)
        block = de[at]
        for j in range(ff // 256):
            cols = slice(j * 256, (j + 1) * 256)
            dz = dot32(block, wd[cols], COL_PAIR)
            g = gp[at, cols].astype(F32)
            u = up[at, cols].astype(F32)
            sg = 1.0 / (1.0 + jnp.exp(-g))
            gp[at, cols] = (dz * u * sg * (1.0 + g * (1.0 - sg))).astype(BF16)
            up[at, cols] = (dz * g * sg).astype(BF16)
        dgp = gp[at]
        dup = up[at]
        for j in range(d // 256):
            cols = slice(j * 256, (j + 1) * 256)
            res = dot32(dgp, wg[cols], COL_PAIR) + dot32(dup, wu[cols], COL_PAIR)
            part[pl.ds(pl.multiple_of(c * n, n), n), :, cols] = (
                res.astype(BF16).reshape(n, r, 256)
            )

        @pl.when(s == 1)
        def _():
            plane.scatter_near(0)

        @pl.when(s == 2)
        def _():
            plane.scatter_near(1)

        return carry

    lax.fori_loop(0, 4, column, 0)
    plane.scatter_far()

    def saving(i, refs):
        at = pl.ds(pl.multiple_of(i * 256, 256), 256)
        for k, (src, ref) in enumerate(zip((out_gate, out_up, out_down), refs)):
            where = (slice(None), at) if k == 2 else (at, slice(None))
            yield pltpu.make_async_copy(src.at[where], ref.at[where], osem.at[k, i])

    def weight_grads(first, last):
        def chunk(i, carry):
            at = pl.ds(pl.multiple_of(i * 256, 256), 256)
            left = arrived[:, at]
            out_gate[at] = dot32(left, gp[...], ROW_PAIR).astype(BF16)
            out_up[at] = dot32(left, up[...], ROW_PAIR).astype(BF16)
            out_down[:, at] = dot32(inner[...], de[:, at], ROW_PAIR).astype(BF16)

            @pl.when(section == layer)
            def _():
                for copy in saving(i, keep_refs):
                    copy.start()

            @pl.when(section != layer)
            def _():
                for copy in saving(i, give_refs):
                    copy.start()

            return carry

        lax.fori_loop(first, last, chunk, 0)

    chunks = d // 256
    cut = [0, chunks * 2 // 8, chunks * 4 // 8, chunks * 6 // 8, chunks]
    weight_grads(cut[0], cut[1])
    plane.each(plane.scatter_pass_on)
    weight_grads(cut[1], cut[2])

    def line(z, k):
        plane.scatter_line(total, z, k)

    plane.each(line)
    weight_grads(cut[2], cut[4])
    plane.scatter_finish(total)

    mid = mid_ref[...]
    scale = lax.rsqrt(jnp.mean(mid * mid, axis=-1, keepdims=True) + EPSILON)
    unit = mid * scale
    db = total[...]
    dgain_ref[...] = jnp.sum(db * unit, axis=0, keepdims=True)
    dmid_ref[...] = cot_ref[...].astype(F32) + norm_back(db * gain_ref[...], unit, scale)
    plane.gather_drain(slot)

    def settle(i, carry):
        for copy in saving(i, keep_refs):
            copy.wait()
        return carry

    lax.fori_loop(0, chunks, settle, 0)


def moe_backward(layer, n, cot, mid, gain, weight, arrived, gp, up, inner, own, other, so_far, cid):
    r, d = mid.shape
    ff = own[0].shape[1]
    total_rows = 4 * n * r
    sums = [jax.ShapeDtypeStruct(shape, BF16) for shape in ((d, ff), (d, ff), (ff, d))] * 2
    return pl.pallas_call(
        functools.partial(moe_backward_kernel, n, layer),
        out_shape=(
            jax.ShapeDtypeStruct((r, d), F32),
            jax.ShapeDtypeStruct((1, d), F32),
            *sums,
        ),
        in_specs=in_vmem(4) + in_place(10 + len(so_far)),
        out_specs=tuple(in_vmem(2) + in_place(6)),
        input_output_aliases={14 + k: 2 + k for k in range(len(so_far))},
        scratch_shapes=[
            pltpu.VMEM((total_rows, d), BF16),
            pltpu.VMEM((d, ff), BF16),
            pltpu.VMEM((d, ff), BF16),
            pltpu.VMEM((ff, d), BF16),
        ]
        + scatter_buffers(n, r, d)
        + [pltpu.VMEM((total_rows, d), BF16)]
        + [pltpu.VMEM((total_rows, ff), BF16)] * 3
        + [pltpu.VMEM((total_rows, d), BF16)]
        + [pltpu.VMEM((d, ff), BF16)] * 2
        + [pltpu.VMEM((ff, d), BF16)]
        + [
            pltpu.SemaphoreType.DMA((3,)),
            pltpu.SemaphoreType.DMA((4,)),
        ]
        + [pltpu.SemaphoreType.DMA((3, d // 256))]
        + [pltpu.SemaphoreType.DMA((n,))] * 14
        + [pltpu.SemaphoreType.DMA((2, n))] * 2
        + [pltpu.SemaphoreType.DMA((n,))] * 2,
        compiler_params=pltpu.CompilerParams(
            collective_id=cid, has_side_effects=True, vmem_limit_bytes=63 << 20
        ),
        name="moe_backward",
    )(cot, mid, gain, weight, arrived, gp, up, inner, *own, *other, *so_far)


class Share:
    def __init__(self, layer, shard, full, scratch):
        self.shard, self.full = shard, full
        self.held, self.plane_sems, self.to_sems, self.from_sems = scratch
        self.section = lax.axis_index("section")
        self.mine = self.section == layer
        gy = lax.axis_index("gy")
        self.cols = [gy_flip(gy, bits) if bits else gy for bits in range(4)]
        self.rows = shard.shape[0]

    def at(self, column, half=None):
        rows = self.rows
        if half is None:
            return self.full.at[pl.ds(pl.multiple_of(column * rows, rows), rows)]
        few = rows // 2
        return self.full.at[pl.ds(pl.multiple_of(column * rows + half * few, few), few)]

    def own(self, step):
        src, dst = ((self.shard, self.held), (self.held, self.at(self.cols[0])))[step]
        return pltpu.make_async_copy(src, dst, self.plane_sems.at[9 * step])

    def direct(self, bit):
        s = self.plane_sems
        k = 1 if bit == 1 else 3
        return remote(
            self.shard, self.at(self.cols[0]), s.at[k], s.at[k + 1], gy=self.cols[bit]
        )

    def onward(self, bit):
        s = self.plane_sems
        k = 5 if bit == 1 else 7
        half = 1 if bit == 1 else 0
        ref = self.at(self.cols[3 - bit], half)
        return remote(ref, ref, s.at[k], s.at[k + 1], gy=self.cols[bit])

    def hand(self, k):
        if k == 0:
            src, dst = self.shard, self.at(self.cols[0])
        elif k < 3:
            src = dst = self.at(self.cols[k])
        else:
            src = dst = self.at(self.cols[3], k - 3)
        return remote(src, dst, self.to_sems.at[k], self.from_sems.at[k], section=1 - self.section)

    def start(self):
        @pl.when(self.mine)
        def _():
            self.direct(1).start()
            self.direct(2).start()
            self.own(0).start()
            self.hand(0).start()

    def pass_on(self):
        @pl.when(self.mine)
        def _():
            self.own(0).wait()
            self.own(1).start()
            self.direct(1).wait_recv()
            self.onward(2).start()
            self.hand(1).start()
            self.direct(2).wait_recv()
            self.onward(1).start()
            self.hand(2).start()

    def finish(self):
        @pl.when(self.mine)
        def _():
            self.onward(2).wait_recv()
            self.hand(3).start()
            self.onward(1).wait_recv()
            self.hand(4).start()
            self.own(1).wait()

        @pl.when(jnp.logical_not(self.mine))
        def _():
            for k in range(5):
                self.hand(k).wait_recv()

    def drain(self):
        @pl.when(self.mine)
        def _():
            for bit in (1, 2):
                self.direct(bit).wait_send()
                self.onward(bit).wait_send()
            for k in range(5):
                self.hand(k).wait_send()


def share_scratch(shard):
    dma = pltpu.SemaphoreType.DMA
    return [pltpu.VMEM(shard.shape, BF16), dma((10,)), dma((5,)), dma((5,))]


def share_kernel(n, layer, count, *refs):
    shards, fulls, scratch = refs[:count], refs[count : 2 * count], refs[2 * count :]
    shares = [
        Share(layer, shards[k], fulls[k], scratch[4 * k : 4 * k + 4]) for k in range(count)
    ]
    hello(n, lax.axis_index("gx"), lax.axis_index("gy"), True, True)
    for share in shares:
        share.start()
    for share in shares:
        share.pass_on()
    for share in shares:
        share.finish()
    for share in shares:
        share.drain()


def share_weights(layer, n, shards, cid):
    return pl.pallas_call(
        functools.partial(share_kernel, n, layer, len(shards)),
        out_shape=tuple(jax.ShapeDtypeStruct((4 * w.shape[0], w.shape[1]), BF16) for w in shards),
        in_specs=in_place(len(shards)),
        out_specs=tuple(in_place(len(shards))),
        scratch_shapes=[item for shard in shards for item in share_scratch(shard)],
        compiler_params=pltpu.CompilerParams(collective_id=cid, has_side_effects=True),
        name="share_weights",
    )(*shards)


def finish_kernel(
    n,
    gains_ref,
    kv_ref,
    lo_ref,
    ig_ref,
    gain_ref,
    key_ref,
    value_ref,
    lo_all_ref,
    ig_all_ref,
    gbuf,
    kv_all_ref,
    stage,
    incoming,
    lsem,
    psem,
    qsem,
    rsem,
    *sems,
):
    me = lax.axis_index("gx")
    gy = lax.axis_index("gy")
    section = lax.axis_index("section")
    other = 1 - section
    gbuf[me] = gains_ref[...]
    kv_all_ref[me] = kv_ref[...]
    hello(n, me, gy, True, True)
    few = Line(n, None, lambda z: gbuf.at[z], None, sems[:4])
    many = Line(n, None, lambda z: kv_all_ref.at[z], None, sems[4:8])
    many.gather_step(0)
    few.gather_step(0)
    keeps = []
    for k, (src, dst) in enumerate(((lo_ref, lo_all_ref), (ig_ref, ig_all_ref))):
        keep = pltpu.make_async_copy(src.at[section], dst.at[section], lsem.at[k])
        give = remote(src.at[other], dst.at[section], psem.at[k], qsem.at[k], section=other)
        keep.start()
        give.start()
        keeps.append((keep, give))
    steps = [functools.partial(many.gather_step, k) for k in range(1, n)]
    for k in range(1, n):
        few.gather_step(k)
        if k == n // 2:
            steps.pop(0)()
    total = gbuf[0]
    for z in range(1, n):
        total = total + gbuf[z]
    for k, where in enumerate(({"gy": gy_flip(gy, 1)}, {"gy": gy_flip(gy, 2)}, {"section": other})):
        stage[k] = total
        swap = remote(stage.at[k], incoming.at[k], rsem.at[0, k], rsem.at[1, k], **where)
        swap.start()
        if k and steps:
            steps.pop(0)()
        swap.wait()
        total = total + incoming[k]

    @pl.when(section == 0)
    def _():
        gain_ref[...] = total[0:1]

    @pl.when(section == 1)
    def _():
        gain_ref[...] = total[1:2]

    for step in steps:
        step()
    for z in range(n):
        cols = slice(z * HD, (z + 1) * HD)
        key_ref[:, cols] = kv_all_ref[z, :, :HD].astype(F32)
        value_ref[:, cols] = kv_all_ref[z, :, HD:].astype(F32)
    for keep, give in keeps:
        keep.wait()
        give.wait()
    few.gather_drain()
    many.gather_drain()


def finish(n, gains, kv, lo, ig, cid):
    dma = pltpu.SemaphoreType.DMA
    shape = jax.ShapeDtypeStruct
    return pl.pallas_call(
        functools.partial(finish_kernel, n),
        out_shape=(
            shape((1, gains.shape[1]), F32),
            shape((kv.shape[0], n * HD), F32),
            shape((kv.shape[0], n * HD), F32),
            shape(lo.shape, BF16),
            shape(ig.shape, BF16),
        ),
        in_specs=in_vmem(4),
        out_specs=tuple(in_vmem(5)),
        scratch_shapes=[
            pltpu.VMEM((n,) + gains.shape, F32),
            pltpu.VMEM((n,) + kv.shape, BF16),
            pltpu.VMEM((3,) + gains.shape, F32),
            pltpu.VMEM((3,) + gains.shape, F32),
            dma((2,)),
            dma((2,)),
            dma((2,)),
            dma((2, 3)),
        ]
        + [dma((n,))] * 8,
        compiler_params=pltpu.CompilerParams(collective_id=cid, has_side_effects=True),
        name="finish",
    )(gains, kv, lo, ig)


class Reduce:
    def __init__(self, layer, part, inbox, xin, yin, din, sems):
        self.part, self.inbox = part, inbox
        self.xin, self.yin, self.din = xin, yin, din
        self.give_sems, self.take_sems, self.send_sems, self.recv_sems = sems
        self.section = lax.axis_index("section")
        self.mine = self.section == layer
        gy = lax.axis_index("gy")
        self.cols = [gy_flip(gy, bits) if bits else gy for bits in range(4)]
        self.few = xin.shape[0] // 2

    def give(self, k, src):
        return remote(
            src,
            self.inbox.at[self.cols[k]],
            self.give_sems.at[k],
            self.take_sems.at[k],
            section=1 - self.section,
        )

    def half(self, ref, h):
        return ref.at[pl.ds(h * self.few, self.few)]

    def far(self, bit):
        k = bit - 1
        src = self.half(self.part(self.cols[3]), k)
        return remote(
            src, self.din.at[k], self.send_sems.at[k], self.recv_sems.at[k], gy=self.cols[bit]
        )

    def near(self, bit, h):
        k = 2 * bit + h
        into = self.xin if bit == 1 else self.yin
        return remote(
            self.half(self.part(self.cols[bit]), h),
            self.half(into, h),
            self.send_sems.at[k],
            self.recv_sems.at[k],
            gy=self.cols[bit],
        )

    def send_term(self, k):
        @pl.when(self.mine)
        def _():
            ref = self.part(self.cols[k])
            self.give(k, ref).wait_recv()
            add_rows(ref, ref, self.inbox.at[self.cols[k]])
            if k == 3:
                self.far(1).start()
                self.far(2).start()
            elif k:
                self.near(k, k - 1).start()

    def pass_on(self):
        @pl.when(self.mine)
        def _():
            self.far(1).wait_recv()
            ref = self.half(self.part(self.cols[2]), 0)
            add_rows(ref, ref, self.din.at[0])
            self.near(2, 0).start()
            self.far(2).wait_recv()
            ref = self.half(self.part(self.cols[1]), 1)
            add_rows(ref, ref, self.din.at[1])
            self.near(1, 1).start()

    def close(self, outs):
        @pl.when(self.mine)
        def _():
            for bit in (1, 2):
                for h in (0, 1):
                    self.near(bit, h).wait_recv()
            for ref, first, last in outs:
                cols = slice(first, last)
                own = self.part(self.cols[0])
                add_rows(ref, own.at[:, cols], self.xin.at[:, cols], self.yin.at[:, cols])
            for bit in (1, 2):
                self.far(bit).wait_send()
                for h in (0, 1):
                    self.near(bit, h).wait_send()


def reduce_sems():
    dma = pltpu.SemaphoreType.DMA
    return [dma((4,)), dma((4,)), dma((6,)), dma((6,))]


class Line:
    def __init__(self, n, m, slot, terms, sems):
        self.n, self.m, self.slot = n, m, slot
        self.me = lax.axis_index("gx")
        if terms is not None:
            self.col, self.zup, self.zdn, self.stage = (ref.at[m] for ref in terms)
        self.sems = [sem if m is None else sem.at[m] for sem in sems]

    def gather_up(self, k):
        ref = self.slot(self.me - k)
        return remote(ref, ref, self.sems[0].at[k], self.sems[1].at[k], gx=self.me + 1)

    def gather_down(self, k):
        ref = self.slot(self.me + k)
        return remote(ref, ref, self.sems[2].at[k], self.sems[3].at[k], gx=self.me - 1)

    def gather_step(self, k):
        n, me = self.n, self.me

        @pl.when(me - k >= 0)
        def _():
            if k:
                ref = self.slot(me - k)
                sems = self.sems
                remote(ref, ref, sems[0].at[k - 1], sems[1].at[k - 1], gx=me + 1).wait_recv()
            if k < n - 1:

                @pl.when(me + 1 < n)
                def _():
                    self.gather_up(k).start()

        @pl.when(me + k < n)
        def _():
            if k:
                ref = self.slot(me + k)
                sems = self.sems
                remote(ref, ref, sems[2].at[k - 1], sems[3].at[k - 1], gx=me - 1).wait_recv()
            if k < n - 1:

                @pl.when(me > 0)
                def _():
                    self.gather_down(k).start()

    def up(self, z):
        send, recv = self.sems[4:6]
        return remote(self.stage.at[z], self.zup.at[z], send.at[z], recv.at[z], gx=self.me + 1)

    def down(self, z):
        send, recv = self.sems[6:8]
        return remote(self.stage.at[z], self.zdn.at[z], send.at[z], recv.at[z], gx=self.me - 1)

    def scatter_tick(self, hop):
        n, me = self.n, self.me

        @pl.when(me == hop)
        def _():
            for z in reversed(range(hop + 1, n)):
                if hop:
                    self.up(z).wait_recv()
                    add_rows(self.stage.at[z], self.col.at[z], self.zup.at[z])
                else:
                    add_rows(self.stage.at[z], self.col.at[z])
                self.up(z).start()

        @pl.when(me == n - 1 - hop)
        def _():
            for z in range(n - 1 - hop):
                if hop:
                    self.down(z).wait_recv()
                    add_rows(self.stage.at[z], self.col.at[z], self.zdn.at[z])
                else:
                    add_rows(self.stage.at[z], self.col.at[z])
                self.down(z).start()

    def scatter_finish(self, total):
        n, me = self.n, self.me
        add_rows(total, self.col.at[me])

        @pl.when(me > 0)
        def _():
            self.up(me).wait_recv()
            add_rows(total, total, self.zup.at[me])

        @pl.when(me < n - 1)
        def _():
            self.down(me).wait_recv()
            add_rows(total, total, self.zdn.at[me])

    def gather_drain(self):
        n, me = self.n, self.me
        for k in range(n - 1):

            @pl.when((me - k >= 0) & (me + 1 < n))
            def _():
                self.gather_up(k).wait_send()

            @pl.when((me + k < n) & (me > 0))
            def _():
                self.gather_down(k).wait_send()

    def drain(self):
        n, me = self.n, self.me
        self.gather_drain()
        for z in range(n):

            @pl.when(me < z)
            def _():
                self.up(z).wait_send()

            @pl.when(me > z)
            def _():
                self.down(z).wait_send()


def unit_of(value):
    scale = lax.rsqrt(jnp.mean(value * value, axis=-1, keepdims=True) + EPSILON)
    return value * scale, scale


def half_turn(value):
    return pltpu.roll(value, value.shape[-1] // 2, axis=value.ndim - 1)


def attn_forward_kernel(
    n,
    layer,
    heads,
    x_ref,
    gain_attn,
    gain_ffn,
    gain_query,
    gain_key,
    cos_ref,
    sin_ref,
    mask_ref,
    gates_ref,
    win_hbm,
    wout_hbm,
    *rest,
):
    count = 2 if layer == 0 else 0
    shards, rest = rest[:count], rest[count:]
    mid_ref, pay_ref, normed_hbm, proj_hbm, qr_hbm, kr_ref, v_ref, prob_hbm, mixed_hbm = rest[:9]
    fulls, rest = rest[9 : 9 + count], rest[9 + count :]
    (
    win,
    wout,
    normed,
    proj,
    qr,
    prob,
    mixed,
    col,
    zup,
    zdn,
    stage,
    total,
    wsem,
    osem,
    *sems,
    ) = rest
    mb, length, d = normed.shape
    t = length // n
    r = mb * t
    span = heads * HD
    me = lax.axis_index("gx")
    shares = [
        Share(1, shards[k], fulls[k], sems[8 + 4 * k : 12 + 4 * k]) for k in range(count)
    ]
    fetch_in = pltpu.make_async_copy(win_hbm, win, wsem.at[0])
    fetch_out = pltpu.make_async_copy(wout_hbm, wout, wsem.at[1])
    fetch_in.start()
    fetch_out.start()
    hello(n, me, lax.axis_index("gy"), count > 0, count > 0)
    for share in shares:
        share.start()
    hidden = x_ref[...].astype(F32)
    unit, _ = unit_of(hidden)
    low = (unit * gain_attn[...]).astype(BF16)
    normed[:, pl.ds(pl.multiple_of(me * t, t), t)] = low.reshape(mb, t, d)
    lines = [
        Line(
            n,
            m,
            lambda z, m=m: normed.at[m, pl.ds(z * t, t)],
            (col, zup, zdn, stage),
            sems[:8],
        )
        for m in range(mb)
    ]
    waiting = []

    def tick():
        if waiting:
            waiting.pop(0)()

    for k in range(n):
        lines[0].gather_step(k)
        if k == min(1, n - 1):
            for line in lines[1:]:
                line.gather_step(0)
    fetch_in.wait()
    cosine, sine = cos_ref[...], sin_ref[...]
    for m, line in enumerate(lines):
        first = m * length
        rows = slice(first, first + length)
        if m + 1 < mb:
            waiting += [functools.partial(lines[m + 1].gather_step, k) for k in range(1, n)]
        for j in range((span + 2 * HD) // 256):
            cols = slice(j * 256, (j + 1) * 256)
            proj[rows, cols] = jnp.dot(normed[m], win[:, cols], preferred_element_type=F32)
            if j == 2:
                tick()
        tick()
        key_unit, _ = unit_of(proj[rows, span : span + HD])
        key = key_unit * gain_key[...]
        kr_ref[rows] = (key * cosine[rows] + half_turn(key) * sine[rows]).astype(BF16)
        v_ref[rows] = proj[rows, span + HD :].astype(BF16)

        def head(h, carry, m=m, rows=rows):
            at = pl.ds(pl.multiple_of(h * HD, HD), HD)
            query_unit, _ = unit_of(proj[rows, at])
            query = query_unit * gain_query[...]
            turned = (query * cosine[rows] + half_turn(query) * sine[rows]).astype(BF16)
            qr[rows, at] = turned
            scores = dot32(turned, kr_ref[rows], COL_PAIR) * (1.0 / math.sqrt(HD))
            exponent = jnp.where(mask_ref[m] > 0.5, jnp.exp(scores), 0.0)
            p = (exponent / jnp.sum(exponent, axis=-1, keepdims=True)).astype(BF16)
            prob[m * heads + h] = p
            mixed[rows, at] = jnp.dot(p, v_ref[rows], preferred_element_type=F32).astype(BF16)
            return carry

        lax.fori_loop(0, heads // 2, head, 0, unroll=2)
        tick()
        lax.fori_loop(heads // 2, heads, head, 0, unroll=2)
        while waiting:
            tick()
        if m == 0:
            for share in shares:
                share.pass_on()
            fetch_out.wait()

        def out_cols(j, carry, m=m, rows=rows):
            at = pl.ds(pl.multiple_of(j * 256, 256), 256)
            res = dot32(mixed[rows], wout[at], COL_PAIR).astype(BF16)
            for z in range(n):
                col[m, z, :, at] = res[z * t : (z + 1) * t]
            return carry

        lax.fori_loop(0, d // 256, out_cols, 0)
        line.scatter_tick(0)
        waiting += [functools.partial(line.scatter_tick, hop) for hop in range(1, n - 1)]
    saves = [
        pltpu.make_async_copy(normed, normed_hbm, osem.at[0]),
        pltpu.make_async_copy(proj, proj_hbm, osem.at[1]),
        pltpu.make_async_copy(qr, qr_hbm, osem.at[2]),
        pltpu.make_async_copy(prob, prob_hbm, osem.at[3]),
        pltpu.make_async_copy(mixed, mixed_hbm, osem.at[4]),
    ]
    for save in saves:
        save.start()
    while waiting:
        tick()
    for m, line in enumerate(lines):
        line.scatter_finish(total.at[m * t : (m + 1) * t])
    mid = x_ref[...].astype(F32) + total[...]
    mid_ref[...] = mid
    unit, _ = unit_of(mid)
    pay_ref[:, :d] = (unit * gain_ffn[...]).astype(BF16)
    pay_ref[:, d:] = gates_ref[...]
    for share in shares:
        share.finish()
    for share in shares:
        share.drain()
    for line in lines:
        line.drain()
    for save in saves:
        save.wait()


def line_buffers(mb, n, r, d):
    return [pltpu.VMEM((mb, n, r // mb, d), BF16)] * 4 + [pltpu.VMEM((r, d), F32)]


def attn_forward(layer, n, x, gains, tables, gate_cols, w_in, w_out, shards, cid, mb):
    r, d = x.shape
    cosine, sine, mask = tables
    total_rows = cosine.shape[0]
    length = total_rows // mb
    width = w_in.shape[1]
    heads = w_out.shape[1] // HD
    span = heads * HD
    shape = jax.ShapeDtypeStruct
    return pl.pallas_call(
        functools.partial(attn_forward_kernel, n, layer, heads),
        out_shape=(
            shape((r, d), F32),
            shape((r, d + 128), BF16),
            shape((mb, length, d), BF16),
            shape((total_rows, width), F32),
            shape((total_rows, span), BF16),
            shape((total_rows, HD), BF16),
            shape((total_rows, HD), BF16),
            shape((mb * heads, length, length), BF16),
            shape((total_rows, span), BF16),
            *(shape((4 * w.shape[0], w.shape[1]), BF16) for w in shards),
        ),
        in_specs=in_vmem(9) + in_place(2 + len(shards)),
        out_specs=tuple(in_vmem(2) + in_place(3) + in_vmem(2) + in_place(2 + len(shards))),
        scratch_shapes=[
            pltpu.VMEM((d, width), BF16),
            pltpu.VMEM((d, span), BF16),
            pltpu.VMEM((mb, length, d), BF16),
            pltpu.VMEM((total_rows, width), F32),
            pltpu.VMEM((total_rows, span), BF16),
            pltpu.VMEM((mb * heads, length, length), BF16),
            pltpu.VMEM((total_rows, span), BF16),
        ]
        + line_buffers(mb, n, r, d)
        + [pltpu.SemaphoreType.DMA((2,)), pltpu.SemaphoreType.DMA((5,))]
        + [pltpu.SemaphoreType.DMA((mb, n))] * 8
        + [item for shard in shards for item in share_scratch(shard)],
        compiler_params=pltpu.CompilerParams(
            collective_id=cid, has_side_effects=True, vmem_limit_bytes=60 << 20
        ),
        name="attn_forward",
    )(x, *gains, cosine, sine, mask, gate_cols, w_in, w_out, *shards)


def attn_backward_kernel(
    n,
    layer,
    heads,
    dmid_ref,
    x_ref,
    gain_attn,
    gain_query,
    gain_key,
    cos_ref,
    sin_ref,
    kr_ref,
    v_ref,
    normed_hbm,
    proj_hbm,
    qr_hbm,
    prob_hbm,
    mixed_hbm,
    win_hbm,
    wout_hbm,
    *rest,
):
    last = layer == 0
    if last:
        later_hbm, gives, rest = rest[0], rest[1:4], rest[4:]
    cot_ref, dgain_attn, dgain_query, dgain_key = rest[:4]
    outs, rest = rest[4 : 10 if last else 5], rest[10 if last else 5 :]
    (
    win,
    wout,
    normed,
    proj,
    qr,
    prob,
    mixed,
    dmids,
    dheads,
    dproj,
    dkey,
    dvalue,
    grads,
    col,
    zup,
    zdn,
    stage,
    total,
    wsem,
    isem,
    osem,
    *sems,
    ) = rest
    mb, length, d = normed.shape
    t = length // n
    span = heads * HD
    me = lax.axis_index("gx")
    inv_root = 1.0 / math.sqrt(HD)
    gy = lax.axis_index("gy")
    section = lax.axis_index("section")
    fetch_out = pltpu.make_async_copy(wout_hbm, wout, wsem.at[0])
    fetch_in = pltpu.make_async_copy(win_hbm, win, wsem.at[1])
    fetch_out.start()
    fetch_in.start()
    loads = [
        pltpu.make_async_copy(prob_hbm, prob, isem.at[0]),
        pltpu.make_async_copy(mixed_hbm, mixed, isem.at[1]),
        pltpu.make_async_copy(qr_hbm, qr, isem.at[2]),
        pltpu.make_async_copy(proj_hbm, proj, isem.at[3]),
        pltpu.make_async_copy(normed_hbm, normed, isem.at[4]),
    ]
    for load in loads:
        load.start()
    if last:
        later, inbox, xin, yin, din = sems[8:13]
        block = d // 4
        job_later = Reduce(
            1, lambda c: later.at[pl.ds(c * block, block)], inbox, xin, yin, din, sems[13:17]
        )
        job = Reduce(
            0, lambda c: grads.at[pl.ds(c * block, block)], inbox, xin, yin, din, sems[17:21]
        )
        swaps = [
            remote(gives[k], outs[3 + k], sems[21].at[k], sems[22].at[k], section=1 - section)
            for k in range(3)
        ]
        load_later = pltpu.make_async_copy(later_hbm, later, osem.at[0])

        @pl.when(job_later.mine)
        def _():
            load_later.start()

        hello(n, me, gy, True, True)

        @pl.when(jnp.logical_not(job_later.mine))
        def _():
            for k in (3, 1, 2, 0):
                c = job_later.cols[k]
                job_later.give(k, later_hbm.at[pl.ds(c * block, block)]).start()

        for swap in swaps:
            swap.start()
    else:
        hello(n, me, None, False)
    dmids[:, pl.ds(pl.multiple_of(me * t, t), t)] = dmid_ref[...].astype(BF16).reshape(mb, t, d)
    lines = [
        Line(
            n,
            m,
            lambda z, m=m: dmids.at[m, pl.ds(z * t, t)],
            (col, zup, zdn, stage),
            sems[:8],
        )
        for m in range(mb)
    ]
    waiting = []
    sums = []

    def tick():
        if waiting:
            waiting.pop(0)()
        if sums:
            sums.pop(0)()

    for k in range(n):
        lines[0].gather_step(k)
        if k == min(1, n - 1):
            for line in lines[1:]:
                line.gather_step(0)
    if last:

        @pl.when(job_later.mine)
        def _():
            load_later.wait()

        sums += [functools.partial(job_later.send_term, k) for k in (3, 1, 2, 0)]
        sums += [job_later.pass_on]
    tick()
    fetch_out.wait()
    for load in loads:
        load.wait()
    cosine, sine = cos_ref[...], sin_ref[...]
    dkey[...] = jnp.zeros_like(dkey)
    dvalue[...] = jnp.zeros_like(dvalue)
    dgain_query[...] = jnp.zeros_like(dgain_query)
    dgain_key[...] = jnp.zeros_like(dgain_key)
    for m, line in enumerate(lines):
        first = m * length
        rows = slice(first, first + length)
        if m + 1 < mb:
            waiting += [functools.partial(lines[m + 1].gather_step, k) for k in range(1, n)]
        for j in range(span // 256):
            cols = slice(j * 256, (j + 1) * 256)
            dheads[rows, cols] = jnp.dot(
                dmids[m], wout[:, cols], preferred_element_type=F32
            ).astype(BF16)
        tick()

        def head(h, carry, m=m, rows=rows):
            at = pl.ds(pl.multiple_of(h * HD, HD), HD)
            p = prob[m * heads + h]
            dh = dheads[rows, at]
            dvalue[rows] += dot32(p, dh, ROW_PAIR)
            dp = dot32(dh, v_ref[rows], COL_PAIR)
            delta = jnp.sum(
                dh.astype(F32) * mixed[rows, at].astype(F32), axis=-1, keepdims=True
            )
            ds = (p.astype(F32) * (dp - delta)).astype(BF16)
            dkey[rows] += dot32(ds, qr[rows, at], ROW_PAIR) * inv_root
            dq = jnp.dot(ds, kr_ref[rows], preferred_element_type=F32) * inv_root
            turned = dq * cosine[rows] - half_turn(dq) * sine[rows]
            unit, scale = unit_of(proj[rows, at])
            dgain_query[...] += jnp.sum(turned * unit, axis=0, keepdims=True)
            dproj[rows, at] = norm_back(turned * gain_query[...], unit, scale).astype(BF16)
            return carry

        lax.fori_loop(0, heads // 2, head, 0, unroll=2)
        tick()
        lax.fori_loop(heads // 2, heads, head, 0, unroll=2)
        tick()
        dk = dkey[rows]
        turned = dk * cosine[rows] - half_turn(dk) * sine[rows]
        unit, scale = unit_of(proj[rows, span : span + HD])
        dgain_key[...] += jnp.sum(turned * unit, axis=0, keepdims=True)
        dproj[rows, span : span + HD] = norm_back(turned * gain_key[...], unit, scale).astype(BF16)
        dproj[rows, span + HD :] = dvalue[rows].astype(BF16)
        if m == 0:
            fetch_in.wait()
        while waiting:
            tick()

        def in_cols(j, carry, m=m, rows=rows):
            at = pl.ds(pl.multiple_of(j * 256, 256), 256)
            res = dot32(dproj[rows], win[at], COL_PAIR).astype(BF16)
            for z in range(n):
                col[m, z, :, at] = res[z * t : (z + 1) * t]
            return carry

        lax.fori_loop(0, d // 256, in_cols, 0)
        line.scatter_tick(0)
        waiting += [functools.partial(line.scatter_tick, hop) for hop in range(1, n - 1)]
    while sums:
        sums.pop(0)()

    def weight_grads(c):
        def chunk(i, carry):
            at = pl.ds(pl.multiple_of(c * (d // 4) + i * 256, 256), 256)
            left = normed[:, :, at].reshape(mb * length, 256)
            grads[at, : span + 2 * HD] = dot32(left, dproj[...], ROW_PAIR).astype(BF16)
            left = dmids[:, :, at].reshape(mb * length, 256)
            grads[at, span + 2 * HD :] = dot32(left, mixed[...], ROW_PAIR).astype(BF16)
            return carry

        lax.fori_loop(0, d // 4 // 256, chunk, 0)

    for bits in (3, 1, 2, 0):
        c = gy_flip(gy, bits)
        weight_grads(c)
        if last:

            @pl.when(jnp.logical_not(job.mine))
            def _():
                job.give(bits, job.part(c)).start()

        tick()
    while waiting:
        tick()
    if last:
        for k in (3, 1, 2, 0):
            job.send_term(k)
    else:
        save = pltpu.make_async_copy(grads, outs[0], osem.at[0])
        save.start()
    for m, line in enumerate(lines):
        line.scatter_finish(total.at[m * t : (m + 1) * t])
    hidden = x_ref[...].astype(F32)
    unit, scale = unit_of(hidden)
    da = total[...]
    dgain_attn[...] = jnp.sum(da * unit, axis=0, keepdims=True)
    cot_ref[...] = (dmid_ref[...] + norm_back(da * gain_attn[...], unit, scale)).astype(BF16)
    for line in lines:
        line.drain()
    if not last:
        save.wait()
        return
    job.pass_on()
    closing = [(outs[0], 0, span), (outs[1], span, span + 2 * HD), (outs[2], span + 2 * HD, None)]
    job_later.close(closing)
    job.close(closing)
    for swap in swaps:
        swap.wait()

    @pl.when(jnp.logical_not(job.mine))
    def _():
        for k in range(4):
            job.give(k, job.part(job.cols[k])).wait_send()

    @pl.when(jnp.logical_not(job_later.mine))
    def _():
        for k in range(4):
            c = job_later.cols[k]
            job_later.give(k, later_hbm.at[pl.ds(c * block, block)]).wait_send()


def attn_backward(layer, n, dmid, x, gains, tables, kept, w_in, w_out, later, gives, cid, mb):
    r, d = x.shape
    cosine, sine, _ = tables
    normed, proj, qr, kr, v, prob, mixed = kept
    total_rows = cosine.shape[0]
    length = total_rows // mb
    width = w_in.shape[1]
    heads = w_out.shape[1] // HD
    span = heads * HD
    shape = jax.ShapeDtypeStruct
    both = width + span
    grad_shapes = [shape((d, both), BF16)]
    extra = []
    if later:
        block = d // 4
        grad_shapes = [
            shape((block, span), F32),
            shape((block, 2 * HD), BF16),
            shape((block, span), F32),
            *(shape(piece.shape, BF16) for piece in gives),
        ]
        extra = [
            pltpu.VMEM((d, both), BF16),
            pltpu.VMEM((4, block, both), BF16),
            pltpu.VMEM((block, both), BF16),
            pltpu.VMEM((block, both), BF16),
            pltpu.VMEM((2, block // 2, both), BF16),
        ] + reduce_sems() * 2 + [pltpu.SemaphoreType.DMA((3,))] * 2
    return pl.pallas_call(
        functools.partial(attn_backward_kernel, n, layer, heads),
        out_shape=(
            shape((r, d), BF16),
            shape((1, d), F32),
            shape((1, HD), F32),
            shape((1, HD), F32),
            *grad_shapes,
        ),
        in_specs=in_vmem(9) + in_place(7 + len(later) + len(gives)),
        out_specs=tuple(in_vmem(4) + (in_vmem(3) + in_place(3) if later else in_place(1))),
        scratch_shapes=[
            pltpu.VMEM((d, width), BF16),
            pltpu.VMEM((d, span), BF16),
            pltpu.VMEM((mb, length, d), BF16),
            pltpu.VMEM((total_rows, width), F32),
            pltpu.VMEM((total_rows, span), BF16),
            pltpu.VMEM((mb * heads, length, length), BF16),
            pltpu.VMEM((total_rows, span), BF16),
            pltpu.VMEM((mb, length, d), BF16),
            pltpu.VMEM((total_rows, span), BF16),
            pltpu.VMEM((total_rows, width), BF16),
            pltpu.VMEM((total_rows, HD), F32),
            pltpu.VMEM((total_rows, HD), F32),
            pltpu.VMEM((d, both), BF16),
        ]
        + line_buffers(mb, n, r, d)
        + [
            pltpu.SemaphoreType.DMA((2,)),
            pltpu.SemaphoreType.DMA((5,)),
            pltpu.SemaphoreType.DMA((1,)),
        ]
        + [pltpu.SemaphoreType.DMA((mb, n))] * 8
        + extra,
        compiler_params=pltpu.CompilerParams(
            collective_id=cid, has_side_effects=True, vmem_limit_bytes=63 << 20
        ),
        name="attn_backward",
    )(
        dmid,
        x,
        *gains,
        cosine,
        sine,
        kr,
        v,
        normed,
        proj,
        qr,
        prob,
        mixed,
        w_in,
        w_out,
        *later,
        *gives,
    )


def local_wide(
    inputs,
    out_grad,
    segments,
    routes,
    gates,
    gain_attn,
    gain_ffn,
    gain_query,
    gain_key,
    w_query,
    w_key,
    w_value,
    w_out,
    w_gate,
    w_up,
    w_down,
):
    micro_count, _, local_rows, width = inputs.shape
    n_sec = lax.axis_size("section")
    n_gx = lax.axis_size("gx")
    n_gy = lax.axis_size("gy")
    heads = w_query.shape[2] // HD
    span = heads * HD
    experts = n_gx * n_gy
    group_len = segments.shape[2]
    mb = micro_count // n_sec
    rows_own = mb * local_rows
    rows_attn = mb * group_len
    section = lax.axis_index("section")
    gx = lax.axis_index("gx")
    gy = lax.axis_index("gy")
    expert_own = gx * n_gy + gy
    inv_root = 1.0 / math.sqrt(HD)
    first = section * mb

    kv_head = gx * heads // (HQ // KVH)
    key_own = lax.dynamic_slice_in_dim(w_key[0], kv_head * HD, HD, 1)
    value_own = lax.dynamic_slice_in_dim(w_value[0], kv_head * HD, HD, 1)
    w_in_shard = jnp.concatenate([w_query[0], key_own, value_own], axis=1)
    w_in_all = both_layers(lax.all_gather(w_in_shard, "gy", axis=0, tiled=True))
    w_out_all = both_layers(lax.all_gather(w_out[0], "gy", axis=0, tiled=True))
    w_gate_all = both_layers(w_gate[0, 0])
    w_up_all = both_layers(w_up[0, 0])
    w_down_all = both_layers(w_down[0, 0])
    table = dense_gates(routes[0, :, 0], gates[0, :, 0], experts)
    small = jnp.concatenate(
        [
            table.reshape(-1),
            gain_attn[0],
            gain_ffn[0],
            gain_query[0],
            gain_key[0],
        ]
    )
    small_all = both_layers(small)
    table_size = micro_count * local_rows * experts
    table_all = small_all[:, :table_size].reshape(n_sec, micro_count, local_rows, experts)
    gains_all = small_all[:, table_size:]

    table_mine = lax.dynamic_slice_in_dim(table_all, first, mb, 1).reshape(
        n_sec, rows_own, experts
    )
    x_mine = lax.dynamic_slice_in_dim(inputs[:, 0], first, mb, 0).reshape(rows_own, width)
    cot_mine = lax.dynamic_slice_in_dim(out_grad[:, 0], first, mb, 0).reshape(rows_own, width)
    segs = lax.dynamic_slice_in_dim(segments[:, 0], first, mb, 0)
    allowed, cosine, sine = seq_tables(segs, HD)
    cos_q = cosine.reshape(rows_attn, 1, HD // 2)
    sin_q = sine.reshape(rows_attn, 1, HD // 2)
    cos_k = cosine.reshape(rows_attn, HD // 2)
    sin_k = sine.reshape(rows_attn, HD // 2)

    def split_gains(layer):
        g = gains_all[layer]
        return (
            g[:width],
            g[width : 2 * width],
            g[2 * width : 2 * width + HD],
            g[2 * width + HD :],
        )

    saved_all = []
    outs = []
    layer_in = x_mine
    for layer in range(n_sec):
        g_attn, g_ffn, g_query, g_key = split_gains(layer)
        hidden = layer_in.astype(F32)
        attn_unit, attn_scale = normalize(hidden)
        normed = (attn_unit * g_attn).astype(BF16)
        normed_all = gather_z(normed.reshape(mb, local_rows, width)).reshape(rows_attn, width)
        projected = dot32(normed_all, w_in_all[layer])
        query = projected[:, :span].reshape(rows_attn, heads, HD)
        key = projected[:, span : span + HD]
        value_low = projected[:, span + HD :].astype(BF16).reshape(mb, group_len, HD)
        query_unit, query_scale = normalize(query)
        key_unit, key_scale = normalize(key)
        query_rope = (
            rotate(query_unit * g_query, cos_q, sin_q)
            .astype(BF16)
            .reshape(mb, group_len, heads, HD)
        )
        key_rope = rotate(key_unit * g_key, cos_k, sin_k).astype(BF16).reshape(mb, group_len, HD)
        scores = (
            jnp.einsum("mthd,msd->mhts", query_rope, key_rope, preferred_element_type=F32)
            * inv_root
        )
        exponent = jnp.where(allowed[:, None], jnp.exp(scores), 0.0)
        log_total = jnp.log(jnp.sum(exponent, axis=-1, keepdims=True))
        prob = jnp.where(allowed[:, None], jnp.exp(scores - log_total), 0.0)
        mixed = (
            jnp.einsum("mhts,msd->mthd", prob.astype(BF16), value_low, preferred_element_type=F32)
            .astype(BF16)
            .reshape(rows_attn, span)
        )
        attn_part = dot32(mixed, w_out_all[layer], COL_PAIR).astype(BF16)
        attn_out = scatter_z(attn_part.reshape(mb, group_len, width)).reshape(rows_own, width)
        middle = hidden + attn_out.astype(F32)
        ffn_unit, ffn_scale = normalize(middle)
        expert_in = (ffn_unit * g_ffn).astype(BF16)
        tab = table_mine[layer]
        tab_hi = tab.astype(BF16)
        tab_lo = (tab - tab_hi.astype(F32)).astype(BF16)
        payload = jnp.concatenate([expert_in, tab_hi, tab_lo], axis=1)
        arrived_all = gather_all(payload)
        arrived = arrived_all[:, :width]
        gate_cols = arrived_all[:, width:].astype(F32)
        is_mine = jnp.arange(2 * experts) % experts == expert_own
        weight = jnp.sum(jnp.where(is_mine[None], gate_cols, 0.0), axis=1, keepdims=True)
        gate_pre = dot32(arrived, w_gate_all[layer])
        up_proj = dot32(arrived, w_up_all[layer])
        inner = (jax.nn.silu(gate_pre) * up_proj).astype(BF16)
        result = dot32(inner, w_down_all[layer])
        weighted = (result * weight).astype(BF16)
        expert_sum = scatter_all(weighted)
        layer_out = (middle + expert_sum.astype(F32)).astype(BF16)
        outs.append(layer_out)
        layer_in = layer_out
        saved_all.append(
            (
                attn_unit,
                attn_scale,
                normed_all,
                query_unit,
                query_scale,
                key_unit,
                key_scale,
                query_rope,
                key_rope,
                value_low,
                prob,
                mixed,
                ffn_unit,
                ffn_scale,
                arrived,
                weight,
                gate_pre,
                up_proj,
                inner,
            )
        )

    cot = cot_mine
    in_grads = [None] * n_sec
    expert_grads = [None] * n_sec
    attn_grads = [None] * n_sec
    gain_grads = [None] * n_sec
    for layer in reversed(range(n_sec)):
        g_attn, g_ffn, g_query, g_key = split_gains(layer)
        (
            attn_unit,
            attn_scale,
            normed_all,
            query_unit,
            query_scale,
            key_unit,
            key_scale,
            query_rope,
            key_rope,
            value_low,
            prob,
            mixed,
            ffn_unit,
            ffn_scale,
            arrived,
            weight,
            gate_pre,
            up_proj,
            inner,
        ) = saved_all[layer]
        gradient = cot.astype(F32)
        grad_all = gather_all(cot)
        grad_result = (grad_all.astype(F32) * weight).astype(BF16)
        grad_inner = dot32(grad_result, w_down_all[layer], COL_PAIR)
        grad_down = dot32(inner, grad_result, ROW_PAIR)
        sig = jax.nn.sigmoid(gate_pre)
        grad_gate_pre = (grad_inner * up_proj * sig * (1.0 + gate_pre * (1.0 - sig))).astype(BF16)
        grad_up_proj = (grad_inner * gate_pre * sig).astype(BF16)
        grad_gate = dot32(arrived, grad_gate_pre, ROW_PAIR)
        grad_up = dot32(arrived, grad_up_proj, ROW_PAIR)
        grad_arrived = (
            dot32(grad_gate_pre, w_gate_all[layer], COL_PAIR)
            + dot32(grad_up_proj, w_up_all[layer], COL_PAIR)
        ).astype(BF16)
        expert_grads[layer] = (grad_gate, grad_up, grad_down)
        grad_expert_in = scatter_all(grad_arrived).astype(F32)
        grad_ffn_gain = jnp.sum(grad_expert_in * ffn_unit, axis=0)
        grad_middle = gradient + norm_back(grad_expert_in * g_ffn, ffn_unit, ffn_scale)
        middle_low = grad_middle.astype(BF16)
        middle_all = gather_z(middle_low.reshape(mb, local_rows, width)).reshape(rows_attn, width)
        grad_out_w = dot32(middle_all, mixed, ROW_PAIR)
        grad_heads = (
            dot32(middle_all, w_out_all[layer]).astype(BF16).reshape(mb, group_len, heads, HD)
        )
        grad_value = jnp.einsum(
            "mhts,mthd->mshd", prob.astype(BF16), grad_heads, preferred_element_type=F32
        )
        grad_prob = jnp.einsum(
            "mthd,msd->mhts", grad_heads, value_low, preferred_element_type=F32
        )
        mixed_split = mixed.reshape(mb, group_len, heads, HD)
        delta = jnp.sum(grad_heads.astype(F32) * mixed_split.astype(F32), axis=-1)
        delta = jnp.swapaxes(delta, 1, 2)[..., None]
        grad_scores = (prob * (grad_prob - delta)).astype(BF16)
        grad_query = (
            jnp.einsum("mhts,msd->mthd", grad_scores, key_rope, preferred_element_type=F32)
            * inv_root
        ).reshape(rows_attn, heads, HD)
        grad_key = (
            jnp.einsum("mhts,mthd->mshd", grad_scores, query_rope, preferred_element_type=F32)
            * inv_root
        ).reshape(rows_attn, heads, HD)
        query_turn = rotate_back(grad_query, cos_q, sin_q)
        grad_query_gain = jnp.sum(query_turn * query_unit, axis=(0, 1))
        grad_query_pre = norm_back(query_turn * g_query, query_unit, query_scale)
        key_turn = rotate_back(jnp.sum(grad_key, axis=1), cos_k, sin_k)
        grad_key_gain = jnp.sum(key_turn * key_unit, axis=0)
        grad_key_pre = norm_back(key_turn * g_key, key_unit, key_scale)
        grad_proj = jnp.concatenate(
            [
                grad_query_pre.reshape(rows_attn, span),
                grad_key_pre,
                jnp.sum(grad_value, axis=2).reshape(rows_attn, HD),
            ],
            axis=1,
        ).astype(BF16)
        grad_in_w = dot32(normed_all, grad_proj, ROW_PAIR)
        normed_part = dot32(grad_proj, w_in_all[layer], COL_PAIR).astype(BF16)
        grad_normed = (
            scatter_z(normed_part.reshape(mb, group_len, width))
            .reshape(rows_own, width)
            .astype(F32)
        )
        grad_attn_gain = jnp.sum(grad_normed * attn_unit, axis=0)
        cot = (grad_middle + norm_back(grad_normed * g_attn, attn_unit, attn_scale)).astype(BF16)
        in_grads[layer] = cot
        attn_grads[layer] = jnp.concatenate([grad_in_w, grad_out_w], axis=1).astype(BF16)
        gain_grads[layer] = jnp.concatenate(
            [grad_attn_gain, grad_ffn_gain, grad_query_gain, grad_key_gain]
        )

    def own_layer_sum(pieces):
        return lax.psum_scatter(
            jnp.stack([piece.astype(BF16) for piece in pieces]),
            "section",
            scatter_dimension=0,
            tiled=True,
        ).astype(F32)

    grad_gate, grad_up, grad_down = (
        own_layer_sum([expert_grads[layer][k] for layer in range(n_sec)]) for k in range(3)
    )
    attn_sum = lax.psum_scatter(
        jnp.concatenate(attn_grads, axis=0), ("section", "gy"), scatter_dimension=0, tiled=True
    ).astype(F32)
    query_grad = attn_sum[:, :span]
    out_w_grad = attn_sum[:, span + 2 * HD :]
    kv_all = lax.all_gather(attn_sum[:, span : span + 2 * HD], "gx", axis=0, tiled=False)
    kv_all = jnp.sum(kv_all.reshape(KVH, n_gx // KVH, -1, 2, HD), axis=1)
    key_part = jnp.swapaxes(kv_all[:, :, 0], 0, 1).reshape(-1, KVH * HD)
    value_part = jnp.swapaxes(kv_all[:, :, 1], 0, 1).reshape(-1, KVH * HD)
    gain_sum = lax.psum(jnp.stack(gain_grads), ("section", "gx", "gy"))
    gain_sum = lax.dynamic_index_in_dim(gain_sum, section, 0, keepdims=True)

    def own_layer_rows(pieces):
        stacked = jnp.stack(pieces).reshape(n_sec, mb, local_rows, width)
        return lax.all_to_all(stacked, "section", split_axis=0, concat_axis=0, tiled=True).reshape(
            1, micro_count, 1, local_rows, width
        )

    return (
        own_layer_rows(outs),
        own_layer_rows(in_grads),
        gain_sum[:, :width],
        gain_sum[:, width : 2 * width],
        gain_sum[:, 2 * width : 2 * width + HD],
        gain_sum[:, 2 * width + HD :],
        query_grad[None],
        key_part[None],
        value_part[None],
        out_w_grad[None],
        grad_gate[:, None],
        grad_up[:, None],
        grad_down[:, None],
    )


def local_fused(
    inputs,
    out_grad,
    segments,
    routes,
    gates,
    gain_attn,
    gain_ffn,
    gain_query,
    gain_key,
    w_query,
    w_key,
    w_value,
    w_out,
    w_gate,
    w_up,
    w_down,
):
    micro_count, _, local_rows, width = inputs.shape
    n_sec = lax.axis_size("section")
    n_gx = lax.axis_size("gx")
    n_gy = lax.axis_size("gy")
    heads = w_query.shape[2] // HD
    span = heads * HD
    experts = n_gx * n_gy
    group_len = segments.shape[2]
    mb = micro_count // n_sec
    rows_own = mb * local_rows
    rows_attn = mb * group_len
    section = lax.axis_index("section")
    gx = lax.axis_index("gx")
    first = section * mb

    kv_head = gx * heads // (HQ // KVH)
    key_own = lax.dynamic_slice_in_dim(w_key[0], kv_head * HD, HD, 1)
    value_own = lax.dynamic_slice_in_dim(w_value[0], kv_head * HD, HD, 1)
    w_in_shard = jnp.concatenate([w_query[0], key_own, value_own], axis=1)
    attn_shards = (w_in_shard, w_out[0])
    attn_all = [share_weights(0, n_gx, attn_shards, 9)]
    moe_own = (w_gate[0, 0], w_up[0, 0], w_down[0, 0])
    moe_other = tuple(swap_sections(w) for w in moe_own)
    table = dense_gates(routes[0, :, 0], gates[0, :, 0], experts)
    small = jnp.concatenate(
        [table.reshape(-1), gain_attn[0], gain_ffn[0], gain_query[0], gain_key[0]]
    )
    small_other = swap_sections(small)
    is_first = section == 0
    small_all = jnp.stack(
        [jnp.where(is_first, small, small_other), jnp.where(is_first, small_other, small)]
    )
    table_size = micro_count * local_rows * experts
    table_all = small_all[:, :table_size].reshape(n_sec, micro_count, local_rows, experts)
    gains_all = small_all[:, table_size:]
    table_mine = lax.dynamic_slice_in_dim(table_all, first, mb, 1).reshape(
        n_sec, rows_own, experts
    )
    x_mine = lax.dynamic_slice_in_dim(inputs[:, 0], first, mb, 0).reshape(rows_own, width)
    cot = lax.dynamic_slice_in_dim(out_grad[:, 0], first, mb, 0).reshape(rows_own, width)
    segs = lax.dynamic_slice_in_dim(segments[:, 0], first, mb, 0)
    allowed, cosine, sine = seq_tables(segs, HD)
    tables = (
        jnp.concatenate([cosine, cosine], axis=-1).reshape(rows_attn, HD),
        jnp.concatenate([-sine, sine], axis=-1).reshape(rows_attn, HD),
        allowed.astype(F32),
    )

    def split_gains(layer):
        g = gains_all[layer : layer + 1]
        return (
            g[:, :width],
            g[:, width : 2 * width],
            g[:, 2 * width : 2 * width + HD],
            g[:, 2 * width + HD :],
        )

    kept = []
    outs = []
    layer_in = x_mine
    for layer in range(n_sec):
        tab = table_mine[layer]
        tab_hi = tab.astype(BF16)
        tab_lo = (tab - tab_hi.astype(F32)).astype(BF16)
        pad = jnp.zeros((rows_own, 128 - 2 * experts), BF16)
        gate_cols = jnp.concatenate([tab_hi, tab_lo, pad], axis=1)
        mid, payload, normed, proj, qr, kr, v, prob, mixed, *next_all = attn_forward(
            layer,
            n_gx,
            layer_in,
            split_gains(layer),
            tables,
            gate_cols,
            *attn_all[layer],
            attn_shards if layer == 0 else (),
            1 + layer,
            mb,
        )
        attn_all.append(next_all)
        layer_out, *moe_kept = moe_forward(
            layer, n_gx, mid, payload, moe_own, moe_other, 3 + layer
        )
        kept.append((layer_in, mid, (normed, proj, qr, kr, v, prob, mixed), moe_kept))
        outs.append(layer_out)
        layer_in = layer_out

    in_grads = [None] * n_sec
    moe_sums = ()
    later = ()
    gain_grads = [None] * n_sec
    for layer in reversed(range(n_sec)):
        g_attn, g_ffn, g_query, g_key = split_gains(layer)
        layer_in, mid, attn_kept, (arrived, weight, gp, up, inner) = kept[layer]
        dmid, d_ffn, *moe_sums = moe_backward(
            layer,
            n_gx,
            cot,
            mid,
            g_ffn,
            weight,
            arrived,
            gp,
            up,
            inner,
            moe_own,
            moe_other,
            moe_sums,
            5 + layer,
        )
        cot, d_attn, d_query, d_key, *later = attn_backward(
            layer,
            n_gx,
            dmid,
            layer_in,
            (g_attn, g_query, g_key),
            tables,
            attn_kept,
            *attn_all[layer],
            later,
            moe_sums[3:] if layer == 0 else (),
            7 + layer,
            mb,
        )
        in_grads[layer] = cot
        gain_grads[layer] = jnp.concatenate([d_attn, d_ffn, d_query, d_key], axis=1)

    query_grad, kv_shard, out_grad_w, *from_other = later
    grad_gate, grad_up, grad_down = (
        (moe_sums[k].astype(F32) + from_other[k].astype(F32))[None] for k in range(3)
    )
    gain_sum, key_part, value_part, out_rows, grad_rows = finish(
        n_gx,
        jnp.concatenate(gain_grads[::1], axis=0),
        kv_shard,
        jnp.stack(outs),
        jnp.stack(in_grads),
        10,
    )
    whole_rows = (1, micro_count, 1, local_rows, width)

    return (
        out_rows.reshape(whole_rows),
        grad_rows.reshape(whole_rows),
        gain_sum[:, :width],
        gain_sum[:, width : 2 * width],
        gain_sum[:, 2 * width : 2 * width + HD],
        gain_sum[:, 2 * width + HD :],
        query_grad[None],
        key_part[None],
        value_part[None],
        out_grad_w[None],
        grad_gate[:, None],
        grad_up[:, None],
        grad_down[:, None],
    )


def local(*args):
    inputs = args[0]
    n = lax.axis_size("gx")
    rows_own = inputs.shape[0] // lax.axis_size("section") * inputs.shape[2]
    if 4 * n * rows_own > MOST_ROWS or n != KVH:
        return local_wide(*args)
    return local_fused(*args)


def solution(mesh):
    return jax.shard_map(
        local,
        mesh=mesh,
        in_specs=(
            P(None, "gy", "gx", None),
            P(None, "gy", "gx", None),
            P(None, "gy", None),
            P("section", None, "gy", "gx", None),
            P("section", None, "gy", "gx", None),
            P("section", None),
            P("section", None),
            P("section", None),
            P("section", None),
            P("section", "gy", "gx"),
            P("section", "gy", None),
            P("section", "gy", None),
            P("section", "gy", "gx"),
            P("section", ("gx", "gy"), None, None),
            P("section", ("gx", "gy"), None, None),
            P("section", ("gx", "gy"), None, None),
        ),
        out_specs=(
            P("section", None, "gy", "gx", None),
            P("section", None, "gy", "gx", None),
            P("section", None),
            P("section", None),
            P("section", None),
            P("section", None),
            P("section", "gy", "gx"),
            P("section", "gy", None),
            P("section", "gy", None),
            P("section", "gy", "gx"),
            P("section", ("gx", "gy"), None, None),
            P("section", ("gx", "gy"), None, None),
            P("section", ("gx", "gy"), None, None),
        ),
        check_vma=False,
    )
```

```python
import functools
import math

import jax
import jax.numpy as jnp
from jax import lax
from jax.experimental import pallas as pl
from jax.experimental.pallas import tpu as pltpu
from jax.sharding import PartitionSpec as P

HQ = 32
KVH = 4
HD = 128
TOPK = 8

EPSILON = 1e-06
ROPE_BASE = 1000000.0
ROW_PAIR = (((0,), (0,)), ((), ()))
COL_PAIR = (((1,), (1,)), ((), ()))
F32 = jnp.float32
BF16 = jnp.bfloat16
MOST_ROWS = 1024


def normalize(tensor):
    scaling = lax.rsqrt(jnp.mean(tensor * tensor, axis=-1, keepdims=True) + EPSILON)
    return (tensor * scaling, scaling)


def norm_back(gradient, unit_vec, scaling):
    return scaling * (gradient - unit_vec * jnp.mean(gradient * unit_vec, axis=-1, keepdims=True))


def rotate(tensor, cosine, sine_part):
    halfway = tensor.shape[-1] // 2
    leading = tensor[..., :halfway]
    trailing = tensor[..., halfway:]
    return jnp.concatenate(
        [leading * cosine - trailing * sine_part, trailing * cosine + leading * sine_part], axis=-1
    )


def rotate_back(gradient, cosine, sine_part):
    return rotate(gradient, cosine, -sine_part)


def seq_tables(segment_ids, head_dim):
    length_all = segment_ids.shape[-1]
    position_ids = jnp.arange(length_all, dtype=jnp.int32)
    allowed = (segment_ids[:, :, None] == segment_ids[:, None, :]) & (
        position_ids[:, None] >= position_ids[None, :]
    )
    positions = jnp.sum(allowed.astype(jnp.int32), axis=-1) - 1
    halfway = head_dim // 2
    inverse = ROPE_BASE ** (-2.0 * jnp.arange(halfway, dtype=jnp.float32) / head_dim)
    angles = positions.astype(jnp.float32)[..., None] * inverse
    return (allowed, jnp.cos(angles), jnp.sin(angles))


def dot32(left, right, dims=None):
    if dims is None:
        return jnp.dot(left, right, preferred_element_type=F32)
    return lax.dot_general(left, right, dims, preferred_element_type=F32)


def gather_z(rows):
    return lax.all_gather(rows, "gx", axis=1, tiled=True)


def scatter_z(rows):
    return lax.psum_scatter(rows, "gx", scatter_dimension=1, tiled=True)


def gather_all(rows):
    return lax.all_gather(rows, ("gx", "gy"), axis=0, tiled=True)


def scatter_all(rows):
    return lax.psum_scatter(rows, ("gx", "gy"), scatter_dimension=0, tiled=True)


def both_layers(tensor):
    return lax.all_gather(tensor, "section", axis=0, tiled=False)


def dense_gates(route_ids, gate_vals, experts):
    onehot = route_ids[..., None] == jnp.arange(experts, dtype=jnp.int32)
    return jnp.sum(jnp.where(onehot, gate_vals[..., None], 0.0), axis=-2)


def swap_sections(tensor):
    return lax.ppermute(tensor, "section", [(0, 1), (1, 0)])


def remote(src, dst, send_sem, recv_sem, **where):
    return pltpu.make_async_remote_copy(
        src_ref=src,
        dst_ref=dst,
        send_sem=send_sem,
        recv_sem=recv_sem,
        device_id=where,
        device_id_type=pl.DeviceIdType.MESH,
    )


def hello(n, me, gy, with_plane, with_section=False):
    barrier = pltpu.get_barrier_semaphore()
    mesh_ids = pl.DeviceIdType.MESH

    @pl.when(me + 1 < n)
    def _():
        pl.semaphore_signal(barrier, 1, device_id={"gx": me + 1}, device_id_type=mesh_ids)

    @pl.when(me > 0)
    def _():
        pl.semaphore_signal(barrier, 1, device_id={"gx": me - 1}, device_id_type=mesh_ids)

    peers = 0
    if with_plane:
        for bit in (1, 2):
            pl.semaphore_signal(
                barrier, 1, device_id={"gy": gy_flip(gy, bit)}, device_id_type=mesh_ids
            )
        peers += 2
    if with_section:
        other = 1 - lax.axis_index("section")
        pl.semaphore_signal(barrier, 1, device_id={"section": other}, device_id_type=mesh_ids)
        peers += 1
    at_end = (me == 0) | (me == n - 1)

    @pl.when(at_end)
    def _():
        pl.semaphore_wait(barrier, peers + 1)

    @pl.when(jnp.logical_not(at_end))
    def _():
        pl.semaphore_wait(barrier, peers + 2)


def gy_flip(gy, bits):
    low = lax.rem(gy, 2)
    high = gy // 2
    if bits & 1:
        low = 1 - low
    if bits & 2:
        high = 1 - high
    return high * 2 + low


def z_gather_steps(n, me, slot, sems, after):
    send_up, recv_up, send_down, recv_down = sems
    sends = []

    def up(k):
        return remote(slot(me - k), slot(me - k), send_up.at[k], recv_up.at[k], gx=me + 1)

    def down(k):
        return remote(slot(me + k), slot(me + k), send_down.at[k], recv_down.at[k], gx=me - 1)

    for k in range(n):
        @pl.when(me - k >= 0)
        def _():
            if k:
                remote(
                    slot(me - k), slot(me - k), send_up.at[k - 1], recv_up.at[k - 1], gx=me
                ).wait_recv()
            if k < n - 1:

                @pl.when(me + 1 < n)
                def _():
                    up(k).start()

            if k == 0:

                @pl.when(me > 0)
                def _():
                    down(0).start()

            after(me - k, k)

        if k:

            @pl.when(me + k < n)
            def _():
                remote(
                    slot(me + k), slot(me + k), send_down.at[k - 1], recv_down.at[k - 1], gx=me
                ).wait_recv()
                if k < n - 1:

                    @pl.when(me > 0)
                    def _():
                        down(k).start()

                after(me + k, k)


def z_gather_drain(n, me, slot, sems):
    send_up, recv_up, send_down, recv_down = sems
    for k in range(n - 1):

        @pl.when((me - k >= 0) & (me + 1 < n))
        def _():
            remote(slot(me - k), slot(me - k), send_up.at[k], recv_up.at[k], gx=me + 1).wait_send()

        @pl.when((me + k < n) & (me > 0))
        def _():
            remote(
                slot(me + k), slot(me + k), send_down.at[k], recv_down.at[k], gx=me - 1
            ).wait_send()


def flip_by(gy, step):
    low = lax.rem(lax.rem(gy, 2) + lax.rem(step, 2), 2)
    high = lax.rem(gy // 2 + step // 2, 2)
    return high * 2 + low


class Plane:
    def __init__(self, n, sems):
        self.n = n
        self.me = lax.axis_index("gx")
        self.gy = lax.axis_index("gy")
        self.cx, self.cy, self.cd = (gy_flip(self.gy, bits) for bits in (1, 2, 3))
        self.gather_sems = sems[:10]
        self.scatter_sems = sems[10:]


    def gather_own_column(self, slot):
        su, ru, sd, rd, sx, rx, sy, ry, sf, rf = self.gather_sems
        c = self.gy

        def after(z, k):
            remote(slot(z, c), slot(z, c), sx.at[z], rx.at[z], gy=self.cx).start()
            remote(slot(z, c), slot(z, c), sy.at[z], ry.at[z], gy=self.cy).start()

        z_gather_steps(self.n, self.me, lambda z: slot(z, c), (su, ru, sd, rd), after)

    def gather_pass_on(self, slot):
        su, ru, sd, rd, sx, rx, sy, ry, sf, rf = self.gather_sems

        def forward(z):
            remote(slot(z, self.cx), slot(z, self.cx), sx.at[z], rx.at[z], gy=self.cx).wait_recv()
            remote(slot(z, self.cy), slot(z, self.cy), sy.at[z], ry.at[z], gy=self.cy).wait_recv()

            @pl.when(lax.rem(z, 2) == 0)
            def _():
                remote(
                    slot(z, self.cy), slot(z, self.cy), sf.at[z], rf.at[z], gy=self.cx
                ).start()

            @pl.when(lax.rem(z, 2) == 1)
            def _():
                remote(
                    slot(z, self.cx), slot(z, self.cx), sf.at[z], rf.at[z], gy=self.cy
                ).start()

        for k in range(self.n):

            @pl.when(self.me - k >= 0)
            def _():
                forward(self.me - k)

            if k:

                @pl.when(self.me + k < self.n)
                def _():
                    forward(self.me + k)

    def gather_far_column(self, slot):
        sf, rf = self.gather_sems[8:]
        for z in range(self.n):
            remote(slot(z, self.cd), slot(z, self.cd), sf.at[z], rf.at[z], gy=self.cx).wait_recv()

    def gather_drain(self, slot):
        su, ru, sd, rd, sx, rx, sy, ry, sf, rf = self.gather_sems
        z_gather_drain(self.n, self.me, lambda z: slot(z, self.gy), (su, ru, sd, rd))
        for z in range(self.n):
            one = slot(z, self.gy)
            remote(one, one, sx.at[z], rx.at[z], gy=self.cx).wait_send()
            remote(one, one, sy.at[z], ry.at[z], gy=self.cy).wait_send()
            remote(one, one, sf.at[z], rf.at[z], gy=self.cx).wait_send()


    def scatter_setup(self, part, sides, din, zup, zdn, stage, acc):
        self.part, self.sides, self.din = part, sides, din
        self.zup, self.zdn, self.stage, self.acc = zup, zdn, stage, acc

    def column_of(self, side):
        return self.cx * (1 - side) + self.cy * side

    def near(self, side, z):
        send, recv = self.scatter_sems[4:6]
        column = self.column_of(side)
        return remote(
            self.part(z, column), self.sides.at[side, z], send.at[side, z], recv.at[side, z], gy=column
        )

    def far(self, z):
        send, recv = self.scatter_sems[6:]
        return remote(
            self.part(z, self.cd),
            self.din.at[z],
            send.at[z],
            recv.at[z],
            gy=self.column_of(lax.rem(z, 2)),
        )

    def each(self, call):
        for k in [sign * far for far in reversed(range(1, self.n)) for sign in (-1, 1)] + [0]:

            @pl.when((self.me + k >= 0) & (self.me + k < self.n))
            def _():
                call(self.me + k, k)

    def scatter_near(self, side):
        def send(z, k):
            @pl.when(lax.rem(z, 2) == side)
            def _():
                self.near(side, z).start()

        self.each(send)

    def scatter_far(self):
        self.each(lambda z, k: self.far(z).start())

    def scatter_pass_on(self, z, k):
        self.far(z).wait_recv()
        side = 1 - lax.rem(z, 2)
        mine = self.part(z, self.column_of(side))
        add_rows(mine, mine, self.din.at[z])
        self.near(side, z).start()

    def along(self, z, up):
        send, recv = self.scatter_sems[:2] if up else self.scatter_sems[2:4]
        into = self.zup if up else self.zdn
        return remote(
            self.stage.at[z],
            into.at[z],
            send.at[z],
            recv.at[z],
            gx=self.me + 1 if up else self.me - 1,
        )

    def scatter_line(self, total, z, k):
        n, me, acc = self.n, self.me, self.acc
        self.near(0, z).wait_recv()
        self.near(1, z).wait_recv()
        terms = (self.part(z, self.gy), self.sides.at[0, z], self.sides.at[1, z])
        if k == 0:
            add_rows(total, *terms)
            return
        came = me > 0 if k > 0 else me < n - 1

        @pl.when(came)
        def _():
            self.along(z, k > 0).wait_recv()
            add_rows(self.stage.at[z], *terms, (self.zup if k > 0 else self.zdn).at[z])

        @pl.when(jnp.logical_not(came))
        def _():
            add_rows(self.stage.at[z], *terms)

        self.along(z, k > 0).start()

    def scatter_finish(self, total):
        n, me = self.n, self.me

        @pl.when(me > 0)
        def _():
            self.along(me, True).wait_recv()
            add_rows(total, total, self.zup.at[me])

        @pl.when(me < n - 1)
        def _():
            self.along(me, False).wait_recv()
            add_rows(total, total, self.zdn.at[me])

        for z in range(n):
            self.near(0, z).wait_send()
            self.near(1, z).wait_send()
            self.far(z).wait_send()

            @pl.when(me < z)
            def _():
                self.along(z, True).wait_send()

            @pl.when(me > z)
            def _():
                self.along(z, False).wait_send()


def add_rows(out, *terms):
    rows = out.shape[0]
    step = 16
    short = len(terms) == 2 and all(ref.dtype == BF16 for ref in (out, *terms))
    kind = BF16 if short else F32

    def body(i, carry):
        at = pl.ds(pl.multiple_of(i * step, step), step)
        value = terms[0][at].astype(kind)
        for term in terms[1:]:
            value = value + term[at].astype(kind)
        out[at] = value.astype(out.dtype)
        return carry

    lax.fori_loop(0, rows // step, body, 0)


def fetch_layer(layer, own, other, held, sems):
    section = lax.axis_index("section")

    @pl.when(section == layer)
    def _():
        for k, ref in enumerate(own):
            pltpu.make_async_copy(ref, held[k], sems.at[k]).start()

    @pl.when(section != layer)
    def _():
        for k, ref in enumerate(other):
            pltpu.make_async_copy(ref, held[k], sems.at[k]).start()


def fetch_wait(own, held, sems, which):
    for k in which:
        pltpu.make_async_copy(own[k], held[k], sems.at[k]).wait()


def moe_forward_kernel(
    n,
    layer,
    mid_ref,
    pay_ref,
    wg_own,
    wu_own,
    wd_own,
    wg_other,
    wu_other,
    wd_other,
    out_ref,
    arrived_ref,
    weight_ref,
    gp_ref,
    up_ref,
    inner_ref,
    pay,
    wg,
    wu,
    wd,
    part,
    sides,
    din,
    zup,
    zdn,
    stage,
    acc,
    total,
    gp,
    up,
    inner,
    wsem,
    osem,
    *sems,
):
    r, d = mid_ref.shape
    ff = wg.shape[1]
    rows = n * r
    experts = 4 * n
    own, other, held = (
        (wg_own, wu_own, wd_own),
        (wg_other, wu_other, wd_other),
        (wg, wu, wd),
    )
    fetch_layer(layer, own, other, held, wsem)
    plane = Plane(n, sems)
    me, gy = plane.me, plane.gy
    hello(n, me, gy, True)
    pay[pl.ds(pl.multiple_of((gy * n + me) * r, r), r)] = pay_ref[...]

    def slot(z, c):
        return pay.at[pl.ds((c * n + z) * r, r)]

    plane.scatter_setup(lambda z, c: part.at[c * n + z], sides, din, zup, zdn, stage, acc)
    plane.gather_own_column(slot)
    fetch_wait(own, held, wsem, range(3))
    expert = me * 4 + gy

    def column(s, carry):
        c = flip_by(gy, s)

        @pl.when(s == 1)
        def _():
            plane.gather_pass_on(slot)

        @pl.when(s == 3)
        def _():
            plane.gather_far_column(slot)

        at = pl.ds(pl.multiple_of(c * rows, rows), rows)
        gate_cols = pay[at, d : d + 128].astype(F32)
        lane = lax.broadcasted_iota(jnp.int32, (rows, 128), 1)
        hit = ((lane == expert) | (lane == expert + experts)) & (lane < 2 * experts)
        weight = jnp.sum(jnp.where(hit, gate_cols, 0.0), axis=1, keepdims=True)
        weight_ref[at] = weight
        block = pay[at, :d]

        def mid_cols(j, carry):
            cols = pl.ds(pl.multiple_of(j * 256, 256), 256)
            g = jnp.dot(block, wg[:, cols], preferred_element_type=F32)
            u = jnp.dot(block, wu[:, cols], preferred_element_type=F32)
            gp[at, cols] = g.astype(BF16)
            up[at, cols] = u.astype(BF16)
            inner[at, cols] = (g / (1.0 + jnp.exp(-g)) * u).astype(BF16)
            return carry

        lax.fori_loop(0, ff // 256, mid_cols, 0)
        act = inner[at]

        def out_cols(j, carry):
            cols = pl.ds(pl.multiple_of(j * 256, 256), 256)
            res = jnp.dot(act, wd[:, cols], preferred_element_type=F32) * weight
            part[pl.ds(pl.multiple_of(c * n, n), n), :, cols] = (
                res.astype(BF16).reshape(n, r, 256)
            )
            return carry

        lax.fori_loop(0, d // 256, out_cols, 0)

        @pl.when(s == 1)
        def _():
            plane.scatter_near(0)

        @pl.when(s == 2)
        def _():
            plane.scatter_near(1)

        return carry

    lax.fori_loop(0, 4, column, 0)
    plane.scatter_far()
    saves = [
        pltpu.make_async_copy(pay.at[:, pl.ds(0, d)], arrived_ref, osem.at[0]),
        pltpu.make_async_copy(gp, gp_ref, osem.at[1]),
        pltpu.make_async_copy(up, up_ref, osem.at[2]),
        pltpu.make_async_copy(inner, inner_ref, osem.at[3]),
    ]
    for save in saves:
        save.start()
    plane.each(plane.scatter_pass_on)
    plane.each(functools.partial(plane.scatter_line, total))
    plane.scatter_finish(total)
    add_rows(out_ref, mid_ref, total)
    plane.gather_drain(slot)
    for save in saves:
        save.wait()


def scatter_buffers(n, r, d):
    block = pltpu.VMEM((n, r, d), BF16)
    return [
        pltpu.VMEM((4 * n, r, d), BF16),
        pltpu.VMEM((2, n, r, d), BF16),
        *[block] * 4,
        *[pltpu.VMEM((r, d), F32)] * 2,
    ]


def in_vmem(count):
    return [pl.BlockSpec(memory_space=pltpu.VMEM)] * count


def in_place(count):
    return [pl.BlockSpec(memory_space=pl.ANY)] * count


def moe_forward(layer, n, mid, payload, own, other, cid):
    r, d = mid.shape
    ff = own[0].shape[1]
    total_rows = 4 * n * r
    width = payload.shape[1]
    return pl.pallas_call(
        functools.partial(moe_forward_kernel, n, layer),
        out_shape=(
            jax.ShapeDtypeStruct((r, d), BF16),
            jax.ShapeDtypeStruct((total_rows, d), BF16),
            jax.ShapeDtypeStruct((total_rows, 1), F32),
            jax.ShapeDtypeStruct((total_rows, ff), BF16),
            jax.ShapeDtypeStruct((total_rows, ff), BF16),
            jax.ShapeDtypeStruct((total_rows, ff), BF16),
        ),
        in_specs=in_vmem(2) + in_place(6),
        out_specs=tuple(in_vmem(1) + in_place(1) + in_vmem(1) + in_place(3)),
        scratch_shapes=[
            pltpu.VMEM((total_rows, width), BF16),
            pltpu.VMEM((d, ff), BF16),
            pltpu.VMEM((d, ff), BF16),
            pltpu.VMEM((ff, d), BF16),
        ]
        + scatter_buffers(n, r, d)
        + [pltpu.VMEM((total_rows, ff), BF16)] * 3
        + [pltpu.SemaphoreType.DMA((3,)), pltpu.SemaphoreType.DMA((4,))]
        + [pltpu.SemaphoreType.DMA((n,))] * 14
        + [pltpu.SemaphoreType.DMA((2, n))] * 2
        + [pltpu.SemaphoreType.DMA((n,))] * 2,
        compiler_params=pltpu.CompilerParams(
            collective_id=cid, has_side_effects=True, vmem_limit_bytes=63 << 20
        ),
        name="moe_forward",
    )(mid, payload, *own, *other)


def moe_backward_kernel(
    n,
    layer,
    cot_ref,
    mid_ref,
    gain_ref,
    weight_ref,
    arrived_hbm,
    gp_hbm,
    up_hbm,
    inner_hbm,
    wg_own,
    wu_own,
    wd_own,
    wg_other,
    wu_other,
    wd_other,
    *rest,
):
    rest = rest[0 if layer else 6 :]
    dmid_ref, dgain_ref = rest[:2]
    keep_refs, give_refs = rest[2:5], rest[5:8]
    (
    cots,
    wg,
    wu,
    wd,
    part,
    sides,
    din,
    zup,
    zdn,
    stage,
    acc,
    total,
    arrived,
    gp,
    up,
    inner,
    de,
    out_gate,
    out_up,
    out_down,
    wsem,
    isem,
    osem,
    *sems,
    ) = rest[8:]
    section = lax.axis_index("section")
    r, d = mid_ref.shape
    ff = wg.shape[1]
    rows = n * r
    own, other, held = (
        (wg_own, wu_own, wd_own),
        (wg_other, wu_other, wd_other),
        (wg, wu, wd),
    )
    loads = [
        pltpu.make_async_copy(gp_hbm, gp, isem.at[0]),
        pltpu.make_async_copy(up_hbm, up, isem.at[1]),
        pltpu.make_async_copy(arrived_hbm, arrived, isem.at[2]),
        pltpu.make_async_copy(inner_hbm, inner, isem.at[3]),
    ]
    fetch_layer(layer, own, other, held, wsem)
    for load in loads:
        load.start()
    plane = Plane(n, sems)
    me, gy = plane.me, plane.gy
    hello(n, me, gy, True)
    cots[pl.ds(pl.multiple_of((gy * n + me) * r, r), r)] = cot_ref[...]

    def slot(z, c):
        return cots.at[pl.ds((c * n + z) * r, r)]

    plane.scatter_setup(lambda z, c: part.at[c * n + z], sides, din, zup, zdn, stage, acc)
    plane.gather_own_column(slot)
    fetch_wait(own, held, wsem, range(3))
    for load in loads:
        load.wait()

    def column(s, carry):
        c = flip_by(gy, s)

        @pl.when(s == 1)
        def _():
            plane.gather_pass_on(slot)

        @pl.when(s == 3)
        def _():
            plane.gather_far_column(slot)

        at = pl.ds(pl.multiple_of(c * rows, rows), rows)
        de[at] = (cots[at].astype(F32) * weight_ref[at]).astype(BF16)
        block = de[at]

        def mid_cols(j, carry):
            cols = pl.ds(pl.multiple_of(j * 256, 256), 256)
            dz = dot32(block, wd[cols], COL_PAIR)
            g = gp[at, cols].astype(F32)
            u = up[at, cols].astype(F32)
            sg = 1.0 / (1.0 + jnp.exp(-g))
            gp[at, cols] = (dz * u * sg * (1.0 + g * (1.0 - sg))).astype(BF16)
            up[at, cols] = (dz * g * sg).astype(BF16)
            return carry

        lax.fori_loop(0, ff // 256, mid_cols, 0)
        dgp = gp[at]
        dup = up[at]

        def in_cols(j, carry):
            cols = pl.ds(pl.multiple_of(j * 256, 256), 256)
            res = dot32(dgp, wg[cols], COL_PAIR) + dot32(dup, wu[cols], COL_PAIR)
            part[pl.ds(pl.multiple_of(c * n, n), n), :, cols] = (
                res.astype(BF16).reshape(n, r, 256)
            )
            return carry

        lax.fori_loop(0, d // 256, in_cols, 0)

        @pl.when(s == 1)
        def _():
            plane.scatter_near(0)

        @pl.when(s == 2)
        def _():
            plane.scatter_near(1)

        return carry

    lax.fori_loop(0, 4, column, 0)
    plane.scatter_far()

    def saving(i, refs):
        at = pl.ds(pl.multiple_of(i * 256, 256), 256)
        for k, (src, ref) in enumerate(zip((out_gate, out_up, out_down), refs)):
            where = (slice(None), at) if k == 2 else (at, slice(None))
            yield pltpu.make_async_copy(src.at[where], ref.at[where], osem.at[k, i])

    chunks = d // 256

    def weight_grads(i, carry):
        at = pl.ds(pl.multiple_of(i * 256, 256), 256)
        left = arrived[:, at]
        out_gate[at] = dot32(left, gp[...], ROW_PAIR).astype(BF16)
        out_up[at] = dot32(left, up[...], ROW_PAIR).astype(BF16)
        out_down[:, at] = dot32(inner[...], de[:, at], ROW_PAIR).astype(BF16)

        @pl.when(section == layer)
        def _():
            for copy in saving(i, keep_refs):
                copy.start()

        @pl.when(section != layer)
        def _():
            for copy in saving(i, give_refs):
                copy.start()

        @pl.when(i == chunks // 4 - 1)
        def _():
            plane.each(plane.scatter_pass_on)

        @pl.when(i == chunks // 2 - 1)
        def _():
            plane.each(functools.partial(plane.scatter_line, total))

        return carry

    lax.fori_loop(0, chunks, weight_grads, 0)
    plane.scatter_finish(total)

    mid = mid_ref[...]
    scale = lax.rsqrt(jnp.mean(mid * mid, axis=-1, keepdims=True) + EPSILON)
    unit = mid * scale
    db = total[...]
    dgain_ref[...] = jnp.sum(db * unit, axis=0, keepdims=True)
    dmid_ref[...] = cot_ref[...].astype(F32) + norm_back(db * gain_ref[...], unit, scale)
    plane.gather_drain(slot)

    def settle(i, carry):
        for copy in saving(i, keep_refs):
            copy.wait()
        return carry

    lax.fori_loop(0, chunks, settle, 0)


def moe_backward(layer, n, cot, mid, gain, weight, arrived, gp, up, inner, own, other, so_far, cid):
    r, d = mid.shape
    ff = own[0].shape[1]
    total_rows = 4 * n * r
    sums = [jax.ShapeDtypeStruct(shape, BF16) for shape in ((d, ff), (d, ff), (ff, d))] * 2
    return pl.pallas_call(
        functools.partial(moe_backward_kernel, n, layer),
        out_shape=(
            jax.ShapeDtypeStruct((r, d), F32),
            jax.ShapeDtypeStruct((1, d), F32),
            *sums,
        ),
        in_specs=in_vmem(4) + in_place(10 + len(so_far)),
        out_specs=tuple(in_vmem(2) + in_place(6)),
        input_output_aliases={14 + k: 2 + k for k in range(len(so_far))},
        scratch_shapes=[
            pltpu.VMEM((total_rows, d), BF16),
            pltpu.VMEM((d, ff), BF16),
            pltpu.VMEM((d, ff), BF16),
            pltpu.VMEM((ff, d), BF16),
        ]
        + scatter_buffers(n, r, d)
        + [pltpu.VMEM((total_rows, d), BF16)]
        + [pltpu.VMEM((total_rows, ff), BF16)] * 3
        + [pltpu.VMEM((total_rows, d), BF16)]
        + [pltpu.VMEM((d, ff), BF16)] * 2
        + [pltpu.VMEM((ff, d), BF16)]
        + [
            pltpu.SemaphoreType.DMA((3,)),
            pltpu.SemaphoreType.DMA((4,)),
        ]
        + [pltpu.SemaphoreType.DMA((3, d // 256))]
        + [pltpu.SemaphoreType.DMA((n,))] * 14
        + [pltpu.SemaphoreType.DMA((2, n))] * 2
        + [pltpu.SemaphoreType.DMA((n,))] * 2,
        compiler_params=pltpu.CompilerParams(
            collective_id=cid, has_side_effects=True, vmem_limit_bytes=63 << 20
        ),
        name="moe_backward",
    )(cot, mid, gain, weight, arrived, gp, up, inner, *own, *other, *so_far)


class Share:
    def __init__(self, layer, pieces, full, scratch):
        self.full = full
        self.held, self.load_sems, self.plane_sems, self.to_sems, self.from_sems = scratch
        self.loads, first = [], 0
        for k, piece in enumerate(pieces):
            last = first + piece.shape[1]
            into = self.held.at[:, first:last]
            self.loads.append(pltpu.make_async_copy(piece, into, self.load_sems.at[k]))
            first = last
        self.section = lax.axis_index("section")
        self.mine = self.section == layer
        gy = lax.axis_index("gy")
        self.cols = [gy_flip(gy, bits) if bits else gy for bits in range(4)]
        self.rows = self.held.shape[0]

    def at(self, column, half=None):
        rows = self.rows
        if half is None:
            return self.full.at[pl.ds(pl.multiple_of(column * rows, rows), rows)]
        few = rows // 2
        return self.full.at[pl.ds(pl.multiple_of(column * rows + half * few, few), few)]

    def own(self):
        return pltpu.make_async_copy(self.held, self.at(self.cols[0]), self.plane_sems.at[0])

    def direct(self, bit):
        s = self.plane_sems
        k = 1 if bit == 1 else 3
        return remote(
            self.held, self.at(self.cols[0]), s.at[k], s.at[k + 1], gy=self.cols[bit]
        )

    def onward(self, bit):
        s = self.plane_sems
        k = 5 if bit == 1 else 7
        half = 1 if bit == 1 else 0
        ref = self.at(self.cols[3 - bit], half)
        return remote(ref, ref, s.at[k], s.at[k + 1], gy=self.cols[bit])

    def hand(self, k):
        if k == 0:
            src, dst = self.held, self.at(self.cols[0])
        elif k < 3:
            src = dst = self.at(self.cols[k])
        else:
            src = dst = self.at(self.cols[3], k - 3)
        return remote(src, dst, self.to_sems.at[k], self.from_sems.at[k], section=1 - self.section)

    def start(self):
        @pl.when(self.mine)
        def _():
            for load in self.loads:
                load.start()
            for load in self.loads:
                load.wait()
            self.direct(1).start()
            self.direct(2).start()
            self.own().start()
            self.hand(0).start()

    def pass_on(self):
        @pl.when(self.mine)
        def _():
            self.direct(1).wait_recv()
            self.onward(2).start()
            self.hand(1).start()
            self.direct(2).wait_recv()
            self.onward(1).start()
            self.hand(2).start()

    def finish(self):
        @pl.when(self.mine)
        def _():
            self.onward(2).wait_recv()
            self.hand(3).start()
            self.onward(1).wait_recv()
            self.hand(4).start()
            self.own().wait()

        @pl.when(jnp.logical_not(self.mine))
        def _():
            for k in range(5):
                self.hand(k).wait_recv()

    def drain(self):
        @pl.when(self.mine)
        def _():
            for bit in (1, 2):
                self.direct(bit).wait_send()
                self.onward(bit).wait_send()
            for k in range(5):
                self.hand(k).wait_send()


def share_scratch(shape):
    dma = pltpu.SemaphoreType.DMA
    return [pltpu.VMEM(shape, BF16), dma((3,)), dma((9,)), dma((5,)), dma((5,))]


def shard_pieces(query, key, value, out):
    heads = query.shape[2] // HD
    kv_head = lax.axis_index("gx") * heads // (HQ // KVH)
    own = pl.ds(pl.multiple_of(kv_head * HD, HD), HD)
    return [(query.at[0], key.at[0, :, own], value.at[0, :, own]), (out.at[0],)]


def shard_shapes(shards):
    rows, span = shards[0].shape[1:]
    return [(rows, span + 2 * HD), (rows, span)]


def full_shapes(shards):
    return [jax.ShapeDtypeStruct((4 * rows, cols), BF16) for rows, cols in shard_shapes(shards)]


def share_kernel(n, layer, *refs):
    fulls, scratch = refs[4:6], refs[6:]
    shares = [
        Share(layer, pieces, fulls[k], scratch[5 * k : 5 * k + 5])
        for k, pieces in enumerate(shard_pieces(*refs[:4]))
    ]
    hello(n, lax.axis_index("gx"), lax.axis_index("gy"), True, True)
    for share in shares:
        share.start()
    for share in shares:
        share.pass_on()
    for share in shares:
        share.finish()
    for share in shares:
        share.drain()


def share_weights(layer, n, shards, cid):
    return pl.pallas_call(
        functools.partial(share_kernel, n, layer),
        out_shape=tuple(full_shapes(shards)),
        in_specs=in_place(4),
        out_specs=tuple(in_place(2)),
        scratch_shapes=[item for shape in shard_shapes(shards) for item in share_scratch(shape)],
        compiler_params=pltpu.CompilerParams(collective_id=cid, has_side_effects=True),
        name="share_weights",
    )(*shards)


def finish_line_kernel(n, *refs):
    gains, rest = refs[:8], refs[8:]
    kv_ref, gain_ref, key_ref, value_ref, gbuf, kv_all, stage, incoming, rsem, *sems = rest
    me = lax.axis_index("gx")
    gy = lax.axis_index("gy")
    kv_all[me] = kv_ref[...]
    for k in range(2):
        first = 0
        for ref in gains[4 * k : 4 * k + 4]:
            last = first + ref.shape[1]
            gbuf[me, k : k + 1, first:last] = ref[...]
            first = last
    hello(n, me, gy, True)
    few = Line(n, None, lambda z: gbuf.at[z], None, sems[:4])
    many = Line(n, None, lambda z: kv_all.at[z], None, sems[4:8])
    few.gather_step(0)
    many.gather_step(0)
    steps = [functools.partial(many.gather_step, k) for k in range(1, n)]
    for k in range(1, n):
        few.gather_step(k)
        if k == n // 2:
            steps.pop(0)()
    total = gbuf[0]
    for z in range(1, n):
        total = total + gbuf[z]
    for k, where in enumerate(({"gy": gy_flip(gy, 1)}, {"gy": gy_flip(gy, 2)})):
        stage[k] = total
        swap = remote(stage.at[k], incoming.at[k], rsem.at[0, k], rsem.at[1, k], **where)
        swap.start()
        if steps:
            steps.pop(0)()
        swap.wait()
        total = total + incoming[k]
    gain_ref[...] = total
    for step in steps:
        step()
    for z in range(n):
        cols = slice(z * HD, (z + 1) * HD)
        key_ref[:, cols] = kv_all[z, :, :HD].astype(F32)
        value_ref[:, cols] = kv_all[z, :, HD:].astype(F32)
    few.gather_drain()
    many.gather_drain()


def finish_line(n, gains, kv, cid):
    dma = pltpu.SemaphoreType.DMA
    shape = jax.ShapeDtypeStruct
    width = sum(gain.shape[1] for gain in gains[:4])
    return pl.pallas_call(
        functools.partial(finish_line_kernel, n),
        out_shape=(
            shape((2, width), F32),
            shape((kv.shape[0], n * HD), F32),
            shape((kv.shape[0], n * HD), F32),
        ),
        in_specs=in_vmem(9),
        out_specs=tuple(in_vmem(3)),
        scratch_shapes=[
            pltpu.VMEM((n, 2, width), F32),
            pltpu.VMEM((n,) + kv.shape, BF16),
            pltpu.VMEM((2, 2, width), F32),
            pltpu.VMEM((2, 2, width), F32),
            dma((2, 2)),
        ]
        + [dma((n,))] * 8,
        compiler_params=pltpu.CompilerParams(collective_id=cid, has_side_effects=True),
        name="finish_line",
    )(*gains, kv)


def finish_pair_kernel(*refs):
    gain_ref, *rows = refs[:5]
    out_rows, out_gains = refs[5:7], refs[7:11]
    incoming, send, recv = refs[11:]
    section = lax.axis_index("section")
    other = 1 - section
    barrier = pltpu.get_barrier_semaphore()
    mesh_ids = pl.DeviceIdType.MESH
    pl.semaphore_signal(barrier, 1, device_id={"section": other}, device_id_type=mesh_ids)
    pl.semaphore_wait(barrier, 1)
    swap = remote(gain_ref, incoming, send.at[2], recv.at[2], section=other)
    swap.start()
    for mine in range(2):

        @pl.when(section == mine)
        def _():
            for k in range(2):
                src, dst = rows[2 * k + 1 - mine], out_rows[k].at[mine]
                remote(src, dst, send.at[k], recv.at[k], section=other).start()
            for k in range(2):
                out_rows[k][mine] = rows[2 * k + mine][...]

    swap.wait()
    for mine in range(2):

        @pl.when(section == mine)
        def _():
            first = 0
            for ref in out_gains:
                last = first + ref.shape[1]
                at = (slice(mine, mine + 1), slice(first, last))
                ref[...] = gain_ref[at] + incoming[at]
                first = last
            for k in range(2):
                src, dst = rows[2 * k + 1 - mine], out_rows[k].at[mine]
                remote(src, dst, send.at[k], recv.at[k], section=other).wait()


def finish_pair(gains, widths, lo, ig, cid):
    dma = pltpu.SemaphoreType.DMA
    shape = jax.ShapeDtypeStruct
    both = shape((2,) + lo[0].shape, BF16)
    return pl.pallas_call(
        finish_pair_kernel,
        out_shape=(both, both, *(shape((1, width), F32) for width in widths)),
        in_specs=in_vmem(5),
        out_specs=tuple(in_vmem(6)),
        scratch_shapes=[pltpu.VMEM(gains.shape, F32), dma((3,)), dma((3,))],
        compiler_params=pltpu.CompilerParams(collective_id=cid, has_side_effects=True),
        name="finish_pair",
    )(gains, *lo, *ig)


class Reduce:
    def __init__(self, layer, part, inbox, xin, yin, din, sems):
        self.part, self.inbox = part, inbox
        self.xin, self.yin, self.din = xin, yin, din
        self.give_sems, self.take_sems, self.send_sems, self.recv_sems = sems
        self.section = lax.axis_index("section")
        self.mine = self.section == layer
        gy = lax.axis_index("gy")
        self.cols = [gy_flip(gy, bits) if bits else gy for bits in range(4)]
        self.few = xin.shape[0] // 2

    def give(self, k, src):
        return remote(
            src,
            self.inbox.at[self.cols[k]],
            self.give_sems.at[k],
            self.take_sems.at[k],
            section=1 - self.section,
        )

    def half(self, ref, h):
        return ref.at[pl.ds(h * self.few, self.few)]

    def far(self, bit):
        k = bit - 1
        src = self.half(self.part(self.cols[3]), k)
        return remote(
            src, self.din.at[k], self.send_sems.at[k], self.recv_sems.at[k], gy=self.cols[bit]
        )

    def near(self, bit, h):
        k = 2 * bit + h
        into = self.xin if bit == 1 else self.yin
        return remote(
            self.half(self.part(self.cols[bit]), h),
            self.half(into, h),
            self.send_sems.at[k],
            self.recv_sems.at[k],
            gy=self.cols[bit],
        )

    def send_term(self, k):
        @pl.when(self.mine)
        def _():
            ref = self.part(self.cols[k])
            self.give(k, ref).wait_recv()
            add_rows(ref, ref, self.inbox.at[self.cols[k]])
            if k == 3:
                self.far(1).start()
                self.far(2).start()
            elif k:
                self.near(k, k - 1).start()

    def pass_on(self):
        @pl.when(self.mine)
        def _():
            self.far(1).wait_recv()
            ref = self.half(self.part(self.cols[2]), 0)
            add_rows(ref, ref, self.din.at[0])
            self.near(2, 0).start()
            self.far(2).wait_recv()
            ref = self.half(self.part(self.cols[1]), 1)
            add_rows(ref, ref, self.din.at[1])
            self.near(1, 1).start()

    def close(self, outs):
        @pl.when(self.mine)
        def _():
            for bit in (1, 2):
                for h in (0, 1):
                    self.near(bit, h).wait_recv()
            for ref, first, last in outs:
                cols = slice(first, last)
                own = self.part(self.cols[0])
                add_rows(ref, own.at[:, cols], self.xin.at[:, cols], self.yin.at[:, cols])
            for bit in (1, 2):
                self.far(bit).wait_send()
                for h in (0, 1):
                    self.near(bit, h).wait_send()


def reduce_sems():
    dma = pltpu.SemaphoreType.DMA
    return [dma((4,)), dma((4,)), dma((6,)), dma((6,))]


class Line:
    def __init__(self, n, m, slot, terms, sems):
        self.n, self.m, self.slot = n, m, slot
        self.me = lax.axis_index("gx")
        if terms is not None:
            self.col, self.zup, self.zdn, self.stage = (ref.at[m] for ref in terms)
        self.sems = [sem if m is None else sem.at[m] for sem in sems]

    def gather_up(self, k):
        ref = self.slot(self.me - k)
        return remote(ref, ref, self.sems[0].at[k], self.sems[1].at[k], gx=self.me + 1)

    def gather_down(self, k):
        ref = self.slot(self.me + k)
        return remote(ref, ref, self.sems[2].at[k], self.sems[3].at[k], gx=self.me - 1)

    def gather_step(self, k):
        n, me = self.n, self.me

        @pl.when(me - k >= 0)
        def _():
            if k:
                ref = self.slot(me - k)
                sems = self.sems
                remote(ref, ref, sems[0].at[k - 1], sems[1].at[k - 1], gx=me + 1).wait_recv()
            if k < n - 1:

                @pl.when(me + 1 < n)
                def _():
                    self.gather_up(k).start()

        @pl.when(me + k < n)
        def _():
            if k:
                ref = self.slot(me + k)
                sems = self.sems
                remote(ref, ref, sems[2].at[k - 1], sems[3].at[k - 1], gx=me - 1).wait_recv()
            if k < n - 1:

                @pl.when(me > 0)
                def _():
                    self.gather_down(k).start()

    def up(self, z):
        send, recv = self.sems[4:6]
        return remote(self.stage.at[z], self.zup.at[z], send.at[z], recv.at[z], gx=self.me + 1)

    def down(self, z):
        send, recv = self.sems[6:8]
        return remote(self.stage.at[z], self.zdn.at[z], send.at[z], recv.at[z], gx=self.me - 1)

    def scatter_tick(self, hop):
        n, me = self.n, self.me

        @pl.when(me == hop)
        def _():
            for z in reversed(range(hop + 1, n)):
                if hop:
                    self.up(z).wait_recv()
                    add_rows(self.stage.at[z], self.col.at[z], self.zup.at[z])
                else:
                    add_rows(self.stage.at[z], self.col.at[z])
                self.up(z).start()

        @pl.when(me == n - 1 - hop)
        def _():
            for z in range(n - 1 - hop):
                if hop:
                    self.down(z).wait_recv()
                    add_rows(self.stage.at[z], self.col.at[z], self.zdn.at[z])
                else:
                    add_rows(self.stage.at[z], self.col.at[z])
                self.down(z).start()

    def scatter_finish(self, total):
        n, me = self.n, self.me
        add_rows(total, self.col.at[me])

        @pl.when(me > 0)
        def _():
            self.up(me).wait_recv()
            add_rows(total, total, self.zup.at[me])

        @pl.when(me < n - 1)
        def _():
            self.down(me).wait_recv()
            add_rows(total, total, self.zdn.at[me])

    def gather_drain(self):
        n, me = self.n, self.me
        for k in range(n - 1):

            @pl.when((me - k >= 0) & (me + 1 < n))
            def _():
                self.gather_up(k).wait_send()

            @pl.when((me + k < n) & (me > 0))
            def _():
                self.gather_down(k).wait_send()

    def drain(self):
        n, me = self.n, self.me
        self.gather_drain()
        for z in range(n):

            @pl.when(me < z)
            def _():
                self.up(z).wait_send()

            @pl.when(me > z)
            def _():
                self.down(z).wait_send()


def unit_of(value):
    scale = lax.rsqrt(jnp.mean(value * value, axis=-1, keepdims=True) + EPSILON)
    return value * scale, scale


def half_turn(value):
    return pltpu.roll(value, value.shape[-1] // 2, axis=value.ndim - 1)


def attn_forward_kernel(
    n,
    layer,
    heads,
    x_ref,
    gain_attn,
    gain_ffn,
    gain_query,
    gain_key,
    cos_ref,
    sin_ref,
    mask_ref,
    gates_ref,
    win_hbm,
    wout_hbm,
    *rest,
):
    ahead = layer == 0
    shards, rest = (rest[:4], rest[4:]) if ahead else ((), rest)
    mid_ref, pay_ref, normed_hbm, proj_hbm, qr_hbm, kr_ref, v_ref, prob_hbm, mixed_hbm = rest[:9]
    fulls, rest = (rest[9:11], rest[11:]) if ahead else ((), rest[9:])
    (
    win,
    wout,
    normed,
    proj,
    qr,
    prob,
    mixed,
    col,
    zup,
    zdn,
    stage,
    total,
    wsem,
    osem,
    *sems,
    ) = rest
    mb, length, d = normed.shape
    t = length // n
    r = mb * t
    span = heads * HD
    me = lax.axis_index("gx")
    shares = []
    if ahead:
        shares = [
            Share(1, pieces, fulls[k], sems[8 + 5 * k : 13 + 5 * k])
            for k, pieces in enumerate(shard_pieces(*shards))
        ]
    fetch_in = pltpu.make_async_copy(win_hbm, win, wsem.at[0])
    fetch_out = pltpu.make_async_copy(wout_hbm, wout, wsem.at[1])
    fetch_in.start()
    fetch_out.start()
    hello(n, me, lax.axis_index("gy"), ahead, ahead)
    for share in shares:
        share.start()
    hidden = x_ref[...].astype(F32)
    unit, _ = unit_of(hidden)
    low = (unit * gain_attn[...]).astype(BF16)
    normed[:, pl.ds(pl.multiple_of(me * t, t), t)] = low.reshape(mb, t, d)
    lines = [
        Line(
            n,
            m,
            lambda z, m=m: normed.at[m, pl.ds(z * t, t)],
            (col, zup, zdn, stage),
            sems[:8],
        )
        for m in range(mb)
    ]
    waiting = []

    def tick():
        if waiting:
            waiting.pop(0)()

    for k in range(n):
        lines[0].gather_step(k)
        if k == min(1, n - 1):
            for line in lines[1:]:
                line.gather_step(0)
    fetch_in.wait()
    cosine, sine = cos_ref[...], sin_ref[...]
    for m, line in enumerate(lines):
        first = m * length
        rows = slice(first, first + length)
        if m + 1 < mb:
            waiting += [functools.partial(lines[m + 1].gather_step, k) for k in range(1, n)]

        def project(j, carry, m=m, rows=rows):
            cols = pl.ds(pl.multiple_of(j * 256, 256), 256)
            proj[rows, cols] = jnp.dot(normed[m], win[:, cols], preferred_element_type=F32)
            return carry

        blocks = (span + 2 * HD) // 256
        lax.fori_loop(0, blocks // 2, project, 0)
        tick()
        lax.fori_loop(blocks // 2, blocks, project, 0)
        tick()
        key_unit, _ = unit_of(proj[rows, span : span + HD])
        key = key_unit * gain_key[...]
        kr_ref[rows] = (key * cosine[rows] + half_turn(key) * sine[rows]).astype(BF16)
        v_ref[rows] = proj[rows, span + HD :].astype(BF16)

        def head(h, carry, m=m, rows=rows):
            at = pl.ds(pl.multiple_of(h * HD, HD), HD)
            query_unit, _ = unit_of(proj[rows, at])
            query = query_unit * gain_query[...]
            turned = (query * cosine[rows] + half_turn(query) * sine[rows]).astype(BF16)
            qr[rows, at] = turned
            scores = dot32(turned, kr_ref[rows], COL_PAIR) * (1.0 / math.sqrt(HD))
            exponent = jnp.where(mask_ref[m] > 0.5, jnp.exp(scores), 0.0)
            p = (exponent * (1.0 / jnp.sum(exponent, axis=-1, keepdims=True))).astype(BF16)
            prob[m * heads + h] = p
            mixed[rows, at] = jnp.dot(p, v_ref[rows], preferred_element_type=F32).astype(BF16)
            return carry

        lax.fori_loop(0, heads // 2, head, 0, unroll=2)
        tick()
        lax.fori_loop(heads // 2, heads, head, 0, unroll=2)
        while waiting:
            tick()
        if m == mb - 1:
            for share in shares:
                share.pass_on()
        if m == 0:
            fetch_out.wait()

        def out_cols(j, carry, m=m, rows=rows):
            at = pl.ds(pl.multiple_of(j * 256, 256), 256)
            res = dot32(mixed[rows], wout[at], COL_PAIR).astype(BF16)
            for z in range(n):
                col[m, z, :, at] = res[z * t : (z + 1) * t]
            return carry

        lax.fori_loop(0, d // 256, out_cols, 0)
        line.scatter_tick(0)
        waiting += [functools.partial(line.scatter_tick, hop) for hop in range(1, n - 1)]
    saves = [
        pltpu.make_async_copy(normed, normed_hbm, osem.at[0]),
        pltpu.make_async_copy(proj, proj_hbm, osem.at[1]),
        pltpu.make_async_copy(qr, qr_hbm, osem.at[2]),
        pltpu.make_async_copy(prob, prob_hbm, osem.at[3]),
        pltpu.make_async_copy(mixed, mixed_hbm, osem.at[4]),
    ]
    for save in saves:
        save.start()
    while waiting:
        tick()
    for m, line in enumerate(lines):
        line.scatter_finish(total.at[m * t : (m + 1) * t])
    mid = x_ref[...].astype(F32) + total[...]
    mid_ref[...] = mid
    unit, _ = unit_of(mid)
    pay_ref[:, :d] = (unit * gain_ffn[...]).astype(BF16)
    pay_ref[:, d:] = gates_ref[...]
    for share in shares:
        share.finish()
    for share in shares:
        share.drain()
    for line in lines:
        line.drain()
    for save in saves:
        save.wait()


def line_buffers(mb, n, r, d):
    return [pltpu.VMEM((mb, n, r // mb, d), BF16)] * 4 + [pltpu.VMEM((r, d), F32)]


def attn_forward(layer, n, x, gains, tables, gate_cols, w_in, w_out, shards, cid, mb):
    r, d = x.shape
    cosine, sine, mask = tables
    total_rows = cosine.shape[0]
    length = total_rows // mb
    width = w_in.shape[1]
    heads = w_out.shape[1] // HD
    span = heads * HD
    shape = jax.ShapeDtypeStruct
    return pl.pallas_call(
        functools.partial(attn_forward_kernel, n, layer, heads),
        out_shape=(
            shape((r, d), F32),
            shape((r, d + 128), BF16),
            shape((mb, length, d), BF16),
            shape((total_rows, width), F32),
            shape((total_rows, span), BF16),
            shape((total_rows, HD), BF16),
            shape((total_rows, HD), BF16),
            shape((mb * heads, length, length), BF16),
            shape((total_rows, span), BF16),
            *(full_shapes(shards) if shards else ()),
        ),
        in_specs=in_vmem(9) + in_place(2 + len(shards)),
        out_specs=tuple(in_vmem(2) + in_place(3) + in_vmem(2) + in_place(4 if shards else 2)),
        scratch_shapes=[
            pltpu.VMEM((d, width), BF16),
            pltpu.VMEM((d, span), BF16),
            pltpu.VMEM((mb, length, d), BF16),
            pltpu.VMEM((total_rows, width), F32),
            pltpu.VMEM((total_rows, span), BF16),
            pltpu.VMEM((mb * heads, length, length), BF16),
            pltpu.VMEM((total_rows, span), BF16),
        ]
        + line_buffers(mb, n, r, d)
        + [pltpu.SemaphoreType.DMA((2,)), pltpu.SemaphoreType.DMA((5,))]
        + [pltpu.SemaphoreType.DMA((mb, n))] * 8
        + [
            item
            for size in (shard_shapes(shards) if shards else ())
            for item in share_scratch(size)
        ],
        compiler_params=pltpu.CompilerParams(
            collective_id=cid, has_side_effects=True, vmem_limit_bytes=60 << 20
        ),
        name="attn_forward",
    )(x, *gains, cosine, sine, mask, gate_cols, w_in, w_out, *shards)


def attn_backward_kernel(
    n,
    layer,
    heads,
    dmid_ref,
    x_ref,
    gain_attn,
    gain_query,
    gain_key,
    cos_ref,
    sin_ref,
    kr_ref,
    v_ref,
    normed_hbm,
    proj_hbm,
    qr_hbm,
    prob_hbm,
    mixed_hbm,
    win_hbm,
    wout_hbm,
    *rest,
):
    last = layer == 0
    if last:
        later_hbm, gives, rest = rest[0], rest[1:4], rest[4:]
    cot_ref, dgain_attn, dgain_query, dgain_key = rest[:4]
    outs, rest = rest[4 : 10 if last else 5], rest[10 if last else 5 :]
    (
    win,
    wout,
    normed,
    proj,
    qr,
    prob,
    mixed,
    dmids,
    dheads,
    dproj,
    dkey,
    dvalue,
    grads,
    col,
    zup,
    zdn,
    stage,
    total,
    wsem,
    isem,
    osem,
    *sems,
    ) = rest
    mb, length, d = normed.shape
    t = length // n
    span = heads * HD
    me = lax.axis_index("gx")
    inv_root = 1.0 / math.sqrt(HD)
    gy = lax.axis_index("gy")
    section = lax.axis_index("section")
    fetch_out = pltpu.make_async_copy(wout_hbm, wout, wsem.at[0])
    fetch_in = pltpu.make_async_copy(win_hbm, win, wsem.at[1])
    fetch_out.start()
    fetch_in.start()
    loads = [
        pltpu.make_async_copy(prob_hbm, prob, isem.at[0]),
        pltpu.make_async_copy(mixed_hbm, mixed, isem.at[1]),
        pltpu.make_async_copy(qr_hbm, qr, isem.at[2]),
        pltpu.make_async_copy(proj_hbm, proj, isem.at[3]),
        pltpu.make_async_copy(normed_hbm, normed, isem.at[4]),
    ]
    for load in loads:
        load.start()
    if last:
        later, inbox, xin, yin, din = sems[8:13]
        block = d // 4

        def reduce(layer, terms, first, last, sems):
            cols = slice(first, last)
            buffers = [ref.at[..., cols] for ref in (inbox, xin, yin, din)]
            return Reduce(layer, lambda c: terms.at[pl.ds(c * block, block), cols], *buffers, sems)

        wide = span + 2 * HD
        job_later = reduce(1, later, 0, wide + span, sems[13:17])
        job = reduce(0, grads, 0, wide, sems[17:21])
        job_out = reduce(0, grads, wide, wide + span, sems[21:25])
        swaps = [
            remote(gives[k], outs[3 + k], sems[25].at[k], sems[26].at[k], section=1 - section)
            for k in range(3)
        ]
        load_later = pltpu.make_async_copy(later_hbm, later, osem.at[0])

        @pl.when(job_later.mine)
        def _():
            load_later.start()

        hello(n, me, gy, True, True)

        @pl.when(jnp.logical_not(job_later.mine))
        def _():
            for k in (3, 1, 2, 0):
                c = job_later.cols[k]
                job_later.give(k, later_hbm.at[pl.ds(c * block, block)]).start()

        for swap in swaps:
            swap.start()
    else:
        hello(n, me, None, False)
    dmids[:, pl.ds(pl.multiple_of(me * t, t), t)] = dmid_ref[...].astype(BF16).reshape(mb, t, d)
    lines = [
        Line(
            n,
            m,
            lambda z, m=m: dmids.at[m, pl.ds(z * t, t)],
            (col, zup, zdn, stage),
            sems[:8],
        )
        for m in range(mb)
    ]
    waiting = []
    sums = []

    def tick():
        if waiting:
            waiting.pop(0)()
        if sums:
            sums.pop(0)()

    for k in range(n):
        lines[0].gather_step(k)
        if k == min(1, n - 1):
            for line in lines[1:]:
                line.gather_step(0)
    if last:

        @pl.when(job_later.mine)
        def _():
            load_later.wait()

        sums += [functools.partial(job_later.send_term, k) for k in (3, 1, 2, 0)]
        sums += [job_later.pass_on]
    tick()
    fetch_out.wait()
    for load in loads:
        load.wait()
    cosine, sine = cos_ref[...], sin_ref[...]
    dkey[...] = jnp.zeros_like(dkey)
    dvalue[...] = jnp.zeros_like(dvalue)
    dgain_query[...] = jnp.zeros_like(dgain_query)
    dgain_key[...] = jnp.zeros_like(dgain_key)
    per = d // 4 // 256

    def out_grads(at):
        left = dmids[:, :, at].reshape(mb * length, 256)
        grads[at, span + 2 * HD :] = dot32(left, mixed[...], ROW_PAIR).astype(BF16)

    def in_grads(at):
        left = normed[:, :, at].reshape(mb * length, 256)
        grads[at, : span + 2 * HD] = dot32(left, dproj[...], ROW_PAIR).astype(BF16)

    def chunked(compute, job):
        def chunk(i, carry):
            first = flip_by(gy, 3 - i // per) * (d // 4) + lax.rem(i, per) * 256
            compute(pl.ds(pl.multiple_of(first, 256), 256))
            for q in range(4):

                @pl.when(i == per * (q + 1) - 1)
                def _():
                    if job is not None:

                        @pl.when(jnp.logical_not(job.mine))
                        def _():
                            job.give(3 - q, job.part(job.cols[3 - q])).start()

                    tick()

            return carry

        lax.fori_loop(0, 4 * per, chunk, 0)

    for m, line in enumerate(lines):
        first = m * length
        rows = slice(first, first + length)
        if m + 1 < mb:
            waiting += [functools.partial(lines[m + 1].gather_step, k) for k in range(1, n)]

        def to_heads(j, carry, m=m, rows=rows):
            cols = pl.ds(pl.multiple_of(j * 256, 256), 256)
            dheads[rows, cols] = jnp.dot(
                dmids[m], wout[:, cols], preferred_element_type=F32
            ).astype(BF16)
            return carry

        lax.fori_loop(0, span // 256, to_heads, 0)
        tick()

        def head(h, carry, m=m, rows=rows):
            at = pl.ds(pl.multiple_of(h * HD, HD), HD)
            p = prob[m * heads + h]
            dh = dheads[rows, at]
            dvalue[rows] += dot32(p, dh, ROW_PAIR)
            dp = dot32(dh, v_ref[rows], COL_PAIR)
            delta = jnp.sum(
                dh.astype(F32) * mixed[rows, at].astype(F32), axis=-1, keepdims=True
            )
            ds = (p.astype(F32) * (dp - delta)).astype(BF16)
            dkey[rows] += dot32(ds, qr[rows, at], ROW_PAIR) * inv_root
            dq = jnp.dot(ds, kr_ref[rows], preferred_element_type=F32) * inv_root
            turned = dq * cosine[rows] - half_turn(dq) * sine[rows]
            unit, scale = unit_of(proj[rows, at])
            dgain_query[...] += jnp.sum(turned * unit, axis=0, keepdims=True)
            dproj[rows, at] = norm_back(turned * gain_query[...], unit, scale).astype(BF16)
            return carry

        lax.fori_loop(0, heads // 2, head, 0, unroll=2)
        tick()
        lax.fori_loop(heads // 2, heads, head, 0, unroll=2)
        tick()
        dk = dkey[rows]
        turned = dk * cosine[rows] - half_turn(dk) * sine[rows]
        unit, scale = unit_of(proj[rows, span : span + HD])
        dgain_key[...] += jnp.sum(turned * unit, axis=0, keepdims=True)
        dproj[rows, span : span + HD] = norm_back(turned * gain_key[...], unit, scale).astype(BF16)
        dproj[rows, span + HD :] = dvalue[rows].astype(BF16)
        if m == 0:
            fetch_in.wait()
        while waiting:
            tick()

        def in_cols(j, carry, m=m, rows=rows):
            at = pl.ds(pl.multiple_of(j * 256, 256), 256)
            res = dot32(dproj[rows], win[at], COL_PAIR).astype(BF16)
            for z in range(n):
                col[m, z, :, at] = res[z * t : (z + 1) * t]
            return carry

        lax.fori_loop(0, d // 256, in_cols, 0)
        line.scatter_tick(0)
        waiting += [functools.partial(line.scatter_tick, hop) for hop in range(1, n - 1)]
        if m == 0 and last:
            chunked(out_grads, job_out)
            sums += [functools.partial(job_out.send_term, k) for k in (3, 2, 1, 0)]
            sums += [job_out.pass_on]
    while sums:
        sums.pop(0)()

    if not last:
        chunked(out_grads, None)
    chunked(in_grads, job if last else None)
    while waiting:
        tick()
    if last:
        for k in (3, 2, 1, 0):
            job.send_term(k)
    else:
        save = pltpu.make_async_copy(grads, outs[0], osem.at[0])
        save.start()
    for m, line in enumerate(lines):
        line.scatter_finish(total.at[m * t : (m + 1) * t])
    hidden = x_ref[...].astype(F32)
    unit, scale = unit_of(hidden)
    da = total[...]
    dgain_attn[...] = jnp.sum(da * unit, axis=0, keepdims=True)
    cot_ref[...] = (dmid_ref[...] + norm_back(da * gain_attn[...], unit, scale)).astype(BF16)
    for line in lines:
        line.drain()
    if not last:
        save.wait()
        return
    job.pass_on()
    closing = [(outs[0], 0, span), (outs[1], span, wide), (outs[2], wide, wide + span)]
    job_later.close(closing)
    job_out.close([(outs[2], 0, span)])
    job.close(closing[:2])
    for swap in swaps:
        swap.wait()

    @pl.when(jnp.logical_not(job.mine))
    def _():
        for k in range(4):
            job.give(k, job.part(job.cols[k])).wait_send()
            job_out.give(k, job_out.part(job_out.cols[k])).wait_send()

    @pl.when(jnp.logical_not(job_later.mine))
    def _():
        for k in range(4):
            c = job_later.cols[k]
            job_later.give(k, later_hbm.at[pl.ds(c * block, block)]).wait_send()


def attn_backward(layer, n, dmid, x, gains, tables, kept, w_in, w_out, later, gives, cid, mb):
    r, d = x.shape
    cosine, sine, _ = tables
    normed, proj, qr, kr, v, prob, mixed = kept
    total_rows = cosine.shape[0]
    length = total_rows // mb
    width = w_in.shape[1]
    heads = w_out.shape[1] // HD
    span = heads * HD
    shape = jax.ShapeDtypeStruct
    both = width + span
    grad_shapes = [shape((d, both), BF16)]
    extra = []
    if later:
        block = d // 4
        grad_shapes = [
            shape((block, span), F32),
            shape((block, 2 * HD), BF16),
            shape((block, span), F32),
            *(shape(piece.shape, BF16) for piece in gives),
        ]
        extra = [
            pltpu.VMEM((d, both), BF16),
            pltpu.VMEM((4, block, both), BF16),
            pltpu.VMEM((block, both), BF16),
            pltpu.VMEM((block, both), BF16),
            pltpu.VMEM((2, block // 2, both), BF16),
        ] + reduce_sems() * 3 + [pltpu.SemaphoreType.DMA((3,))] * 2
    return pl.pallas_call(
        functools.partial(attn_backward_kernel, n, layer, heads),
        out_shape=(
            shape((r, d), BF16),
            shape((1, d), F32),
            shape((1, HD), F32),
            shape((1, HD), F32),
            *grad_shapes,
        ),
        in_specs=in_vmem(9) + in_place(7 + len(later) + len(gives)),
        out_specs=tuple(in_vmem(4) + (in_vmem(3) + in_place(3) if later else in_place(1))),
        scratch_shapes=[
            pltpu.VMEM((d, width), BF16),
            pltpu.VMEM((d, span), BF16),
            pltpu.VMEM((mb, length, d), BF16),
            pltpu.VMEM((total_rows, width), F32),
            pltpu.VMEM((total_rows, span), BF16),
            pltpu.VMEM((mb * heads, length, length), BF16),
            pltpu.VMEM((total_rows, span), BF16),
            pltpu.VMEM((mb, length, d), BF16),
            pltpu.VMEM((total_rows, span), BF16),
            pltpu.VMEM((total_rows, width), BF16),
            pltpu.VMEM((total_rows, HD), F32),
            pltpu.VMEM((total_rows, HD), F32),
            pltpu.VMEM((d, both), BF16),
        ]
        + line_buffers(mb, n, r, d)
        + [
            pltpu.SemaphoreType.DMA((2,)),
            pltpu.SemaphoreType.DMA((5,)),
            pltpu.SemaphoreType.DMA((1,)),
        ]
        + [pltpu.SemaphoreType.DMA((mb, n))] * 8
        + extra,
        compiler_params=pltpu.CompilerParams(
            collective_id=cid, has_side_effects=True, vmem_limit_bytes=63 << 20
        ),
        name="attn_backward",
    )(
        dmid,
        x,
        *gains,
        cosine,
        sine,
        kr,
        v,
        normed,
        proj,
        qr,
        prob,
        mixed,
        w_in,
        w_out,
        *later,
        *gives,
    )


def local_wide(
    inputs,
    out_grad,
    segments,
    routes,
    gates,
    gain_attn,
    gain_ffn,
    gain_query,
    gain_key,
    w_query,
    w_key,
    w_value,
    w_out,
    w_gate,
    w_up,
    w_down,
):
    micro_count, _, local_rows, width = inputs.shape
    n_sec = lax.axis_size("section")
    n_gx = lax.axis_size("gx")
    n_gy = lax.axis_size("gy")
    heads = w_query.shape[2] // HD
    span = heads * HD
    experts = n_gx * n_gy
    group_len = segments.shape[2]
    mb = micro_count // n_sec
    rows_own = mb * local_rows
    rows_attn = mb * group_len
    section = lax.axis_index("section")
    gx = lax.axis_index("gx")
    gy = lax.axis_index("gy")
    expert_own = gx * n_gy + gy
    inv_root = 1.0 / math.sqrt(HD)
    first = section * mb

    kv_head = gx * heads // (HQ // KVH)
    key_own = lax.dynamic_slice_in_dim(w_key[0], kv_head * HD, HD, 1)
    value_own = lax.dynamic_slice_in_dim(w_value[0], kv_head * HD, HD, 1)
    w_in_shard = jnp.concatenate([w_query[0], key_own, value_own], axis=1)
    w_in_all = both_layers(lax.all_gather(w_in_shard, "gy", axis=0, tiled=True))
    w_out_all = both_layers(lax.all_gather(w_out[0], "gy", axis=0, tiled=True))
    w_gate_all = both_layers(w_gate[0, 0])
    w_up_all = both_layers(w_up[0, 0])
    w_down_all = both_layers(w_down[0, 0])
    table = dense_gates(routes[0, :, 0], gates[0, :, 0], experts)
    small = jnp.concatenate(
        [
            table.reshape(-1),
            gain_attn[0],
            gain_ffn[0],
            gain_query[0],
            gain_key[0],
        ]
    )
    small_all = both_layers(small)
    table_size = micro_count * local_rows * experts
    table_all = small_all[:, :table_size].reshape(n_sec, micro_count, local_rows, experts)
    gains_all = small_all[:, table_size:]

    table_mine = lax.dynamic_slice_in_dim(table_all, first, mb, 1).reshape(
        n_sec, rows_own, experts
    )
    x_mine = lax.dynamic_slice_in_dim(inputs[:, 0], first, mb, 0).reshape(rows_own, width)
    cot_mine = lax.dynamic_slice_in_dim(out_grad[:, 0], first, mb, 0).reshape(rows_own, width)
    segs = lax.dynamic_slice_in_dim(segments[:, 0], first, mb, 0)
    allowed, cosine, sine = seq_tables(segs, HD)
    cos_q = cosine.reshape(rows_attn, 1, HD // 2)
    sin_q = sine.reshape(rows_attn, 1, HD // 2)
    cos_k = cosine.reshape(rows_attn, HD // 2)
    sin_k = sine.reshape(rows_attn, HD // 2)

    def split_gains(layer):
        g = gains_all[layer]
        return (
            g[:width],
            g[width : 2 * width],
            g[2 * width : 2 * width + HD],
            g[2 * width + HD :],
        )

    saved_all = []
    outs = []
    layer_in = x_mine
    for layer in range(n_sec):
        g_attn, g_ffn, g_query, g_key = split_gains(layer)
        hidden = layer_in.astype(F32)
        attn_unit, attn_scale = normalize(hidden)
        normed = (attn_unit * g_attn).astype(BF16)
        normed_all = gather_z(normed.reshape(mb, local_rows, width)).reshape(rows_attn, width)
        projected = dot32(normed_all, w_in_all[layer])
        query = projected[:, :span].reshape(rows_attn, heads, HD)
        key = projected[:, span : span + HD]
        value_low = projected[:, span + HD :].astype(BF16).reshape(mb, group_len, HD)
        query_unit, query_scale = normalize(query)
        key_unit, key_scale = normalize(key)
        query_rope = (
            rotate(query_unit * g_query, cos_q, sin_q)
            .astype(BF16)
            .reshape(mb, group_len, heads, HD)
        )
        key_rope = rotate(key_unit * g_key, cos_k, sin_k).astype(BF16).reshape(mb, group_len, HD)
        scores = (
            jnp.einsum("mthd,msd->mhts", query_rope, key_rope, preferred_element_type=F32)
            * inv_root
        )
        exponent = jnp.where(allowed[:, None], jnp.exp(scores), 0.0)
        log_total = jnp.log(jnp.sum(exponent, axis=-1, keepdims=True))
        prob = jnp.where(allowed[:, None], jnp.exp(scores - log_total), 0.0)
        mixed = (
            jnp.einsum("mhts,msd->mthd", prob.astype(BF16), value_low, preferred_element_type=F32)
            .astype(BF16)
            .reshape(rows_attn, span)
        )
        attn_part = dot32(mixed, w_out_all[layer], COL_PAIR).astype(BF16)
        attn_out = scatter_z(attn_part.reshape(mb, group_len, width)).reshape(rows_own, width)
        middle = hidden + attn_out.astype(F32)
        ffn_unit, ffn_scale = normalize(middle)
        expert_in = (ffn_unit * g_ffn).astype(BF16)
        tab = table_mine[layer]
        tab_hi = tab.astype(BF16)
        tab_lo = (tab - tab_hi.astype(F32)).astype(BF16)
        payload = jnp.concatenate([expert_in, tab_hi, tab_lo], axis=1)
        arrived_all = gather_all(payload)
        arrived = arrived_all[:, :width]
        gate_cols = arrived_all[:, width:].astype(F32)
        is_mine = jnp.arange(2 * experts) % experts == expert_own
        weight = jnp.sum(jnp.where(is_mine[None], gate_cols, 0.0), axis=1, keepdims=True)
        gate_pre = dot32(arrived, w_gate_all[layer])
        up_proj = dot32(arrived, w_up_all[layer])
        inner = (jax.nn.silu(gate_pre) * up_proj).astype(BF16)
        result = dot32(inner, w_down_all[layer])
        weighted = (result * weight).astype(BF16)
        expert_sum = scatter_all(weighted)
        layer_out = (middle + expert_sum.astype(F32)).astype(BF16)
        outs.append(layer_out)
        layer_in = layer_out
        saved_all.append(
            (
                attn_unit,
                attn_scale,
                normed_all,
                query_unit,
                query_scale,
                key_unit,
                key_scale,
                query_rope,
                key_rope,
                value_low,
                prob,
                mixed,
                ffn_unit,
                ffn_scale,
                arrived,
                weight,
                gate_pre,
                up_proj,
                inner,
            )
        )

    cot = cot_mine
    in_grads = [None] * n_sec
    expert_grads = [None] * n_sec
    attn_grads = [None] * n_sec
    gain_grads = [None] * n_sec
    for layer in reversed(range(n_sec)):
        g_attn, g_ffn, g_query, g_key = split_gains(layer)
        (
            attn_unit,
            attn_scale,
            normed_all,
            query_unit,
            query_scale,
            key_unit,
            key_scale,
            query_rope,
            key_rope,
            value_low,
            prob,
            mixed,
            ffn_unit,
            ffn_scale,
            arrived,
            weight,
            gate_pre,
            up_proj,
            inner,
        ) = saved_all[layer]
        gradient = cot.astype(F32)
        grad_all = gather_all(cot)
        grad_result = (grad_all.astype(F32) * weight).astype(BF16)
        grad_inner = dot32(grad_result, w_down_all[layer], COL_PAIR)
        grad_down = dot32(inner, grad_result, ROW_PAIR)
        sig = jax.nn.sigmoid(gate_pre)
        grad_gate_pre = (grad_inner * up_proj * sig * (1.0 + gate_pre * (1.0 - sig))).astype(BF16)
        grad_up_proj = (grad_inner * gate_pre * sig).astype(BF16)
        grad_gate = dot32(arrived, grad_gate_pre, ROW_PAIR)
        grad_up = dot32(arrived, grad_up_proj, ROW_PAIR)
        grad_arrived = (
            dot32(grad_gate_pre, w_gate_all[layer], COL_PAIR)
            + dot32(grad_up_proj, w_up_all[layer], COL_PAIR)
        ).astype(BF16)
        expert_grads[layer] = (grad_gate, grad_up, grad_down)
        grad_expert_in = scatter_all(grad_arrived).astype(F32)
        grad_ffn_gain = jnp.sum(grad_expert_in * ffn_unit, axis=0)
        grad_middle = gradient + norm_back(grad_expert_in * g_ffn, ffn_unit, ffn_scale)
        middle_low = grad_middle.astype(BF16)
        middle_all = gather_z(middle_low.reshape(mb, local_rows, width)).reshape(rows_attn, width)
        grad_out_w = dot32(middle_all, mixed, ROW_PAIR)
        grad_heads = (
            dot32(middle_all, w_out_all[layer]).astype(BF16).reshape(mb, group_len, heads, HD)
        )
        grad_value = jnp.einsum(
            "mhts,mthd->mshd", prob.astype(BF16), grad_heads, preferred_element_type=F32
        )
        grad_prob = jnp.einsum(
            "mthd,msd->mhts", grad_heads, value_low, preferred_element_type=F32
        )
        mixed_split = mixed.reshape(mb, group_len, heads, HD)
        delta = jnp.sum(grad_heads.astype(F32) * mixed_split.astype(F32), axis=-1)
        delta = jnp.swapaxes(delta, 1, 2)[..., None]
        grad_scores = (prob * (grad_prob - delta)).astype(BF16)
        grad_query = (
            jnp.einsum("mhts,msd->mthd", grad_scores, key_rope, preferred_element_type=F32)
            * inv_root
        ).reshape(rows_attn, heads, HD)
        grad_key = (
            jnp.einsum("mhts,mthd->mshd", grad_scores, query_rope, preferred_element_type=F32)
            * inv_root
        ).reshape(rows_attn, heads, HD)
        query_turn = rotate_back(grad_query, cos_q, sin_q)
        grad_query_gain = jnp.sum(query_turn * query_unit, axis=(0, 1))
        grad_query_pre = norm_back(query_turn * g_query, query_unit, query_scale)
        key_turn = rotate_back(jnp.sum(grad_key, axis=1), cos_k, sin_k)
        grad_key_gain = jnp.sum(key_turn * key_unit, axis=0)
        grad_key_pre = norm_back(key_turn * g_key, key_unit, key_scale)
        grad_proj = jnp.concatenate(
            [
                grad_query_pre.reshape(rows_attn, span),
                grad_key_pre,
                jnp.sum(grad_value, axis=2).reshape(rows_attn, HD),
            ],
            axis=1,
        ).astype(BF16)
        grad_in_w = dot32(normed_all, grad_proj, ROW_PAIR)
        normed_part = dot32(grad_proj, w_in_all[layer], COL_PAIR).astype(BF16)
        grad_normed = (
            scatter_z(normed_part.reshape(mb, group_len, width))
            .reshape(rows_own, width)
            .astype(F32)
        )
        grad_attn_gain = jnp.sum(grad_normed * attn_unit, axis=0)
        cot = (grad_middle + norm_back(grad_normed * g_attn, attn_unit, attn_scale)).astype(BF16)
        in_grads[layer] = cot
        attn_grads[layer] = jnp.concatenate([grad_in_w, grad_out_w], axis=1).astype(BF16)
        gain_grads[layer] = jnp.concatenate(
            [grad_attn_gain, grad_ffn_gain, grad_query_gain, grad_key_gain]
        )

    def own_layer_sum(pieces):
        return lax.psum_scatter(
            jnp.stack([piece.astype(BF16) for piece in pieces]),
            "section",
            scatter_dimension=0,
            tiled=True,
        ).astype(F32)

    grad_gate, grad_up, grad_down = (
        own_layer_sum([expert_grads[layer][k] for layer in range(n_sec)]) for k in range(3)
    )
    attn_sum = lax.psum_scatter(
        jnp.concatenate(attn_grads, axis=0), ("section", "gy"), scatter_dimension=0, tiled=True
    ).astype(F32)
    query_grad = attn_sum[:, :span]
    out_w_grad = attn_sum[:, span + 2 * HD :]
    kv_all = lax.all_gather(attn_sum[:, span : span + 2 * HD], "gx", axis=0, tiled=False)
    kv_all = jnp.sum(kv_all.reshape(KVH, n_gx // KVH, -1, 2, HD), axis=1)
    key_part = jnp.swapaxes(kv_all[:, :, 0], 0, 1).reshape(-1, KVH * HD)
    value_part = jnp.swapaxes(kv_all[:, :, 1], 0, 1).reshape(-1, KVH * HD)
    gain_sum = lax.psum(jnp.stack(gain_grads), ("section", "gx", "gy"))
    gain_sum = lax.dynamic_index_in_dim(gain_sum, section, 0, keepdims=True)

    def own_layer_rows(pieces):
        stacked = jnp.stack(pieces).reshape(n_sec, mb, local_rows, width)
        return lax.all_to_all(stacked, "section", split_axis=0, concat_axis=0, tiled=True).reshape(
            1, micro_count, 1, local_rows, width
        )

    return (
        own_layer_rows(outs),
        own_layer_rows(in_grads),
        gain_sum[:, :width],
        gain_sum[:, width : 2 * width],
        gain_sum[:, 2 * width : 2 * width + HD],
        gain_sum[:, 2 * width + HD :],
        query_grad[None],
        key_part[None],
        value_part[None],
        out_w_grad[None],
        grad_gate[:, None],
        grad_up[:, None],
        grad_down[:, None],
    )


def local_fused(
    inputs,
    out_grad,
    segments,
    routes,
    gates,
    gain_attn,
    gain_ffn,
    gain_query,
    gain_key,
    w_query,
    w_key,
    w_value,
    w_out,
    w_gate,
    w_up,
    w_down,
):
    micro_count, _, local_rows, width = inputs.shape
    n_sec = lax.axis_size("section")
    n_gx = lax.axis_size("gx")
    n_gy = lax.axis_size("gy")
    heads = w_query.shape[2] // HD
    span = heads * HD
    experts = n_gx * n_gy
    group_len = segments.shape[2]
    mb = micro_count // n_sec
    rows_own = mb * local_rows
    rows_attn = mb * group_len
    section = lax.axis_index("section")
    first = section * mb

    attn_shards = (w_query, w_key, w_value, w_out)
    attn_all = [share_weights(0, n_gx, attn_shards, 9)]
    moe_own = (w_gate[0, 0], w_up[0, 0], w_down[0, 0])
    moe_other = tuple(swap_sections(w) for w in moe_own)
    table = dense_gates(routes[0, :, 0], gates[0, :, 0], experts)
    small = jnp.concatenate(
        [table.reshape(-1), gain_attn[0], gain_ffn[0], gain_query[0], gain_key[0]]
    )
    small_other = swap_sections(small)
    is_first = section == 0
    small_all = jnp.stack(
        [jnp.where(is_first, small, small_other), jnp.where(is_first, small_other, small)]
    )
    table_size = micro_count * local_rows * experts
    table_all = small_all[:, :table_size].reshape(n_sec, micro_count, local_rows, experts)
    gains_all = small_all[:, table_size:]
    table_mine = lax.dynamic_slice_in_dim(table_all, first, mb, 1).reshape(
        n_sec, rows_own, experts
    )
    x_mine = lax.dynamic_slice_in_dim(inputs[:, 0], first, mb, 0).reshape(rows_own, width)
    cot = lax.dynamic_slice_in_dim(out_grad[:, 0], first, mb, 0).reshape(rows_own, width)
    segs = lax.dynamic_slice_in_dim(segments[:, 0], first, mb, 0)
    allowed, cosine, sine = seq_tables(segs, HD)
    tables = (
        jnp.concatenate([cosine, cosine], axis=-1).reshape(rows_attn, HD),
        jnp.concatenate([-sine, sine], axis=-1).reshape(rows_attn, HD),
        allowed.astype(F32),
    )

    def split_gains(layer):
        g = gains_all[layer : layer + 1]
        return (
            g[:, :width],
            g[:, width : 2 * width],
            g[:, 2 * width : 2 * width + HD],
            g[:, 2 * width + HD :],
        )

    kept = []
    outs = []
    layer_in = x_mine
    for layer in range(n_sec):
        tab = table_mine[layer]
        tab_hi = tab.astype(BF16)
        tab_lo = (tab - tab_hi.astype(F32)).astype(BF16)
        pad = jnp.zeros((rows_own, 128 - 2 * experts), BF16)
        gate_cols = jnp.concatenate([tab_hi, tab_lo, pad], axis=1)
        mid, payload, normed, proj, qr, kr, v, prob, mixed, *next_all = attn_forward(
            layer,
            n_gx,
            layer_in,
            split_gains(layer),
            tables,
            gate_cols,
            *attn_all[layer],
            attn_shards if layer == 0 else (),
            1 + layer,
            mb,
        )
        attn_all.append(next_all)
        layer_out, *moe_kept = moe_forward(
            layer, n_gx, mid, payload, moe_own, moe_other, 3 + layer
        )
        kept.append((layer_in, mid, (normed, proj, qr, kr, v, prob, mixed), moe_kept))
        outs.append(layer_out)
        layer_in = layer_out

    in_grads = [None] * n_sec
    moe_sums = ()
    later = ()
    gain_grads = [None] * n_sec
    for layer in reversed(range(n_sec)):
        g_attn, g_ffn, g_query, g_key = split_gains(layer)
        layer_in, mid, attn_kept, (arrived, weight, gp, up, inner) = kept[layer]
        dmid, d_ffn, *moe_sums = moe_backward(
            layer,
            n_gx,
            cot,
            mid,
            g_ffn,
            weight,
            arrived,
            gp,
            up,
            inner,
            moe_own,
            moe_other,
            moe_sums,
            5 + layer,
        )
        cot, d_attn, d_query, d_key, *later = attn_backward(
            layer,
            n_gx,
            dmid,
            layer_in,
            (g_attn, g_query, g_key),
            tables,
            attn_kept,
            *attn_all[layer],
            later,
            moe_sums[3:] if layer == 0 else (),
            7 + layer,
            mb,
        )
        in_grads[layer] = cot
        gain_grads[layer] = [d_attn, d_ffn, d_query, d_key]

    query_grad, kv_shard, out_grad_w, *from_other = later
    grad_gate, grad_up, grad_down = (
        (moe_sums[k].astype(F32) + from_other[k].astype(F32))[None] for k in range(3)
    )
    gain_sum, key_part, value_part = finish_line(
        n_gx, [grad for grads in gain_grads for grad in grads], kv_shard, 10
    )
    out_rows, grad_rows, *gain_sums = finish_pair(
        gain_sum, [grad.shape[1] for grad in gain_grads[0]], outs, in_grads, 11
    )
    whole_rows = (1, micro_count, 1, local_rows, width)

    return (
        out_rows.reshape(whole_rows),
        grad_rows.reshape(whole_rows),
        *gain_sums,
        query_grad[None],
        key_part[None],
        value_part[None],
        out_grad_w[None],
        grad_gate[:, None],
        grad_up[:, None],
        grad_down[:, None],
    )


def local(*args):
    inputs = args[0]
    n = lax.axis_size("gx")
    rows_own = inputs.shape[0] // lax.axis_size("section") * inputs.shape[2]
    if 4 * n * rows_own > MOST_ROWS or n != KVH:
        return local_wide(*args)
    return local_fused(*args)


def solution(mesh):
    return jax.shard_map(
        local,
        mesh=mesh,
        in_specs=(
            P(None, "gy", "gx", None),
            P(None, "gy", "gx", None),
            P(None, "gy", None),
            P("section", None, "gy", "gx", None),
            P("section", None, "gy", "gx", None),
            P("section", None),
            P("section", None),
            P("section", None),
            P("section", None),
            P("section", "gy", "gx"),
            P("section", "gy", None),
            P("section", "gy", None),
            P("section", "gy", "gx"),
            P("section", ("gx", "gy"), None, None),
            P("section", ("gx", "gy"), None, None),
            P("section", ("gx", "gy"), None, None),
        ),
        out_specs=(
            P("section", None, "gy", "gx", None),
            P("section", None, "gy", "gx", None),
            P("section", None),
            P("section", None),
            P("section", None),
            P("section", None),
            P("section", "gy", "gx"),
            P("section", "gy", None),
            P("section", "gy", None),
            P("section", "gy", "gx"),
            P("section", ("gx", "gy"), None, None),
            P("section", ("gx", "gy"), None, None),
            P("section", ("gx", "gy"), None, None),
        ),
        check_vma=False,
    )
```

```python
import functools
import math

import jax
import jax.numpy as jnp
from jax import lax
from jax.experimental import pallas as pl
from jax.experimental.pallas import tpu as pltpu
from jax.sharding import PartitionSpec as P

HQ = 32
KVH = 4
HD = 128
TOPK = 8

EPSILON = 1e-06
ROPE_BASE = 1000000.0
ROW_PAIR = (((0,), (0,)), ((), ()))
COL_PAIR = (((1,), (1,)), ((), ()))
F32 = jnp.float32
BF16 = jnp.bfloat16
MOST_ROWS = 1024


def normalize(tensor):
    scaling = lax.rsqrt(jnp.mean(tensor * tensor, axis=-1, keepdims=True) + EPSILON)
    return (tensor * scaling, scaling)


def norm_back(gradient, unit_vec, scaling):
    return scaling * (gradient - unit_vec * jnp.mean(gradient * unit_vec, axis=-1, keepdims=True))


def rotate(tensor, cosine, sine_part):
    halfway = tensor.shape[-1] // 2
    leading = tensor[..., :halfway]
    trailing = tensor[..., halfway:]
    return jnp.concatenate(
        [leading * cosine - trailing * sine_part, trailing * cosine + leading * sine_part], axis=-1
    )


def rotate_back(gradient, cosine, sine_part):
    return rotate(gradient, cosine, -sine_part)


def seq_tables(segment_ids, head_dim):
    length_all = segment_ids.shape[-1]
    position_ids = jnp.arange(length_all, dtype=jnp.int32)
    allowed = (segment_ids[:, :, None] == segment_ids[:, None, :]) & (
        position_ids[:, None] >= position_ids[None, :]
    )
    positions = jnp.sum(allowed.astype(jnp.int32), axis=-1) - 1
    halfway = head_dim // 2
    inverse = ROPE_BASE ** (-2.0 * jnp.arange(halfway, dtype=jnp.float32) / head_dim)
    angles = positions.astype(jnp.float32)[..., None] * inverse
    return (allowed, jnp.cos(angles), jnp.sin(angles))


def dot32(left, right, dims=None):
    if dims is None:
        return jnp.dot(left, right, preferred_element_type=F32)
    return lax.dot_general(left, right, dims, preferred_element_type=F32)


def gather_z(rows):
    return lax.all_gather(rows, "gx", axis=1, tiled=True)


def scatter_z(rows):
    return lax.psum_scatter(rows, "gx", scatter_dimension=1, tiled=True)


def gather_all(rows):
    return lax.all_gather(rows, ("gx", "gy"), axis=0, tiled=True)


def scatter_all(rows):
    return lax.psum_scatter(rows, ("gx", "gy"), scatter_dimension=0, tiled=True)


def both_layers(tensor):
    return lax.all_gather(tensor, "section", axis=0, tiled=False)


def dense_gates(route_ids, gate_vals, experts):
    onehot = route_ids[..., None] == jnp.arange(experts, dtype=jnp.int32)
    return jnp.sum(jnp.where(onehot, gate_vals[..., None], 0.0), axis=-2)


def swap_sections(tensor):
    return lax.ppermute(tensor, "section", [(0, 1), (1, 0)])


def remote(src, dst, send_sem, recv_sem, **where):
    return pltpu.make_async_remote_copy(
        src_ref=src,
        dst_ref=dst,
        send_sem=send_sem,
        recv_sem=recv_sem,
        device_id=where,
        device_id_type=pl.DeviceIdType.MESH,
    )


def hello(n, me, gy, with_plane, with_section=False):
    barrier = pltpu.get_barrier_semaphore()
    mesh_ids = pl.DeviceIdType.MESH

    @pl.when(me + 1 < n)
    def _():
        pl.semaphore_signal(barrier, 1, device_id={"gx": me + 1}, device_id_type=mesh_ids)

    @pl.when(me > 0)
    def _():
        pl.semaphore_signal(barrier, 1, device_id={"gx": me - 1}, device_id_type=mesh_ids)

    peers = 0
    if with_plane:
        for bit in (1, 2):
            pl.semaphore_signal(
                barrier, 1, device_id={"gy": gy_flip(gy, bit)}, device_id_type=mesh_ids
            )
        peers += 2
    if with_section:
        other = 1 - lax.axis_index("section")
        pl.semaphore_signal(barrier, 1, device_id={"section": other}, device_id_type=mesh_ids)
        peers += 1
    at_end = (me == 0) | (me == n - 1)

    @pl.when(at_end)
    def _():
        pl.semaphore_wait(barrier, peers + 1)

    @pl.when(jnp.logical_not(at_end))
    def _():
        pl.semaphore_wait(barrier, peers + 2)


def gy_flip(gy, bits):
    low = lax.rem(gy, 2)
    high = gy // 2
    if bits & 1:
        low = 1 - low
    if bits & 2:
        high = 1 - high
    return high * 2 + low


def z_gather_steps(n, me, slot, sems, after):
    send_up, recv_up, send_down, recv_down = sems
    sends = []

    def up(k):
        return remote(slot(me - k), slot(me - k), send_up.at[k], recv_up.at[k], gx=me + 1)

    def down(k):
        return remote(slot(me + k), slot(me + k), send_down.at[k], recv_down.at[k], gx=me - 1)

    for k in range(n):
        @pl.when(me - k >= 0)
        def _():
            if k:
                remote(
                    slot(me - k), slot(me - k), send_up.at[k - 1], recv_up.at[k - 1], gx=me
                ).wait_recv()
            if k < n - 1:

                @pl.when(me + 1 < n)
                def _():
                    up(k).start()

            if k == 0:

                @pl.when(me > 0)
                def _():
                    down(0).start()

            after(me - k, k)

        if k:

            @pl.when(me + k < n)
            def _():
                remote(
                    slot(me + k), slot(me + k), send_down.at[k - 1], recv_down.at[k - 1], gx=me
                ).wait_recv()
                if k < n - 1:

                    @pl.when(me > 0)
                    def _():
                        down(k).start()

                after(me + k, k)


def z_gather_drain(n, me, slot, sems):
    send_up, recv_up, send_down, recv_down = sems
    for k in range(n - 1):

        @pl.when((me - k >= 0) & (me + 1 < n))
        def _():
            remote(slot(me - k), slot(me - k), send_up.at[k], recv_up.at[k], gx=me + 1).wait_send()

        @pl.when((me + k < n) & (me > 0))
        def _():
            remote(
                slot(me + k), slot(me + k), send_down.at[k], recv_down.at[k], gx=me - 1
            ).wait_send()


def flip_by(gy, step):
    low = lax.rem(lax.rem(gy, 2) + lax.rem(step, 2), 2)
    high = lax.rem(gy // 2 + step // 2, 2)
    return high * 2 + low


class Plane:
    def __init__(self, n, sems):
        self.n = n
        self.me = lax.axis_index("gx")
        self.gy = lax.axis_index("gy")
        self.cx, self.cy, self.cd = (gy_flip(self.gy, bits) for bits in (1, 2, 3))
        self.gather_sems = sems[:10]
        self.scatter_sems = sems[10:]


    def gather_own_column(self, slot):
        su, ru, sd, rd, sx, rx, sy, ry, sf, rf = self.gather_sems
        c = self.gy

        def after(z, k):
            remote(slot(z, c), slot(z, c), sx.at[z], rx.at[z], gy=self.cx).start()
            remote(slot(z, c), slot(z, c), sy.at[z], ry.at[z], gy=self.cy).start()

        z_gather_steps(self.n, self.me, lambda z: slot(z, c), (su, ru, sd, rd), after)

    def gather_pass_on(self, slot):
        su, ru, sd, rd, sx, rx, sy, ry, sf, rf = self.gather_sems

        def forward(z):
            remote(slot(z, self.cx), slot(z, self.cx), sx.at[z], rx.at[z], gy=self.cx).wait_recv()
            remote(slot(z, self.cy), slot(z, self.cy), sy.at[z], ry.at[z], gy=self.cy).wait_recv()

            @pl.when(lax.rem(z, 2) == 0)
            def _():
                remote(
                    slot(z, self.cy), slot(z, self.cy), sf.at[z], rf.at[z], gy=self.cx
                ).start()

            @pl.when(lax.rem(z, 2) == 1)
            def _():
                remote(
                    slot(z, self.cx), slot(z, self.cx), sf.at[z], rf.at[z], gy=self.cy
                ).start()

        for k in range(self.n):

            @pl.when(self.me - k >= 0)
            def _():
                forward(self.me - k)

            if k:

                @pl.when(self.me + k < self.n)
                def _():
                    forward(self.me + k)

    def gather_far_column(self, slot):
        sf, rf = self.gather_sems[8:]
        for z in range(self.n):
            remote(slot(z, self.cd), slot(z, self.cd), sf.at[z], rf.at[z], gy=self.cx).wait_recv()

    def gather_drain(self, slot):
        su, ru, sd, rd, sx, rx, sy, ry, sf, rf = self.gather_sems
        z_gather_drain(self.n, self.me, lambda z: slot(z, self.gy), (su, ru, sd, rd))
        for z in range(self.n):
            one = slot(z, self.gy)
            remote(one, one, sx.at[z], rx.at[z], gy=self.cx).wait_send()
            remote(one, one, sy.at[z], ry.at[z], gy=self.cy).wait_send()
            remote(one, one, sf.at[z], rf.at[z], gy=self.cx).wait_send()


    def scatter_setup(self, part, sides, din, zup, zdn, stage, acc):
        self.part, self.sides, self.din = part, sides, din
        self.zup, self.zdn, self.stage, self.acc = zup, zdn, stage, acc

    def column_of(self, side):
        return self.cx * (1 - side) + self.cy * side

    def near(self, side, z):
        send, recv = self.scatter_sems[4:6]
        column = self.column_of(side)
        return remote(
            self.part(z, column), self.sides.at[side, z], send.at[side, z], recv.at[side, z], gy=column
        )

    def far(self, z):
        send, recv = self.scatter_sems[6:]
        return remote(
            self.part(z, self.cd),
            self.din.at[z],
            send.at[z],
            recv.at[z],
            gy=self.column_of(lax.rem(z, 2)),
        )

    def each(self, call):
        for k in [sign * far for far in reversed(range(1, self.n)) for sign in (-1, 1)] + [0]:

            @pl.when((self.me + k >= 0) & (self.me + k < self.n))
            def _():
                call(self.me + k, k)

    def scatter_near(self, side):
        def send(z, k):
            if abs(k) > 1:

                @pl.when(lax.rem(z, 2) == side)
                def _():
                    self.near(side, z).start()

        self.each(send)

    def scatter_far(self):
        self.each(lambda z, k: self.far(z).start())

    def scatter_pass_on(self, z, k):
        self.far(z).wait_recv()
        side = 1 - lax.rem(z, 2)
        mine = self.part(z, self.column_of(side))
        add_rows(mine, mine, self.din.at[z])
        self.near(side, z).start()
        if abs(k) < 2:
            self.near(1 - side, z).start()

    def along(self, z, up):
        send, recv = self.scatter_sems[:2] if up else self.scatter_sems[2:4]
        into = self.zup if up else self.zdn
        return remote(
            self.stage.at[z],
            into.at[z],
            send.at[z],
            recv.at[z],
            gx=self.me + 1 if up else self.me - 1,
        )

    def scatter_line(self, total, z, k):
        n, me, acc = self.n, self.me, self.acc
        self.near(0, z).wait_recv()
        self.near(1, z).wait_recv()
        terms = (self.part(z, self.gy), self.sides.at[0, z], self.sides.at[1, z])
        if k == 0:
            add_rows(total, *terms)
            return
        came = me > 0 if k > 0 else me < n - 1

        @pl.when(came)
        def _():
            self.along(z, k > 0).wait_recv()
            add_rows(self.stage.at[z], *terms, (self.zup if k > 0 else self.zdn).at[z])

        @pl.when(jnp.logical_not(came))
        def _():
            add_rows(self.stage.at[z], *terms)

        self.along(z, k > 0).start()

    def scatter_finish(self, total):
        n, me = self.n, self.me

        @pl.when(me > 0)
        def _():
            self.along(me, True).wait_recv()
            add_rows(total, total, self.zup.at[me])

        @pl.when(me < n - 1)
        def _():
            self.along(me, False).wait_recv()
            add_rows(total, total, self.zdn.at[me])

        for z in range(n):
            self.near(0, z).wait_send()
            self.near(1, z).wait_send()
            self.far(z).wait_send()

            @pl.when(me < z)
            def _():
                self.along(z, True).wait_send()

            @pl.when(me > z)
            def _():
                self.along(z, False).wait_send()


def add_rows(out, *terms):
    rows = out.shape[0]
    step = 16
    short = len(terms) == 2 and all(ref.dtype == BF16 for ref in (out, *terms))
    kind = BF16 if short else F32

    def body(i, carry):
        at = pl.ds(pl.multiple_of(i * step, step), step)
        value = terms[0][at].astype(kind)
        for term in terms[1:]:
            value = value + term[at].astype(kind)
        out[at] = value.astype(out.dtype)
        return carry

    lax.fori_loop(0, rows // step, body, 0)


def fetch_layer(layer, own, other, held, sems):
    section = lax.axis_index("section")

    @pl.when(section == layer)
    def _():
        for k, ref in enumerate(own):
            pltpu.make_async_copy(ref, held[k], sems.at[k]).start()

    @pl.when(section != layer)
    def _():
        for k, ref in enumerate(other):
            pltpu.make_async_copy(ref, held[k], sems.at[k]).start()


def fetch_wait(own, held, sems, which):
    for k in which:
        pltpu.make_async_copy(own[k], held[k], sems.at[k]).wait()


def moe_forward_kernel(
    n,
    layer,
    mid_ref,
    pay_ref,
    wg_own,
    wu_own,
    wd_own,
    wg_other,
    wu_other,
    wd_other,
    out_ref,
    arrived_ref,
    weight_ref,
    gp_ref,
    up_ref,
    inner_ref,
    pay,
    wg,
    wu,
    wd,
    part,
    sides,
    din,
    zup,
    zdn,
    stage,
    acc,
    total,
    gp,
    up,
    inner,
    wsem,
    osem,
    *sems,
):
    r, d = mid_ref.shape
    ff = wg.shape[1]
    rows = n * r
    experts = 4 * n
    own, other, held = (
        (wg_own, wu_own, wd_own),
        (wg_other, wu_other, wd_other),
        (wg, wu, wd),
    )
    fetch_layer(layer, own, other, held, wsem)
    plane = Plane(n, sems)
    me, gy = plane.me, plane.gy
    hello(n, me, gy, True)
    pay[pl.ds(pl.multiple_of((gy * n + me) * r, r), r)] = pay_ref[...]

    def slot(z, c):
        return pay.at[pl.ds((c * n + z) * r, r)]

    plane.scatter_setup(lambda z, c: part.at[c * n + z], sides, din, zup, zdn, stage, acc)
    plane.gather_own_column(slot)
    fetch_wait(own, held, wsem, range(3))
    expert = me * 4 + gy

    def column(s, carry):
        c = flip_by(gy, s)

        @pl.when(s == 1)
        def _():
            plane.gather_pass_on(slot)

        @pl.when(s == 3)
        def _():
            plane.gather_far_column(slot)

        at = pl.ds(pl.multiple_of(c * rows, rows), rows)
        gate_cols = pay[at, d : d + 128].astype(F32)
        lane = lax.broadcasted_iota(jnp.int32, (rows, 128), 1)
        hit = ((lane == expert) | (lane == expert + experts)) & (lane < 2 * experts)
        weight = jnp.sum(jnp.where(hit, gate_cols, 0.0), axis=1, keepdims=True)
        weight_ref[at] = weight
        block = pay[at, :d]

        def mid_cols(j, carry):
            cols = pl.ds(pl.multiple_of(j * 256, 256), 256)
            g = jnp.dot(block, wg[:, cols], preferred_element_type=F32)
            u = jnp.dot(block, wu[:, cols], preferred_element_type=F32)
            gp[at, cols] = g.astype(BF16)
            up[at, cols] = u.astype(BF16)
            inner[at, cols] = (g / (1.0 + jnp.exp(-g)) * u).astype(BF16)
            return carry

        lax.fori_loop(0, ff // 256, mid_cols, 0)
        act = inner[at]

        def out_cols(j, carry):
            cols = pl.ds(pl.multiple_of(j * 256, 256), 256)
            res = jnp.dot(act, wd[:, cols], preferred_element_type=F32) * weight
            part[pl.ds(pl.multiple_of(c * n, n), n), :, cols] = (
                res.astype(BF16).reshape(n, r, 256)
            )
            return carry

        lax.fori_loop(0, d // 256, out_cols, 0)

        @pl.when(s == 1)
        def _():
            plane.scatter_near(0)

        @pl.when(s == 2)
        def _():
            plane.scatter_near(1)

        return carry

    lax.fori_loop(0, 4, column, 0)
    plane.scatter_far()
    saves = [
        pltpu.make_async_copy(pay.at[:, pl.ds(0, d)], arrived_ref, osem.at[0]),
        pltpu.make_async_copy(gp, gp_ref, osem.at[1]),
        pltpu.make_async_copy(up, up_ref, osem.at[2]),
        pltpu.make_async_copy(inner, inner_ref, osem.at[3]),
    ]
    for save in saves:
        save.start()
    plane.each(plane.scatter_pass_on)
    plane.each(functools.partial(plane.scatter_line, total))
    plane.scatter_finish(total)
    add_rows(out_ref, mid_ref, total)
    plane.gather_drain(slot)
    for save in saves:
        save.wait()


def scatter_buffers(n, r, d):
    block = pltpu.VMEM((n, r, d), BF16)
    return [
        pltpu.VMEM((4 * n, r, d), BF16),
        pltpu.VMEM((2, n, r, d), BF16),
        *[block] * 4,
        *[pltpu.VMEM((r, d), F32)] * 2,
    ]


def in_vmem(count):
    return [pl.BlockSpec(memory_space=pltpu.VMEM)] * count


def in_place(count):
    return [pl.BlockSpec(memory_space=pl.ANY)] * count


def moe_forward(layer, n, mid, payload, own, other, cid):
    r, d = mid.shape
    ff = own[0].shape[1]
    total_rows = 4 * n * r
    width = payload.shape[1]
    return pl.pallas_call(
        functools.partial(moe_forward_kernel, n, layer),
        out_shape=(
            jax.ShapeDtypeStruct((r, d), BF16),
            jax.ShapeDtypeStruct((total_rows, d), BF16),
            jax.ShapeDtypeStruct((total_rows, 1), F32),
            jax.ShapeDtypeStruct((total_rows, ff), BF16),
            jax.ShapeDtypeStruct((total_rows, ff), BF16),
            jax.ShapeDtypeStruct((total_rows, ff), BF16),
        ),
        in_specs=in_vmem(2) + in_place(6),
        out_specs=tuple(in_vmem(1) + in_place(1) + in_vmem(1) + in_place(3)),
        scratch_shapes=[
            pltpu.VMEM((total_rows, width), BF16),
            pltpu.VMEM((d, ff), BF16),
            pltpu.VMEM((d, ff), BF16),
            pltpu.VMEM((ff, d), BF16),
        ]
        + scatter_buffers(n, r, d)
        + [pltpu.VMEM((total_rows, ff), BF16)] * 3
        + [pltpu.SemaphoreType.DMA((3,)), pltpu.SemaphoreType.DMA((4,))]
        + [pltpu.SemaphoreType.DMA((n,))] * 14
        + [pltpu.SemaphoreType.DMA((2, n))] * 2
        + [pltpu.SemaphoreType.DMA((n,))] * 2,
        compiler_params=pltpu.CompilerParams(
            collective_id=cid, has_side_effects=True, vmem_limit_bytes=63 << 20
        ),
        name="moe_forward",
    )(mid, payload, *own, *other)


def moe_backward_kernel(
    n,
    layer,
    cot_ref,
    mid_ref,
    gain_ref,
    weight_ref,
    arrived_hbm,
    gp_hbm,
    up_hbm,
    inner_hbm,
    wg_own,
    wu_own,
    wd_own,
    wg_other,
    wu_other,
    wd_other,
    *rest,
):
    rest = rest[0 if layer else 6 :]
    dmid_ref, dgain_ref = rest[:2]
    keep_refs, give_refs = rest[2:5], rest[5:8]
    (
    cots,
    wg,
    wu,
    wd,
    part,
    sides,
    din,
    zup,
    zdn,
    stage,
    acc,
    total,
    arrived,
    gp,
    up,
    inner,
    de,
    out_gate,
    out_up,
    out_down,
    wsem,
    isem,
    osem,
    *sems,
    ) = rest[8:]
    section = lax.axis_index("section")
    r, d = mid_ref.shape
    ff = wg.shape[1]
    rows = n * r
    own, other, held = (
        (wg_own, wu_own, wd_own),
        (wg_other, wu_other, wd_other),
        (wg, wu, wd),
    )
    loads = [
        pltpu.make_async_copy(gp_hbm, gp, isem.at[0]),
        pltpu.make_async_copy(up_hbm, up, isem.at[1]),
        pltpu.make_async_copy(arrived_hbm, arrived, isem.at[2]),
        pltpu.make_async_copy(inner_hbm, inner, isem.at[3]),
    ]
    fetch_layer(layer, own, other, held, wsem)
    for load in loads:
        load.start()
    plane = Plane(n, sems)
    me, gy = plane.me, plane.gy
    hello(n, me, gy, True)
    cots[pl.ds(pl.multiple_of((gy * n + me) * r, r), r)] = cot_ref[...]

    def slot(z, c):
        return cots.at[pl.ds((c * n + z) * r, r)]

    plane.scatter_setup(lambda z, c: part.at[c * n + z], sides, din, zup, zdn, stage, acc)
    plane.gather_own_column(slot)
    fetch_wait(own, held, wsem, range(3))
    for load in loads:
        load.wait()

    def column(s, carry):
        c = flip_by(gy, s)

        @pl.when(s == 1)
        def _():
            plane.gather_pass_on(slot)

        @pl.when(s == 3)
        def _():
            plane.gather_far_column(slot)

        at = pl.ds(pl.multiple_of(c * rows, rows), rows)
        de[at] = (cots[at].astype(F32) * weight_ref[at]).astype(BF16)
        block = de[at]

        def mid_cols(j, carry):
            cols = pl.ds(pl.multiple_of(j * 256, 256), 256)
            dz = dot32(block, wd[cols], COL_PAIR)
            g = gp[at, cols].astype(F32)
            u = up[at, cols].astype(F32)
            sg = 1.0 / (1.0 + jnp.exp(-g))
            gp[at, cols] = (dz * u * sg * (1.0 + g * (1.0 - sg))).astype(BF16)
            up[at, cols] = (dz * g * sg).astype(BF16)
            return carry

        lax.fori_loop(0, ff // 256, mid_cols, 0)
        dgp = gp[at]
        dup = up[at]

        def in_cols(j, carry):
            cols = pl.ds(pl.multiple_of(j * 256, 256), 256)
            res = dot32(dgp, wg[cols], COL_PAIR) + dot32(dup, wu[cols], COL_PAIR)
            part[pl.ds(pl.multiple_of(c * n, n), n), :, cols] = (
                res.astype(BF16).reshape(n, r, 256)
            )
            return carry

        lax.fori_loop(0, d // 256, in_cols, 0)

        @pl.when(s == 1)
        def _():
            plane.scatter_near(0)

        @pl.when(s == 2)
        def _():
            plane.scatter_near(1)

        return carry

    lax.fori_loop(0, 4, column, 0)
    plane.scatter_far()

    def saving(i, refs):
        at = pl.ds(pl.multiple_of(i * 256, 256), 256)
        for k, (src, ref) in enumerate(zip((out_gate, out_up, out_down), refs)):
            where = (slice(None), at) if k == 2 else (at, slice(None))
            yield pltpu.make_async_copy(src.at[where], ref.at[where], osem.at[k, i])

    chunks = d // 256

    def weight_grads(i, carry):
        at = pl.ds(pl.multiple_of(i * 256, 256), 256)
        left = arrived[:, at]
        out_gate[at] = dot32(left, gp[...], ROW_PAIR).astype(BF16)
        out_up[at] = dot32(left, up[...], ROW_PAIR).astype(BF16)
        out_down[:, at] = dot32(inner[...], de[:, at], ROW_PAIR).astype(BF16)

        @pl.when(section == layer)
        def _():
            for copy in saving(i, keep_refs):
                copy.start()

        @pl.when(section != layer)
        def _():
            for copy in saving(i, give_refs):
                copy.start()

        @pl.when(i == chunks // 4 - 1)
        def _():
            plane.each(plane.scatter_pass_on)

        @pl.when(i == chunks // 2 - 1)
        def _():
            plane.each(functools.partial(plane.scatter_line, total))

        return carry

    lax.fori_loop(0, chunks, weight_grads, 0)
    plane.scatter_finish(total)

    mid = mid_ref[...]
    scale = lax.rsqrt(jnp.mean(mid * mid, axis=-1, keepdims=True) + EPSILON)
    unit = mid * scale
    db = total[...]
    dgain_ref[...] = jnp.sum(db * unit, axis=0, keepdims=True)
    dmid_ref[...] = cot_ref[...].astype(F32) + norm_back(db * gain_ref[...], unit, scale)
    plane.gather_drain(slot)

    def settle(i, carry):
        for copy in saving(i, keep_refs):
            copy.wait()
        return carry

    lax.fori_loop(0, chunks, settle, 0)


def moe_backward(layer, n, cot, mid, gain, weight, arrived, gp, up, inner, own, other, so_far, cid):
    r, d = mid.shape
    ff = own[0].shape[1]
    total_rows = 4 * n * r
    sums = [jax.ShapeDtypeStruct(shape, BF16) for shape in ((d, ff), (d, ff), (ff, d))] * 2
    return pl.pallas_call(
        functools.partial(moe_backward_kernel, n, layer),
        out_shape=(
            jax.ShapeDtypeStruct((r, d), F32),
            jax.ShapeDtypeStruct((1, d), F32),
            *sums,
        ),
        in_specs=in_vmem(4) + in_place(10 + len(so_far)),
        out_specs=tuple(in_vmem(2) + in_place(6)),
        input_output_aliases={14 + k: 2 + k for k in range(len(so_far))},
        scratch_shapes=[
            pltpu.VMEM((total_rows, d), BF16),
            pltpu.VMEM((d, ff), BF16),
            pltpu.VMEM((d, ff), BF16),
            pltpu.VMEM((ff, d), BF16),
        ]
        + scatter_buffers(n, r, d)
        + [pltpu.VMEM((total_rows, d), BF16)]
        + [pltpu.VMEM((total_rows, ff), BF16)] * 3
        + [pltpu.VMEM((total_rows, d), BF16)]
        + [pltpu.VMEM((d, ff), BF16)] * 2
        + [pltpu.VMEM((ff, d), BF16)]
        + [
            pltpu.SemaphoreType.DMA((3,)),
            pltpu.SemaphoreType.DMA((4,)),
        ]
        + [pltpu.SemaphoreType.DMA((3, d // 256))]
        + [pltpu.SemaphoreType.DMA((n,))] * 14
        + [pltpu.SemaphoreType.DMA((2, n))] * 2
        + [pltpu.SemaphoreType.DMA((n,))] * 2,
        compiler_params=pltpu.CompilerParams(
            collective_id=cid, has_side_effects=True, vmem_limit_bytes=63 << 20
        ),
        name="moe_backward",
    )(cot, mid, gain, weight, arrived, gp, up, inner, *own, *other, *so_far)


class Share:
    def __init__(self, layer, pieces, full, scratch):
        self.full = full
        self.held, self.load_sems, self.plane_sems, self.to_sems, self.from_sems = scratch
        self.loads, first = [], 0
        for k, piece in enumerate(pieces):
            last = first + piece.shape[1]
            into = self.held.at[:, first:last]
            self.loads.append(pltpu.make_async_copy(piece, into, self.load_sems.at[k]))
            first = last
        self.section = lax.axis_index("section")
        self.mine = self.section == layer
        gy = lax.axis_index("gy")
        self.cols = [gy_flip(gy, bits) if bits else gy for bits in range(4)]
        self.rows = self.held.shape[0]

    def at(self, column, half=None):
        rows = self.rows
        if half is None:
            return self.full.at[pl.ds(pl.multiple_of(column * rows, rows), rows)]
        few = rows // 2
        return self.full.at[pl.ds(pl.multiple_of(column * rows + half * few, few), few)]

    def own(self):
        return pltpu.make_async_copy(self.held, self.at(self.cols[0]), self.plane_sems.at[0])

    def direct(self, bit):
        s = self.plane_sems
        k = 1 if bit == 1 else 3
        return remote(
            self.held, self.at(self.cols[0]), s.at[k], s.at[k + 1], gy=self.cols[bit]
        )

    def onward(self, bit):
        s = self.plane_sems
        k = 5 if bit == 1 else 7
        half = 1 if bit == 1 else 0
        ref = self.at(self.cols[3 - bit], half)
        return remote(ref, ref, s.at[k], s.at[k + 1], gy=self.cols[bit])

    def hand(self, k):
        if k == 0:
            src, dst = self.held, self.at(self.cols[0])
        elif k < 3:
            src = dst = self.at(self.cols[k])
        else:
            src = dst = self.at(self.cols[3], k - 3)
        return remote(src, dst, self.to_sems.at[k], self.from_sems.at[k], section=1 - self.section)

    def start(self):
        @pl.when(self.mine)
        def _():
            for load in self.loads:
                load.start()
            for load in self.loads:
                load.wait()
            self.direct(1).start()
            self.direct(2).start()
            self.own().start()
            self.hand(0).start()

    def pass_on(self):
        @pl.when(self.mine)
        def _():
            self.direct(1).wait_recv()
            self.onward(2).start()
            self.hand(1).start()
            self.direct(2).wait_recv()
            self.onward(1).start()
            self.hand(2).start()

    def finish(self):
        @pl.when(self.mine)
        def _():
            self.onward(2).wait_recv()
            self.hand(3).start()
            self.onward(1).wait_recv()
            self.hand(4).start()
            self.own().wait()

        @pl.when(jnp.logical_not(self.mine))
        def _():
            for k in range(5):
                self.hand(k).wait_recv()

    def drain(self):
        @pl.when(self.mine)
        def _():
            for bit in (1, 2):
                self.direct(bit).wait_send()
                self.onward(bit).wait_send()
            for k in range(5):
                self.hand(k).wait_send()


def share_scratch(shape):
    dma = pltpu.SemaphoreType.DMA
    return [pltpu.VMEM(shape, BF16), dma((3,)), dma((9,)), dma((5,)), dma((5,))]


def shard_pieces(query, key, value, out):
    heads = query.shape[2] // HD
    kv_head = lax.axis_index("gx") * heads // (HQ // KVH)
    own = pl.ds(pl.multiple_of(kv_head * HD, HD), HD)
    return [(query.at[0], key.at[0, :, own], value.at[0, :, own]), (out.at[0],)]


def shard_shapes(shards):
    rows, span = shards[0].shape[1:]
    return [(rows, span + 2 * HD), (rows, span)]


def full_shapes(shards):
    return [jax.ShapeDtypeStruct((4 * rows, cols), BF16) for rows, cols in shard_shapes(shards)]


def share_kernel(n, layer, few, *refs):
    shards, smalls = refs[:4], refs[4 : 4 + few]
    fulls, others = refs[4 + few : 6 + few], refs[6 + few : 6 + 2 * few]
    send, recv, *scratch = refs[6 + 2 * few :]
    other = 1 - lax.axis_index("section")
    swaps = [
        remote(smalls[k], others[k], send.at[k], recv.at[k], section=other) for k in range(few)
    ]
    shares = [
        Share(layer, pieces, fulls[k], scratch[5 * k : 5 * k + 5])
        for k, pieces in enumerate(shard_pieces(*shards))
    ]
    hello(n, lax.axis_index("gx"), lax.axis_index("gy"), True, True)
    for share in shares:
        share.start()
    for swap in swaps:
        swap.start()
    for share in shares:
        share.pass_on()
    for share in shares:
        share.finish()
    for share in shares:
        share.drain()
    for swap in swaps:
        swap.wait()


def share_weights(layer, n, shards, smalls, cid):
    few = len(smalls)
    return pl.pallas_call(
        functools.partial(share_kernel, n, layer, few),
        out_shape=(
            *full_shapes(shards),
            *(jax.ShapeDtypeStruct(small.shape, small.dtype) for small in smalls),
        ),
        in_specs=in_place(4 + few),
        out_specs=tuple(in_place(2 + few)),
        scratch_shapes=[pltpu.SemaphoreType.DMA((few,))] * 2
        + [item for shape in shard_shapes(shards) for item in share_scratch(shape)],
        compiler_params=pltpu.CompilerParams(collective_id=cid, has_side_effects=True),
        name="share_weights",
    )(*shards, *smalls)


def finish_line_kernel(n, *refs):
    gains, rest = refs[:8], refs[8:]
    kv_ref, gain_ref, key_ref, value_ref, gbuf, kv_all, stage, incoming, rsem, *sems = rest
    me = lax.axis_index("gx")
    gy = lax.axis_index("gy")
    kv_all[me] = kv_ref[...]
    for k in range(2):
        first = 0
        for ref in gains[4 * k : 4 * k + 4]:
            last = first + ref.shape[1]
            gbuf[me, k : k + 1, first:last] = ref[...]
            first = last
    hello(n, me, gy, True)
    few = Line(n, None, lambda z: gbuf.at[z], None, sems[:4])
    many = Line(n, None, lambda z: kv_all.at[z], None, sems[4:8])
    few.gather_step(0)
    many.gather_step(0)
    steps = [functools.partial(many.gather_step, k) for k in range(1, n)]
    for k in range(1, n):
        few.gather_step(k)
        if k == n // 2:
            steps.pop(0)()
    total = gbuf[0]
    for z in range(1, n):
        total = total + gbuf[z]
    for k, where in enumerate(({"gy": gy_flip(gy, 1)}, {"gy": gy_flip(gy, 2)})):
        stage[k] = total
        swap = remote(stage.at[k], incoming.at[k], rsem.at[0, k], rsem.at[1, k], **where)
        swap.start()
        if steps:
            steps.pop(0)()
        swap.wait()
        total = total + incoming[k]
    gain_ref[...] = total
    for step in steps:
        step()
    for z in range(n):
        cols = slice(z * HD, (z + 1) * HD)
        key_ref[:, cols] = kv_all[z, :, :HD].astype(F32)
        value_ref[:, cols] = kv_all[z, :, HD:].astype(F32)
    few.gather_drain()
    many.gather_drain()


def finish_line(n, gains, kv, cid):
    dma = pltpu.SemaphoreType.DMA
    shape = jax.ShapeDtypeStruct
    width = sum(gain.shape[1] for gain in gains[:4])
    return pl.pallas_call(
        functools.partial(finish_line_kernel, n),
        out_shape=(
            shape((2, width), F32),
            shape((kv.shape[0], n * HD), F32),
            shape((kv.shape[0], n * HD), F32),
        ),
        in_specs=in_vmem(9),
        out_specs=tuple(in_vmem(3)),
        scratch_shapes=[
            pltpu.VMEM((n, 2, width), F32),
            pltpu.VMEM((n,) + kv.shape, BF16),
            pltpu.VMEM((2, 2, width), F32),
            pltpu.VMEM((2, 2, width), F32),
            dma((2, 2)),
        ]
        + [dma((n,))] * 8,
        compiler_params=pltpu.CompilerParams(collective_id=cid, has_side_effects=True),
        name="finish_line",
    )(*gains, kv)


def finish_pair_kernel(*refs):
    gain_ref, *rows = refs[:5]
    out_rows, out_gains = refs[5:7], refs[7:11]
    incoming, send, recv = refs[11:]
    section = lax.axis_index("section")
    other = 1 - section
    barrier = pltpu.get_barrier_semaphore()
    mesh_ids = pl.DeviceIdType.MESH
    pl.semaphore_signal(barrier, 1, device_id={"section": other}, device_id_type=mesh_ids)
    pl.semaphore_wait(barrier, 1)
    swap = remote(gain_ref, incoming, send.at[2], recv.at[2], section=other)
    swap.start()
    for mine in range(2):

        @pl.when(section == mine)
        def _():
            for k in range(2):
                src, dst = rows[2 * k + 1 - mine], out_rows[k].at[mine]
                remote(src, dst, send.at[k], recv.at[k], section=other).start()
            for k in range(2):
                out_rows[k][mine] = rows[2 * k + mine][...]

    swap.wait()
    for mine in range(2):

        @pl.when(section == mine)
        def _():
            first = 0
            for ref in out_gains:
                last = first + ref.shape[1]
                at = (slice(mine, mine + 1), slice(first, last))
                ref[...] = gain_ref[at] + incoming[at]
                first = last
            for k in range(2):
                src, dst = rows[2 * k + 1 - mine], out_rows[k].at[mine]
                remote(src, dst, send.at[k], recv.at[k], section=other).wait()


def finish_pair(gains, widths, lo, ig, cid):
    dma = pltpu.SemaphoreType.DMA
    shape = jax.ShapeDtypeStruct
    both = shape((2,) + lo[0].shape, BF16)
    return pl.pallas_call(
        finish_pair_kernel,
        out_shape=(both, both, *(shape((1, width), F32) for width in widths)),
        in_specs=in_vmem(5),
        out_specs=tuple(in_vmem(6)),
        scratch_shapes=[pltpu.VMEM(gains.shape, F32), dma((3,)), dma((3,))],
        compiler_params=pltpu.CompilerParams(collective_id=cid, has_side_effects=True),
        name="finish_pair",
    )(gains, *lo, *ig)


class Reduce:
    def __init__(self, layer, part, inbox, xin, yin, din, sems):
        self.part, self.inbox = part, inbox
        self.xin, self.yin, self.din = xin, yin, din
        self.give_sems, self.take_sems, self.send_sems, self.recv_sems = sems
        self.section = lax.axis_index("section")
        self.mine = self.section == layer
        gy = lax.axis_index("gy")
        self.cols = [gy_flip(gy, bits) if bits else gy for bits in range(4)]
        self.few = xin.shape[0] // 2

    def give(self, k, src):
        return remote(
            src,
            self.inbox.at[self.cols[k]],
            self.give_sems.at[k],
            self.take_sems.at[k],
            section=1 - self.section,
        )

    def half(self, ref, h):
        return ref.at[pl.ds(h * self.few, self.few)]

    def far(self, bit):
        k = bit - 1
        src = self.half(self.part(self.cols[3]), k)
        return remote(
            src, self.din.at[k], self.send_sems.at[k], self.recv_sems.at[k], gy=self.cols[bit]
        )

    def near(self, bit, h):
        k = 2 * bit + h
        into = self.xin if bit == 1 else self.yin
        return remote(
            self.half(self.part(self.cols[bit]), h),
            self.half(into, h),
            self.send_sems.at[k],
            self.recv_sems.at[k],
            gy=self.cols[bit],
        )

    def send_term(self, k):
        @pl.when(self.mine)
        def _():
            ref = self.part(self.cols[k])
            self.give(k, ref).wait_recv()
            add_rows(ref, ref, self.inbox.at[self.cols[k]])
            if k == 3:
                self.far(1).start()
                self.far(2).start()
            elif k:
                self.near(k, k - 1).start()

    def pass_on(self):
        @pl.when(self.mine)
        def _():
            self.far(1).wait_recv()
            ref = self.half(self.part(self.cols[2]), 0)
            add_rows(ref, ref, self.din.at[0])
            self.near(2, 0).start()
            self.far(2).wait_recv()
            ref = self.half(self.part(self.cols[1]), 1)
            add_rows(ref, ref, self.din.at[1])
            self.near(1, 1).start()

    def close(self, outs):
        @pl.when(self.mine)
        def _():
            for bit in (1, 2):
                for h in (0, 1):
                    self.near(bit, h).wait_recv()
            for ref, first, last in outs:
                cols = slice(first, last)
                own = self.part(self.cols[0])
                add_rows(ref, own.at[:, cols], self.xin.at[:, cols], self.yin.at[:, cols])
            for bit in (1, 2):
                self.far(bit).wait_send()
                for h in (0, 1):
                    self.near(bit, h).wait_send()


def reduce_sems():
    dma = pltpu.SemaphoreType.DMA
    return [dma((4,)), dma((4,)), dma((6,)), dma((6,))]


class Line:
    def __init__(self, n, m, slot, terms, sems):
        self.n, self.m, self.slot = n, m, slot
        self.me = lax.axis_index("gx")
        if terms is not None:
            self.col, self.zup, self.zdn, self.stage = (ref.at[m] for ref in terms)
        self.sems = [sem if m is None else sem.at[m] for sem in sems]

    def gather_up(self, k):
        ref = self.slot(self.me - k)
        return remote(ref, ref, self.sems[0].at[k], self.sems[1].at[k], gx=self.me + 1)

    def gather_down(self, k):
        ref = self.slot(self.me + k)
        return remote(ref, ref, self.sems[2].at[k], self.sems[3].at[k], gx=self.me - 1)

    def gather_step(self, k):
        n, me = self.n, self.me

        @pl.when(me - k >= 0)
        def _():
            if k:
                ref = self.slot(me - k)
                sems = self.sems
                remote(ref, ref, sems[0].at[k - 1], sems[1].at[k - 1], gx=me + 1).wait_recv()
            if k < n - 1:

                @pl.when(me + 1 < n)
                def _():
                    self.gather_up(k).start()

        @pl.when(me + k < n)
        def _():
            if k:
                ref = self.slot(me + k)
                sems = self.sems
                remote(ref, ref, sems[2].at[k - 1], sems[3].at[k - 1], gx=me - 1).wait_recv()
            if k < n - 1:

                @pl.when(me > 0)
                def _():
                    self.gather_down(k).start()

    def up(self, z):
        send, recv = self.sems[4:6]
        return remote(self.stage.at[z], self.zup.at[z], send.at[z], recv.at[z], gx=self.me + 1)

    def down(self, z):
        send, recv = self.sems[6:8]
        return remote(self.stage.at[z], self.zdn.at[z], send.at[z], recv.at[z], gx=self.me - 1)

    def scatter_tick(self, hop):
        n, me = self.n, self.me

        @pl.when(me == hop)
        def _():
            for z in reversed(range(hop + 1, n)):
                if hop:
                    self.up(z).wait_recv()
                    add_rows(self.stage.at[z], self.col.at[z], self.zup.at[z])
                else:
                    add_rows(self.stage.at[z], self.col.at[z])
                self.up(z).start()

        @pl.when(me == n - 1 - hop)
        def _():
            for z in range(n - 1 - hop):
                if hop:
                    self.down(z).wait_recv()
                    add_rows(self.stage.at[z], self.col.at[z], self.zdn.at[z])
                else:
                    add_rows(self.stage.at[z], self.col.at[z])
                self.down(z).start()

    def scatter_finish(self, total):
        n, me = self.n, self.me
        add_rows(total, self.col.at[me])

        @pl.when(me > 0)
        def _():
            self.up(me).wait_recv()
            add_rows(total, total, self.zup.at[me])

        @pl.when(me < n - 1)
        def _():
            self.down(me).wait_recv()
            add_rows(total, total, self.zdn.at[me])

    def gather_drain(self):
        n, me = self.n, self.me
        for k in range(n - 1):

            @pl.when((me - k >= 0) & (me + 1 < n))
            def _():
                self.gather_up(k).wait_send()

            @pl.when((me + k < n) & (me > 0))
            def _():
                self.gather_down(k).wait_send()

    def drain(self):
        n, me = self.n, self.me
        self.gather_drain()
        for z in range(n):

            @pl.when(me < z)
            def _():
                self.up(z).wait_send()

            @pl.when(me > z)
            def _():
                self.down(z).wait_send()


def unit_of(value):
    scale = lax.rsqrt(jnp.mean(value * value, axis=-1, keepdims=True) + EPSILON)
    return value * scale, scale


def half_turn(value):
    return pltpu.roll(value, value.shape[-1] // 2, axis=value.ndim - 1)


def attn_forward_kernel(
    n,
    layer,
    heads,
    x_ref,
    gain_attn,
    gain_ffn,
    gain_query,
    gain_key,
    cos_ref,
    sin_ref,
    mask_ref,
    gates_ref,
    win_hbm,
    wout_hbm,
    *rest,
):
    ahead = layer == 0
    shards, rest = (rest[:4], rest[4:]) if ahead else ((), rest)
    mid_ref, pay_ref, normed_hbm, proj_hbm, qr_hbm, kr_ref, v_ref, prob_hbm, mixed_hbm = rest[:9]
    fulls, rest = (rest[9:11], rest[11:]) if ahead else ((), rest[9:])
    (
    win,
    wout,
    normed,
    proj,
    qr,
    prob,
    mixed,
    col,
    zup,
    zdn,
    stage,
    total,
    wsem,
    osem,
    *sems,
    ) = rest
    mb, length, d = normed.shape
    t = length // n
    r = mb * t
    span = heads * HD
    me = lax.axis_index("gx")
    shares = []
    if ahead:
        shares = [
            Share(1, pieces, fulls[k], sems[8 + 5 * k : 13 + 5 * k])
            for k, pieces in enumerate(shard_pieces(*shards))
        ]
    fetch_in = pltpu.make_async_copy(win_hbm, win, wsem.at[0])
    fetch_out = pltpu.make_async_copy(wout_hbm, wout, wsem.at[1])
    fetch_in.start()
    fetch_out.start()
    hello(n, me, lax.axis_index("gy"), ahead, ahead)
    for share in shares:
        share.start()
    hidden = x_ref[...].astype(F32)
    unit, _ = unit_of(hidden)
    low = (unit * gain_attn[...]).astype(BF16)
    normed[:, pl.ds(pl.multiple_of(me * t, t), t)] = low.reshape(mb, t, d)
    lines = [
        Line(
            n,
            m,
            lambda z, m=m: normed.at[m, pl.ds(z * t, t)],
            (col, zup, zdn, stage),
            sems[:8],
        )
        for m in range(mb)
    ]
    waiting = []

    def tick():
        if waiting:
            waiting.pop(0)()

    for k in range(n):
        lines[0].gather_step(k)
        if k == min(1, n - 1):
            for line in lines[1:]:
                line.gather_step(0)
    fetch_in.wait()
    cosine, sine = cos_ref[...], sin_ref[...]
    for m, line in enumerate(lines):
        first = m * length
        rows = slice(first, first + length)
        if m + 1 < mb:
            waiting += [functools.partial(lines[m + 1].gather_step, k) for k in range(1, n)]

        def project(j, carry, m=m, rows=rows):
            cols = pl.ds(pl.multiple_of(j * 256, 256), 256)
            proj[rows, cols] = jnp.dot(normed[m], win[:, cols], preferred_element_type=F32)
            return carry

        blocks = (span + 2 * HD) // 256
        lax.fori_loop(0, blocks // 2, project, 0)
        tick()
        lax.fori_loop(blocks // 2, blocks, project, 0)
        tick()
        key_unit, _ = unit_of(proj[rows, span : span + HD])
        key = key_unit * gain_key[...]
        kr_ref[rows] = (key * cosine[rows] + half_turn(key) * sine[rows]).astype(BF16)
        v_ref[rows] = proj[rows, span + HD :].astype(BF16)

        def head(h, carry, m=m, rows=rows):
            at = pl.ds(pl.multiple_of(h * HD, HD), HD)
            query_unit, _ = unit_of(proj[rows, at])
            query = query_unit * gain_query[...]
            turned = (query * cosine[rows] + half_turn(query) * sine[rows]).astype(BF16)
            qr[rows, at] = turned
            scores = dot32(turned, kr_ref[rows], COL_PAIR) * (1.0 / math.sqrt(HD))
            exponent = jnp.where(mask_ref[m] > 0.5, jnp.exp(scores), 0.0)
            p = (exponent * (1.0 / jnp.sum(exponent, axis=-1, keepdims=True))).astype(BF16)
            prob[m * heads + h] = p
            mixed[rows, at] = jnp.dot(p, v_ref[rows], preferred_element_type=F32).astype(BF16)
            return carry

        lax.fori_loop(0, heads // 2, head, 0, unroll=2)
        tick()
        lax.fori_loop(heads // 2, heads, head, 0, unroll=2)
        while waiting:
            tick()
        if m == mb - 1:
            for share in shares:
                share.pass_on()
        if m == 0:
            fetch_out.wait()

        def out_cols(j, carry, m=m, rows=rows):
            at = pl.ds(pl.multiple_of(j * 256, 256), 256)
            res = dot32(mixed[rows], wout[at], COL_PAIR).astype(BF16)
            for z in range(n):
                col[m, z, :, at] = res[z * t : (z + 1) * t]
            return carry

        lax.fori_loop(0, d // 256, out_cols, 0)
        line.scatter_tick(0)
        waiting += [functools.partial(line.scatter_tick, hop) for hop in range(1, n - 1)]
    saves = [
        pltpu.make_async_copy(normed, normed_hbm, osem.at[0]),
        pltpu.make_async_copy(proj, proj_hbm, osem.at[1]),
        pltpu.make_async_copy(qr, qr_hbm, osem.at[2]),
        pltpu.make_async_copy(prob, prob_hbm, osem.at[3]),
        pltpu.make_async_copy(mixed, mixed_hbm, osem.at[4]),
    ]
    for save in saves:
        save.start()
    while waiting:
        tick()
    for m, line in enumerate(lines):
        line.scatter_finish(total.at[m * t : (m + 1) * t])
    mid = x_ref[...].astype(F32) + total[...]
    mid_ref[...] = mid
    unit, _ = unit_of(mid)
    pay_ref[:, :d] = (unit * gain_ffn[...]).astype(BF16)
    pay_ref[:, d:] = gates_ref[...]
    for share in shares:
        share.finish()
    for share in shares:
        share.drain()
    for line in lines:
        line.drain()
    for save in saves:
        save.wait()


def line_buffers(mb, n, r, d):
    return [pltpu.VMEM((mb, n, r // mb, d), BF16)] * 4 + [pltpu.VMEM((r, d), F32)]


def attn_forward(layer, n, x, gains, tables, gate_cols, w_in, w_out, shards, cid, mb):
    r, d = x.shape
    cosine, sine, mask = tables
    total_rows = cosine.shape[0]
    length = total_rows // mb
    width = w_in.shape[1]
    heads = w_out.shape[1] // HD
    span = heads * HD
    shape = jax.ShapeDtypeStruct
    return pl.pallas_call(
        functools.partial(attn_forward_kernel, n, layer, heads),
        out_shape=(
            shape((r, d), F32),
            shape((r, d + 128), BF16),
            shape((mb, length, d), BF16),
            shape((total_rows, width), F32),
            shape((total_rows, span), BF16),
            shape((total_rows, HD), BF16),
            shape((total_rows, HD), BF16),
            shape((mb * heads, length, length), BF16),
            shape((total_rows, span), BF16),
            *(full_shapes(shards) if shards else ()),
        ),
        in_specs=in_vmem(9) + in_place(2 + len(shards)),
        out_specs=tuple(in_vmem(2) + in_place(3) + in_vmem(2) + in_place(4 if shards else 2)),
        scratch_shapes=[
            pltpu.VMEM((d, width), BF16),
            pltpu.VMEM((d, span), BF16),
            pltpu.VMEM((mb, length, d), BF16),
            pltpu.VMEM((total_rows, width), F32),
            pltpu.VMEM((total_rows, span), BF16),
            pltpu.VMEM((mb * heads, length, length), BF16),
            pltpu.VMEM((total_rows, span), BF16),
        ]
        + line_buffers(mb, n, r, d)
        + [pltpu.SemaphoreType.DMA((2,)), pltpu.SemaphoreType.DMA((5,))]
        + [pltpu.SemaphoreType.DMA((mb, n))] * 8
        + [
            item
            for size in (shard_shapes(shards) if shards else ())
            for item in share_scratch(size)
        ],
        compiler_params=pltpu.CompilerParams(
            collective_id=cid, has_side_effects=True, vmem_limit_bytes=60 << 20
        ),
        name="attn_forward",
    )(x, *gains, cosine, sine, mask, gate_cols, w_in, w_out, *shards)


def attn_backward_kernel(
    n,
    layer,
    heads,
    dmid_ref,
    x_ref,
    gain_attn,
    gain_query,
    gain_key,
    cos_ref,
    sin_ref,
    kr_ref,
    v_ref,
    normed_hbm,
    proj_hbm,
    qr_hbm,
    prob_hbm,
    mixed_hbm,
    win_hbm,
    wout_hbm,
    *rest,
):
    last = layer == 0
    if last:
        later_hbm, gives, rest = rest[0], rest[1:4], rest[4:]
    cot_ref, dgain_attn, dgain_query, dgain_key = rest[:4]
    outs, rest = rest[4 : 10 if last else 5], rest[10 if last else 5 :]
    (
    win,
    wout,
    normed,
    proj,
    qr,
    prob,
    mixed,
    dmids,
    dheads,
    dproj,
    dkey,
    dvalue,
    grads,
    col,
    zup,
    zdn,
    stage,
    total,
    wsem,
    isem,
    osem,
    *sems,
    ) = rest
    mb, length, d = normed.shape
    t = length // n
    span = heads * HD
    me = lax.axis_index("gx")
    inv_root = 1.0 / math.sqrt(HD)
    gy = lax.axis_index("gy")
    section = lax.axis_index("section")
    fetch_out = pltpu.make_async_copy(wout_hbm, wout, wsem.at[0])
    fetch_in = pltpu.make_async_copy(win_hbm, win, wsem.at[1])
    fetch_out.start()
    fetch_in.start()
    loads = [
        pltpu.make_async_copy(prob_hbm, prob, isem.at[0]),
        pltpu.make_async_copy(mixed_hbm, mixed, isem.at[1]),
        pltpu.make_async_copy(qr_hbm, qr, isem.at[2]),
        pltpu.make_async_copy(proj_hbm, proj, isem.at[3]),
        pltpu.make_async_copy(normed_hbm, normed, isem.at[4]),
    ]
    for load in loads:
        load.start()
    if last:
        later, inbox, xin, yin, din = sems[8:13]
        block = d // 4

        def reduce(layer, terms, first, last, sems):
            cols = slice(first, last)
            buffers = [ref.at[..., cols] for ref in (inbox, xin, yin, din)]
            return Reduce(layer, lambda c: terms.at[pl.ds(c * block, block), cols], *buffers, sems)

        wide = span + 2 * HD
        job_later = reduce(1, later, 0, wide + span, sems[13:17])
        job = reduce(0, grads, 0, wide, sems[17:21])
        job_out = reduce(0, grads, wide, wide + span, sems[21:25])
        swaps = [
            remote(gives[k], outs[3 + k], sems[25].at[k], sems[26].at[k], section=1 - section)
            for k in range(3)
        ]
        load_later = pltpu.make_async_copy(later_hbm, later, osem.at[0])

        @pl.when(job_later.mine)
        def _():
            load_later.start()

        hello(n, me, gy, True, True)

        @pl.when(jnp.logical_not(job_later.mine))
        def _():
            for k in (3, 1, 2, 0):
                c = job_later.cols[k]
                job_later.give(k, later_hbm.at[pl.ds(c * block, block)]).start()

        for swap in swaps:
            swap.start()
    else:
        hello(n, me, None, False)
    dmids[:, pl.ds(pl.multiple_of(me * t, t), t)] = dmid_ref[...].astype(BF16).reshape(mb, t, d)
    lines = [
        Line(
            n,
            m,
            lambda z, m=m: dmids.at[m, pl.ds(z * t, t)],
            (col, zup, zdn, stage),
            sems[:8],
        )
        for m in range(mb)
    ]
    waiting = []
    sums = []

    def tick():
        if waiting:
            waiting.pop(0)()
        if sums:
            sums.pop(0)()

    if last:
        sums += [functools.partial(job_later.send_term, k) for k in (3, 1, 2, 0)]
        sums += [job_later.pass_on]
    for k in range(n):
        lines[0].gather_step(k)
        if k == min(1, n - 1):
            for line in lines[1:]:
                line.gather_step(0)
        if k == 0 and last:

            @pl.when(job_later.mine)
            def _():
                load_later.wait()

        if k < n - 1:
            tick()
    fetch_out.wait()
    for load in loads:
        load.wait()
    cosine, sine = cos_ref[...], sin_ref[...]
    dkey[...] = jnp.zeros_like(dkey)
    dvalue[...] = jnp.zeros_like(dvalue)
    dgain_query[...] = jnp.zeros_like(dgain_query)
    dgain_key[...] = jnp.zeros_like(dgain_key)
    per = d // 4 // 256

    def out_grads(at):
        left = dmids[:, :, at].reshape(mb * length, 256)
        grads[at, span + 2 * HD :] = dot32(left, mixed[...], ROW_PAIR).astype(BF16)

    def in_grads(at):
        left = normed[:, :, at].reshape(mb * length, 256)
        grads[at, : span + 2 * HD] = dot32(left, dproj[...], ROW_PAIR).astype(BF16)

    def chunked(compute, job):
        def chunk(i, carry):
            first = flip_by(gy, 3 - i // per) * (d // 4) + lax.rem(i, per) * 256
            compute(pl.ds(pl.multiple_of(first, 256), 256))
            for q in range(4):

                @pl.when(i == per * (q + 1) - 1)
                def _():
                    if job is not None:

                        @pl.when(jnp.logical_not(job.mine))
                        def _():
                            job.give(3 - q, job.part(job.cols[3 - q])).start()

                    tick()

            return carry

        lax.fori_loop(0, 4 * per, chunk, 0)

    for m, line in enumerate(lines):
        first = m * length
        rows = slice(first, first + length)
        if m + 1 < mb:
            waiting += [functools.partial(lines[m + 1].gather_step, k) for k in range(1, n)]

        def to_heads(j, carry, m=m, rows=rows):
            cols = pl.ds(pl.multiple_of(j * 256, 256), 256)
            dheads[rows, cols] = jnp.dot(
                dmids[m], wout[:, cols], preferred_element_type=F32
            ).astype(BF16)
            return carry

        lax.fori_loop(0, span // 256, to_heads, 0)
        tick()

        def head(h, carry, m=m, rows=rows):
            at = pl.ds(pl.multiple_of(h * HD, HD), HD)
            p = prob[m * heads + h]
            dh = dheads[rows, at]
            dvalue[rows] += dot32(p, dh, ROW_PAIR)
            dp = dot32(dh, v_ref[rows], COL_PAIR)
            delta = jnp.sum(
                dh.astype(F32) * mixed[rows, at].astype(F32), axis=-1, keepdims=True
            )
            ds = (p.astype(F32) * (dp - delta)).astype(BF16)
            dkey[rows] += dot32(ds, qr[rows, at], ROW_PAIR) * inv_root
            dq = jnp.dot(ds, kr_ref[rows], preferred_element_type=F32) * inv_root
            turned = dq * cosine[rows] - half_turn(dq) * sine[rows]
            unit, scale = unit_of(proj[rows, at])
            dgain_query[...] += jnp.sum(turned * unit, axis=0, keepdims=True)
            dproj[rows, at] = norm_back(turned * gain_query[...], unit, scale).astype(BF16)
            return carry

        lax.fori_loop(0, heads // 2, head, 0, unroll=2)
        tick()
        lax.fori_loop(heads // 2, heads, head, 0, unroll=2)
        tick()
        dk = dkey[rows]
        turned = dk * cosine[rows] - half_turn(dk) * sine[rows]
        unit, scale = unit_of(proj[rows, span : span + HD])
        dgain_key[...] += jnp.sum(turned * unit, axis=0, keepdims=True)
        dproj[rows, span : span + HD] = norm_back(turned * gain_key[...], unit, scale).astype(BF16)
        dproj[rows, span + HD :] = dvalue[rows].astype(BF16)
        if m == 0:
            fetch_in.wait()
        while waiting:
            waiting.pop(0)()

        def in_cols(j, carry, m=m, rows=rows):
            at = pl.ds(pl.multiple_of(j * 256, 256), 256)
            res = dot32(dproj[rows], win[at], COL_PAIR).astype(BF16)
            for z in range(n):
                col[m, z, :, at] = res[z * t : (z + 1) * t]
            return carry

        lax.fori_loop(0, d // 256, in_cols, 0)
        line.scatter_tick(0)
        waiting += [functools.partial(line.scatter_tick, hop) for hop in range(1, n - 1)]
        if m == 0 and last:
            chunked(out_grads, job_out)
            sums += [functools.partial(job_out.send_term, k) for k in (3, 2, 1, 0)]
            sums += [job_out.pass_on]

    if not last:
        chunked(out_grads, None)
    chunked(in_grads, job if last else None)
    while waiting or sums:
        tick()
    if last:
        for k in (3, 2, 1, 0):
            job.send_term(k)
    else:
        save = pltpu.make_async_copy(grads, outs[0], osem.at[0])
        save.start()
    for m, line in enumerate(lines):
        line.scatter_finish(total.at[m * t : (m + 1) * t])
    hidden = x_ref[...].astype(F32)
    unit, scale = unit_of(hidden)
    da = total[...]
    dgain_attn[...] = jnp.sum(da * unit, axis=0, keepdims=True)
    cot_ref[...] = (dmid_ref[...] + norm_back(da * gain_attn[...], unit, scale)).astype(BF16)
    for line in lines:
        line.drain()
    if not last:
        save.wait()
        return
    job.pass_on()
    closing = [(outs[0], 0, span), (outs[1], span, wide), (outs[2], wide, wide + span)]
    job_later.close(closing)
    job_out.close([(outs[2], 0, span)])
    job.close(closing[:2])
    for swap in swaps:
        swap.wait()

    @pl.when(jnp.logical_not(job.mine))
    def _():
        for k in range(4):
            job.give(k, job.part(job.cols[k])).wait_send()
            job_out.give(k, job_out.part(job_out.cols[k])).wait_send()

    @pl.when(jnp.logical_not(job_later.mine))
    def _():
        for k in range(4):
            c = job_later.cols[k]
            job_later.give(k, later_hbm.at[pl.ds(c * block, block)]).wait_send()


def attn_backward(layer, n, dmid, x, gains, tables, kept, w_in, w_out, later, gives, cid, mb):
    r, d = x.shape
    cosine, sine, _ = tables
    normed, proj, qr, kr, v, prob, mixed = kept
    total_rows = cosine.shape[0]
    length = total_rows // mb
    width = w_in.shape[1]
    heads = w_out.shape[1] // HD
    span = heads * HD
    shape = jax.ShapeDtypeStruct
    both = width + span
    grad_shapes = [shape((d, both), BF16)]
    extra = []
    if later:
        block = d // 4
        grad_shapes = [
            shape((block, span), F32),
            shape((block, 2 * HD), BF16),
            shape((block, span), F32),
            *(shape(piece.shape, BF16) for piece in gives),
        ]
        extra = [
            pltpu.VMEM((d, both), BF16),
            pltpu.VMEM((4, block, both), BF16),
            pltpu.VMEM((block, both), BF16),
            pltpu.VMEM((block, both), BF16),
            pltpu.VMEM((2, block // 2, both), BF16),
        ] + reduce_sems() * 3 + [pltpu.SemaphoreType.DMA((3,))] * 2
    return pl.pallas_call(
        functools.partial(attn_backward_kernel, n, layer, heads),
        out_shape=(
            shape((r, d), BF16),
            shape((1, d), F32),
            shape((1, HD), F32),
            shape((1, HD), F32),
            *grad_shapes,
        ),
        in_specs=in_vmem(9) + in_place(7 + len(later) + len(gives)),
        out_specs=tuple(in_vmem(4) + (in_vmem(3) + in_place(3) if later else in_place(1))),
        scratch_shapes=[
            pltpu.VMEM((d, width), BF16),
            pltpu.VMEM((d, span), BF16),
            pltpu.VMEM((mb, length, d), BF16),
            pltpu.VMEM((total_rows, width), F32),
            pltpu.VMEM((total_rows, span), BF16),
            pltpu.VMEM((mb * heads, length, length), BF16),
            pltpu.VMEM((total_rows, span), BF16),
            pltpu.VMEM((mb, length, d), BF16),
            pltpu.VMEM((total_rows, span), BF16),
            pltpu.VMEM((total_rows, width), BF16),
            pltpu.VMEM((total_rows, HD), F32),
            pltpu.VMEM((total_rows, HD), F32),
            pltpu.VMEM((d, both), BF16),
        ]
        + line_buffers(mb, n, r, d)
        + [
            pltpu.SemaphoreType.DMA((2,)),
            pltpu.SemaphoreType.DMA((5,)),
            pltpu.SemaphoreType.DMA((1,)),
        ]
        + [pltpu.SemaphoreType.DMA((mb, n))] * 8
        + extra,
        compiler_params=pltpu.CompilerParams(
            collective_id=cid, has_side_effects=True, vmem_limit_bytes=63 << 20
        ),
        name="attn_backward",
    )(
        dmid,
        x,
        *gains,
        cosine,
        sine,
        kr,
        v,
        normed,
        proj,
        qr,
        prob,
        mixed,
        w_in,
        w_out,
        *later,
        *gives,
    )


def local_wide(
    inputs,
    out_grad,
    segments,
    routes,
    gates,
    gain_attn,
    gain_ffn,
    gain_query,
    gain_key,
    w_query,
    w_key,
    w_value,
    w_out,
    w_gate,
    w_up,
    w_down,
):
    micro_count, _, local_rows, width = inputs.shape
    n_sec = lax.axis_size("section")
    n_gx = lax.axis_size("gx")
    n_gy = lax.axis_size("gy")
    heads = w_query.shape[2] // HD
    span = heads * HD
    experts = n_gx * n_gy
    group_len = segments.shape[2]
    mb = micro_count // n_sec
    rows_own = mb * local_rows
    rows_attn = mb * group_len
    section = lax.axis_index("section")
    gx = lax.axis_index("gx")
    gy = lax.axis_index("gy")
    expert_own = gx * n_gy + gy
    inv_root = 1.0 / math.sqrt(HD)
    first = section * mb

    kv_head = gx * heads // (HQ // KVH)
    key_own = lax.dynamic_slice_in_dim(w_key[0], kv_head * HD, HD, 1)
    value_own = lax.dynamic_slice_in_dim(w_value[0], kv_head * HD, HD, 1)
    w_in_shard = jnp.concatenate([w_query[0], key_own, value_own], axis=1)
    w_in_all = both_layers(lax.all_gather(w_in_shard, "gy", axis=0, tiled=True))
    w_out_all = both_layers(lax.all_gather(w_out[0], "gy", axis=0, tiled=True))
    w_gate_all = both_layers(w_gate[0, 0])
    w_up_all = both_layers(w_up[0, 0])
    w_down_all = both_layers(w_down[0, 0])
    table = dense_gates(routes[0, :, 0], gates[0, :, 0], experts)
    small = jnp.concatenate(
        [
            table.reshape(-1),
            gain_attn[0],
            gain_ffn[0],
            gain_query[0],
            gain_key[0],
        ]
    )
    small_all = both_layers(small)
    table_size = micro_count * local_rows * experts
    table_all = small_all[:, :table_size].reshape(n_sec, micro_count, local_rows, experts)
    gains_all = small_all[:, table_size:]

    table_mine = lax.dynamic_slice_in_dim(table_all, first, mb, 1).reshape(
        n_sec, rows_own, experts
    )
    x_mine = lax.dynamic_slice_in_dim(inputs[:, 0], first, mb, 0).reshape(rows_own, width)
    cot_mine = lax.dynamic_slice_in_dim(out_grad[:, 0], first, mb, 0).reshape(rows_own, width)
    segs = lax.dynamic_slice_in_dim(segments[:, 0], first, mb, 0)
    allowed, cosine, sine = seq_tables(segs, HD)
    cos_q = cosine.reshape(rows_attn, 1, HD // 2)
    sin_q = sine.reshape(rows_attn, 1, HD // 2)
    cos_k = cosine.reshape(rows_attn, HD // 2)
    sin_k = sine.reshape(rows_attn, HD // 2)

    def split_gains(layer):
        g = gains_all[layer]
        return (
            g[:width],
            g[width : 2 * width],
            g[2 * width : 2 * width + HD],
            g[2 * width + HD :],
        )

    saved_all = []
    outs = []
    layer_in = x_mine
    for layer in range(n_sec):
        g_attn, g_ffn, g_query, g_key = split_gains(layer)
        hidden = layer_in.astype(F32)
        attn_unit, attn_scale = normalize(hidden)
        normed = (attn_unit * g_attn).astype(BF16)
        normed_all = gather_z(normed.reshape(mb, local_rows, width)).reshape(rows_attn, width)
        projected = dot32(normed_all, w_in_all[layer])
        query = projected[:, :span].reshape(rows_attn, heads, HD)
        key = projected[:, span : span + HD]
        value_low = projected[:, span + HD :].astype(BF16).reshape(mb, group_len, HD)
        query_unit, query_scale = normalize(query)
        key_unit, key_scale = normalize(key)
        query_rope = (
            rotate(query_unit * g_query, cos_q, sin_q)
            .astype(BF16)
            .reshape(mb, group_len, heads, HD)
        )
        key_rope = rotate(key_unit * g_key, cos_k, sin_k).astype(BF16).reshape(mb, group_len, HD)
        scores = (
            jnp.einsum("mthd,msd->mhts", query_rope, key_rope, preferred_element_type=F32)
            * inv_root
        )
        exponent = jnp.where(allowed[:, None], jnp.exp(scores), 0.0)
        log_total = jnp.log(jnp.sum(exponent, axis=-1, keepdims=True))
        prob = jnp.where(allowed[:, None], jnp.exp(scores - log_total), 0.0)
        mixed = (
            jnp.einsum("mhts,msd->mthd", prob.astype(BF16), value_low, preferred_element_type=F32)
            .astype(BF16)
            .reshape(rows_attn, span)
        )
        attn_part = dot32(mixed, w_out_all[layer], COL_PAIR).astype(BF16)
        attn_out = scatter_z(attn_part.reshape(mb, group_len, width)).reshape(rows_own, width)
        middle = hidden + attn_out.astype(F32)
        ffn_unit, ffn_scale = normalize(middle)
        expert_in = (ffn_unit * g_ffn).astype(BF16)
        tab = table_mine[layer]
        tab_hi = tab.astype(BF16)
        tab_lo = (tab - tab_hi.astype(F32)).astype(BF16)
        payload = jnp.concatenate([expert_in, tab_hi, tab_lo], axis=1)
        arrived_all = gather_all(payload)
        arrived = arrived_all[:, :width]
        gate_cols = arrived_all[:, width:].astype(F32)
        is_mine = jnp.arange(2 * experts) % experts == expert_own
        weight = jnp.sum(jnp.where(is_mine[None], gate_cols, 0.0), axis=1, keepdims=True)
        gate_pre = dot32(arrived, w_gate_all[layer])
        up_proj = dot32(arrived, w_up_all[layer])
        inner = (jax.nn.silu(gate_pre) * up_proj).astype(BF16)
        result = dot32(inner, w_down_all[layer])
        weighted = (result * weight).astype(BF16)
        expert_sum = scatter_all(weighted)
        layer_out = (middle + expert_sum.astype(F32)).astype(BF16)
        outs.append(layer_out)
        layer_in = layer_out
        saved_all.append(
            (
                attn_unit,
                attn_scale,
                normed_all,
                query_unit,
                query_scale,
                key_unit,
                key_scale,
                query_rope,
                key_rope,
                value_low,
                prob,
                mixed,
                ffn_unit,
                ffn_scale,
                arrived,
                weight,
                gate_pre,
                up_proj,
                inner,
            )
        )

    cot = cot_mine
    in_grads = [None] * n_sec
    expert_grads = [None] * n_sec
    attn_grads = [None] * n_sec
    gain_grads = [None] * n_sec
    for layer in reversed(range(n_sec)):
        g_attn, g_ffn, g_query, g_key = split_gains(layer)
        (
            attn_unit,
            attn_scale,
            normed_all,
            query_unit,
            query_scale,
            key_unit,
            key_scale,
            query_rope,
            key_rope,
            value_low,
            prob,
            mixed,
            ffn_unit,
            ffn_scale,
            arrived,
            weight,
            gate_pre,
            up_proj,
            inner,
        ) = saved_all[layer]
        gradient = cot.astype(F32)
        grad_all = gather_all(cot)
        grad_result = (grad_all.astype(F32) * weight).astype(BF16)
        grad_inner = dot32(grad_result, w_down_all[layer], COL_PAIR)
        grad_down = dot32(inner, grad_result, ROW_PAIR)
        sig = jax.nn.sigmoid(gate_pre)
        grad_gate_pre = (grad_inner * up_proj * sig * (1.0 + gate_pre * (1.0 - sig))).astype(BF16)
        grad_up_proj = (grad_inner * gate_pre * sig).astype(BF16)
        grad_gate = dot32(arrived, grad_gate_pre, ROW_PAIR)
        grad_up = dot32(arrived, grad_up_proj, ROW_PAIR)
        grad_arrived = (
            dot32(grad_gate_pre, w_gate_all[layer], COL_PAIR)
            + dot32(grad_up_proj, w_up_all[layer], COL_PAIR)
        ).astype(BF16)
        expert_grads[layer] = (grad_gate, grad_up, grad_down)
        grad_expert_in = scatter_all(grad_arrived).astype(F32)
        grad_ffn_gain = jnp.sum(grad_expert_in * ffn_unit, axis=0)
        grad_middle = gradient + norm_back(grad_expert_in * g_ffn, ffn_unit, ffn_scale)
        middle_low = grad_middle.astype(BF16)
        middle_all = gather_z(middle_low.reshape(mb, local_rows, width)).reshape(rows_attn, width)
        grad_out_w = dot32(middle_all, mixed, ROW_PAIR)
        grad_heads = (
            dot32(middle_all, w_out_all[layer]).astype(BF16).reshape(mb, group_len, heads, HD)
        )
        grad_value = jnp.einsum(
            "mhts,mthd->mshd", prob.astype(BF16), grad_heads, preferred_element_type=F32
        )
        grad_prob = jnp.einsum(
            "mthd,msd->mhts", grad_heads, value_low, preferred_element_type=F32
        )
        mixed_split = mixed.reshape(mb, group_len, heads, HD)
        delta = jnp.sum(grad_heads.astype(F32) * mixed_split.astype(F32), axis=-1)
        delta = jnp.swapaxes(delta, 1, 2)[..., None]
        grad_scores = (prob * (grad_prob - delta)).astype(BF16)
        grad_query = (
            jnp.einsum("mhts,msd->mthd", grad_scores, key_rope, preferred_element_type=F32)
            * inv_root
        ).reshape(rows_attn, heads, HD)
        grad_key = (
            jnp.einsum("mhts,mthd->mshd", grad_scores, query_rope, preferred_element_type=F32)
            * inv_root
        ).reshape(rows_attn, heads, HD)
        query_turn = rotate_back(grad_query, cos_q, sin_q)
        grad_query_gain = jnp.sum(query_turn * query_unit, axis=(0, 1))
        grad_query_pre = norm_back(query_turn * g_query, query_unit, query_scale)
        key_turn = rotate_back(jnp.sum(grad_key, axis=1), cos_k, sin_k)
        grad_key_gain = jnp.sum(key_turn * key_unit, axis=0)
        grad_key_pre = norm_back(key_turn * g_key, key_unit, key_scale)
        grad_proj = jnp.concatenate(
            [
                grad_query_pre.reshape(rows_attn, span),
                grad_key_pre,
                jnp.sum(grad_value, axis=2).reshape(rows_attn, HD),
            ],
            axis=1,
        ).astype(BF16)
        grad_in_w = dot32(normed_all, grad_proj, ROW_PAIR)
        normed_part = dot32(grad_proj, w_in_all[layer], COL_PAIR).astype(BF16)
        grad_normed = (
            scatter_z(normed_part.reshape(mb, group_len, width))
            .reshape(rows_own, width)
            .astype(F32)
        )
        grad_attn_gain = jnp.sum(grad_normed * attn_unit, axis=0)
        cot = (grad_middle + norm_back(grad_normed * g_attn, attn_unit, attn_scale)).astype(BF16)
        in_grads[layer] = cot
        attn_grads[layer] = jnp.concatenate([grad_in_w, grad_out_w], axis=1).astype(BF16)
        gain_grads[layer] = jnp.concatenate(
            [grad_attn_gain, grad_ffn_gain, grad_query_gain, grad_key_gain]
        )

    def own_layer_sum(pieces):
        return lax.psum_scatter(
            jnp.stack([piece.astype(BF16) for piece in pieces]),
            "section",
            scatter_dimension=0,
            tiled=True,
        ).astype(F32)

    grad_gate, grad_up, grad_down = (
        own_layer_sum([expert_grads[layer][k] for layer in range(n_sec)]) for k in range(3)
    )
    attn_sum = lax.psum_scatter(
        jnp.concatenate(attn_grads, axis=0), ("section", "gy"), scatter_dimension=0, tiled=True
    ).astype(F32)
    query_grad = attn_sum[:, :span]
    out_w_grad = attn_sum[:, span + 2 * HD :]
    kv_all = lax.all_gather(attn_sum[:, span : span + 2 * HD], "gx", axis=0, tiled=False)
    kv_all = jnp.sum(kv_all.reshape(KVH, n_gx // KVH, -1, 2, HD), axis=1)
    key_part = jnp.swapaxes(kv_all[:, :, 0], 0, 1).reshape(-1, KVH * HD)
    value_part = jnp.swapaxes(kv_all[:, :, 1], 0, 1).reshape(-1, KVH * HD)
    gain_sum = lax.psum(jnp.stack(gain_grads), ("section", "gx", "gy"))
    gain_sum = lax.dynamic_index_in_dim(gain_sum, section, 0, keepdims=True)

    def own_layer_rows(pieces):
        stacked = jnp.stack(pieces).reshape(n_sec, mb, local_rows, width)
        return lax.all_to_all(stacked, "section", split_axis=0, concat_axis=0, tiled=True).reshape(
            1, micro_count, 1, local_rows, width
        )

    return (
        own_layer_rows(outs),
        own_layer_rows(in_grads),
        gain_sum[:, :width],
        gain_sum[:, width : 2 * width],
        gain_sum[:, 2 * width : 2 * width + HD],
        gain_sum[:, 2 * width + HD :],
        query_grad[None],
        key_part[None],
        value_part[None],
        out_w_grad[None],
        grad_gate[:, None],
        grad_up[:, None],
        grad_down[:, None],
    )


def local_fused(
    inputs,
    out_grad,
    segments,
    routes,
    gates,
    gain_attn,
    gain_ffn,
    gain_query,
    gain_key,
    w_query,
    w_key,
    w_value,
    w_out,
    w_gate,
    w_up,
    w_down,
):
    micro_count, _, local_rows, width = inputs.shape
    n_sec = lax.axis_size("section")
    n_gx = lax.axis_size("gx")
    n_gy = lax.axis_size("gy")
    heads = w_query.shape[2] // HD
    span = heads * HD
    experts = n_gx * n_gy
    group_len = segments.shape[2]
    mb = micro_count // n_sec
    rows_own = mb * local_rows
    rows_attn = mb * group_len
    section = lax.axis_index("section")
    first = section * mb

    attn_shards = (w_query, w_key, w_value, w_out)
    table = dense_gates(routes[0, :, 0], gates[0, :, 0], experts)
    smalls = (table, gain_attn, gain_ffn, gain_query, gain_key)
    full_in, full_out, *others = share_weights(0, n_gx, attn_shards, smalls, 9)
    attn_all = [(full_in, full_out)]
    is_first = section == 0
    by_layer = [
        (jnp.where(is_first, own, other), jnp.where(is_first, other, own))
        for own, other in zip(smalls, others)
    ]
    moe_own = (w_gate[0, 0], w_up[0, 0], w_down[0, 0])
    moe_other = tuple(swap_sections(w) for w in moe_own)
    table_mine = [
        lax.dynamic_slice_in_dim(part, first, mb, 0).reshape(rows_own, experts)
        for part in by_layer[0]
    ]
    x_mine = lax.dynamic_slice_in_dim(inputs[:, 0], first, mb, 0).reshape(rows_own, width)
    cot = lax.dynamic_slice_in_dim(out_grad[:, 0], first, mb, 0).reshape(rows_own, width)
    segs = lax.dynamic_slice_in_dim(segments[:, 0], first, mb, 0)
    allowed, cosine, sine = seq_tables(segs, HD)
    tables = (
        jnp.concatenate([cosine, cosine], axis=-1).reshape(rows_attn, HD),
        jnp.concatenate([-sine, sine], axis=-1).reshape(rows_attn, HD),
        allowed.astype(F32),
    )

    def split_gains(layer):
        return tuple(pair[layer] for pair in by_layer[1:])

    kept = []
    outs = []
    layer_in = x_mine
    for layer in range(n_sec):
        tab = table_mine[layer]
        tab_hi = tab.astype(BF16)
        tab_lo = (tab - tab_hi.astype(F32)).astype(BF16)
        pad = jnp.zeros((rows_own, 128 - 2 * experts), BF16)
        gate_cols = jnp.concatenate([tab_hi, tab_lo, pad], axis=1)
        mid, payload, normed, proj, qr, kr, v, prob, mixed, *next_all = attn_forward(
            layer,
            n_gx,
            layer_in,
            split_gains(layer),
            tables,
            gate_cols,
            *attn_all[layer],
            attn_shards if layer == 0 else (),
            1 + layer,
            mb,
        )
        attn_all.append(next_all)
        layer_out, *moe_kept = moe_forward(
            layer, n_gx, mid, payload, moe_own, moe_other, 3 + layer
        )
        kept.append((layer_in, mid, (normed, proj, qr, kr, v, prob, mixed), moe_kept))
        outs.append(layer_out)
        layer_in = layer_out

    in_grads = [None] * n_sec
    moe_sums = ()
    later = ()
    gain_grads = [None] * n_sec
    for layer in reversed(range(n_sec)):
        g_attn, g_ffn, g_query, g_key = split_gains(layer)
        layer_in, mid, attn_kept, (arrived, weight, gp, up, inner) = kept[layer]
        dmid, d_ffn, *moe_sums = moe_backward(
            layer,
            n_gx,
            cot,
            mid,
            g_ffn,
            weight,
            arrived,
            gp,
            up,
            inner,
            moe_own,
            moe_other,
            moe_sums,
            5 + layer,
        )
        cot, d_attn, d_query, d_key, *later = attn_backward(
            layer,
            n_gx,
            dmid,
            layer_in,
            (g_attn, g_query, g_key),
            tables,
            attn_kept,
            *attn_all[layer],
            later,
            moe_sums[3:] if layer == 0 else (),
            7 + layer,
            mb,
        )
        in_grads[layer] = cot
        gain_grads[layer] = [d_attn, d_ffn, d_query, d_key]

    query_grad, kv_shard, out_grad_w, *from_other = later
    grad_gate, grad_up, grad_down = (
        (moe_sums[k].astype(F32) + from_other[k].astype(F32))[None] for k in range(3)
    )
    gain_sum, key_part, value_part = finish_line(
        n_gx, [grad for grads in gain_grads for grad in grads], kv_shard, 10
    )
    out_rows, grad_rows, *gain_sums = finish_pair(
        gain_sum, [grad.shape[1] for grad in gain_grads[0]], outs, in_grads, 11
    )
    whole_rows = (1, micro_count, 1, local_rows, width)

    return (
        out_rows.reshape(whole_rows),
        grad_rows.reshape(whole_rows),
        *gain_sums,
        query_grad[None],
        key_part[None],
        value_part[None],
        out_grad_w[None],
        grad_gate[:, None],
        grad_up[:, None],
        grad_down[:, None],
    )


def local(*args):
    inputs = args[0]
    n = lax.axis_size("gx")
    rows_own = inputs.shape[0] // lax.axis_size("section") * inputs.shape[2]
    if 4 * n * rows_own > MOST_ROWS or n != KVH:
        return local_wide(*args)
    return local_fused(*args)


def solution(mesh):
    return jax.shard_map(
        local,
        mesh=mesh,
        in_specs=(
            P(None, "gy", "gx", None),
            P(None, "gy", "gx", None),
            P(None, "gy", None),
            P("section", None, "gy", "gx", None),
            P("section", None, "gy", "gx", None),
            P("section", None),
            P("section", None),
            P("section", None),
            P("section", None),
            P("section", "gy", "gx"),
            P("section", "gy", None),
            P("section", "gy", None),
            P("section", "gy", "gx"),
            P("section", ("gx", "gy"), None, None),
            P("section", ("gx", "gy"), None, None),
            P("section", ("gx", "gy"), None, None),
        ),
        out_specs=(
            P("section", None, "gy", "gx", None),
            P("section", None, "gy", "gx", None),
            P("section", None),
            P("section", None),
            P("section", None),
            P("section", None),
            P("section", "gy", "gx"),
            P("section", "gy", None),
            P("section", "gy", None),
            P("section", "gy", "gx"),
            P("section", ("gx", "gy"), None, None),
            P("section", ("gx", "gy"), None, None),
            P("section", ("gx", "gy"), None, None),
        ),
        check_vma=False,
    )
```

```python
import functools
import math

import jax
import jax.numpy as jnp
from jax import lax
from jax.experimental import pallas as pl
from jax.experimental.pallas import tpu as pltpu
from jax.sharding import PartitionSpec as P

HQ = 32
KVH = 4
HD = 128
TOPK = 8

EPSILON = 1e-06
ROPE_BASE = 1000000.0
ROW_PAIR = (((0,), (0,)), ((), ()))
COL_PAIR = (((1,), (1,)), ((), ()))
F32 = jnp.float32
BF16 = jnp.bfloat16
MOST_ROWS = 1024


def normalize(tensor):
    scaling = lax.rsqrt(jnp.mean(tensor * tensor, axis=-1, keepdims=True) + EPSILON)
    return (tensor * scaling, scaling)


def norm_back(gradient, unit_vec, scaling):
    return scaling * (gradient - unit_vec * jnp.mean(gradient * unit_vec, axis=-1, keepdims=True))


def rotate(tensor, cosine, sine_part):
    halfway = tensor.shape[-1] // 2
    leading = tensor[..., :halfway]
    trailing = tensor[..., halfway:]
    return jnp.concatenate(
        [leading * cosine - trailing * sine_part, trailing * cosine + leading * sine_part], axis=-1
    )


def rotate_back(gradient, cosine, sine_part):
    return rotate(gradient, cosine, -sine_part)


def seq_tables(segment_ids, head_dim):
    length_all = segment_ids.shape[-1]
    position_ids = jnp.arange(length_all, dtype=jnp.int32)
    allowed = (segment_ids[:, :, None] == segment_ids[:, None, :]) & (
        position_ids[:, None] >= position_ids[None, :]
    )
    positions = jnp.sum(allowed.astype(jnp.int32), axis=-1) - 1
    halfway = head_dim // 2
    inverse = ROPE_BASE ** (-2.0 * jnp.arange(halfway, dtype=jnp.float32) / head_dim)
    angles = positions.astype(jnp.float32)[..., None] * inverse
    return (allowed, jnp.cos(angles), jnp.sin(angles))


def dot32(left, right, dims=None):
    if dims is None:
        return jnp.dot(left, right, preferred_element_type=F32)
    return lax.dot_general(left, right, dims, preferred_element_type=F32)


def gather_z(rows):
    return lax.all_gather(rows, "gx", axis=1, tiled=True)


def scatter_z(rows):
    return lax.psum_scatter(rows, "gx", scatter_dimension=1, tiled=True)


def gather_all(rows):
    return lax.all_gather(rows, ("gx", "gy"), axis=0, tiled=True)


def scatter_all(rows):
    return lax.psum_scatter(rows, ("gx", "gy"), scatter_dimension=0, tiled=True)


def both_layers(tensor):
    return lax.all_gather(tensor, "section", axis=0, tiled=False)


def dense_gates(route_ids, gate_vals, experts):
    onehot = route_ids[..., None] == jnp.arange(experts, dtype=jnp.int32)
    return jnp.sum(jnp.where(onehot, gate_vals[..., None], 0.0), axis=-2)


def swap_sections(tensor):
    return lax.ppermute(tensor, "section", [(0, 1), (1, 0)])


def remote(src, dst, send_sem, recv_sem, **where):
    return pltpu.make_async_remote_copy(
        src_ref=src,
        dst_ref=dst,
        send_sem=send_sem,
        recv_sem=recv_sem,
        device_id=where,
        device_id_type=pl.DeviceIdType.MESH,
    )


def hello(n, me, gy, with_plane, with_section=False):
    barrier = pltpu.get_barrier_semaphore()
    mesh_ids = pl.DeviceIdType.MESH

    @pl.when(me + 1 < n)
    def _():
        pl.semaphore_signal(barrier, 1, device_id={"gx": me + 1}, device_id_type=mesh_ids)

    @pl.when(me > 0)
    def _():
        pl.semaphore_signal(barrier, 1, device_id={"gx": me - 1}, device_id_type=mesh_ids)

    peers = 0
    if with_plane:
        for bit in (1, 2):
            pl.semaphore_signal(
                barrier, 1, device_id={"gy": gy_flip(gy, bit)}, device_id_type=mesh_ids
            )
        peers += 2
    if with_section:
        other = 1 - lax.axis_index("section")
        pl.semaphore_signal(barrier, 1, device_id={"section": other}, device_id_type=mesh_ids)
        peers += 1
    at_end = (me == 0) | (me == n - 1)

    @pl.when(at_end)
    def _():
        pl.semaphore_wait(barrier, peers + 1)

    @pl.when(jnp.logical_not(at_end))
    def _():
        pl.semaphore_wait(barrier, peers + 2)


def gy_flip(gy, bits):
    low = lax.rem(gy, 2)
    high = gy // 2
    if bits & 1:
        low = 1 - low
    if bits & 2:
        high = 1 - high
    return high * 2 + low


def z_gather_steps(n, me, slot, sems, after):
    send_up, recv_up, send_down, recv_down = sems
    sends = []

    def up(k):
        return remote(slot(me - k), slot(me - k), send_up.at[k], recv_up.at[k], gx=me + 1)

    def down(k):
        return remote(slot(me + k), slot(me + k), send_down.at[k], recv_down.at[k], gx=me - 1)

    for k in range(n):
        @pl.when(me - k >= 0)
        def _():
            if k:
                remote(
                    slot(me - k), slot(me - k), send_up.at[k - 1], recv_up.at[k - 1], gx=me
                ).wait_recv()
            if k < n - 1:

                @pl.when(me + 1 < n)
                def _():
                    up(k).start()

            if k == 0:

                @pl.when(me > 0)
                def _():
                    down(0).start()

            after(me - k, k)

        if k:

            @pl.when(me + k < n)
            def _():
                remote(
                    slot(me + k), slot(me + k), send_down.at[k - 1], recv_down.at[k - 1], gx=me
                ).wait_recv()
                if k < n - 1:

                    @pl.when(me > 0)
                    def _():
                        down(k).start()

                after(me + k, k)


def z_gather_drain(n, me, slot, sems):
    send_up, recv_up, send_down, recv_down = sems
    for k in range(n - 1):

        @pl.when((me - k >= 0) & (me + 1 < n))
        def _():
            remote(slot(me - k), slot(me - k), send_up.at[k], recv_up.at[k], gx=me + 1).wait_send()

        @pl.when((me + k < n) & (me > 0))
        def _():
            remote(
                slot(me + k), slot(me + k), send_down.at[k], recv_down.at[k], gx=me - 1
            ).wait_send()


def flip_by(gy, step):
    low = lax.rem(lax.rem(gy, 2) + lax.rem(step, 2), 2)
    high = lax.rem(gy // 2 + step // 2, 2)
    return high * 2 + low


class Plane:
    def __init__(self, n, sems):
        self.n = n
        self.me = lax.axis_index("gx")
        self.gy = lax.axis_index("gy")
        self.cx, self.cy, self.cd = (gy_flip(self.gy, bits) for bits in (1, 2, 3))
        self.gather_sems = sems[:10]
        self.scatter_sems = sems[10:]


    def gather_own_column(self, slot):
        su, ru, sd, rd, sx, rx, sy, ry, sf, rf = self.gather_sems
        c = self.gy

        def after(z, k):
            remote(slot(z, c), slot(z, c), sx.at[z], rx.at[z], gy=self.cx).start()
            remote(slot(z, c), slot(z, c), sy.at[z], ry.at[z], gy=self.cy).start()

        z_gather_steps(self.n, self.me, lambda z: slot(z, c), (su, ru, sd, rd), after)

    def gather_pass_on(self, slot):
        su, ru, sd, rd, sx, rx, sy, ry, sf, rf = self.gather_sems

        def forward(z):
            remote(slot(z, self.cx), slot(z, self.cx), sx.at[z], rx.at[z], gy=self.cx).wait_recv()
            remote(slot(z, self.cy), slot(z, self.cy), sy.at[z], ry.at[z], gy=self.cy).wait_recv()

            @pl.when(lax.rem(z, 2) == 0)
            def _():
                remote(
                    slot(z, self.cy), slot(z, self.cy), sf.at[z], rf.at[z], gy=self.cx
                ).start()

            @pl.when(lax.rem(z, 2) == 1)
            def _():
                remote(
                    slot(z, self.cx), slot(z, self.cx), sf.at[z], rf.at[z], gy=self.cy
                ).start()

        for k in range(self.n):

            @pl.when(self.me - k >= 0)
            def _():
                forward(self.me - k)

            if k:

                @pl.when(self.me + k < self.n)
                def _():
                    forward(self.me + k)

    def gather_far_column(self, slot):
        sf, rf = self.gather_sems[8:]
        for z in range(self.n):
            remote(slot(z, self.cd), slot(z, self.cd), sf.at[z], rf.at[z], gy=self.cx).wait_recv()

    def gather_drain(self, slot):
        su, ru, sd, rd, sx, rx, sy, ry, sf, rf = self.gather_sems
        z_gather_drain(self.n, self.me, lambda z: slot(z, self.gy), (su, ru, sd, rd))
        for z in range(self.n):
            one = slot(z, self.gy)
            remote(one, one, sx.at[z], rx.at[z], gy=self.cx).wait_send()
            remote(one, one, sy.at[z], ry.at[z], gy=self.cy).wait_send()
            remote(one, one, sf.at[z], rf.at[z], gy=self.cx).wait_send()


    def scatter_setup(self, part, sides, din, zup, zdn, stage, acc):
        self.part, self.sides, self.din = part, sides, din
        self.zup, self.zdn, self.stage, self.acc = zup, zdn, stage, acc

    def column_of(self, side):
        return self.cx * (1 - side) + self.cy * side

    def near(self, side, z):
        send, recv = self.scatter_sems[4:6]
        column = self.column_of(side)
        return remote(
            self.part(z, column), self.sides.at[side, z], send.at[side, z], recv.at[side, z], gy=column
        )

    def far(self, z):
        send, recv = self.scatter_sems[6:]
        return remote(
            self.part(z, self.cd),
            self.din.at[z],
            send.at[z],
            recv.at[z],
            gy=self.column_of(lax.rem(z, 2)),
        )

    def each(self, call, nearest=0, farthest=None):
        hops = reversed(range(nearest, self.n if farthest is None else farthest + 1))
        for k in [sign * far for far in hops for sign in ((-1, 1) if far else (1,))]:

            @pl.when((self.me + k >= 0) & (self.me + k < self.n))
            def _():
                call(self.me + k, k)

    def early(self, z, k):
        at_end = (z == 0) | (z == self.n - 1)
        return (abs(k) > 1) | (at_end & (k != 0))

    def scatter_near(self, side):
        def send(z, k):
            if k:

                @pl.when((lax.rem(z, 2) == side) & self.early(z, k))
                def _():
                    self.near(side, z).start()

        self.each(send)

    def scatter_far(self):
        self.each(lambda z, k: self.far(z).start())

    def scatter_pass_on(self, z, k):
        self.far(z).wait_recv()
        side = 1 - lax.rem(z, 2)
        mine = self.part(z, self.column_of(side))
        add_rows(mine, mine, self.din.at[z])
        self.near(side, z).start()
        pl.when(jnp.logical_not(self.early(z, k)))(lambda: self.near(1 - side, z).start())

    def closing_steps(self, total):
        pass_on, line = self.scatter_pass_on, functools.partial(self.scatter_line, total)
        order = [(pass_on, 2, None), (pass_on, 1, 1), (line, 2, None)]
        order += [(pass_on, 0, 0), (line, 1, 1), (line, 0, 0)]
        return [functools.partial(self.each, *step) for step in order]

    def along(self, z, up):
        send, recv = self.scatter_sems[:2] if up else self.scatter_sems[2:4]
        into = self.zup if up else self.zdn
        return remote(
            self.stage.at[z],
            into.at[z],
            send.at[z],
            recv.at[z],
            gx=self.me + 1 if up else self.me - 1,
        )

    def scatter_line(self, total, z, k):
        n, me, acc = self.n, self.me, self.acc
        self.near(0, z).wait_recv()
        self.near(1, z).wait_recv()
        terms = (self.part(z, self.gy), self.sides.at[0, z], self.sides.at[1, z])
        if k == 0:
            add_rows(total, *terms)
            return
        came = me > 0 if k > 0 else me < n - 1

        @pl.when(came)
        def _():
            self.along(z, k > 0).wait_recv()
            add_rows(self.stage.at[z], *terms, (self.zup if k > 0 else self.zdn).at[z])

        @pl.when(jnp.logical_not(came))
        def _():
            add_rows(self.stage.at[z], *terms)

        self.along(z, k > 0).start()

    def scatter_finish(self, total):
        n, me = self.n, self.me

        @pl.when(me > 0)
        def _():
            self.along(me, True).wait_recv()
            add_rows(total, total, self.zup.at[me])

        @pl.when(me < n - 1)
        def _():
            self.along(me, False).wait_recv()
            add_rows(total, total, self.zdn.at[me])

        for z in range(n):
            self.near(0, z).wait_send()
            self.near(1, z).wait_send()
            self.far(z).wait_send()

            @pl.when(me < z)
            def _():
                self.along(z, True).wait_send()

            @pl.when(me > z)
            def _():
                self.along(z, False).wait_send()


def add_rows(out, *terms):
    rows = out.shape[0]
    step = 16
    short = len(terms) == 2 and all(ref.dtype == BF16 for ref in (out, *terms))
    kind = BF16 if short else F32

    def body(i, carry):
        at = pl.ds(pl.multiple_of(i * step, step), step)
        value = terms[0][at].astype(kind)
        for term in terms[1:]:
            value = value + term[at].astype(kind)
        out[at] = value.astype(out.dtype)
        return carry

    lax.fori_loop(0, rows // step, body, 0)


def fetch_layer(layer, own, other, held, sems):
    section = lax.axis_index("section")

    @pl.when(section == layer)
    def _():
        for k, ref in enumerate(own):
            pltpu.make_async_copy(ref, held[k], sems.at[k]).start()

    @pl.when(section != layer)
    def _():
        for k, ref in enumerate(other):
            pltpu.make_async_copy(ref, held[k], sems.at[k]).start()


def fetch_wait(own, held, sems, which):
    for k in which:
        pltpu.make_async_copy(own[k], held[k], sems.at[k]).wait()


def moe_forward_kernel(
    n,
    layer,
    mid_ref,
    pay_ref,
    wg_own,
    wu_own,
    wd_own,
    wg_other,
    wu_other,
    wd_other,
    out_ref,
    arrived_ref,
    weight_ref,
    gp_ref,
    up_ref,
    inner_ref,
    pay,
    wg,
    wu,
    wd,
    part,
    sides,
    din,
    zup,
    zdn,
    stage,
    acc,
    total,
    gp,
    up,
    inner,
    wsem,
    osem,
    *sems,
):
    r, d = mid_ref.shape
    ff = wg.shape[1]
    rows = n * r
    experts = 4 * n
    own, other, held = (
        (wg_own, wu_own, wd_own),
        (wg_other, wu_other, wd_other),
        (wg, wu, wd),
    )
    fetch_layer(layer, own, other, held, wsem)
    plane = Plane(n, sems)
    me, gy = plane.me, plane.gy
    hello(n, me, gy, True)
    pay[pl.ds(pl.multiple_of((gy * n + me) * r, r), r)] = pay_ref[...]

    def slot(z, c):
        return pay.at[pl.ds((c * n + z) * r, r)]

    plane.scatter_setup(lambda z, c: part.at[c * n + z], sides, din, zup, zdn, stage, acc)
    plane.gather_own_column(slot)
    fetch_wait(own, held, wsem, range(3))
    expert = me * 4 + gy

    def column(s, carry):
        c = flip_by(gy, s)

        @pl.when(s == 1)
        def _():
            plane.gather_pass_on(slot)

        @pl.when(s == 3)
        def _():
            plane.gather_far_column(slot)

        at = pl.ds(pl.multiple_of(c * rows, rows), rows)
        gate_cols = pay[at, d : d + 128].astype(F32)
        lane = lax.broadcasted_iota(jnp.int32, (rows, 128), 1)
        hit = ((lane == expert) | (lane == expert + experts)) & (lane < 2 * experts)
        weight = jnp.sum(jnp.where(hit, gate_cols, 0.0), axis=1, keepdims=True)
        weight_ref[at] = weight
        block = pay[at, :d]

        def mid_cols(j, carry):
            cols = pl.ds(pl.multiple_of(j * 256, 256), 256)
            g = jnp.dot(block, wg[:, cols], preferred_element_type=F32)
            u = jnp.dot(block, wu[:, cols], preferred_element_type=F32)
            gp[at, cols] = g.astype(BF16)
            up[at, cols] = u.astype(BF16)
            inner[at, cols] = (g / (1.0 + jnp.exp(-g)) * u).astype(BF16)
            return carry

        lax.fori_loop(0, ff // 256, mid_cols, 0)
        act = inner[at]

        def out_cols(j, carry):
            cols = pl.ds(pl.multiple_of(j * 256, 256), 256)
            res = jnp.dot(act, wd[:, cols], preferred_element_type=F32) * weight
            part[pl.ds(pl.multiple_of(c * n, n), n), :, cols] = (
                res.astype(BF16).reshape(n, r, 256)
            )
            return carry

        lax.fori_loop(0, d // 256, out_cols, 0)

        @pl.when(s == 1)
        def _():
            plane.scatter_near(0)

        @pl.when(s == 2)
        def _():
            plane.scatter_near(1)

        return carry

    lax.fori_loop(0, 4, column, 0)
    plane.scatter_far()
    saves = [
        pltpu.make_async_copy(pay.at[:, pl.ds(0, d)], arrived_ref, osem.at[0]),
        pltpu.make_async_copy(gp, gp_ref, osem.at[1]),
        pltpu.make_async_copy(up, up_ref, osem.at[2]),
        pltpu.make_async_copy(inner, inner_ref, osem.at[3]),
    ]
    for save in saves:
        save.start()
    for step in plane.closing_steps(total):
        step()
    plane.scatter_finish(total)
    add_rows(out_ref, mid_ref, total)
    plane.gather_drain(slot)
    for save in saves:
        save.wait()


def scatter_buffers(n, r, d):
    block = pltpu.VMEM((n, r, d), BF16)
    return [
        pltpu.VMEM((4 * n, r, d), BF16),
        pltpu.VMEM((2, n, r, d), BF16),
        *[block] * 4,
        *[pltpu.VMEM((r, d), F32)] * 2,
    ]


def in_vmem(count):
    return [pl.BlockSpec(memory_space=pltpu.VMEM)] * count


def in_place(count):
    return [pl.BlockSpec(memory_space=pl.ANY)] * count


def moe_forward(layer, n, mid, payload, own, other, cid):
    r, d = mid.shape
    ff = own[0].shape[1]
    total_rows = 4 * n * r
    width = payload.shape[1]
    return pl.pallas_call(
        functools.partial(moe_forward_kernel, n, layer),
        out_shape=(
            jax.ShapeDtypeStruct((r, d), BF16),
            jax.ShapeDtypeStruct((total_rows, d), BF16),
            jax.ShapeDtypeStruct((total_rows, 1), F32),
            jax.ShapeDtypeStruct((total_rows, ff), BF16),
            jax.ShapeDtypeStruct((total_rows, ff), BF16),
            jax.ShapeDtypeStruct((total_rows, ff), BF16),
        ),
        in_specs=in_vmem(2) + in_place(6),
        out_specs=tuple(in_vmem(1) + in_place(1) + in_vmem(1) + in_place(3)),
        scratch_shapes=[
            pltpu.VMEM((total_rows, width), BF16),
            pltpu.VMEM((d, ff), BF16),
            pltpu.VMEM((d, ff), BF16),
            pltpu.VMEM((ff, d), BF16),
        ]
        + scatter_buffers(n, r, d)
        + [pltpu.VMEM((total_rows, ff), BF16)] * 3
        + [pltpu.SemaphoreType.DMA((3,)), pltpu.SemaphoreType.DMA((4,))]
        + [pltpu.SemaphoreType.DMA((n,))] * 14
        + [pltpu.SemaphoreType.DMA((2, n))] * 2
        + [pltpu.SemaphoreType.DMA((n,))] * 2,
        compiler_params=pltpu.CompilerParams(
            collective_id=cid, has_side_effects=True, vmem_limit_bytes=63 << 20
        ),
        name="moe_forward",
    )(mid, payload, *own, *other)


def moe_backward_kernel(
    n,
    layer,
    cot_ref,
    mid_ref,
    gain_ref,
    weight_ref,
    arrived_hbm,
    gp_hbm,
    up_hbm,
    inner_hbm,
    wg_own,
    wu_own,
    wd_own,
    wg_other,
    wu_other,
    wd_other,
    *rest,
):
    rest = rest[0 if layer else 6 :]
    dmid_ref, dgain_ref = rest[:2]
    keep_refs, give_refs = rest[2:5], rest[5:8]
    (
    cots,
    wg,
    wu,
    wd,
    part,
    sides,
    din,
    zup,
    zdn,
    stage,
    acc,
    total,
    arrived,
    gp,
    up,
    inner,
    de,
    out_gate,
    out_up,
    out_down,
    wsem,
    isem,
    osem,
    *sems,
    ) = rest[8:]
    section = lax.axis_index("section")
    r, d = mid_ref.shape
    ff = wg.shape[1]
    rows = n * r
    own, other, held = (
        (wg_own, wu_own, wd_own),
        (wg_other, wu_other, wd_other),
        (wg, wu, wd),
    )
    loads = [
        pltpu.make_async_copy(gp_hbm, gp, isem.at[0]),
        pltpu.make_async_copy(up_hbm, up, isem.at[1]),
        pltpu.make_async_copy(arrived_hbm, arrived, isem.at[2]),
        pltpu.make_async_copy(inner_hbm, inner, isem.at[3]),
    ]
    fetch_layer(layer, own, other, held, wsem)
    for load in loads:
        load.start()
    plane = Plane(n, sems)
    me, gy = plane.me, plane.gy
    hello(n, me, gy, True)
    cots[pl.ds(pl.multiple_of((gy * n + me) * r, r), r)] = cot_ref[...]

    def slot(z, c):
        return cots.at[pl.ds((c * n + z) * r, r)]

    plane.scatter_setup(lambda z, c: part.at[c * n + z], sides, din, zup, zdn, stage, acc)
    plane.gather_own_column(slot)
    fetch_wait(own, held, wsem, range(3))
    for load in loads:
        load.wait()

    def column(s, carry):
        c = flip_by(gy, s)

        @pl.when(s == 1)
        def _():
            plane.gather_pass_on(slot)

        @pl.when(s == 3)
        def _():
            plane.gather_far_column(slot)

        at = pl.ds(pl.multiple_of(c * rows, rows), rows)
        de[at] = (cots[at].astype(F32) * weight_ref[at]).astype(BF16)
        block = de[at]

        def mid_cols(j, carry):
            cols = pl.ds(pl.multiple_of(j * 256, 256), 256)
            dz = dot32(block, wd[cols], COL_PAIR)
            g = gp[at, cols].astype(F32)
            u = up[at, cols].astype(F32)
            sg = 1.0 / (1.0 + jnp.exp(-g))
            gp[at, cols] = (dz * u * sg * (1.0 + g * (1.0 - sg))).astype(BF16)
            up[at, cols] = (dz * g * sg).astype(BF16)
            return carry

        lax.fori_loop(0, ff // 256, mid_cols, 0)
        dgp = gp[at]
        dup = up[at]

        def in_cols(j, carry):
            cols = pl.ds(pl.multiple_of(j * 256, 256), 256)
            res = dot32(dgp, wg[cols], COL_PAIR) + dot32(dup, wu[cols], COL_PAIR)
            part[pl.ds(pl.multiple_of(c * n, n), n), :, cols] = (
                res.astype(BF16).reshape(n, r, 256)
            )
            return carry

        lax.fori_loop(0, d // 256, in_cols, 0)

        @pl.when(s == 1)
        def _():
            plane.scatter_near(0)

        @pl.when(s == 2)
        def _():
            plane.scatter_near(1)

        return carry

    lax.fori_loop(0, 4, column, 0)
    plane.scatter_far()

    def saving(i, refs):
        at = pl.ds(pl.multiple_of(i * 256, 256), 256)
        for k, (src, ref) in enumerate(zip((out_gate, out_up, out_down), refs)):
            where = (slice(None), at) if k == 2 else (at, slice(None))
            yield pltpu.make_async_copy(src.at[where], ref.at[where], osem.at[k, i])

    chunks = d // 256

    def weight_grads(i, carry):
        at = pl.ds(pl.multiple_of(i * 256, 256), 256)
        left = arrived[:, at]
        out_gate[at] = dot32(left, gp[...], ROW_PAIR).astype(BF16)
        out_up[at] = dot32(left, up[...], ROW_PAIR).astype(BF16)
        out_down[:, at] = dot32(inner[...], de[:, at], ROW_PAIR).astype(BF16)

        @pl.when(section == layer)
        def _():
            for copy in saving(i, keep_refs):
                copy.start()

        @pl.when(section != layer)
        def _():
            for copy in saving(i, give_refs):
                copy.start()

        for k, step in enumerate(plane.closing_steps(total)):
            pl.when(i == min(k + 1, chunks - 1))(step)

        return carry

    lax.fori_loop(0, chunks, weight_grads, 0)
    plane.scatter_finish(total)

    mid = mid_ref[...]
    scale = lax.rsqrt(jnp.mean(mid * mid, axis=-1, keepdims=True) + EPSILON)
    unit = mid * scale
    db = total[...]
    dgain_ref[...] = jnp.sum(db * unit, axis=0, keepdims=True)
    dmid_ref[...] = cot_ref[...].astype(F32) + norm_back(db * gain_ref[...], unit, scale)
    plane.gather_drain(slot)

    def settle(i, carry):
        for copy in saving(i, keep_refs):
            copy.wait()
        return carry

    lax.fori_loop(0, chunks, settle, 0)


def moe_backward(layer, n, cot, mid, gain, weight, arrived, gp, up, inner, own, other, so_far, cid):
    r, d = mid.shape
    ff = own[0].shape[1]
    total_rows = 4 * n * r
    sums = [jax.ShapeDtypeStruct(shape, BF16) for shape in ((d, ff), (d, ff), (ff, d))] * 2
    return pl.pallas_call(
        functools.partial(moe_backward_kernel, n, layer),
        out_shape=(
            jax.ShapeDtypeStruct((r, d), F32),
            jax.ShapeDtypeStruct((1, d), F32),
            *sums,
        ),
        in_specs=in_vmem(4) + in_place(10 + len(so_far)),
        out_specs=tuple(in_vmem(2) + in_place(6)),
        input_output_aliases={14 + k: 2 + k for k in range(len(so_far))},
        scratch_shapes=[
            pltpu.VMEM((total_rows, d), BF16),
            pltpu.VMEM((d, ff), BF16),
            pltpu.VMEM((d, ff), BF16),
            pltpu.VMEM((ff, d), BF16),
        ]
        + scatter_buffers(n, r, d)
        + [pltpu.VMEM((total_rows, d), BF16)]
        + [pltpu.VMEM((total_rows, ff), BF16)] * 3
        + [pltpu.VMEM((total_rows, d), BF16)]
        + [pltpu.VMEM((d, ff), BF16)] * 2
        + [pltpu.VMEM((ff, d), BF16)]
        + [
            pltpu.SemaphoreType.DMA((3,)),
            pltpu.SemaphoreType.DMA((4,)),
        ]
        + [pltpu.SemaphoreType.DMA((3, d // 256))]
        + [pltpu.SemaphoreType.DMA((n,))] * 14
        + [pltpu.SemaphoreType.DMA((2, n))] * 2
        + [pltpu.SemaphoreType.DMA((n,))] * 2,
        compiler_params=pltpu.CompilerParams(
            collective_id=cid, has_side_effects=True, vmem_limit_bytes=63 << 20
        ),
        name="moe_backward",
    )(cot, mid, gain, weight, arrived, gp, up, inner, *own, *other, *so_far)


class Share:
    def __init__(self, layer, pieces, full, scratch):
        self.full = full
        self.held, self.load_sems, self.plane_sems, self.to_sems, self.from_sems = scratch
        self.loads, first = [], 0
        for k, piece in enumerate(pieces):
            last = first + piece.shape[1]
            into = self.held.at[:, first:last]
            self.loads.append(pltpu.make_async_copy(piece, into, self.load_sems.at[k]))
            first = last
        self.section = lax.axis_index("section")
        self.mine = self.section == layer
        gy = lax.axis_index("gy")
        self.cols = [gy_flip(gy, bits) if bits else gy for bits in range(4)]
        self.rows = self.held.shape[0]

    def at(self, column, half=None):
        rows = self.rows
        if half is None:
            return self.full.at[pl.ds(pl.multiple_of(column * rows, rows), rows)]
        few = rows // 2
        return self.full.at[pl.ds(pl.multiple_of(column * rows + half * few, few), few)]

    def own(self):
        return pltpu.make_async_copy(self.held, self.at(self.cols[0]), self.plane_sems.at[0])

    def direct(self, bit):
        s = self.plane_sems
        k = 1 if bit == 1 else 3
        return remote(
            self.held, self.at(self.cols[0]), s.at[k], s.at[k + 1], gy=self.cols[bit]
        )

    def onward(self, bit):
        s = self.plane_sems
        k = 5 if bit == 1 else 7
        half = 1 if bit == 1 else 0
        ref = self.at(self.cols[3 - bit], half)
        return remote(ref, ref, s.at[k], s.at[k + 1], gy=self.cols[bit])

    def hand(self, k):
        if k == 0:
            src, dst = self.held, self.at(self.cols[0])
        elif k < 3:
            src = dst = self.at(self.cols[k])
        else:
            src = dst = self.at(self.cols[3], k - 3)
        return remote(src, dst, self.to_sems.at[k], self.from_sems.at[k], section=1 - self.section)

    def start(self):
        @pl.when(self.mine)
        def _():
            for load in self.loads:
                load.start()
            for load in self.loads:
                load.wait()
            self.direct(1).start()
            self.direct(2).start()
            self.own().start()
            self.hand(0).start()

    def pass_on(self):
        @pl.when(self.mine)
        def _():
            self.direct(1).wait_recv()
            self.onward(2).start()
            self.hand(1).start()
            self.direct(2).wait_recv()
            self.onward(1).start()
            self.hand(2).start()

    def finish(self):
        @pl.when(self.mine)
        def _():
            self.onward(2).wait_recv()
            self.hand(3).start()
            self.onward(1).wait_recv()
            self.hand(4).start()
            self.own().wait()

        @pl.when(jnp.logical_not(self.mine))
        def _():
            for k in range(5):
                self.hand(k).wait_recv()

    def drain(self):
        @pl.when(self.mine)
        def _():
            for bit in (1, 2):
                self.direct(bit).wait_send()
                self.onward(bit).wait_send()
            for k in range(5):
                self.hand(k).wait_send()


def share_scratch(shape):
    dma = pltpu.SemaphoreType.DMA
    return [pltpu.VMEM(shape, BF16), dma((3,)), dma((9,)), dma((5,)), dma((5,))]


def shard_pieces(query, key, value, out):
    heads = query.shape[2] // HD
    kv_head = lax.axis_index("gx") * heads // (HQ // KVH)
    own = pl.ds(pl.multiple_of(kv_head * HD, HD), HD)
    return [(query.at[0], key.at[0, :, own], value.at[0, :, own]), (out.at[0],)]


def shard_shapes(shards):
    rows, span = shards[0].shape[1:]
    return [(rows, span + 2 * HD), (rows, span)]


def full_shapes(shards):
    return [jax.ShapeDtypeStruct((4 * rows, cols), BF16) for rows, cols in shard_shapes(shards)]


def share_kernel(n, layer, few, *refs):
    shards, smalls = refs[:4], refs[4 : 4 + few]
    fulls, others = refs[4 + few : 6 + few], refs[6 + few : 6 + 2 * few]
    send, recv, *scratch = refs[6 + 2 * few :]
    other = 1 - lax.axis_index("section")
    swaps = [
        remote(smalls[k], others[k], send.at[k], recv.at[k], section=other) for k in range(few)
    ]
    shares = [
        Share(layer, pieces, fulls[k], scratch[5 * k : 5 * k + 5])
        for k, pieces in enumerate(shard_pieces(*shards))
    ]
    hello(n, lax.axis_index("gx"), lax.axis_index("gy"), True, True)
    for share in shares:
        share.start()
    for swap in swaps:
        swap.start()
    for share in shares:
        share.pass_on()
    for share in shares:
        share.finish()
    for share in shares:
        share.drain()
    for swap in swaps:
        swap.wait()


def share_weights(layer, n, shards, smalls, cid):
    few = len(smalls)
    return pl.pallas_call(
        functools.partial(share_kernel, n, layer, few),
        out_shape=(
            *full_shapes(shards),
            *(jax.ShapeDtypeStruct(small.shape, small.dtype) for small in smalls),
        ),
        in_specs=in_place(4 + few),
        out_specs=tuple(in_place(2 + few)),
        scratch_shapes=[pltpu.SemaphoreType.DMA((few,))] * 2
        + [item for shape in shard_shapes(shards) for item in share_scratch(shape)],
        compiler_params=pltpu.CompilerParams(collective_id=cid, has_side_effects=True),
        name="share_weights",
    )(*shards, *smalls)


def finish_line_kernel(n, *refs):
    gains, rest = refs[:8], refs[8:]
    kv_ref, gain_ref, key_ref, value_ref, gbuf, kv_all, stage, incoming, rsem, *sems = rest
    me = lax.axis_index("gx")
    gy = lax.axis_index("gy")
    kv_all[me] = kv_ref[...]
    for k in range(2):
        first = 0
        for ref in gains[4 * k : 4 * k + 4]:
            last = first + ref.shape[1]
            gbuf[me, k : k + 1, first:last] = ref[...]
            first = last
    hello(n, me, gy, True)
    few = Line(n, None, lambda z: gbuf.at[z], None, sems[:4])
    many = Line(n, None, lambda z: kv_all.at[z], None, sems[4:8])
    few.gather_step(0)
    many.gather_step(0)
    steps = [functools.partial(many.gather_step, k) for k in range(1, n)]
    for k in range(1, n):
        few.gather_step(k)
        if k == n // 2:
            steps.pop(0)()
    total = gbuf[0]
    for z in range(1, n):
        total = total + gbuf[z]
    for k, where in enumerate(({"gy": gy_flip(gy, 1)}, {"gy": gy_flip(gy, 2)})):
        stage[k] = total
        swap = remote(stage.at[k], incoming.at[k], rsem.at[0, k], rsem.at[1, k], **where)
        swap.start()
        if steps:
            steps.pop(0)()
        swap.wait()
        total = total + incoming[k]
    gain_ref[...] = total
    for step in steps:
        step()
    for z in range(n):
        cols = slice(z * HD, (z + 1) * HD)
        key_ref[:, cols] = kv_all[z, :, :HD].astype(F32)
        value_ref[:, cols] = kv_all[z, :, HD:].astype(F32)
    few.gather_drain()
    many.gather_drain()


def finish_line(n, gains, kv, cid):
    dma = pltpu.SemaphoreType.DMA
    shape = jax.ShapeDtypeStruct
    width = sum(gain.shape[1] for gain in gains[:4])
    return pl.pallas_call(
        functools.partial(finish_line_kernel, n),
        out_shape=(
            shape((2, width), F32),
            shape((kv.shape[0], n * HD), F32),
            shape((kv.shape[0], n * HD), F32),
        ),
        in_specs=in_vmem(9),
        out_specs=tuple(in_vmem(3)),
        scratch_shapes=[
            pltpu.VMEM((n, 2, width), F32),
            pltpu.VMEM((n,) + kv.shape, BF16),
            pltpu.VMEM((2, 2, width), F32),
            pltpu.VMEM((2, 2, width), F32),
            dma((2, 2)),
        ]
        + [dma((n,))] * 8,
        compiler_params=pltpu.CompilerParams(collective_id=cid, has_side_effects=True),
        name="finish_line",
    )(*gains, kv)


def finish_pair_kernel(*refs):
    gain_ref, *rows = refs[:5]
    out_rows, out_gains = refs[5:7], refs[7:11]
    incoming, send, recv = refs[11:]
    section = lax.axis_index("section")
    other = 1 - section
    barrier = pltpu.get_barrier_semaphore()
    mesh_ids = pl.DeviceIdType.MESH
    pl.semaphore_signal(barrier, 1, device_id={"section": other}, device_id_type=mesh_ids)
    pl.semaphore_wait(barrier, 1)
    swap = remote(gain_ref, incoming, send.at[2], recv.at[2], section=other)
    swap.start()
    for mine in range(2):

        @pl.when(section == mine)
        def _():
            for k in range(2):
                src, dst = rows[2 * k + 1 - mine], out_rows[k].at[mine]
                remote(src, dst, send.at[k], recv.at[k], section=other).start()
            for k in range(2):
                out_rows[k][mine] = rows[2 * k + mine][...]

    swap.wait()
    for mine in range(2):

        @pl.when(section == mine)
        def _():
            first = 0
            for ref in out_gains:
                last = first + ref.shape[1]
                at = (slice(mine, mine + 1), slice(first, last))
                ref[...] = gain_ref[at] + incoming[at]
                first = last
            for k in range(2):
                src, dst = rows[2 * k + 1 - mine], out_rows[k].at[mine]
                remote(src, dst, send.at[k], recv.at[k], section=other).wait()


def finish_pair(gains, widths, lo, ig, cid):
    dma = pltpu.SemaphoreType.DMA
    shape = jax.ShapeDtypeStruct
    both = shape((2,) + lo[0].shape, BF16)
    return pl.pallas_call(
        finish_pair_kernel,
        out_shape=(both, both, *(shape((1, width), F32) for width in widths)),
        in_specs=in_vmem(5),
        out_specs=tuple(in_vmem(6)),
        scratch_shapes=[pltpu.VMEM(gains.shape, F32), dma((3,)), dma((3,))],
        compiler_params=pltpu.CompilerParams(collective_id=cid, has_side_effects=True),
        name="finish_pair",
    )(gains, *lo, *ig)


class Reduce:
    def __init__(self, layer, part, inbox, xin, yin, din, sems):
        self.part, self.inbox = part, inbox
        self.xin, self.yin, self.din = xin, yin, din
        self.give_sems, self.take_sems, self.send_sems, self.recv_sems = sems
        self.section = lax.axis_index("section")
        self.mine = self.section == layer
        gy = lax.axis_index("gy")
        self.cols = [gy_flip(gy, bits) if bits else gy for bits in range(4)]
        self.few = xin.shape[0] // 2

    def give(self, k, src):
        return remote(
            src,
            self.inbox.at[self.cols[k]],
            self.give_sems.at[k],
            self.take_sems.at[k],
            section=1 - self.section,
        )

    def half(self, ref, h):
        return ref.at[pl.ds(h * self.few, self.few)]

    def far(self, bit):
        k = bit - 1
        src = self.half(self.part(self.cols[3]), k)
        return remote(
            src, self.din.at[k], self.send_sems.at[k], self.recv_sems.at[k], gy=self.cols[bit]
        )

    def near(self, bit, h):
        k = 2 * bit + h
        into = self.xin if bit == 1 else self.yin
        return remote(
            self.half(self.part(self.cols[bit]), h),
            self.half(into, h),
            self.send_sems.at[k],
            self.recv_sems.at[k],
            gy=self.cols[bit],
        )

    def send_term(self, k):
        @pl.when(self.mine)
        def _():
            ref = self.part(self.cols[k])
            self.give(k, ref).wait_recv()
            add_rows(ref, ref, self.inbox.at[self.cols[k]])
            if k == 3:
                self.far(1).start()
                self.far(2).start()
            elif k:
                self.near(k, k - 1).start()

    def pass_on(self):
        @pl.when(self.mine)
        def _():
            self.far(1).wait_recv()
            ref = self.half(self.part(self.cols[2]), 0)
            add_rows(ref, ref, self.din.at[0])
            self.near(2, 0).start()
            self.far(2).wait_recv()
            ref = self.half(self.part(self.cols[1]), 1)
            add_rows(ref, ref, self.din.at[1])
            self.near(1, 1).start()

    def close(self, outs):
        @pl.when(self.mine)
        def _():
            for bit in (1, 2):
                for h in (0, 1):
                    self.near(bit, h).wait_recv()
            for ref, first, last in outs:
                cols = slice(first, last)
                own = self.part(self.cols[0])
                add_rows(ref, own.at[:, cols], self.xin.at[:, cols], self.yin.at[:, cols])
            for bit in (1, 2):
                self.far(bit).wait_send()
                for h in (0, 1):
                    self.near(bit, h).wait_send()


def reduce_sems():
    dma = pltpu.SemaphoreType.DMA
    return [dma((4,)), dma((4,)), dma((6,)), dma((6,))]


class Line:
    def __init__(self, n, m, slot, terms, sems):
        self.n, self.m, self.slot = n, m, slot
        self.me = lax.axis_index("gx")
        if terms is not None:
            self.col, self.zup, self.zdn, self.stage = (ref.at[m] for ref in terms)
        self.sems = [sem if m is None else sem.at[m] for sem in sems]

    def gather_up(self, k):
        ref = self.slot(self.me - k)
        return remote(ref, ref, self.sems[0].at[k], self.sems[1].at[k], gx=self.me + 1)

    def gather_down(self, k):
        ref = self.slot(self.me + k)
        return remote(ref, ref, self.sems[2].at[k], self.sems[3].at[k], gx=self.me - 1)

    def gather_step(self, k):
        n, me = self.n, self.me

        @pl.when(me - k >= 0)
        def _():
            if k:
                ref = self.slot(me - k)
                sems = self.sems
                remote(ref, ref, sems[0].at[k - 1], sems[1].at[k - 1], gx=me + 1).wait_recv()
            if k < n - 1:

                @pl.when(me + 1 < n)
                def _():
                    self.gather_up(k).start()

        @pl.when(me + k < n)
        def _():
            if k:
                ref = self.slot(me + k)
                sems = self.sems
                remote(ref, ref, sems[2].at[k - 1], sems[3].at[k - 1], gx=me - 1).wait_recv()
            if k < n - 1:

                @pl.when(me > 0)
                def _():
                    self.gather_down(k).start()

    def up(self, z):
        send, recv = self.sems[4:6]
        return remote(self.stage.at[z], self.zup.at[z], send.at[z], recv.at[z], gx=self.me + 1)

    def down(self, z):
        send, recv = self.sems[6:8]
        return remote(self.stage.at[z], self.zdn.at[z], send.at[z], recv.at[z], gx=self.me - 1)

    def scatter_tick(self, hop):
        n, me = self.n, self.me

        @pl.when(me == hop)
        def _():
            for z in reversed(range(hop + 1, n)):
                if hop:
                    self.up(z).wait_recv()
                    add_rows(self.stage.at[z], self.col.at[z], self.zup.at[z])
                else:
                    add_rows(self.stage.at[z], self.col.at[z])
                self.up(z).start()

        @pl.when(me == n - 1 - hop)
        def _():
            for z in range(n - 1 - hop):
                if hop:
                    self.down(z).wait_recv()
                    add_rows(self.stage.at[z], self.col.at[z], self.zdn.at[z])
                else:
                    add_rows(self.stage.at[z], self.col.at[z])
                self.down(z).start()

    def scatter_finish(self, total):
        n, me = self.n, self.me
        add_rows(total, self.col.at[me])

        @pl.when(me > 0)
        def _():
            self.up(me).wait_recv()
            add_rows(total, total, self.zup.at[me])

        @pl.when(me < n - 1)
        def _():
            self.down(me).wait_recv()
            add_rows(total, total, self.zdn.at[me])

    def gather_drain(self):
        n, me = self.n, self.me
        for k in range(n - 1):

            @pl.when((me - k >= 0) & (me + 1 < n))
            def _():
                self.gather_up(k).wait_send()

            @pl.when((me + k < n) & (me > 0))
            def _():
                self.gather_down(k).wait_send()

    def drain(self):
        n, me = self.n, self.me
        self.gather_drain()
        for z in range(n):

            @pl.when(me < z)
            def _():
                self.up(z).wait_send()

            @pl.when(me > z)
            def _():
                self.down(z).wait_send()


def unit_of(value):
    scale = lax.rsqrt(jnp.mean(value * value, axis=-1, keepdims=True) + EPSILON)
    return value * scale, scale


def half_turn(value):
    return pltpu.roll(value, value.shape[-1] // 2, axis=value.ndim - 1)


def attn_forward_kernel(
    n,
    layer,
    heads,
    x_ref,
    gain_attn,
    gain_ffn,
    gain_query,
    gain_key,
    cos_ref,
    sin_ref,
    mask_ref,
    gates_ref,
    win_hbm,
    wout_hbm,
    *rest,
):
    ahead = layer == 0
    shards, rest = (rest[:4], rest[4:]) if ahead else ((), rest)
    mid_ref, pay_ref, normed_hbm, proj_hbm, qr_hbm, kr_ref, v_ref, prob_hbm, mixed_hbm = rest[:9]
    fulls, rest = (rest[9:11], rest[11:]) if ahead else ((), rest[9:])
    (
    win,
    wout,
    normed,
    proj,
    qr,
    prob,
    mixed,
    col,
    zup,
    zdn,
    stage,
    total,
    wsem,
    osem,
    *sems,
    ) = rest
    mb, length, d = normed.shape
    t = length // n
    r = mb * t
    span = heads * HD
    me = lax.axis_index("gx")
    shares = []
    if ahead:
        shares = [
            Share(1, pieces, fulls[k], sems[8 + 5 * k : 13 + 5 * k])
            for k, pieces in enumerate(shard_pieces(*shards))
        ]
    fetch_in = pltpu.make_async_copy(win_hbm, win, wsem.at[0])
    fetch_out = pltpu.make_async_copy(wout_hbm, wout, wsem.at[1])
    fetch_in.start()
    fetch_out.start()
    hello(n, me, lax.axis_index("gy"), ahead, ahead)
    for share in shares:
        share.start()
    hidden = x_ref[...].astype(F32)
    unit, _ = unit_of(hidden)
    low = (unit * gain_attn[...]).astype(BF16)
    normed[:, pl.ds(pl.multiple_of(me * t, t), t)] = low.reshape(mb, t, d)
    lines = [
        Line(
            n,
            m,
            lambda z, m=m: normed.at[m, pl.ds(z * t, t)],
            (col, zup, zdn, stage),
            sems[:8],
        )
        for m in range(mb)
    ]
    waiting = []

    def tick():
        if waiting:
            waiting.pop(0)()

    for k in range(n):
        lines[0].gather_step(k)
        if k == min(1, n - 1):
            for line in lines[1:]:
                line.gather_step(0)
    fetch_in.wait()
    cosine, sine = cos_ref[...], sin_ref[...]
    for m, line in enumerate(lines):
        first = m * length
        rows = slice(first, first + length)
        if m + 1 < mb:
            waiting += [functools.partial(lines[m + 1].gather_step, k) for k in range(1, n)]

        def project(j, carry, m=m, rows=rows):
            cols = pl.ds(pl.multiple_of(j * 256, 256), 256)
            proj[rows, cols] = jnp.dot(normed[m], win[:, cols], preferred_element_type=F32)
            return carry

        blocks = (span + 2 * HD) // 256
        lax.fori_loop(0, blocks // 2, project, 0)
        tick()
        lax.fori_loop(blocks // 2, blocks, project, 0)
        tick()
        key_unit, _ = unit_of(proj[rows, span : span + HD])
        key = key_unit * gain_key[...]
        kr_ref[rows] = (key * cosine[rows] + half_turn(key) * sine[rows]).astype(BF16)
        v_ref[rows] = proj[rows, span + HD :].astype(BF16)

        def head(h, carry, m=m, rows=rows):
            at = pl.ds(pl.multiple_of(h * HD, HD), HD)
            query_unit, _ = unit_of(proj[rows, at])
            query = query_unit * gain_query[...]
            turned = (query * cosine[rows] + half_turn(query) * sine[rows]).astype(BF16)
            qr[rows, at] = turned
            scores = dot32(turned, kr_ref[rows], COL_PAIR) * (1.0 / math.sqrt(HD))
            exponent = jnp.where(mask_ref[m] > 0.5, jnp.exp(scores), 0.0)
            p = (exponent * (1.0 / jnp.sum(exponent, axis=-1, keepdims=True))).astype(BF16)
            prob[m * heads + h] = p
            mixed[rows, at] = jnp.dot(p, v_ref[rows], preferred_element_type=F32).astype(BF16)
            return carry

        lax.fori_loop(0, heads // 2, head, 0, unroll=2)
        tick()
        lax.fori_loop(heads // 2, heads, head, 0, unroll=2)
        while waiting:
            tick()
        if m == mb - 1:
            for share in shares:
                share.pass_on()
        if m == 0:
            fetch_out.wait()

        def out_cols(j, carry, m=m, rows=rows):
            at = pl.ds(pl.multiple_of(j * 256, 256), 256)
            res = dot32(mixed[rows], wout[at], COL_PAIR).astype(BF16)
            for z in range(n):
                col[m, z, :, at] = res[z * t : (z + 1) * t]
            return carry

        lax.fori_loop(0, d // 256, out_cols, 0)
        line.scatter_tick(0)
        waiting += [functools.partial(line.scatter_tick, hop) for hop in range(1, n - 1)]
    saves = [
        pltpu.make_async_copy(normed, normed_hbm, osem.at[0]),
        pltpu.make_async_copy(proj, proj_hbm, osem.at[1]),
        pltpu.make_async_copy(qr, qr_hbm, osem.at[2]),
        pltpu.make_async_copy(prob, prob_hbm, osem.at[3]),
        pltpu.make_async_copy(mixed, mixed_hbm, osem.at[4]),
    ]
    for save in saves:
        save.start()
    while waiting:
        tick()
    for m, line in enumerate(lines):
        line.scatter_finish(total.at[m * t : (m + 1) * t])
    mid = x_ref[...].astype(F32) + total[...]
    mid_ref[...] = mid
    unit, _ = unit_of(mid)
    pay_ref[:, :d] = (unit * gain_ffn[...]).astype(BF16)
    pay_ref[:, d:] = gates_ref[...]
    for share in shares:
        share.finish()
    for share in shares:
        share.drain()
    for line in lines:
        line.drain()
    for save in saves:
        save.wait()


def line_buffers(mb, n, r, d):
    return [pltpu.VMEM((mb, n, r // mb, d), BF16)] * 4 + [pltpu.VMEM((r, d), F32)]


def attn_forward(layer, n, x, gains, tables, gate_cols, w_in, w_out, shards, cid, mb):
    r, d = x.shape
    cosine, sine, mask = tables
    total_rows = cosine.shape[0]
    length = total_rows // mb
    width = w_in.shape[1]
    heads = w_out.shape[1] // HD
    span = heads * HD
    shape = jax.ShapeDtypeStruct
    return pl.pallas_call(
        functools.partial(attn_forward_kernel, n, layer, heads),
        out_shape=(
            shape((r, d), F32),
            shape((r, d + 128), BF16),
            shape((mb, length, d), BF16),
            shape((total_rows, width), F32),
            shape((total_rows, span), BF16),
            shape((total_rows, HD), BF16),
            shape((total_rows, HD), BF16),
            shape((mb * heads, length, length), BF16),
            shape((total_rows, span), BF16),
            *(full_shapes(shards) if shards else ()),
        ),
        in_specs=in_vmem(9) + in_place(2 + len(shards)),
        out_specs=tuple(in_vmem(2) + in_place(3) + in_vmem(2) + in_place(4 if shards else 2)),
        scratch_shapes=[
            pltpu.VMEM((d, width), BF16),
            pltpu.VMEM((d, span), BF16),
            pltpu.VMEM((mb, length, d), BF16),
            pltpu.VMEM((total_rows, width), F32),
            pltpu.VMEM((total_rows, span), BF16),
            pltpu.VMEM((mb * heads, length, length), BF16),
            pltpu.VMEM((total_rows, span), BF16),
        ]
        + line_buffers(mb, n, r, d)
        + [pltpu.SemaphoreType.DMA((2,)), pltpu.SemaphoreType.DMA((5,))]
        + [pltpu.SemaphoreType.DMA((mb, n))] * 8
        + [
            item
            for size in (shard_shapes(shards) if shards else ())
            for item in share_scratch(size)
        ],
        compiler_params=pltpu.CompilerParams(
            collective_id=cid, has_side_effects=True, vmem_limit_bytes=60 << 20
        ),
        name="attn_forward",
    )(x, *gains, cosine, sine, mask, gate_cols, w_in, w_out, *shards)


def attn_backward_kernel(
    n,
    layer,
    heads,
    dmid_ref,
    x_ref,
    gain_attn,
    gain_query,
    gain_key,
    cos_ref,
    sin_ref,
    kr_ref,
    v_ref,
    normed_hbm,
    proj_hbm,
    qr_hbm,
    prob_hbm,
    mixed_hbm,
    win_hbm,
    wout_hbm,
    *rest,
):
    last = layer == 0
    if last:
        later_hbm, gives, rest = rest[0], rest[1:4], rest[4:]
    cot_ref, dgain_attn, dgain_query, dgain_key = rest[:4]
    outs, rest = rest[4 : 10 if last else 5], rest[10 if last else 5 :]
    (
    win,
    wout,
    normed,
    proj,
    qr,
    prob,
    mixed,
    dmids,
    dheads,
    dproj,
    dkey,
    dvalue,
    grads,
    col,
    zup,
    zdn,
    stage,
    total,
    wsem,
    isem,
    osem,
    *sems,
    ) = rest
    mb, length, d = normed.shape
    t = length // n
    span = heads * HD
    me = lax.axis_index("gx")
    inv_root = 1.0 / math.sqrt(HD)
    gy = lax.axis_index("gy")
    section = lax.axis_index("section")
    fetch_out = pltpu.make_async_copy(wout_hbm, wout, wsem.at[0])
    fetch_in = pltpu.make_async_copy(win_hbm, win, wsem.at[1])
    fetch_out.start()
    fetch_in.start()
    loads = [
        pltpu.make_async_copy(prob_hbm, prob, isem.at[0]),
        pltpu.make_async_copy(mixed_hbm, mixed, isem.at[1]),
        pltpu.make_async_copy(qr_hbm, qr, isem.at[2]),
        pltpu.make_async_copy(proj_hbm, proj, isem.at[3]),
        pltpu.make_async_copy(normed_hbm, normed, isem.at[4]),
    ]
    for load in loads:
        load.start()
    if last:
        later, inbox, xin, yin, din = sems[8:13]
        block = d // 4

        def reduce(layer, terms, first, last, sems):
            cols = slice(first, last)
            buffers = [ref.at[..., cols] for ref in (inbox, xin, yin, din)]
            return Reduce(layer, lambda c: terms.at[pl.ds(c * block, block), cols], *buffers, sems)

        wide = span + 2 * HD
        job_later = reduce(1, later, 0, wide + span, sems[13:17])
        job = reduce(0, grads, 0, wide, sems[17:21])
        job_out = reduce(0, grads, wide, wide + span, sems[21:25])
        swaps = [
            remote(gives[k], outs[3 + k], sems[25].at[k], sems[26].at[k], section=1 - section)
            for k in range(3)
        ]
        load_later = pltpu.make_async_copy(later_hbm, later, osem.at[0])

        @pl.when(job_later.mine)
        def _():
            load_later.start()

        hello(n, me, gy, True, True)

        @pl.when(jnp.logical_not(job_later.mine))
        def _():
            for k in (3, 1, 2, 0):
                c = job_later.cols[k]
                job_later.give(k, later_hbm.at[pl.ds(c * block, block)]).start()

        for swap in swaps:
            swap.start()
    else:
        hello(n, me, None, False)
    dmids[:, pl.ds(pl.multiple_of(me * t, t), t)] = dmid_ref[...].astype(BF16).reshape(mb, t, d)
    lines = [
        Line(
            n,
            m,
            lambda z, m=m: dmids.at[m, pl.ds(z * t, t)],
            (col, zup, zdn, stage),
            sems[:8],
        )
        for m in range(mb)
    ]
    waiting = []
    sums = []

    def tick():
        if waiting:
            waiting.pop(0)()
        if sums:
            sums.pop(0)()

    if last:
        sums += [functools.partial(job_later.send_term, k) for k in (3, 1, 2, 0)]
        sums += [job_later.pass_on]
    for k in range(n):
        lines[0].gather_step(k)
        if k == min(1, n - 1):
            for line in lines[1:]:
                line.gather_step(0)
        if k == 0 and last:

            @pl.when(job_later.mine)
            def _():
                load_later.wait()

        if k < n - 1:
            tick()
    fetch_out.wait()
    for load in loads:
        load.wait()
    cosine, sine = cos_ref[...], sin_ref[...]
    dkey[...] = jnp.zeros_like(dkey)
    dvalue[...] = jnp.zeros_like(dvalue)
    dgain_query[...] = jnp.zeros_like(dgain_query)
    dgain_key[...] = jnp.zeros_like(dgain_key)
    per = d // 4 // 256

    def out_grads(at):
        left = dmids[:, :, at].reshape(mb * length, 256)
        grads[at, span + 2 * HD :] = dot32(left, mixed[...], ROW_PAIR).astype(BF16)

    def in_grads(at):
        left = normed[:, :, at].reshape(mb * length, 256)
        grads[at, : span + 2 * HD] = dot32(left, dproj[...], ROW_PAIR).astype(BF16)

    def chunked(compute, job):
        def chunk(i, carry):
            first = flip_by(gy, 3 - i // per) * (d // 4) + lax.rem(i, per) * 256
            compute(pl.ds(pl.multiple_of(first, 256), 256))
            for q in range(4):

                @pl.when(i == per * (q + 1) - 1)
                def _():
                    if job is not None:

                        @pl.when(jnp.logical_not(job.mine))
                        def _():
                            job.give(3 - q, job.part(job.cols[3 - q])).start()

                    tick()

            return carry

        lax.fori_loop(0, 4 * per, chunk, 0)

    for m, line in enumerate(lines):
        first = m * length
        rows = slice(first, first + length)
        if m + 1 < mb:
            waiting += [functools.partial(lines[m + 1].gather_step, k) for k in range(1, n)]

        def to_heads(j, carry, m=m, rows=rows):
            cols = pl.ds(pl.multiple_of(j * 256, 256), 256)
            dheads[rows, cols] = jnp.dot(
                dmids[m], wout[:, cols], preferred_element_type=F32
            ).astype(BF16)
            return carry

        lax.fori_loop(0, span // 256, to_heads, 0)
        tick()

        def head(h, carry, m=m, rows=rows):
            at = pl.ds(pl.multiple_of(h * HD, HD), HD)
            p = prob[m * heads + h]
            dh = dheads[rows, at]
            dvalue[rows] += dot32(p, dh, ROW_PAIR)
            dp = dot32(dh, v_ref[rows], COL_PAIR)
            delta = jnp.sum(
                dh.astype(F32) * mixed[rows, at].astype(F32), axis=-1, keepdims=True
            )
            ds = (p.astype(F32) * (dp - delta)).astype(BF16)
            dkey[rows] += dot32(ds, qr[rows, at], ROW_PAIR) * inv_root
            dq = jnp.dot(ds, kr_ref[rows], preferred_element_type=F32) * inv_root
            turned = dq * cosine[rows] - half_turn(dq) * sine[rows]
            unit, scale = unit_of(proj[rows, at])
            dgain_query[...] += jnp.sum(turned * unit, axis=0, keepdims=True)
            dproj[rows, at] = norm_back(turned * gain_query[...], unit, scale).astype(BF16)
            return carry

        lax.fori_loop(0, heads // 2, head, 0, unroll=2)
        tick()
        lax.fori_loop(heads // 2, heads, head, 0, unroll=2)
        tick()
        dk = dkey[rows]
        turned = dk * cosine[rows] - half_turn(dk) * sine[rows]
        unit, scale = unit_of(proj[rows, span : span + HD])
        dgain_key[...] += jnp.sum(turned * unit, axis=0, keepdims=True)
        dproj[rows, span : span + HD] = norm_back(turned * gain_key[...], unit, scale).astype(BF16)
        dproj[rows, span + HD :] = dvalue[rows].astype(BF16)
        if m == 0:
            fetch_in.wait()
        while waiting:
            waiting.pop(0)()

        def in_cols(j, carry, m=m, rows=rows):
            at = pl.ds(pl.multiple_of(j * 256, 256), 256)
            res = dot32(dproj[rows], win[at], COL_PAIR).astype(BF16)
            for z in range(n):
                col[m, z, :, at] = res[z * t : (z + 1) * t]
            return carry

        lax.fori_loop(0, d // 256, in_cols, 0)
        line.scatter_tick(0)
        waiting += [functools.partial(line.scatter_tick, hop) for hop in range(1, n - 1)]
        if m == 0 and last:
            chunked(out_grads, job_out)
            sums += [functools.partial(job_out.send_term, k) for k in (3, 2, 1, 0)]
            sums += [job_out.pass_on]

    if not last:
        chunked(out_grads, None)
    chunked(in_grads, job if last else None)
    while waiting or sums:
        tick()
    if last:
        for k in (3, 2, 1, 0):
            job.send_term(k)
    else:
        save = pltpu.make_async_copy(grads, outs[0], osem.at[0])
        save.start()
    for m, line in enumerate(lines):
        line.scatter_finish(total.at[m * t : (m + 1) * t])
    hidden = x_ref[...].astype(F32)
    unit, scale = unit_of(hidden)
    da = total[...]
    dgain_attn[...] = jnp.sum(da * unit, axis=0, keepdims=True)
    cot_ref[...] = (dmid_ref[...] + norm_back(da * gain_attn[...], unit, scale)).astype(BF16)
    for line in lines:
        line.drain()
    if not last:
        save.wait()
        return
    job.pass_on()
    closing = [(outs[0], 0, span), (outs[1], span, wide), (outs[2], wide, wide + span)]
    job_later.close(closing)
    job_out.close([(outs[2], 0, span)])
    job.close(closing[:2])
    for swap in swaps:
        swap.wait()

    @pl.when(jnp.logical_not(job.mine))
    def _():
        for k in range(4):
            job.give(k, job.part(job.cols[k])).wait_send()
            job_out.give(k, job_out.part(job_out.cols[k])).wait_send()

    @pl.when(jnp.logical_not(job_later.mine))
    def _():
        for k in range(4):
            c = job_later.cols[k]
            job_later.give(k, later_hbm.at[pl.ds(c * block, block)]).wait_send()


def attn_backward(layer, n, dmid, x, gains, tables, kept, w_in, w_out, later, gives, cid, mb):
    r, d = x.shape
    cosine, sine, _ = tables
    normed, proj, qr, kr, v, prob, mixed = kept
    total_rows = cosine.shape[0]
    length = total_rows // mb
    width = w_in.shape[1]
    heads = w_out.shape[1] // HD
    span = heads * HD
    shape = jax.ShapeDtypeStruct
    both = width + span
    grad_shapes = [shape((d, both), BF16)]
    extra = []
    if later:
        block = d // 4
        grad_shapes = [
            shape((block, span), F32),
            shape((block, 2 * HD), BF16),
            shape((block, span), F32),
            *(shape(piece.shape, BF16) for piece in gives),
        ]
        extra = [
            pltpu.VMEM((d, both), BF16),
            pltpu.VMEM((4, block, both), BF16),
            pltpu.VMEM((block, both), BF16),
            pltpu.VMEM((block, both), BF16),
            pltpu.VMEM((2, block // 2, both), BF16),
        ] + reduce_sems() * 3 + [pltpu.SemaphoreType.DMA((3,))] * 2
    return pl.pallas_call(
        functools.partial(attn_backward_kernel, n, layer, heads),
        out_shape=(
            shape((r, d), BF16),
            shape((1, d), F32),
            shape((1, HD), F32),
            shape((1, HD), F32),
            *grad_shapes,
        ),
        in_specs=in_vmem(9) + in_place(7 + len(later) + len(gives)),
        out_specs=tuple(in_vmem(4) + (in_vmem(3) + in_place(3) if later else in_place(1))),
        scratch_shapes=[
            pltpu.VMEM((d, width), BF16),
            pltpu.VMEM((d, span), BF16),
            pltpu.VMEM((mb, length, d), BF16),
            pltpu.VMEM((total_rows, width), F32),
            pltpu.VMEM((total_rows, span), BF16),
            pltpu.VMEM((mb * heads, length, length), BF16),
            pltpu.VMEM((total_rows, span), BF16),
            pltpu.VMEM((mb, length, d), BF16),
            pltpu.VMEM((total_rows, span), BF16),
            pltpu.VMEM((total_rows, width), BF16),
            pltpu.VMEM((total_rows, HD), F32),
            pltpu.VMEM((total_rows, HD), F32),
            pltpu.VMEM((d, both), BF16),
        ]
        + line_buffers(mb, n, r, d)
        + [
            pltpu.SemaphoreType.DMA((2,)),
            pltpu.SemaphoreType.DMA((5,)),
            pltpu.SemaphoreType.DMA((1,)),
        ]
        + [pltpu.SemaphoreType.DMA((mb, n))] * 8
        + extra,
        compiler_params=pltpu.CompilerParams(
            collective_id=cid, has_side_effects=True, vmem_limit_bytes=63 << 20
        ),
        name="attn_backward",
    )(
        dmid,
        x,
        *gains,
        cosine,
        sine,
        kr,
        v,
        normed,
        proj,
        qr,
        prob,
        mixed,
        w_in,
        w_out,
        *later,
        *gives,
    )


def local_wide(
    inputs,
    out_grad,
    segments,
    routes,
    gates,
    gain_attn,
    gain_ffn,
    gain_query,
    gain_key,
    w_query,
    w_key,
    w_value,
    w_out,
    w_gate,
    w_up,
    w_down,
):
    micro_count, _, local_rows, width = inputs.shape
    n_sec = lax.axis_size("section")
    n_gx = lax.axis_size("gx")
    n_gy = lax.axis_size("gy")
    heads = w_query.shape[2] // HD
    span = heads * HD
    experts = n_gx * n_gy
    group_len = segments.shape[2]
    mb = micro_count // n_sec
    rows_own = mb * local_rows
    rows_attn = mb * group_len
    section = lax.axis_index("section")
    gx = lax.axis_index("gx")
    gy = lax.axis_index("gy")
    expert_own = gx * n_gy + gy
    inv_root = 1.0 / math.sqrt(HD)
    first = section * mb

    kv_head = gx * heads // (HQ // KVH)
    key_own = lax.dynamic_slice_in_dim(w_key[0], kv_head * HD, HD, 1)
    value_own = lax.dynamic_slice_in_dim(w_value[0], kv_head * HD, HD, 1)
    w_in_shard = jnp.concatenate([w_query[0], key_own, value_own], axis=1)
    w_in_all = both_layers(lax.all_gather(w_in_shard, "gy", axis=0, tiled=True))
    w_out_all = both_layers(lax.all_gather(w_out[0], "gy", axis=0, tiled=True))
    w_gate_all = both_layers(w_gate[0, 0])
    w_up_all = both_layers(w_up[0, 0])
    w_down_all = both_layers(w_down[0, 0])
    table = dense_gates(routes[0, :, 0], gates[0, :, 0], experts)
    small = jnp.concatenate(
        [
            table.reshape(-1),
            gain_attn[0],
            gain_ffn[0],
            gain_query[0],
            gain_key[0],
        ]
    )
    small_all = both_layers(small)
    table_size = micro_count * local_rows * experts
    table_all = small_all[:, :table_size].reshape(n_sec, micro_count, local_rows, experts)
    gains_all = small_all[:, table_size:]

    table_mine = lax.dynamic_slice_in_dim(table_all, first, mb, 1).reshape(
        n_sec, rows_own, experts
    )
    x_mine = lax.dynamic_slice_in_dim(inputs[:, 0], first, mb, 0).reshape(rows_own, width)
    cot_mine = lax.dynamic_slice_in_dim(out_grad[:, 0], first, mb, 0).reshape(rows_own, width)
    segs = lax.dynamic_slice_in_dim(segments[:, 0], first, mb, 0)
    allowed, cosine, sine = seq_tables(segs, HD)
    cos_q = cosine.reshape(rows_attn, 1, HD // 2)
    sin_q = sine.reshape(rows_attn, 1, HD // 2)
    cos_k = cosine.reshape(rows_attn, HD // 2)
    sin_k = sine.reshape(rows_attn, HD // 2)

    def split_gains(layer):
        g = gains_all[layer]
        return (
            g[:width],
            g[width : 2 * width],
            g[2 * width : 2 * width + HD],
            g[2 * width + HD :],
        )

    saved_all = []
    outs = []
    layer_in = x_mine
    for layer in range(n_sec):
        g_attn, g_ffn, g_query, g_key = split_gains(layer)
        hidden = layer_in.astype(F32)
        attn_unit, attn_scale = normalize(hidden)
        normed = (attn_unit * g_attn).astype(BF16)
        normed_all = gather_z(normed.reshape(mb, local_rows, width)).reshape(rows_attn, width)
        projected = dot32(normed_all, w_in_all[layer])
        query = projected[:, :span].reshape(rows_attn, heads, HD)
        key = projected[:, span : span + HD]
        value_low = projected[:, span + HD :].astype(BF16).reshape(mb, group_len, HD)
        query_unit, query_scale = normalize(query)
        key_unit, key_scale = normalize(key)
        query_rope = (
            rotate(query_unit * g_query, cos_q, sin_q)
            .astype(BF16)
            .reshape(mb, group_len, heads, HD)
        )
        key_rope = rotate(key_unit * g_key, cos_k, sin_k).astype(BF16).reshape(mb, group_len, HD)
        scores = (
            jnp.einsum("mthd,msd->mhts", query_rope, key_rope, preferred_element_type=F32)
            * inv_root
        )
        exponent = jnp.where(allowed[:, None], jnp.exp(scores), 0.0)
        log_total = jnp.log(jnp.sum(exponent, axis=-1, keepdims=True))
        prob = jnp.where(allowed[:, None], jnp.exp(scores - log_total), 0.0)
        mixed = (
            jnp.einsum("mhts,msd->mthd", prob.astype(BF16), value_low, preferred_element_type=F32)
            .astype(BF16)
            .reshape(rows_attn, span)
        )
        attn_part = dot32(mixed, w_out_all[layer], COL_PAIR).astype(BF16)
        attn_out = scatter_z(attn_part.reshape(mb, group_len, width)).reshape(rows_own, width)
        middle = hidden + attn_out.astype(F32)
        ffn_unit, ffn_scale = normalize(middle)
        expert_in = (ffn_unit * g_ffn).astype(BF16)
        tab = table_mine[layer]
        tab_hi = tab.astype(BF16)
        tab_lo = (tab - tab_hi.astype(F32)).astype(BF16)
        payload = jnp.concatenate([expert_in, tab_hi, tab_lo], axis=1)
        arrived_all = gather_all(payload)
        arrived = arrived_all[:, :width]
        gate_cols = arrived_all[:, width:].astype(F32)
        is_mine = jnp.arange(2 * experts) % experts == expert_own
        weight = jnp.sum(jnp.where(is_mine[None], gate_cols, 0.0), axis=1, keepdims=True)
        gate_pre = dot32(arrived, w_gate_all[layer])
        up_proj = dot32(arrived, w_up_all[layer])
        inner = (jax.nn.silu(gate_pre) * up_proj).astype(BF16)
        result = dot32(inner, w_down_all[layer])
        weighted = (result * weight).astype(BF16)
        expert_sum = scatter_all(weighted)
        layer_out = (middle + expert_sum.astype(F32)).astype(BF16)
        outs.append(layer_out)
        layer_in = layer_out
        saved_all.append(
            (
                attn_unit,
                attn_scale,
                normed_all,
                query_unit,
                query_scale,
                key_unit,
                key_scale,
                query_rope,
                key_rope,
                value_low,
                prob,
                mixed,
                ffn_unit,
                ffn_scale,
                arrived,
                weight,
                gate_pre,
                up_proj,
                inner,
            )
        )

    cot = cot_mine
    in_grads = [None] * n_sec
    expert_grads = [None] * n_sec
    attn_grads = [None] * n_sec
    gain_grads = [None] * n_sec
    for layer in reversed(range(n_sec)):
        g_attn, g_ffn, g_query, g_key = split_gains(layer)
        (
            attn_unit,
            attn_scale,
            normed_all,
            query_unit,
            query_scale,
            key_unit,
            key_scale,
            query_rope,
            key_rope,
            value_low,
            prob,
            mixed,
            ffn_unit,
            ffn_scale,
            arrived,
            weight,
            gate_pre,
            up_proj,
            inner,
        ) = saved_all[layer]
        gradient = cot.astype(F32)
        grad_all = gather_all(cot)
        grad_result = (grad_all.astype(F32) * weight).astype(BF16)
        grad_inner = dot32(grad_result, w_down_all[layer], COL_PAIR)
        grad_down = dot32(inner, grad_result, ROW_PAIR)
        sig = jax.nn.sigmoid(gate_pre)
        grad_gate_pre = (grad_inner * up_proj * sig * (1.0 + gate_pre * (1.0 - sig))).astype(BF16)
        grad_up_proj = (grad_inner * gate_pre * sig).astype(BF16)
        grad_gate = dot32(arrived, grad_gate_pre, ROW_PAIR)
        grad_up = dot32(arrived, grad_up_proj, ROW_PAIR)
        grad_arrived = (
            dot32(grad_gate_pre, w_gate_all[layer], COL_PAIR)
            + dot32(grad_up_proj, w_up_all[layer], COL_PAIR)
        ).astype(BF16)
        expert_grads[layer] = (grad_gate, grad_up, grad_down)
        grad_expert_in = scatter_all(grad_arrived).astype(F32)
        grad_ffn_gain = jnp.sum(grad_expert_in * ffn_unit, axis=0)
        grad_middle = gradient + norm_back(grad_expert_in * g_ffn, ffn_unit, ffn_scale)
        middle_low = grad_middle.astype(BF16)
        middle_all = gather_z(middle_low.reshape(mb, local_rows, width)).reshape(rows_attn, width)
        grad_out_w = dot32(middle_all, mixed, ROW_PAIR)
        grad_heads = (
            dot32(middle_all, w_out_all[layer]).astype(BF16).reshape(mb, group_len, heads, HD)
        )
        grad_value = jnp.einsum(
            "mhts,mthd->mshd", prob.astype(BF16), grad_heads, preferred_element_type=F32
        )
        grad_prob = jnp.einsum(
            "mthd,msd->mhts", grad_heads, value_low, preferred_element_type=F32
        )
        mixed_split = mixed.reshape(mb, group_len, heads, HD)
        delta = jnp.sum(grad_heads.astype(F32) * mixed_split.astype(F32), axis=-1)
        delta = jnp.swapaxes(delta, 1, 2)[..., None]
        grad_scores = (prob * (grad_prob - delta)).astype(BF16)
        grad_query = (
            jnp.einsum("mhts,msd->mthd", grad_scores, key_rope, preferred_element_type=F32)
            * inv_root
        ).reshape(rows_attn, heads, HD)
        grad_key = (
            jnp.einsum("mhts,mthd->mshd", grad_scores, query_rope, preferred_element_type=F32)
            * inv_root
        ).reshape(rows_attn, heads, HD)
        query_turn = rotate_back(grad_query, cos_q, sin_q)
        grad_query_gain = jnp.sum(query_turn * query_unit, axis=(0, 1))
        grad_query_pre = norm_back(query_turn * g_query, query_unit, query_scale)
        key_turn = rotate_back(jnp.sum(grad_key, axis=1), cos_k, sin_k)
        grad_key_gain = jnp.sum(key_turn * key_unit, axis=0)
        grad_key_pre = norm_back(key_turn * g_key, key_unit, key_scale)
        grad_proj = jnp.concatenate(
            [
                grad_query_pre.reshape(rows_attn, span),
                grad_key_pre,
                jnp.sum(grad_value, axis=2).reshape(rows_attn, HD),
            ],
            axis=1,
        ).astype(BF16)
        grad_in_w = dot32(normed_all, grad_proj, ROW_PAIR)
        normed_part = dot32(grad_proj, w_in_all[layer], COL_PAIR).astype(BF16)
        grad_normed = (
            scatter_z(normed_part.reshape(mb, group_len, width))
            .reshape(rows_own, width)
            .astype(F32)
        )
        grad_attn_gain = jnp.sum(grad_normed * attn_unit, axis=0)
        cot = (grad_middle + norm_back(grad_normed * g_attn, attn_unit, attn_scale)).astype(BF16)
        in_grads[layer] = cot
        attn_grads[layer] = jnp.concatenate([grad_in_w, grad_out_w], axis=1).astype(BF16)
        gain_grads[layer] = jnp.concatenate(
            [grad_attn_gain, grad_ffn_gain, grad_query_gain, grad_key_gain]
        )

    def own_layer_sum(pieces):
        return lax.psum_scatter(
            jnp.stack([piece.astype(BF16) for piece in pieces]),
            "section",
            scatter_dimension=0,
            tiled=True,
        ).astype(F32)

    grad_gate, grad_up, grad_down = (
        own_layer_sum([expert_grads[layer][k] for layer in range(n_sec)]) for k in range(3)
    )
    attn_sum = lax.psum_scatter(
        jnp.concatenate(attn_grads, axis=0), ("section", "gy"), scatter_dimension=0, tiled=True
    ).astype(F32)
    query_grad = attn_sum[:, :span]
    out_w_grad = attn_sum[:, span + 2 * HD :]
    kv_all = lax.all_gather(attn_sum[:, span : span + 2 * HD], "gx", axis=0, tiled=False)
    kv_all = jnp.sum(kv_all.reshape(KVH, n_gx // KVH, -1, 2, HD), axis=1)
    key_part = jnp.swapaxes(kv_all[:, :, 0], 0, 1).reshape(-1, KVH * HD)
    value_part = jnp.swapaxes(kv_all[:, :, 1], 0, 1).reshape(-1, KVH * HD)
    gain_sum = lax.psum(jnp.stack(gain_grads), ("section", "gx", "gy"))
    gain_sum = lax.dynamic_index_in_dim(gain_sum, section, 0, keepdims=True)

    def own_layer_rows(pieces):
        stacked = jnp.stack(pieces).reshape(n_sec, mb, local_rows, width)
        return lax.all_to_all(stacked, "section", split_axis=0, concat_axis=0, tiled=True).reshape(
            1, micro_count, 1, local_rows, width
        )

    return (
        own_layer_rows(outs),
        own_layer_rows(in_grads),
        gain_sum[:, :width],
        gain_sum[:, width : 2 * width],
        gain_sum[:, 2 * width : 2 * width + HD],
        gain_sum[:, 2 * width + HD :],
        query_grad[None],
        key_part[None],
        value_part[None],
        out_w_grad[None],
        grad_gate[:, None],
        grad_up[:, None],
        grad_down[:, None],
    )


def local_fused(
    inputs,
    out_grad,
    segments,
    routes,
    gates,
    gain_attn,
    gain_ffn,
    gain_query,
    gain_key,
    w_query,
    w_key,
    w_value,
    w_out,
    w_gate,
    w_up,
    w_down,
):
    micro_count, _, local_rows, width = inputs.shape
    n_sec = lax.axis_size("section")
    n_gx = lax.axis_size("gx")
    n_gy = lax.axis_size("gy")
    heads = w_query.shape[2] // HD
    span = heads * HD
    experts = n_gx * n_gy
    group_len = segments.shape[2]
    mb = micro_count // n_sec
    rows_own = mb * local_rows
    rows_attn = mb * group_len
    section = lax.axis_index("section")
    first = section * mb

    attn_shards = (w_query, w_key, w_value, w_out)
    table = dense_gates(routes[0, :, 0], gates[0, :, 0], experts)
    smalls = (table, gain_attn, gain_ffn, gain_query, gain_key)
    full_in, full_out, *others = share_weights(0, n_gx, attn_shards, smalls, 9)
    attn_all = [(full_in, full_out)]
    is_first = section == 0
    by_layer = [
        (jnp.where(is_first, own, other), jnp.where(is_first, other, own))
        for own, other in zip(smalls, others)
    ]
    moe_own = (w_gate[0, 0], w_up[0, 0], w_down[0, 0])
    moe_other = tuple(swap_sections(w) for w in moe_own)
    table_mine = [
        lax.dynamic_slice_in_dim(part, first, mb, 0).reshape(rows_own, experts)
        for part in by_layer[0]
    ]
    x_mine = lax.dynamic_slice_in_dim(inputs[:, 0], first, mb, 0).reshape(rows_own, width)
    cot = lax.dynamic_slice_in_dim(out_grad[:, 0], first, mb, 0).reshape(rows_own, width)
    segs = lax.dynamic_slice_in_dim(segments[:, 0], first, mb, 0)
    allowed, cosine, sine = seq_tables(segs, HD)
    tables = (
        jnp.concatenate([cosine, cosine], axis=-1).reshape(rows_attn, HD),
        jnp.concatenate([-sine, sine], axis=-1).reshape(rows_attn, HD),
        allowed.astype(F32),
    )

    def split_gains(layer):
        return tuple(pair[layer] for pair in by_layer[1:])

    kept = []
    outs = []
    layer_in = x_mine
    for layer in range(n_sec):
        tab = table_mine[layer]
        tab_hi = tab.astype(BF16)
        tab_lo = (tab - tab_hi.astype(F32)).astype(BF16)
        pad = jnp.zeros((rows_own, 128 - 2 * experts), BF16)
        gate_cols = jnp.concatenate([tab_hi, tab_lo, pad], axis=1)
        mid, payload, normed, proj, qr, kr, v, prob, mixed, *next_all = attn_forward(
            layer,
            n_gx,
            layer_in,
            split_gains(layer),
            tables,
            gate_cols,
            *attn_all[layer],
            attn_shards if layer == 0 else (),
            1 + layer,
            mb,
        )
        attn_all.append(next_all)
        layer_out, *moe_kept = moe_forward(
            layer, n_gx, mid, payload, moe_own, moe_other, 3 + layer
        )
        kept.append((layer_in, mid, (normed, proj, qr, kr, v, prob, mixed), moe_kept))
        outs.append(layer_out)
        layer_in = layer_out

    in_grads = [None] * n_sec
    moe_sums = ()
    later = ()
    gain_grads = [None] * n_sec
    for layer in reversed(range(n_sec)):
        g_attn, g_ffn, g_query, g_key = split_gains(layer)
        layer_in, mid, attn_kept, (arrived, weight, gp, up, inner) = kept[layer]
        dmid, d_ffn, *moe_sums = moe_backward(
            layer,
            n_gx,
            cot,
            mid,
            g_ffn,
            weight,
            arrived,
            gp,
            up,
            inner,
            moe_own,
            moe_other,
            moe_sums,
            5 + layer,
        )
        cot, d_attn, d_query, d_key, *later = attn_backward(
            layer,
            n_gx,
            dmid,
            layer_in,
            (g_attn, g_query, g_key),
            tables,
            attn_kept,
            *attn_all[layer],
            later,
            moe_sums[3:] if layer == 0 else (),
            7 + layer,
            mb,
        )
        in_grads[layer] = cot
        gain_grads[layer] = [d_attn, d_ffn, d_query, d_key]

    query_grad, kv_shard, out_grad_w, *from_other = later
    grad_gate, grad_up, grad_down = (
        (moe_sums[k].astype(F32) + from_other[k].astype(F32))[None] for k in range(3)
    )
    gain_sum, key_part, value_part = finish_line(
        n_gx, [grad for grads in gain_grads for grad in grads], kv_shard, 10
    )
    out_rows, grad_rows, *gain_sums = finish_pair(
        gain_sum, [grad.shape[1] for grad in gain_grads[0]], outs, in_grads, 11
    )
    whole_rows = (1, micro_count, 1, local_rows, width)

    return (
        out_rows.reshape(whole_rows),
        grad_rows.reshape(whole_rows),
        *gain_sums,
        query_grad[None],
        key_part[None],
        value_part[None],
        out_grad_w[None],
        grad_gate[:, None],
        grad_up[:, None],
        grad_down[:, None],
    )


def local(*args):
    inputs = args[0]
    n = lax.axis_size("gx")
    rows_own = inputs.shape[0] // lax.axis_size("section") * inputs.shape[2]
    if 4 * n * rows_own > MOST_ROWS or n != KVH:
        return local_wide(*args)
    return local_fused(*args)


def solution(mesh):
    return jax.shard_map(
        local,
        mesh=mesh,
        in_specs=(
            P(None, "gy", "gx", None),
            P(None, "gy", "gx", None),
            P(None, "gy", None),
            P("section", None, "gy", "gx", None),
            P("section", None, "gy", "gx", None),
            P("section", None),
            P("section", None),
            P("section", None),
            P("section", None),
            P("section", "gy", "gx"),
            P("section", "gy", None),
            P("section", "gy", None),
            P("section", "gy", "gx"),
            P("section", ("gx", "gy"), None, None),
            P("section", ("gx", "gy"), None, None),
            P("section", ("gx", "gy"), None, None),
        ),
        out_specs=(
            P("section", None, "gy", "gx", None),
            P("section", None, "gy", "gx", None),
            P("section", None),
            P("section", None),
            P("section", None),
            P("section", None),
            P("section", "gy", "gx"),
            P("section", "gy", None),
            P("section", "gy", None),
            P("section", "gy", "gx"),
            P("section", ("gx", "gy"), None, None),
            P("section", ("gx", "gy"), None, None),
            P("section", ("gx", "gy"), None, None),
        ),
        check_vma=False,
    )
```
